8 devices in a mesh: tp: 8 (over z, y, x, core).
Axes of the slice: x: 2, y: 2, z: 1, core: 2. Of those that a mesh axis runs over, the one named last changes fastest.
Arguments:
- x_input: bfloat16 [2, 2048, 2048], P(None, 'tp')
- w_query: bfloat16 [2048, 2048], P(None, 'tp')
- w_key: bfloat16 [2048, 2048], P(None, 'tp')
- w_value: bfloat16 [2048, 2048], P(None, 'tp')
- w_out: bfloat16 [2048, 2048], P('tp')
- g_query: bfloat16 [2048], P('tp')
- g_key: bfloat16 [2048], P('tp')
- g_attn: bfloat16 [2048], replicated
- grad_y: bfloat16 [2, 2048, 2048], P(None, 'tp')
Outputs:
- output 1: bfloat16 [2, 2048, 2048], P(None, 'tp')
- output 2: bfloat16 [2, 2048, 2048], P(None, 'tp')
- output 3: bfloat16 [2048, 2048], P(None, 'tp')
- output 4: bfloat16 [2048, 2048], P(None, 'tp')
- output 5: bfloat16 [2048, 2048], P(None, 'tp')
- output 6: bfloat16 [2048, 2048], P('tp')
- output 7: bfloat16 [2048], P('tp')
- output 8: bfloat16 [2048], P('tp')
- output 9: bfloat16 [2048], replicated
All inputs are finite; a program needn't handle non-finite values.
Results may differ from the reference program's by a relative error of at most 0.0158848.
Values are sent between devices in bfloat16 or wider.
A program may use at most 1 GiB of HBM per device.

```python
import jax
import jax.numpy as jnp
from jax import lax

BATCH_SIZE = 2
SEQ_LEN = 2048
MODEL_DIM = 2048
NUM_HEADS = 16
HEAD_DIM = 128
ROPE_THETA = 500000
NORM_EPS = 1e-6


def setup_inputs(seed: int = 0) -> dict:
    rng_keys = jax.random.split(jax.random.key(seed), 12)
    fan_scale = MODEL_DIM ** -0.5
    act_shape = (BATCH_SIZE, SEQ_LEN, MODEL_DIM)
    mat_shape = (MODEL_DIM, MODEL_DIM)
    head_q = jnp.exp(jax.random.uniform(rng_keys[0], (NUM_HEADS,), jnp.float32, jnp.log(0.3), jnp.log(3.0)))
    head_k = jnp.exp(jax.random.uniform(rng_keys[1], (NUM_HEADS,), jnp.float32, jnp.log(0.3), jnp.log(3.0)))
    col_q = jnp.repeat(head_q, HEAD_DIM)[None, :]
    col_k = jnp.repeat(head_k, HEAD_DIM)[None, :]
    x_input = jax.random.normal(rng_keys[2], act_shape, jnp.float32)
    w_query = jax.random.normal(rng_keys[3], mat_shape, jnp.float32) * fan_scale * col_q
    w_key = jax.random.normal(rng_keys[4], mat_shape, jnp.float32) * fan_scale * col_k
    w_value = jax.random.normal(rng_keys[5], mat_shape, jnp.float32) * fan_scale
    w_out = jax.random.normal(rng_keys[6], mat_shape, jnp.float32) * fan_scale
    g_query = jax.random.uniform(rng_keys[7], (MODEL_DIM,), jnp.float32, 0.5, 1.5)
    g_key = jax.random.uniform(rng_keys[8], (MODEL_DIM,), jnp.float32, 0.5, 1.5)
    g_attn = jax.random.uniform(rng_keys[9], (MODEL_DIM,), jnp.float32, 0.5, 1.5)
    grad_y = jax.random.normal(rng_keys[10], act_shape, jnp.float32)
    return {'x_input': x_input.astype(jnp.bfloat16), 'w_query': w_query.astype(jnp.bfloat16), 'w_key': w_key.astype(jnp.bfloat16), 'w_value': w_value.astype(jnp.bfloat16), 'w_out': w_out.astype(jnp.bfloat16), 'g_query': g_query.astype(jnp.bfloat16), 'g_key': g_key.astype(jnp.bfloat16), 'g_attn': g_attn.astype(jnp.bfloat16), 'grad_y': grad_y.astype(jnp.bfloat16)}


def rope_tables():
    half_dim = HEAD_DIM // 2
    inv_freq = 1.0 / (ROPE_THETA ** (jnp.arange(half_dim, dtype=jnp.float32) / half_dim))
    angles = jnp.arange(SEQ_LEN, dtype=jnp.float32)[:, None] * inv_freq[None, :]
    return jnp.cos(angles)[:, None, :], jnp.sin(angles)[:, None, :]


def rotate(values, cos_t, sin_t):
    lower_half, upper_half = jnp.split(values, 2, axis=-1)
    return jnp.concatenate([lower_half * cos_t - upper_half * sin_t, upper_half * cos_t + lower_half * sin_t], axis=-1)


def whole_norm(values, gain):
    inv_rms = lax.rsqrt(jnp.mean(values * values, axis=-1, keepdims=True) + NORM_EPS)
    return values * inv_rms * gain.astype(jnp.float32)


def head_attention(operands):
    q_head, k_head, v_head = operands
    scores = jnp.einsum('bqd,bkd->bqk', q_head.astype(jnp.float32), k_head.astype(jnp.float32)) * (HEAD_DIM ** -0.5)
    causal = jnp.arange(SEQ_LEN)[:, None] >= jnp.arange(SEQ_LEN)[None, :]
    attn_probs = jax.nn.softmax(jnp.where(causal[None], scores, -1e30), axis=-1)
    head_out = jnp.einsum('bqk,bkd->bqd', attn_probs.astype(jnp.bfloat16).astype(jnp.float32), v_head.astype(jnp.float32))
    return head_out.astype(jnp.bfloat16)


def block_forward(x_input, w_query, w_key, w_value, w_out, g_query, g_key, g_attn):
    x_rows = x_input.reshape(BATCH_SIZE * SEQ_LEN, MODEL_DIM)
    head_shape = (BATCH_SIZE, SEQ_LEN, NUM_HEADS, HEAD_DIM)
    cos_t, sin_t = rope_tables()
    q_raw = jnp.dot(x_rows, w_query, preferred_element_type=jnp.float32)
    k_raw = jnp.dot(x_rows, w_key, preferred_element_type=jnp.float32)
    v_proj = jnp.dot(x_rows, w_value, preferred_element_type=jnp.float32).astype(jnp.bfloat16)
    q_rot = rotate(whole_norm(q_raw, g_query).reshape(head_shape), cos_t, sin_t).astype(jnp.bfloat16)
    k_rot = rotate(whole_norm(k_raw, g_key).reshape(head_shape), cos_t, sin_t).astype(jnp.bfloat16)
    v_heads = v_proj.reshape(head_shape)
    per_head = lax.map(jax.checkpoint(head_attention), (jnp.moveaxis(q_rot, 2, 0), jnp.moveaxis(k_rot, 2, 0), jnp.moveaxis(v_heads, 2, 0)))
    attn_rows = jnp.moveaxis(per_head, 0, 2).reshape(BATCH_SIZE * SEQ_LEN, MODEL_DIM)
    attn_sum = jnp.dot(attn_rows, w_out, preferred_element_type=jnp.float32)
    post_rms = lax.rsqrt(jnp.mean(attn_sum * attn_sum, axis=-1, keepdims=True) + NORM_EPS)
    y_rows = x_rows.astype(jnp.float32) + attn_sum * post_rms * g_attn.astype(jnp.float32)
    return y_rows.astype(jnp.bfloat16).reshape(BATCH_SIZE, SEQ_LEN, MODEL_DIM)


def reference(x_input, w_query, w_key, w_value, w_out, g_query, g_key, g_attn, grad_y):
    y_out, pullback = jax.vjp(block_forward, x_input, w_query, w_key, w_value, w_out, g_query, g_key, g_attn)
    grad_x, grad_wq, grad_wk, grad_wv, grad_wo, grad_gq, grad_gk, grad_ga = pullback(grad_y)
    return (y_out, grad_x, grad_wq, grad_wk, grad_wv, grad_wo, grad_gq, grad_gk, grad_ga)
```

```python
import functools
import math

import jax
import jax.numpy as jnp
from jax import lax
from jax.experimental import pallas as pl
from jax.experimental.pallas import tpu as pltpu
from jax.sharding import PartitionSpec as P

HD = 128
ROPE_THETA = 500000.0
EPS = 1e-6
DIM = 2048
SEQ = 2048
LOC = 256
TOK = 256
BLK = 512
NB = SEQ // BLK
NDEV = 8
SCALE = HD ** -0.5
C2 = SCALE * math.log2(math.e)
MESH = pl.DeviceIdType.MESH
BF = jnp.bfloat16
F32 = jnp.float32
VMEM_MAX = 60 * 1024 * 1024

NT = (((1,), (1,)), ((), ()))
NN = (((1,), (0,)), ((), ()))


def dot(a, b, dims=NN):
    return lax.dot_general(a, b, dims, preferred_element_type=F32)


def sds(shape, dtype):
    return jax.ShapeDtypeStruct(shape, dtype)


def cost(flops, nbytes, trans=0):
    return pl.CostEstimate(flops=int(flops), bytes_accessed=int(nbytes), transcendentals=int(trans))


def params(**kw):
    return pltpu.CompilerParams(vmem_limit_bytes=VMEM_MAX, **kw)


def peer_of(me, mask):
    core, ax, ay = me % 2, (me // 2) % 2, me // 4
    core = 1 - core if mask & 1 else core
    ax = 1 - ax if mask & 2 else ax
    ay = 1 - ay if mask & 4 else ay
    return ay * 4 + ax * 2 + core


ORDER = (6, 7, 2, 4, 3, 5, 1)


def entry_barrier(me):
    barrier = pltpu.get_barrier_semaphore()
    for mask in ORDER:
        pl.semaphore_signal(barrier, inc=1, device_id=(peer_of(me, mask),), device_id_type=MESH)
    pl.semaphore_wait(barrier, NDEV - 1)


def rope_tables():
    half = HD // 2
    inv_freq = 1.0 / (ROPE_THETA ** (jnp.arange(half, dtype=F32) / half))
    angles = jnp.arange(SEQ, dtype=F32)[:, None] * inv_freq[None, :]
    cos, sin = jnp.cos(angles), jnp.sin(angles)
    return jnp.concatenate([cos, cos], axis=1), jnp.concatenate([-sin, sin], axis=1)


def row_sums(vals):
    folded = vals[:, :HD]
    for start in range(HD, vals.shape[1], HD):
        folded = folded + vals[:, start:start + HD]
    return jnp.sum(folded.T, axis=0, keepdims=True)


def as_column(row):
    return jnp.broadcast_to(row, (HD, row.shape[1])).T


def proj_kernel(x_ref, w_ref, q_ref, k_ref, v_ref, s_ref):
    i = pl.program_id(0)
    x = x_ref[...]
    q = dot(x, w_ref[:, :LOC])
    q_ref[...] = q
    s_ref[pl.ds(i, 1), :] = row_sums(q * q)
    k = dot(x, w_ref[:, LOC:2 * LOC])
    k_ref[...] = k
    s_ref[pl.ds(i + NB, 1), :] = row_sums(k * k)
    v_ref[...] = dot(x, w_ref[:, 2 * LOC:]).astype(BF)


def project(x, w):
    row = pl.BlockSpec((BLK, LOC), lambda i: (i, 0))
    return pl.pallas_call(
        proj_kernel,
        grid=(NB,),
        in_specs=[pl.BlockSpec((BLK, DIM), lambda i: (i, 0)), pl.BlockSpec((DIM, 3 * LOC), lambda i: (0, 0))],
        out_specs=[row, row, row, pl.BlockSpec((2 * NB, BLK), lambda i: (0, 0))],
        out_shape=[sds((SEQ, LOC), F32), sds((SEQ, LOC), F32), sds((SEQ, LOC), BF), sds((2 * NB, BLK), F32)],
        compiler_params=params(dimension_semantics=("arbitrary",)),
        cost_estimate=cost(2 * SEQ * DIM * 3 * LOC, 16e6),
        name="proj",
    )(x, w)


def exchange(me, srcs, slots, send_sems, recv_sems):
    entry_barrier(me)
    copies = []
    for n, (src, slot) in enumerate(zip(srcs, slots)):
        for p, mask in enumerate(ORDER):
            copies.append(pltpu.make_async_remote_copy(
                src_ref=src, dst_ref=slot.at[p], send_sem=send_sems.at[n, p], recv_sem=recv_sems.at[n, p],
                device_id=(peer_of(me, mask),), device_id_type=MESH))
    for c in copies:
        c.start()
    for c in copies:
        c.wait()


def ordered_total(me, src, slot):
    own = src[...]
    total = jnp.zeros_like(own)
    for dev in range(NDEV):
        term = jnp.where(me == dev, own, 0.0)
        for p, mask in enumerate(ORDER):
            term = term + jnp.where(peer_of(me, mask) == dev, slot[p], 0.0)
        total = total + term
    return total


def rotated(v, cos, sin):
    out = []
    for h in range(v.shape[1] // HD):
        part = v[:, h * HD:(h + 1) * HD]
        out.append(part * cos + pltpu.roll(part, HD // 2, 1) * sin)
    return out


def norm_kernel(q_ref, k_ref, s_ref, gq_ref, gk_ref, cos_ref, sin_ref, qo_ref, ko_ref, iq_ref, ik_ref,
                slot, total, send_sems, recv_sems):
    i = pl.program_id(0)
    me = lax.axis_index('tp')

    @pl.when(i == 0)
    def _():
        exchange(me, [s_ref], [slot], send_sems, recv_sems)
        total[...] = lax.rsqrt(ordered_total(me, s_ref, slot) / DIM + EPS)

    cos, sin = cos_ref[...], sin_ref[...]
    for src, dst, inv_ref, g_ref, row in ((q_ref, qo_ref, iq_ref, gq_ref, i), (k_ref, ko_ref, ik_ref, gk_ref, i + NB)):
        inv = as_column(total[pl.ds(row, 1), :])
        inv_ref[...] = inv
        g = g_ref[...].astype(F32)
        for h in range(LOC // HD):
            sl = slice(h * HD, (h + 1) * HD)
            hat = src[:, sl] * inv * g[:, sl]
            dst[:, sl] = (hat * cos + pltpu.roll(hat, HD // 2, 1) * sin).astype(BF)


def norm_rope(q, k, s, gq, gk, cos, sin, cid):
    row = pl.BlockSpec((BLK, LOC), lambda i: (i, 0))
    half = pl.BlockSpec((BLK, HD), lambda i: (i, 0))
    gain = pl.BlockSpec((1, LOC), lambda i: (0, 0))
    return pl.pallas_call(
        norm_kernel,
        grid=(NB,),
        in_specs=[row, row, pl.BlockSpec((2 * NB, BLK), lambda i: (0, 0)), gain, gain, half, half],
        out_specs=[row, row, half, half],
        out_shape=[sds((SEQ, LOC), BF), sds((SEQ, LOC), BF), sds((SEQ, HD), F32), sds((SEQ, HD), F32)],
        scratch_shapes=[pltpu.VMEM((NDEV - 1, 2 * NB, BLK), F32), pltpu.VMEM((2 * NB, BLK), F32),
                        pltpu.SemaphoreType.DMA((1, NDEV - 1)), pltpu.SemaphoreType.DMA((1, NDEV - 1))],
        compiler_params=params(dimension_semantics=("arbitrary",), collective_id=cid, has_side_effects=True),
        cost_estimate=cost(2e9, 10e6),
        name="norm_rope",
    )(q, k, s, gq, gk, cos, sin)


def causal_mask():
    keys = lax.broadcasted_iota(jnp.int32, (BLK, BLK), 0)
    queries = lax.broadcasted_iota(jnp.int32, (BLK, BLK), 1)
    return keys <= queries


def attn_kernel(q_ref, k_ref, v_ref, o_ref, lse_ref, p_scr, vt_scr, acc_scr):
    h, qi = pl.program_id(0), pl.program_id(1)

    @pl.when(qi == 0)
    def _():
        vt_scr[...] = v_ref[...].T

    qb = q_ref[...]

    def scores(j):
        return dot(k_ref[pl.ds(pl.multiple_of(j * BLK, BLK), BLK), :], qb, NT)

    def first(j, m):
        s = scores(j)
        p_scr[j] = s
        return jnp.maximum(m, jnp.max(s.reshape(BLK // 8, 8, BLK), axis=0))

    s = jnp.where(causal_mask(), scores(qi), -1e30)
    p_scr[qi] = s
    m = lax.fori_loop(0, qi, first, jnp.max(s.reshape(BLK // 8, 8, BLK), axis=0))
    m = jnp.max(m, axis=0, keepdims=True)

    def second(j, l):
        p = jnp.exp2((p_scr[j] - m) * C2)
        p_scr[j] = p
        return l + jnp.sum(p.reshape(BLK // 8, 8, BLK), axis=0)

    l = lax.fori_loop(0, qi + 1, second, jnp.zeros((8, BLK), F32))
    l = jnp.sum(l, axis=0, keepdims=True)
    rl = 1.0 / l
    lse_ref[pl.ds(h * NB + qi, 1), :] = m * C2 + jnp.log2(l)

    acc_scr[...] = jnp.zeros_like(acc_scr)

    def third(j, carry):
        p = (p_scr[j] * rl).astype(BF)
        acc_scr[...] += dot(vt_scr[:, pl.ds(pl.multiple_of(j * BLK, BLK), BLK)], p)
        return carry

    lax.fori_loop(0, qi + 1, third, 0)
    o_ref[...] = acc_scr[...].T.astype(BF)


def attention(q, k, v):
    blk = pl.BlockSpec((BLK, HD), lambda h, i: (i, h))
    full = pl.BlockSpec((SEQ, HD), lambda h, i: (0, h))
    return pl.pallas_call(
        attn_kernel,
        grid=(2, NB),
        in_specs=[blk, full, full],
        out_specs=[blk, pl.BlockSpec((2 * NB, BLK), lambda h, i: (0, 0))],
        out_shape=[sds((SEQ, LOC), BF), sds((2 * NB, BLK), F32)],
        scratch_shapes=[pltpu.VMEM((NB, BLK, BLK), F32), pltpu.VMEM((HD, SEQ), BF), pltpu.VMEM((HD, BLK), F32)],
        compiler_params=params(dimension_semantics=("arbitrary", "arbitrary")),
        cost_estimate=cost(9e9, 6e6),
        name="attn_fwd",
    )(q, k, v)


def heads_to_tokens_kernel(src, dst, send_sems, recv_sems, own_sem):
    me = lax.axis_index('tp')
    width = src.shape[1]
    entry_barrier(me)
    here = dst.at[:, pl.ds(pl.multiple_of(me * width, width), width)]
    copies = []
    for p, mask in enumerate(ORDER):
        peer = peer_of(me, mask)
        copies.append(pltpu.make_async_remote_copy(
            src_ref=src.at[pl.ds(pl.multiple_of(peer * TOK, TOK), TOK), :], dst_ref=here,
            send_sem=send_sems.at[p], recv_sem=recv_sems.at[p], device_id=(peer,), device_id_type=MESH))
    for c in copies:
        c.start()
    own = pltpu.make_async_copy(src.at[pl.ds(pl.multiple_of(me * TOK, TOK), TOK), :], here, own_sem)
    own.start()
    own.wait()
    for c in copies:
        c.wait()


def tokens_to_heads_kernel(src, dst, send_sems, recv_sems, own_sem):
    me = lax.axis_index('tp')
    width = dst.shape[1]
    entry_barrier(me)
    here = dst.at[pl.ds(pl.multiple_of(me * TOK, TOK), TOK), :]
    copies = []
    for p, mask in enumerate(ORDER):
        peer = peer_of(me, mask)
        copies.append(pltpu.make_async_remote_copy(
            src_ref=src.at[:, pl.ds(pl.multiple_of(peer * width, width), width)], dst_ref=here,
            send_sem=send_sems.at[p], recv_sem=recv_sems.at[p], device_id=(peer,), device_id_type=MESH))
    for c in copies:
        c.start()
    own = pltpu.make_async_copy(src.at[:, pl.ds(pl.multiple_of(me * width, width), width)], here, own_sem)
    own.start()
    own.wait()
    for c in copies:
        c.wait()


def all_to_all(kernel, src, out_shape, cid):
    return pl.pallas_call(
        kernel,
        in_specs=[pl.BlockSpec(memory_space=pl.ANY)],
        out_specs=pl.BlockSpec(memory_space=pl.ANY),
        out_shape=sds(out_shape, BF),
        scratch_shapes=[pltpu.SemaphoreType.DMA((NDEV - 1,)), pltpu.SemaphoreType.DMA((NDEV - 1,)),
                        pltpu.SemaphoreType.DMA],
        compiler_params=pltpu.CompilerParams(collective_id=cid, has_side_effects=True),
        cost_estimate=cost(5e9, 2 * src.size),
        name="a2a",
    )(src)


def out_kernel(o_ref, wo_ref, x_ref, dy_ref, ga_ref, y_ref, da_ref, dh_ref, gga_ref, a_scr):
    step = DIM // NB
    o = o_ref[...]

    def fwd(j, carry):
        cols = pl.ds(pl.multiple_of(j * step, step), step)
        a_scr[:, cols] = dot(o, wo_ref[:, cols])
        return carry

    lax.fori_loop(0, NB, fwd, 0)
    a = a_scr[...]
    r = lax.rsqrt(jnp.mean(a * a, axis=-1, keepdims=True) + EPS)
    n = a * r
    ga = ga_ref[...].astype(F32)
    dy = dy_ref[...].astype(F32)
    y_ref[...] = (x_ref[...].astype(F32) + n * ga).astype(BF)
    col = jnp.sum(dy * n, axis=0, keepdims=True)
    for i in range(8):
        gga_ref[i:i + 1, :] = col[:, i * (DIM // 8):(i + 1) * (DIM // 8)]
    gn = dy * ga
    da_ref[...] = (r * (gn - n * jnp.mean(gn * n, axis=-1, keepdims=True))).astype(BF)
    da = da_ref[...]

    def bwd(j, carry):
        rows = pl.ds(pl.multiple_of(j * step, step), step)
        dh_ref[:, rows] = dot(da, wo_ref[rows, :], NT).astype(BF)
        return carry

    lax.fori_loop(0, NB, bwd, 0)


def out_block(o, wo, x, dy, ga):
    spec = pl.BlockSpec(memory_space=pltpu.VMEM)
    return pl.pallas_call(
        out_kernel,
        in_specs=[spec] * 5,
        out_specs=[spec] * 4,
        out_shape=[sds((TOK, DIM), BF), sds((TOK, DIM), BF), sds((TOK, DIM), BF), sds((8, DIM // 8), F32)],
        scratch_shapes=[pltpu.VMEM((TOK, DIM), F32)],
        compiler_params=params(),
        cost_estimate=cost(4 * TOK * DIM * DIM, 14e6),
        name="out_block",
    )(o, wo, x, dy, ga)


def attn_bwd_kernel(q_ref, k_ref, v_ref, do_ref, lse_ref, qr_ref, kr_ref, iq_ref, ik_ref, gq_ref, gk_ref, cos_ref, sin_ref,
                    dqu_ref, dku_ref, dv_ref, dots_ref, gg_ref,
                    p_scr, dp_scr, kt_scr, dqt_scr, dq_scr, dk_scr, dv_scr):
    h, qi = pl.program_id(0), pl.program_id(1)

    @pl.when(qi == 0)
    def _():
        kt_scr[...] = k_ref[...].T
        dk_scr[...] = jnp.zeros_like(dk_scr)
        dv_scr[...] = jnp.zeros_like(dv_scr)

    qb = q_ref[...]
    dob = do_ref[...]
    lse = lse_ref[pl.ds(h * NB + qi, 1), :]

    def first(j, acc, diag=False):
        rows = pl.ds(pl.multiple_of(j * BLK, BLK), BLK)
        p = jnp.exp2(dot(k_ref[rows, :], qb, NT) * C2 - lse)
        if diag:
            p = jnp.where(causal_mask(), p, 0.0)
        dp = dot(v_ref[rows, :], dob, NT)
        p_scr[j] = p
        dp_scr[j] = dp
        dv_scr[rows, :] += dot(p.astype(BF), dob)
        return acc + jnp.sum((p * dp).reshape(BLK // 8, 8, BLK), axis=0)

    acc = first(qi, jnp.zeros((8, BLK), F32), True)
    acc = lax.fori_loop(0, qi, first, acc)
    delta = jnp.sum(acc, axis=0, keepdims=True)
    dqt_scr[...] = jnp.zeros_like(dqt_scr)

    def second(j, carry):
        rows = pl.ds(pl.multiple_of(j * BLK, BLK), BLK)
        ds = (p_scr[j] * (dp_scr[j] - delta) * SCALE).astype(BF)
        dk_scr[rows, :] += dot(ds, qb)
        dqt_scr[...] += dot(kt_scr[:, rows], ds)
        return carry

    lax.fori_loop(0, qi + 1, second, 0)
    dq_scr[pl.ds(pl.multiple_of(qi * BLK, BLK), BLK), :] = dqt_scr[...].T

    @pl.when(qi == NB - 1)
    def _():
        dv_ref[...] = dv_scr[...].astype(BF)

        @pl.when(h == 0)
        def _():
            dots_ref[...] = jnp.zeros_like(dots_ref)

        gg_ref[...] = jnp.zeros_like(gg_ref)

        def tail(i, carry):
            rows = pl.ds(pl.multiple_of(i * BLK, BLK), BLK)
            cos, sin = cos_ref[rows, :], sin_ref[rows, :]
            for n, (d_scr, raw_ref, inv_ref, g_ref, out_ref) in enumerate((
                    (dq_scr, qr_ref, iq_ref, gq_ref, dqu_ref), (dk_scr, kr_ref, ik_ref, gk_ref, dku_ref))):
                d = d_scr[rows, :]
                hat = d * cos - pltpu.roll(d, HD // 2, 1) * sin
                unit = raw_ref[rows, :] * inv_ref[rows, :]
                gg_ref[n:n + 1, :] += jnp.sum(hat * unit, axis=0, keepdims=True)
                du = hat * g_ref[...].astype(F32)
                out_ref[rows, :] = du
                dots_ref[pl.ds(i + n * NB, 1), :] += row_sums(du * unit)
            return carry

        lax.fori_loop(0, NB, tail, 0)


def attention_bwd(q, k, v, do, lse, qr, kr, iq, ik, gq, gk, cos, sin):
    blk = pl.BlockSpec((BLK, HD), lambda h, i: (i, h))
    full = pl.BlockSpec((SEQ, HD), lambda h, i: (0, h))
    shared = pl.BlockSpec((SEQ, HD), lambda h, i: (0, 0))
    gain = pl.BlockSpec((1, HD), lambda h, i: (0, h))
    rows = pl.BlockSpec((2 * NB, BLK), lambda h, i: (0, 0))
    return pl.pallas_call(
        attn_bwd_kernel,
        grid=(2, NB),
        in_specs=[blk, full, full, blk, rows, full, full, shared, shared, gain, gain, shared, shared],
        out_specs=[full, full, full, rows, pl.BlockSpec((8, HD), lambda h, i: (0, h))],
        out_shape=[sds((SEQ, LOC), F32), sds((SEQ, LOC), F32), sds((SEQ, LOC), BF), sds((2 * NB, BLK), F32),
                   sds((8, LOC), F32)],
        scratch_shapes=[pltpu.VMEM((NB, BLK, BLK), F32), pltpu.VMEM((NB, BLK, BLK), F32), pltpu.VMEM((HD, SEQ), BF),
                        pltpu.VMEM((HD, BLK), F32), pltpu.VMEM((SEQ, HD), F32), pltpu.VMEM((SEQ, HD), F32),
                        pltpu.VMEM((SEQ, HD), F32)],
        compiler_params=params(dimension_semantics=("arbitrary", "arbitrary")),
        cost_estimate=cost(16e9, 16e6),
        name="attn_bwd",
    )(q, k, v, do, lse, qr, kr, iq, ik, gq, gk, cos, sin)


def norm_bwd_kernel(dqu_ref, dku_ref, dv_ref, qr_ref, kr_ref, iq_ref, ik_ref, dots_ref, ga_ref, out_ref, gga_ref,
                    slot, ga_slot, total, send_sems, recv_sems):
    i = pl.program_id(0)
    me = lax.axis_index('tp')

    @pl.when(i == 0)
    def _():
        exchange(me, [dots_ref, ga_ref], [slot, ga_slot], send_sems, recv_sems)
        total[...] = ordered_total(me, dots_ref, slot) / DIM
        gga_ref[...] = ordered_total(me, ga_ref, ga_slot)

    for n, (du_ref, raw_ref, inv_ref) in enumerate(((dqu_ref, qr_ref, iq_ref), (dku_ref, kr_ref, ik_ref))):
        dots = as_column(total[pl.ds(i + n * NB, 1), :])
        inv = inv_ref[...]
        for h in range(LOC // HD):
            sl = slice(h * HD, (h + 1) * HD)
            unit = raw_ref[:, sl] * inv
            out_ref[:, n * LOC + h * HD:n * LOC + (h + 1) * HD] = (inv * (du_ref[:, sl] - unit * dots)).astype(BF)
    out_ref[:, 2 * LOC:] = dv_ref[...]


def norm_bwd(dqu, dku, dv, qr, kr, iq, ik, dots, gga, cid):
    row = pl.BlockSpec((BLK, LOC), lambda i: (i, 0))
    half = pl.BlockSpec((BLK, HD), lambda i: (i, 0))
    rows = pl.BlockSpec((2 * NB, BLK), lambda i: (0, 0))
    gsp = pl.BlockSpec((8, DIM // 8), lambda i: (0, 0))
    return pl.pallas_call(
        norm_bwd_kernel,
        grid=(NB,),
        in_specs=[row, row, row, row, row, half, half, rows, gsp],
        out_specs=[pl.BlockSpec((BLK, 3 * LOC), lambda i: (i, 0)), gsp],
        out_shape=[sds((SEQ, 3 * LOC), BF), sds((8, DIM // 8), F32)],
        scratch_shapes=[pltpu.VMEM((NDEV - 1, 2 * NB, BLK), F32), pltpu.VMEM((NDEV - 1, 8, DIM // 8), F32),
                        pltpu.VMEM((2 * NB, BLK), F32),
                        pltpu.SemaphoreType.DMA((2, NDEV - 1)), pltpu.SemaphoreType.DMA((2, NDEV - 1))],
        compiler_params=params(dimension_semantics=("arbitrary",), collective_id=cid, has_side_effects=True),
        cost_estimate=cost(2e9, 14e6),
        name="norm_bwd",
    )(dqu, dku, dv, qr, kr, iq, ik, dots, gga)


def dx_kernel(d0_ref, d1_ref, w_ref, dy0_ref, dy1_ref, dx0_ref, dx1_ref, acc0, acc1):
    i = pl.program_id(0)

    @pl.when(i == 0)
    def _():
        acc0[...] = dy0_ref[...].astype(F32)
        acc1[...] = dy1_ref[...].astype(F32)

    w = w_ref[0]
    acc0[...] += dot(d0_ref[...], w, NT)
    acc1[...] += dot(d1_ref[...], w, NT)

    @pl.when(i == NDEV - 1)
    def _():
        dx0_ref[...] = acc0[...].astype(BF)
        dx1_ref[...] = acc1[...].astype(BF)


def dx_block(d0, d1, w, dy0, dy1):
    part = pl.BlockSpec((TOK, 3 * LOC), lambda i: (0, i))
    full = pl.BlockSpec((TOK, DIM), lambda i: (0, 0))
    return pl.pallas_call(
        dx_kernel,
        grid=(NDEV,),
        in_specs=[part, part, pl.BlockSpec((1, DIM, 3 * LOC), lambda i: (i, 0, 0)), full, full],
        out_specs=[full, full],
        out_shape=[sds((TOK, DIM), BF)] * 2,
        scratch_shapes=[pltpu.VMEM((TOK, DIM), F32)] * 2,
        compiler_params=params(dimension_semantics=("arbitrary",)),
        cost_estimate=cost(2 * 2 * TOK * DIM * 3 * DIM, 40e6),
        name="dx",
    )(d0, d1, w, dy0, dy1)


def wgrad_kernel(transposed, l0_ref, l1_ref, r0_ref, r1_ref, *rest):
    *outs, acc = rest
    i = pl.program_id(0)

    @pl.when(i == 0)
    def _():
        acc[...] = jnp.zeros_like(acc)

    @pl.when(i < NB)
    def _():
        acc[...] += dot(l0_ref[...].T, r0_ref[...])

    @pl.when(i >= NB)
    def _():
        acc[...] += dot(l1_ref[...].T, r1_ref[...])

    @pl.when(i == 2 * NB - 1)
    def _():
        for n, out in enumerate(outs):
            part = acc[n * LOC:(n + 1) * LOC, :]
            out[...] = (part.T if transposed else part).astype(BF)


def wgrad(left, right, transposed):
    width = left[0].shape[1]
    count = width // LOC
    first = lambda i: (jnp.minimum(i, NB - 1), 0)
    second = lambda i: (jnp.maximum(i - NB, 0), 0)
    shape = (DIM, LOC) if transposed else (LOC, DIM)
    return pl.pallas_call(
        functools.partial(wgrad_kernel, transposed),
        grid=(2 * NB,),
        in_specs=[pl.BlockSpec((BLK, width), first), pl.BlockSpec((BLK, width), second),
                  pl.BlockSpec((BLK, DIM), first), pl.BlockSpec((BLK, DIM), second)],
        out_specs=[pl.BlockSpec(shape, lambda i: (0, 0))] * count,
        out_shape=[sds(shape, BF)] * count,
        scratch_shapes=[pltpu.VMEM((width, DIM), F32)],
        compiler_params=params(dimension_semantics=("arbitrary",)),
        cost_estimate=cost(2 * 2 * SEQ * width * DIM, 20e6),
        name="wgrad",
    )(*left, *right)


def local_block(x_loc, wq, wk, wv, wo, gq, gk, ga, dy_loc):
    gather = functools.partial(lax.all_gather, axis_name='tp')
    w_loc = jnp.concatenate([wq, wk, wv], axis=1)
    gq, gk, ga = gq[None, :], gk[None, :], ga[None, :]
    cos, sin = rope_tables()
    xs, dys = [x_loc[0], x_loc[1]], [dy_loc[0], dy_loc[1]]
    x_full = []
    for b in range(2):
        src = xs[b] if b == 0 else lax.optimization_barrier((xs[b], x_full[0][:8, :HD]))[0]
        x_full.append(gather(xs[b], axis=0, tiled=True))
    wo_src = lax.optimization_barrier((wo, x_full[1][:8, :HD]))[0]
    wo_full = gather(wo_src, axis=0, tiled=True)
    w_src = lax.optimization_barrier((w_loc, wo_full[:8, :HD]))[0]
    w_full = gather(w_src, axis=0, tiled=False)

    fwd, o_recv = [], []
    for b in range(2):
        q_raw, k_raw, v, s = project(x_full[b], w_loc)
        q_rot, k_rot, iq, ik = norm_rope(q_raw, k_raw, s, gq, gk, cos, sin, 1 + b)
        o, lse = attention(q_rot, k_rot, v)
        o_recv.append(all_to_all(heads_to_tokens_kernel, o, (TOK, DIM), 3 + b))
        fwd.append((q_raw, k_raw, v, q_rot, k_rot, iq, ik, o, lse))
    ys, das, dhs, ggas = [], [], [], []
    for b in range(2):
        y, da, dh, gga = out_block(o_recv[b], wo_full, xs[b], dys[b], ga)
        ys.append(y)
        das.append(da)
        dhs.append(all_to_all(tokens_to_heads_kernel, dh, (SEQ, LOC), 5 + b))
        ggas.append(gga)
    da_full = [gather(das[b], axis=0, tiled=True) for b in range(2)]
    ds, d_recv, gga_sum, ggs = [], [], [], []
    for b in range(2):
        q_raw, k_raw, v, q_rot, k_rot, iq, ik, o, lse = fwd[b]
        dqu, dku, dv, dots, gg = attention_bwd(q_rot, k_rot, v, dhs[b], lse, q_raw, k_raw, iq, ik, gq, gk, cos, sin)
        d, gsum = norm_bwd(dqu, dku, dv, q_raw, k_raw, iq, ik, dots, ggas[b], 7 + b)
        ds.append(d)
        gga_sum.append(gsum)
        ggs.append(gg)
        d_recv.append(all_to_all(heads_to_tokens_kernel, d, (TOK, 3 * DIM), 9 + b))
    gwq, gwk, gwv = wgrad(ds, x_full, True)
    gwo, = wgrad([fwd[0][7], fwd[1][7]], da_full, False)
    dx0, dx1 = dx_block(d_recv[0], d_recv[1], w_full, dys[0], dys[1])
    gg = ggs[0] + ggs[1]
    grad_ga = (gga_sum[0] + gga_sum[1]).reshape(DIM).astype(BF)
    return (jnp.stack(ys), jnp.stack([dx0, dx1]), gwq, gwk, gwv, gwo, gg[0].astype(BF), gg[1].astype(BF), grad_ga)


def solution(mesh):
    act, col, row, vec = P(None, 'tp', None), P(None, 'tp'), P('tp', None), P('tp')
    in_specs = (act, col, col, col, row, vec, vec, P(), act)
    out_specs = (act, act, col, col, col, row, vec, vec, P())
    return jax.shard_map(local_block, mesh=mesh, in_specs=in_specs, out_specs=out_specs, check_vma=False)
```

```python
import functools
import math

import jax
import jax.numpy as jnp
from jax import lax
from jax.experimental import pallas as pl
from jax.experimental.pallas import tpu as pltpu
from jax.sharding import PartitionSpec as P

HD = 128
ROPE_THETA = 500000.0
EPS = 1e-6
DIM = 2048
SEQ = 2048
LOC = 256
TOK = 256
BLK = 512
NB = SEQ // BLK
NDEV = 8
SCALE = HD ** -0.5
C2 = SCALE * math.log2(math.e)
MESH = pl.DeviceIdType.MESH
BF = jnp.bfloat16
F32 = jnp.float32
VMEM_MAX = 60 * 1024 * 1024

NT = (((1,), (1,)), ((), ()))
NN = (((1,), (0,)), ((), ()))


def dot(a, b, dims=NN):
    return lax.dot_general(a, b, dims, preferred_element_type=F32)


def sds(shape, dtype):
    return jax.ShapeDtypeStruct(shape, dtype)


def cost(flops, nbytes, trans=0):
    return pl.CostEstimate(flops=int(flops), bytes_accessed=int(nbytes), transcendentals=int(trans))


def params(**kw):
    return pltpu.CompilerParams(vmem_limit_bytes=VMEM_MAX, **kw)


def peer_of(me, mask):
    core, ax, ay = me % 2, (me // 2) % 2, me // 4
    core = 1 - core if mask & 1 else core
    ax = 1 - ax if mask & 2 else ax
    ay = 1 - ay if mask & 4 else ay
    return ay * 4 + ax * 2 + core


ORDER = (6, 7, 2, 4, 3, 5, 1)


def entry_barrier(me):
    barrier = pltpu.get_barrier_semaphore()
    for mask in ORDER:
        pl.semaphore_signal(barrier, inc=1, device_id=(peer_of(me, mask),), device_id_type=MESH)
    pl.semaphore_wait(barrier, NDEV - 1)


def rope_tables():
    half = HD // 2
    inv_freq = 1.0 / (ROPE_THETA ** (jnp.arange(half, dtype=F32) / half))
    angles = jnp.arange(SEQ, dtype=F32)[:, None] * inv_freq[None, :]
    cos, sin = jnp.cos(angles), jnp.sin(angles)
    return jnp.concatenate([cos, cos], axis=1), jnp.concatenate([-sin, sin], axis=1)


def row_sums(vals):
    folded = vals[:, :HD]
    for start in range(HD, vals.shape[1], HD):
        folded = folded + vals[:, start:start + HD]
    return jnp.sum(folded.T, axis=0, keepdims=True)


def as_column(row):
    return jnp.broadcast_to(row, (HD, row.shape[1])).T


def proj_kernel(x_ref, w_ref, *rest):
    q_ref, k_ref, v_ref, s_ref = rest[-5:-1] if len(rest) == 6 else rest
    i = pl.program_id(0)
    x = x_ref[...]
    q = dot(x, w_ref[:, :LOC])
    q_ref[...] = q
    s_ref[pl.ds(i, 1), :] = row_sums(q * q)
    k = dot(x, w_ref[:, LOC:2 * LOC])
    k_ref[...] = k
    s_ref[pl.ds(i + NB, 1), :] = row_sums(k * k)
    v_ref[...] = dot(x, w_ref[:, 2 * LOC:]).astype(BF)


def project(x, w, through=()):
    row = pl.BlockSpec((BLK, LOC), lambda i: (i, 0))
    whole = [pl.BlockSpec(memory_space=pl.ANY)] * len(through)
    return pl.pallas_call(
        proj_kernel,
        grid=(NB,),
        in_specs=[pl.BlockSpec((BLK, DIM), lambda i: (i, 0)), pl.BlockSpec((DIM, 3 * LOC), lambda i: (0, 0))] + whole,
        out_specs=[row, row, row, pl.BlockSpec((2 * NB, BLK), lambda i: (0, 0))] + whole,
        out_shape=[sds((SEQ, LOC), F32), sds((SEQ, LOC), F32), sds((SEQ, LOC), BF), sds((2 * NB, BLK), F32)]
        + [sds(t.shape, t.dtype) for t in through],
        input_output_aliases={2 + n: 4 + n for n in range(len(through))},
        compiler_params=params(dimension_semantics=("arbitrary",)),
        cost_estimate=cost(2 * SEQ * DIM * 3 * LOC, 16e6),
        name="proj",
    )(x, w, *through)


def exchange(me, srcs, slots, send_sems, recv_sems):
    entry_barrier(me)
    copies = []
    for n, (src, slot) in enumerate(zip(srcs, slots)):
        for p, mask in enumerate(ORDER):
            copies.append(pltpu.make_async_remote_copy(
                src_ref=src, dst_ref=slot.at[p], send_sem=send_sems.at[n, p], recv_sem=recv_sems.at[n, p],
                device_id=(peer_of(me, mask),), device_id_type=MESH))
    for c in copies:
        c.start()
    for c in copies:
        c.wait()


def ordered_total(me, src, slot):
    own = src[...]
    total = jnp.zeros_like(own)
    for dev in range(NDEV):
        term = jnp.where(me == dev, own, 0.0)
        for p, mask in enumerate(ORDER):
            term = term + jnp.where(peer_of(me, mask) == dev, slot[p], 0.0)
        total = total + term
    return total


def rotated(v, cos, sin):
    out = []
    for h in range(v.shape[1] // HD):
        part = v[:, h * HD:(h + 1) * HD]
        out.append(part * cos + pltpu.roll(part, HD // 2, 1) * sin)
    return out


def norm_kernel(q_ref, k_ref, s_ref, gq_ref, gk_ref, cos_ref, sin_ref, qo_ref, ko_ref, iq_ref, ik_ref,
                slot, total, send_sems, recv_sems):
    i = pl.program_id(0)
    me = lax.axis_index('tp')

    @pl.when(i == 0)
    def _():
        exchange(me, [s_ref], [slot], send_sems, recv_sems)
        total[...] = lax.rsqrt(ordered_total(me, s_ref, slot) / DIM + EPS)

    cos, sin = cos_ref[...], sin_ref[...]
    for src, dst, inv_ref, g_ref, row in ((q_ref, qo_ref, iq_ref, gq_ref, i), (k_ref, ko_ref, ik_ref, gk_ref, i + NB)):
        inv = as_column(total[pl.ds(row, 1), :])
        inv_ref[...] = inv
        g = g_ref[...].astype(F32)
        for h in range(LOC // HD):
            sl = slice(h * HD, (h + 1) * HD)
            hat = src[:, sl] * inv * g[:, sl]
            dst[:, sl] = (hat * cos + pltpu.roll(hat, HD // 2, 1) * sin).astype(BF)


def norm_rope(q, k, s, gq, gk, cos, sin, cid):
    row = pl.BlockSpec((BLK, LOC), lambda i: (i, 0))
    half = pl.BlockSpec((BLK, HD), lambda i: (i, 0))
    gain = pl.BlockSpec((1, LOC), lambda i: (0, 0))
    return pl.pallas_call(
        norm_kernel,
        grid=(NB,),
        in_specs=[row, row, pl.BlockSpec((2 * NB, BLK), lambda i: (0, 0)), gain, gain, half, half],
        out_specs=[row, row, half, half],
        out_shape=[sds((SEQ, LOC), BF), sds((SEQ, LOC), BF), sds((SEQ, HD), F32), sds((SEQ, HD), F32)],
        scratch_shapes=[pltpu.VMEM((NDEV - 1, 2 * NB, BLK), F32), pltpu.VMEM((2 * NB, BLK), F32),
                        pltpu.SemaphoreType.DMA((1, NDEV - 1)), pltpu.SemaphoreType.DMA((1, NDEV - 1))],
        compiler_params=params(dimension_semantics=("arbitrary",), collective_id=cid, has_side_effects=True),
        cost_estimate=cost(2e9, 10e6),
        name="norm_rope",
    )(q, k, s, gq, gk, cos, sin)


def causal_mask():
    keys = lax.broadcasted_iota(jnp.int32, (BLK, BLK), 0)
    queries = lax.broadcasted_iota(jnp.int32, (BLK, BLK), 1)
    return keys <= queries


def attn_kernel(q_ref, k_ref, v_ref, o_ref, lse_ref, recv_ref, p_scr, vt_scr, acc_scr, o_scr, send_sems, recv_sems, own_sems):
    h, step = pl.program_id(0), pl.program_id(1)
    me = lax.axis_index('tp')
    qi = (me // 2 + 1 + step) % NB
    rows = pl.ds(pl.multiple_of(qi * BLK, BLK), BLK)

    @pl.when(jnp.logical_and(h == 0, step == 0))
    def _():
        entry_barrier(me)

    @pl.when(step == 0)
    def _():
        vt_scr[...] = v_ref[...].T

    qb = q_ref[rows, :]

    def scores(j):
        return dot(k_ref[pl.ds(pl.multiple_of(j * BLK, BLK), BLK), :], qb, NT)

    def first(j, m):
        s = scores(j)
        p_scr[j] = s
        return jnp.maximum(m, jnp.max(s.reshape(BLK // 8, 8, BLK), axis=0))

    s = jnp.where(causal_mask(), scores(qi), -1e30)
    p_scr[qi] = s
    m = lax.fori_loop(0, qi, first, jnp.max(s.reshape(BLK // 8, 8, BLK), axis=0))
    m = jnp.max(m, axis=0, keepdims=True)

    def second(j, l):
        p = jnp.exp2((p_scr[j] - m) * C2)
        p_scr[j] = p
        return l + jnp.sum(p.reshape(BLK // 8, 8, BLK), axis=0)

    l = lax.fori_loop(0, qi + 1, second, jnp.zeros((8, BLK), F32))
    l = jnp.sum(l, axis=0, keepdims=True)
    rl = 1.0 / l
    lse_ref[pl.ds(h * NB + qi, 1), :] = m * C2 + jnp.log2(l)

    acc_scr[...] = jnp.zeros_like(acc_scr)

    def third(j, carry):
        p = (p_scr[j] * rl).astype(BF)
        acc_scr[...] += dot(vt_scr[:, pl.ds(pl.multiple_of(j * BLK, BLK), BLK)], p)
        return carry

    lax.fori_loop(0, qi + 1, third, 0)
    out = acc_scr[...].T.astype(BF)
    o_scr[h, step] = out
    o_ref[rows, :] = out

    def block_copy(hh, st, half, remote):
        dest = 2 * ((me // 2 + 1 + st) % NB) + half
        src = o_scr.at[hh, st, pl.ds(half * TOK, TOK), :]
        dst = recv_ref.at[:, pl.ds(pl.multiple_of(me * LOC + hh * HD, HD), HD)]
        if remote:
            return dest, pltpu.make_async_remote_copy(
                src_ref=src, dst_ref=dst, send_sem=send_sems.at[hh, st, half], recv_sem=recv_sems.at[hh, me],
                device_id=(dest,), device_id_type=MESH)
        return dest, pltpu.make_async_copy(src, dst, own_sems.at[hh])

    for half in range(2):
        dest, away = block_copy(h, step, half, True)
        _, here = block_copy(h, step, half, False)
        pl.when(dest != me)(away.start)
        pl.when(dest == me)(here.start)

    @pl.when(jnp.logical_and(h == 1, step == NB - 1))
    def _():
        for hh in range(2):
            for st in range(NB):
                for half in range(2):
                    dest, away = block_copy(hh, st, half, True)
                    _, here = block_copy(hh, st, half, False)
                    if st < NB - 1:
                        away.wait_send()
                    else:
                        pl.when(dest != me)(away.wait_send)
                        pl.when(dest == me)(here.wait)
            for mask in ORDER:
                peer = peer_of(me, mask)
                pltpu.make_async_remote_copy(
                    src_ref=o_scr.at[0, 0, pl.ds(0, TOK), :],
                    dst_ref=recv_ref.at[:, pl.ds(pl.multiple_of(peer * LOC + hh * HD, HD), HD)],
                    send_sem=send_sems.at[0, 0, 0], recv_sem=recv_sems.at[hh, peer],
                    device_id=(peer,), device_id_type=MESH).wait_recv()


def attention(q, k, v, cid):
    full = pl.BlockSpec((SEQ, HD), lambda h, i: (0, h))
    return pl.pallas_call(
        attn_kernel,
        grid=(2, NB),
        in_specs=[full, full, full],
        out_specs=[full, pl.BlockSpec((2 * NB, BLK), lambda h, i: (0, 0)), pl.BlockSpec(memory_space=pl.ANY)],
        out_shape=[sds((SEQ, LOC), BF), sds((2 * NB, BLK), F32), sds((TOK, DIM), BF)],
        scratch_shapes=[pltpu.VMEM((NB, BLK, BLK), F32), pltpu.VMEM((HD, SEQ), BF), pltpu.VMEM((HD, BLK), F32),
                        pltpu.VMEM((2, NB, BLK, HD), BF), pltpu.SemaphoreType.DMA((2, NB, 2)),
                        pltpu.SemaphoreType.DMA((2, NDEV)), pltpu.SemaphoreType.DMA((2,))],
        compiler_params=params(dimension_semantics=("arbitrary", "arbitrary"), collective_id=cid, has_side_effects=True),
        cost_estimate=cost(9e9, 6e6),
        name="attn_fwd",
    )(q, k, v)


def out_kernel(o_ref, wo_ref, x_ref, dy_ref, ga_ref, y_ref, da_ref, gga_ref, recv_ref, a_scr, dh_scr, send_sems, recv_sems, own_sem):
    me = lax.axis_index('tp')
    entry_barrier(me)
    step = DIM // NB
    o = o_ref[...]

    def fwd(j, carry):
        cols = pl.ds(pl.multiple_of(j * step, step), step)
        a_scr[:, cols] = dot(o, wo_ref[:, cols])
        return carry

    lax.fori_loop(0, NB, fwd, 0)
    a = a_scr[...]
    r = lax.rsqrt(jnp.mean(a * a, axis=-1, keepdims=True) + EPS)
    n = a * r
    ga = ga_ref[...].astype(F32)
    dy = dy_ref[...].astype(F32)
    y_ref[...] = (x_ref[...].astype(F32) + n * ga).astype(BF)
    col = jnp.sum(dy * n, axis=0, keepdims=True)
    for i in range(8):
        gga_ref[i:i + 1, :] = col[:, i * (DIM // 8):(i + 1) * (DIM // 8)]
    gn = dy * ga
    da_ref[...] = (r * (gn - n * jnp.mean(gn * n, axis=-1, keepdims=True))).astype(BF)
    da = da_ref[...]
    mine = recv_ref.at[pl.ds(pl.multiple_of(me * TOK, TOK), TOK), :]

    def block_copy(st, half):
        dest = 2 * ((me // 2 + 1 + st) % NB) + half
        src = dh_scr.at[st, :, pl.ds(half * LOC, LOC)]
        away = pltpu.make_async_remote_copy(
            src_ref=src, dst_ref=mine, send_sem=send_sems.at[st, half], recv_sem=recv_sems.at[me],
            device_id=(dest,), device_id_type=MESH)
        return dest, away, pltpu.make_async_copy(src, mine, own_sem)

    def bwd(st, carry):
        blk = (me // 2 + 1 + st) % NB
        dh_scr[st] = dot(da, wo_ref[pl.ds(pl.multiple_of(blk * step, step), step), :], NT).astype(BF)
        for half in range(2):
            dest, away, here = block_copy(st, half)
            pl.when(dest != me)(away.start)
            pl.when(dest == me)(here.start)
        return carry

    lax.fori_loop(0, NB, bwd, 0)
    for st in range(NB):
        for half in range(2):
            dest, away, here = block_copy(st, half)
            if st < NB - 1:
                away.wait_send()
            else:
                pl.when(dest != me)(away.wait_send)
                pl.when(dest == me)(here.wait)
    for mask in ORDER:
        peer = peer_of(me, mask)
        pltpu.make_async_remote_copy(
            src_ref=dh_scr.at[0, :, pl.ds(0, LOC)], dst_ref=recv_ref.at[pl.ds(pl.multiple_of(peer * TOK, TOK), TOK), :],
            send_sem=send_sems.at[0, 0], recv_sem=recv_sems.at[peer], device_id=(peer,), device_id_type=MESH).wait_recv()


def out_block(o, wo, x, dy, ga, cid):
    spec = pl.BlockSpec(memory_space=pltpu.VMEM)
    return pl.pallas_call(
        out_kernel,
        in_specs=[spec] * 5,
        out_specs=[spec] * 3 + [pl.BlockSpec(memory_space=pl.ANY)],
        out_shape=[sds((TOK, DIM), BF), sds((TOK, DIM), BF), sds((8, DIM // 8), F32), sds((SEQ, LOC), BF)],
        scratch_shapes=[pltpu.VMEM((TOK, DIM), F32), pltpu.VMEM((NB, TOK, DIM // NB), BF), pltpu.SemaphoreType.DMA((NB, 2)),
                        pltpu.SemaphoreType.DMA((NDEV,)), pltpu.SemaphoreType.DMA],
        compiler_params=params(collective_id=cid, has_side_effects=True),
        cost_estimate=cost(4 * TOK * DIM * DIM + 5e9, 14e6),
        name="out_block",
    )(o, wo, x, dy, ga)


def attn_bwd_kernel(q_ref, k_ref, v_ref, do_ref, lse_ref, qr_ref, kr_ref, iq_ref, ik_ref, gq_ref, gk_ref, cos_ref, sin_ref,
                    dqu_ref, dku_ref, dv_ref, dots_ref, gg_ref,
                    p_scr, dp_scr, kt_scr, dqt_scr, dq_scr, dk_scr, dv_scr):
    h, qi = pl.program_id(0), pl.program_id(1)

    @pl.when(qi == 0)
    def _():
        kt_scr[...] = k_ref[...].T
        dk_scr[...] = jnp.zeros_like(dk_scr)
        dv_scr[...] = jnp.zeros_like(dv_scr)

    qb = q_ref[...]
    dob = do_ref[...]
    lse = lse_ref[pl.ds(h * NB + qi, 1), :]

    def first(j, acc, diag=False):
        rows = pl.ds(pl.multiple_of(j * BLK, BLK), BLK)
        p = jnp.exp2(dot(k_ref[rows, :], qb, NT) * C2 - lse)
        if diag:
            p = jnp.where(causal_mask(), p, 0.0)
        dp = dot(v_ref[rows, :], dob, NT)
        p_scr[j] = p
        dp_scr[j] = dp
        dv_scr[rows, :] += dot(p.astype(BF), dob)
        return acc + jnp.sum((p * dp).reshape(BLK // 8, 8, BLK), axis=0)

    acc = first(qi, jnp.zeros((8, BLK), F32), True)
    acc = lax.fori_loop(0, qi, first, acc)
    delta = jnp.sum(acc, axis=0, keepdims=True)
    dqt_scr[...] = jnp.zeros_like(dqt_scr)

    def second(j, carry):
        rows = pl.ds(pl.multiple_of(j * BLK, BLK), BLK)
        ds = (p_scr[j] * (dp_scr[j] - delta) * SCALE).astype(BF)
        dk_scr[rows, :] += dot(ds, qb)
        dqt_scr[...] += dot(kt_scr[:, rows], ds)
        return carry

    lax.fori_loop(0, qi + 1, second, 0)
    dq_scr[pl.ds(pl.multiple_of(qi * BLK, BLK), BLK), :] = dqt_scr[...].T

    @pl.when(qi == NB - 1)
    def _():
        dv_ref[...] = dv_scr[...].astype(BF)

        @pl.when(h == 0)
        def _():
            dots_ref[...] = jnp.zeros_like(dots_ref)

        gg_ref[...] = jnp.zeros_like(gg_ref)

        def tail(i, carry):
            rows = pl.ds(pl.multiple_of(i * BLK, BLK), BLK)
            cos, sin = cos_ref[rows, :], sin_ref[rows, :]
            for n, (d_scr, raw_ref, inv_ref, g_ref, out_ref) in enumerate((
                    (dq_scr, qr_ref, iq_ref, gq_ref, dqu_ref), (dk_scr, kr_ref, ik_ref, gk_ref, dku_ref))):
                d = d_scr[rows, :]
                hat = d * cos - pltpu.roll(d, HD // 2, 1) * sin
                unit = raw_ref[rows, :] * inv_ref[rows, :]
                gg_ref[n:n + 1, :] += jnp.sum(hat * unit, axis=0, keepdims=True)
                du = hat * g_ref[...].astype(F32)
                out_ref[rows, :] = du
                dots_ref[pl.ds(i + n * NB, 1), :] += row_sums(du * unit)
            return carry

        lax.fori_loop(0, NB, tail, 0)


def attention_bwd(q, k, v, do, lse, qr, kr, iq, ik, gq, gk, cos, sin):
    blk = pl.BlockSpec((BLK, HD), lambda h, i: (i, h))
    full = pl.BlockSpec((SEQ, HD), lambda h, i: (0, h))
    shared = pl.BlockSpec((SEQ, HD), lambda h, i: (0, 0))
    gain = pl.BlockSpec((1, HD), lambda h, i: (0, h))
    rows = pl.BlockSpec((2 * NB, BLK), lambda h, i: (0, 0))
    return pl.pallas_call(
        attn_bwd_kernel,
        grid=(2, NB),
        in_specs=[blk, full, full, blk, rows, full, full, shared, shared, gain, gain, shared, shared],
        out_specs=[full, full, full, rows, pl.BlockSpec((8, HD), lambda h, i: (0, h))],
        out_shape=[sds((SEQ, LOC), F32), sds((SEQ, LOC), F32), sds((SEQ, LOC), BF), sds((2 * NB, BLK), F32),
                   sds((8, LOC), F32)],
        scratch_shapes=[pltpu.VMEM((NB, BLK, BLK), F32), pltpu.VMEM((NB, BLK, BLK), F32), pltpu.VMEM((HD, SEQ), BF),
                        pltpu.VMEM((HD, BLK), F32), pltpu.VMEM((SEQ, HD), F32), pltpu.VMEM((SEQ, HD), F32),
                        pltpu.VMEM((SEQ, HD), F32)],
        compiler_params=params(dimension_semantics=("arbitrary", "arbitrary")),
        cost_estimate=cost(16e9, 16e6),
        name="attn_bwd",
    )(q, k, v, do, lse, qr, kr, iq, ik, gq, gk, cos, sin)


def norm_bwd_kernel(dqu_ref, dku_ref, dv_ref, qr_ref, kr_ref, iq_ref, ik_ref, dots_ref, ga_ref, out_ref, gga_ref,
                    slot, ga_slot, total, send_sems, recv_sems):
    i = pl.program_id(0)
    me = lax.axis_index('tp')

    @pl.when(i == 0)
    def _():
        exchange(me, [dots_ref, ga_ref], [slot, ga_slot], send_sems, recv_sems)
        total[...] = ordered_total(me, dots_ref, slot) / DIM
        gga_ref[...] = ordered_total(me, ga_ref, ga_slot)

    for n, (du_ref, raw_ref, inv_ref) in enumerate(((dqu_ref, qr_ref, iq_ref), (dku_ref, kr_ref, ik_ref))):
        dots = as_column(total[pl.ds(i + n * NB, 1), :])
        inv = inv_ref[...]
        for h in range(LOC // HD):
            sl = slice(h * HD, (h + 1) * HD)
            unit = raw_ref[:, sl] * inv
            out_ref[:, n * LOC + h * HD:n * LOC + (h + 1) * HD] = (inv * (du_ref[:, sl] - unit * dots)).astype(BF)
    out_ref[:, 2 * LOC:] = dv_ref[...]


def norm_bwd(dqu, dku, dv, qr, kr, iq, ik, dots, gga, cid):
    row = pl.BlockSpec((BLK, LOC), lambda i: (i, 0))
    half = pl.BlockSpec((BLK, HD), lambda i: (i, 0))
    rows = pl.BlockSpec((2 * NB, BLK), lambda i: (0, 0))
    gsp = pl.BlockSpec((8, DIM // 8), lambda i: (0, 0))
    return pl.pallas_call(
        norm_bwd_kernel,
        grid=(NB,),
        in_specs=[row, row, row, row, row, half, half, rows, gsp],
        out_specs=[pl.BlockSpec((BLK, 3 * LOC), lambda i: (i, 0)), gsp],
        out_shape=[sds((SEQ, 3 * LOC), BF), sds((8, DIM // 8), F32)],
        scratch_shapes=[pltpu.VMEM((NDEV - 1, 2 * NB, BLK), F32), pltpu.VMEM((NDEV - 1, 8, DIM // 8), F32),
                        pltpu.VMEM((2 * NB, BLK), F32),
                        pltpu.SemaphoreType.DMA((2, NDEV - 1)), pltpu.SemaphoreType.DMA((2, NDEV - 1))],
        compiler_params=params(dimension_semantics=("arbitrary",), collective_id=cid, has_side_effects=True),
        cost_estimate=cost(2e9, 14e6),
        name="norm_bwd",
    )(dqu, dku, dv, qr, kr, iq, ik, dots, gga)


HALF = DIM // 2
CH = 256


def grads_kernel(d0, d1, w, x0, x1, o0, o1, da0, da1, dy_ref, dx_ref, gwq_ref, gwk_ref, gwv_ref, gwo_ref,
                 d_all, w_all, sbuf, r1, r2, fin, acc, xbuf, obuf,
                 dl_sems, dsnd_sems, drcv_sems, w_sems, s1_sems, r1_sems, s2_sems, r2_sems, fs_sems, fr_sems, x_sems, o_sems):
    me = lax.axis_index('tp')
    core, chip = me % 2, me // 2
    partner = peer_of(me, 1)
    first = peer_of(me, 2) * (1 - core) + peer_of(me, 4) * core
    second = peer_of(me, 4) * (1 - core) + peer_of(me, 2) * core
    diag_chip, first_chip, second_chip = peer_of(me, 6) // 2, first // 2, second // 2
    d_src = (d0, d1)

    barrier = pltpu.get_barrier_semaphore()
    for dev in (partner, first, second):
        pl.semaphore_signal(barrier, inc=1, device_id=(dev,), device_id_type=MESH)
    pl.semaphore_wait(barrier, 3)

    def rows_of(blk):
        return pl.ds(pl.multiple_of(blk * BLK, BLK), BLK)

    def half_rows(c):
        return pl.ds(pl.multiple_of(c * HALF, HALF), HALF)

    chips = (diag_chip, first_chip, second_chip, chip)
    w_out = pltpu.make_async_remote_copy(
        src_ref=w.at[half_rows(1 - core), :], dst_ref=w_all.at[1], send_sem=w_sems.at[0], recv_sem=w_sems.at[1],
        device_id=(partner,), device_id_type=MESH)
    w_own = pltpu.make_async_copy(w.at[half_rows(core), :], w_all.at[0], w_sems.at[2])
    w_out.start()
    w_own.start()
    swaps, loads = [], []
    for kind in range(4):
        for b in range(2):
            n = 2 * kind + b
            rows = rows_of(chips[kind])
            loads.append(pltpu.make_async_copy(d_src[b].at[rows, :], d_all.at[0, b, rows, :], dl_sems.at[n]))
            kp = {0: 0, 1: 2, 2: 1, 3: 3}[kind]
            prow = rows_of(chips[kp])
            swaps.append(pltpu.make_async_remote_copy(
                src_ref=d_src[b].at[prow, :], dst_ref=d_all.at[1, b, prow, :], send_sem=dsnd_sems.at[n],
                recv_sem=drcv_sems.at[n], device_id=(partner,), device_id_type=MESH))
    for load, swap in zip(loads, swaps):
        swap.start()
        load.start()
    w_own.wait()
    w_out.wait()

    def arrived(n, b, blk):
        rows = rows_of(blk)
        pltpu.make_async_copy(d0.at[rows, :], d_all.at[0, b, rows, :], dl_sems.at[n]).wait()
        pltpu.make_async_remote_copy(
            src_ref=d0.at[rows, :], dst_ref=d_all.at[1, b, rows, :], send_sem=dsnd_sems.at[n],
            recv_sem=drcv_sems.at[n], device_id=(partner,), device_id_type=MESH).wait()

    def partial(b, blk):
        rows = rows_of(blk)
        return dot(d_all[0, b, rows, :], w_all[0], NT) + dot(d_all[1, b, rows, :], w_all[1], NT)

    def to_first(n):
        return pltpu.make_async_remote_copy(
            src_ref=sbuf.at[n], dst_ref=r1.at[n], send_sem=s1_sems.at[n], recv_sem=r1_sems.at[n],
            device_id=(first,), device_id_type=MESH)

    def to_second(b):
        return pltpu.make_async_remote_copy(
            src_ref=r1.at[b], dst_ref=r2.at[b], send_sem=s2_sems.at[b], recv_sem=r2_sems.at[b],
            device_id=(second,), device_id_type=MESH)

    def to_partner(b):
        return pltpu.make_async_remote_copy(
            src_ref=r1.at[2 + b, pl.ds(pl.multiple_of((1 - core) * TOK, TOK), TOK), :], dst_ref=fin.at[b],
            send_sem=fs_sems.at[b], recv_sem=fr_sems.at[b], device_id=(partner,), device_id_type=MESH)

    def phase1(n, carry):
        kind, b = n // 2, n % 2
        blk = diag_chip * (1 - kind) + first_chip * kind
        arrived(n, b, blk)
        sbuf[n] = partial(b, blk)
        to_first(n).start()
        return carry

    lax.fori_loop(0, 4, phase1, 0)
    for n in range(4, 8):
        arrived(n, n % 2, chips[n // 2])

    steps = SEQ // CH

    def chunk(i):
        return pl.ds(pl.multiple_of(i * CH, CH), CH)

    def stream(pairs, body):
        def fetch(i):
            return [pltpu.make_async_copy(src.at[chunk(i), :], buf.at[i % 2], sems.at[i % 2]) for src, buf, sems in pairs]

        for c in fetch(0):
            c.start()

        def it(i, carry):
            @pl.when(i + 1 < steps)
            def _():
                for c in fetch(i + 1):
                    c.start()

            for c in fetch(i):
                c.wait()
            body(i)
            return carry

        lax.fori_loop(0, steps, it, 0)

    def wgrad(b, src):
        def body(i):
            left = d_all[0, b, chunk(i), :].T
            for c in range(3):
                part = slice(c * LOC, (c + 1) * LOC)
                acc[part, :] += dot(left[part, :], xbuf[i % 2])

        stream([(src, xbuf, x_sems)], body)

    def forward_second(b, carry):
        to_first(b).wait_recv()
        r1[b] += partial(b, second_chip)
        to_second(b).start()
        return carry

    acc[...] = jnp.zeros_like(acc)
    wgrad(0, x0)
    forward_second(0, 0)
    wgrad(1, x1)
    for n, ref in enumerate((gwq_ref, gwk_ref, gwv_ref)):
        ref[...] = acc[n * LOC:(n + 1) * LOC, :].T.astype(BF)
    forward_second(1, 0)
    acc[:LOC, :] = jnp.zeros((LOC, DIM), F32)

    def wo_body(i):
        acc[:LOC, :] += dot(obuf[i % 2].T, xbuf[i % 2])

    for o_src, da_src in ((o0, da0), (o1, da1)):
        stream([(da_src, xbuf, x_sems), (o_src, obuf, o_sems)], wo_body)
    gwo_ref[...] = acc[:LOC, :].astype(BF)

    def own_part(b, carry):
        r1_own = partial(b, chip)
        to_first(2 + b).wait_recv()
        to_second(b).wait_recv()
        r1[2 + b] += r1_own + r2[b]
        to_partner(b).start()
        cols = half_rows(core)
        rows = pl.ds(pl.multiple_of(core * TOK, TOK), TOK)
        dx_ref[b, :, cols] = (r1[2 + b, rows, :] + dy_ref[b, :, cols].astype(F32)).astype(BF)
        return carry

    lax.fori_loop(0, 2, own_part, 0)

    def finish(b, carry):
        to_partner(b).wait()
        cols = half_rows(1 - core)
        dx_ref[b, :, cols] = (fin[b] + dy_ref[b, :, cols].astype(F32)).astype(BF)
        to_second(b).wait_send()
        to_first(b).wait_send()
        to_first(2 + b).wait_send()
        return carry

    lax.fori_loop(0, 2, finish, 0)


def grads(d0, d1, w, x0, x1, o0, o1, da0, da1, dy, cid):
    vm = pl.BlockSpec(memory_space=pltpu.VMEM)
    far = pl.BlockSpec(memory_space=pl.ANY)
    dma = pltpu.SemaphoreType.DMA
    return pl.pallas_call(
        grads_kernel,
        in_specs=[far] * 9 + [vm],
        out_specs=[vm] * 5,
        out_shape=[sds((2, TOK, DIM), BF)] + [sds((DIM, LOC), BF)] * 3 + [sds((LOC, DIM), BF)],
        scratch_shapes=[pltpu.VMEM((2, 2, SEQ, 3 * LOC), BF), pltpu.VMEM((2, HALF, 3 * LOC), BF),
                        pltpu.VMEM((4, BLK, HALF), F32), pltpu.VMEM((4, BLK, HALF), F32), pltpu.VMEM((2, BLK, HALF), F32),
                        pltpu.VMEM((2, TOK, HALF), F32), pltpu.VMEM((3 * LOC, DIM), F32),
                        pltpu.VMEM((2, CH, DIM), BF), pltpu.VMEM((2, CH, LOC), BF),
                        dma((8,)), dma((8,)), dma((8,)), dma((3,)), dma((4,)), dma((4,)), dma((2,)), dma((2,)),
                        dma((2,)), dma((2,)), dma((2,)), dma((2,))],
        compiler_params=pltpu.CompilerParams(vmem_limit_bytes=67043328, collective_id=cid, has_side_effects=True),
        cost_estimate=cost(100e9, 40e6),
        name="grads",
    )(d0, d1, w, x0, x1, o0, o1, da0, da1, dy)


def local_block(x_loc, wq, wk, wv, wo, gq, gk, ga, dy_loc):
    gather = functools.partial(lax.all_gather, axis_name='tp')
    w_loc = jnp.concatenate([wq, wk, wv], axis=1)
    gq, gk, ga = gq[None, :], gk[None, :], ga[None, :]
    cos, sin = rope_tables()
    xs, dys = [x_loc[0], x_loc[1]], [dy_loc[0], dy_loc[1]]
    x_full = [gather(xs[b], axis=0, tiled=True) for b in range(2)]

    fwd, o_recv = [], []
    for b in range(2):
        q_raw, k_raw, v, s, *through = project(x_full[b], w_loc, (wo,) if b == 0 else ())
        if b == 0:
            wo_full = gather(through[0], axis=0, tiled=True)
        q_rot, k_rot, iq, ik = norm_rope(q_raw, k_raw, s, gq, gk, cos, sin, 1 + b)
        o, lse, recv = attention(q_rot, k_rot, v, 3 + b)
        o_recv.append(recv)
        fwd.append((q_raw, k_raw, v, q_rot, k_rot, iq, ik, o, lse))
    ys, das, dhs, ggas = [], [], [], []
    for b in range(2):
        y, da, gga, dh = out_block(o_recv[b], wo_full, xs[b], dys[b], ga, 5 + b)
        ys.append(y)
        das.append(da)
        dhs.append(dh)
        ggas.append(gga)
    da_full = [gather(das[b], axis=0, tiled=True) for b in range(2)]
    ds, gga_sum, ggs = [], [], []
    for b in range(2):
        q_raw, k_raw, v, q_rot, k_rot, iq, ik, o, lse = fwd[b]
        dqu, dku, dv, dots, gg = attention_bwd(q_rot, k_rot, v, dhs[b], lse, q_raw, k_raw, iq, ik, gq, gk, cos, sin)
        d, gsum = norm_bwd(dqu, dku, dv, q_raw, k_raw, iq, ik, dots, ggas[b], 7 + b)
        ds.append(d)
        gga_sum.append(gsum)
        ggs.append(gg)
    dx, gwq, gwk, gwv, gwo = grads(ds[0], ds[1], w_loc, x_full[0], x_full[1], fwd[0][7], fwd[1][7], da_full[0], da_full[1], dy_loc, 9)
    gg = ggs[0] + ggs[1]
    grad_ga = (gga_sum[0] + gga_sum[1]).reshape(DIM).astype(BF)
    return (jnp.stack(ys), dx, gwq, gwk, gwv, gwo, gg[0].astype(BF), gg[1].astype(BF), grad_ga)


def solution(mesh):
    act, col, row, vec = P(None, 'tp', None), P(None, 'tp'), P('tp', None), P('tp')
    in_specs = (act, col, col, col, row, vec, vec, P(), act)
    out_specs = (act, act, col, col, col, row, vec, vec, P())
    return jax.shard_map(local_block, mesh=mesh, in_specs=in_specs, out_specs=out_specs, check_vma=False)
```

```python
import functools
import math

import jax
import jax.numpy as jnp
from jax import lax
from jax.experimental import pallas as pl
from jax.experimental.pallas import tpu as pltpu
from jax.sharding import PartitionSpec as P

HD = 128
ROPE_THETA = 500000.0
EPS = 1e-6
DIM = 2048
SEQ = 2048
LOC = 256
TOK = 256
BLK = 512
NB = SEQ // BLK
NDEV = 8
SCALE = HD ** -0.5
C2 = SCALE * math.log2(math.e)
MESH = pl.DeviceIdType.MESH
BF = jnp.bfloat16
F32 = jnp.float32
VMEM_MAX = 60 * 1024 * 1024

NT = (((1,), (1,)), ((), ()))
NN = (((1,), (0,)), ((), ()))


def dot(a, b, dims=NN):
    return lax.dot_general(a, b, dims, preferred_element_type=F32)


def sds(shape, dtype):
    return jax.ShapeDtypeStruct(shape, dtype)


def cost(flops, nbytes, trans=0):
    return pl.CostEstimate(flops=int(flops), bytes_accessed=int(nbytes), transcendentals=int(trans))


def params(**kw):
    return pltpu.CompilerParams(vmem_limit_bytes=VMEM_MAX, **kw)


def peer_of(me, mask):
    core, ax, ay = me % 2, (me // 2) % 2, me // 4
    core = 1 - core if mask & 1 else core
    ax = 1 - ax if mask & 2 else ax
    ay = 1 - ay if mask & 4 else ay
    return ay * 4 + ax * 2 + core


ORDER = (6, 7, 2, 4, 3, 5, 1)


def entry_barrier(me):
    barrier = pltpu.get_barrier_semaphore()
    for mask in ORDER:
        pl.semaphore_signal(barrier, inc=1, device_id=(peer_of(me, mask),), device_id_type=MESH)
    pl.semaphore_wait(barrier, NDEV - 1)


def nbr_barrier(me):
    barrier = pltpu.get_barrier_semaphore()
    for mask in (1, 2, 4):
        pl.semaphore_signal(barrier, inc=1, device_id=(peer_of(me, mask),), device_id_type=MESH)
    pl.semaphore_wait(barrier, 3)


DMA = pltpu.SemaphoreType.DMA
ANYWHERE = pl.BlockSpec(memory_space=pl.ANY)
BG_SEMS = [DMA((8,)), DMA((8,)), DMA((2,))]


def shard_rows(dev, lo=0, count=TOK):
    return pl.ds(pl.multiple_of(dev * TOK + lo, HD), count)


def stage1(me, src, full, sems, lo=0, count=TOK, at=0):
    send, recv, own = sems
    there = full.at[shard_rows(me, lo, count), :]
    part = src.at[pl.ds(lo, count), :]
    copies = [pltpu.make_async_remote_copy(
        src_ref=part, dst_ref=there, send_sem=send.at[at + k], recv_sem=recv.at[at + k],
        device_id=(peer_of(me, mask),), device_id_type=MESH) for k, mask in enumerate((2, 4, 1))]
    return copies + [pltpu.make_async_copy(part, there, own.at[0])]


def stage2(me, full, sems, at=0):
    send, recv, _ = sems
    xn, yn = peer_of(me, 2), peer_of(me, 4)
    half = TOK // 2
    plan = ((shard_rows(yn, half, half), 2), (shard_rows(xn, 0, half), 4), (shard_rows(xn), 1), (shard_rows(yn), 1))
    return [pltpu.make_async_remote_copy(
        src_ref=full.at[rows, :], dst_ref=full.at[rows, :], send_sem=send.at[at + k], recv_sem=recv.at[at + k],
        device_id=(peer_of(me, mask),), device_id_type=MESH) for k, (rows, mask) in enumerate(plan)]


def stage3(me, full, sems, at=0):
    send, recv, _ = sems
    rows = shard_rows(peer_of(me, 6))
    return [pltpu.make_async_remote_copy(
        src_ref=full.at[rows, :], dst_ref=full.at[rows, :], send_sem=send.at[at], recv_sem=recv.at[at],
        device_id=(peer_of(me, 1),), device_id_type=MESH)]


def start(copies):
    for c in copies:
        c.start()


def wait(copies):
    for c in copies:
        c.wait()


def gather_kernel(x_ref, freq_ref, full_ref, cos_ref, sin_ref, *sems):
    me = lax.axis_index('tp')
    nbr_barrier(me)
    first = stage1(me, x_ref.at[0], full_ref, sems)
    start(first)
    freq = freq_ref[...]
    sign = jnp.where(lax.broadcasted_iota(jnp.int32, (TOK, HD), 1) < HD // 2, -1.0, 1.0)

    def table(i, carry):
        rows = pl.ds(pl.multiple_of(i * TOK, TOK), TOK)
        pos = (lax.broadcasted_iota(jnp.int32, (TOK, HD), 0) + i * TOK).astype(F32)
        angle = pos * freq
        cos_ref[rows, :] = jnp.cos(angle)
        sin_ref[rows, :] = jnp.sin(angle) * sign
        return carry

    lax.fori_loop(0, SEQ // TOK, table, 0)
    wait(first)
    second = stage2(me, full_ref, sems, 3)
    start(second)
    wait(second)
    third = stage3(me, full_ref, sems, 7)
    start(third)
    wait(third)


def first_gather(x, cid):
    half = HD // 2
    inv_freq = 1.0 / (ROPE_THETA ** (jnp.arange(half, dtype=F32) / half))
    freq = jnp.concatenate([inv_freq, inv_freq])[None, :]
    vm = pl.BlockSpec(memory_space=pltpu.VMEM)
    return pl.pallas_call(
        gather_kernel,
        in_specs=[ANYWHERE, vm],
        out_specs=[ANYWHERE, vm, vm],
        out_shape=[sds((SEQ, DIM), BF), sds((SEQ, HD), F32), sds((SEQ, HD), F32)],
        scratch_shapes=BG_SEMS,
        compiler_params=params(collective_id=cid, has_side_effects=True),
        cost_estimate=cost(20e9, 20e6),
        name="gather",
    )(x, freq)


def row_sums(vals):
    folded = vals[:, :HD]
    for start in range(HD, vals.shape[1], HD):
        folded = folded + vals[:, start:start + HD]
    return jnp.sum(folded.T, axis=0, keepdims=True)


def as_column(row):
    return jnp.broadcast_to(row, (HD, row.shape[1])).T


def proj_kernel(pick, x_ref, wq_ref, wk_ref, wv_ref, shard_ref, q_ref, k_ref, v_ref, s_ref, full_ref, *sems):
    i = pl.program_id(0)
    me = lax.axis_index('tp')
    src = shard_ref if pick is None else shard_ref.at[pick]

    @pl.when(i == 0)
    def _():
        nbr_barrier(me)
        start(stage1(me, src, full_ref, sems, 0, TOK // 2))

    x = x_ref[...]
    q = dot(x, wq_ref[...])
    q_ref[...] = q
    s_ref[pl.ds(i, 1), :] = row_sums(q * q)
    k = dot(x, wk_ref[...])
    k_ref[...] = k
    s_ref[pl.ds(i + NB, 1), :] = row_sums(k * k)
    v_ref[...] = dot(x, wv_ref[...]).astype(BF)

    @pl.when(i == NB - 1)
    def _():
        wait(stage1(me, src, full_ref, sems, 0, TOK // 2))


def project(x, wq, wk, wv, shard, pick, cid):
    row = pl.BlockSpec((BLK, LOC), lambda i: (i, 0))
    wspec = pl.BlockSpec((DIM, LOC), lambda i: (0, 0))
    return pl.pallas_call(
        functools.partial(proj_kernel, pick),
        grid=(NB,),
        in_specs=[pl.BlockSpec((BLK, DIM), lambda i: (i, 0)), wspec, wspec, wspec, ANYWHERE],
        out_specs=[row, row, row, pl.BlockSpec((2 * NB, BLK), lambda i: (0, 0)), ANYWHERE],
        out_shape=[sds((SEQ, LOC), F32), sds((SEQ, LOC), F32), sds((SEQ, LOC), BF), sds((2 * NB, BLK), F32),
                   sds((SEQ, DIM), BF)],
        scratch_shapes=BG_SEMS,
        compiler_params=params(dimension_semantics=("arbitrary",), collective_id=cid, has_side_effects=True),
        cost_estimate=cost(2 * SEQ * DIM * 3 * LOC, 16e6),
        name="proj",
    )(x, wq, wk, wv, shard)


def exchange(me, srcs, slots, send_sems, recv_sems):
    copies = []
    for n, (src, slot) in enumerate(zip(srcs, slots)):
        for p, mask in enumerate(ORDER):
            copies.append(pltpu.make_async_remote_copy(
                src_ref=src, dst_ref=slot.at[p], send_sem=send_sems.at[n, p], recv_sem=recv_sems.at[n, p],
                device_id=(peer_of(me, mask),), device_id_type=MESH))
    return copies


def ordered_total(me, src, slot):
    own = src[...]
    total = jnp.zeros_like(own)
    for dev in range(NDEV):
        term = jnp.where(me == dev, own, 0.0)
        for p, mask in enumerate(ORDER):
            term = term + jnp.where(peer_of(me, mask) == dev, slot[p], 0.0)
        total = total + term
    return total


def norm_kernel(pick, q_ref, k_ref, s_ref, gq_ref, gk_ref, cos_ref, sin_ref, shard_ref, full_in, qo_ref, ko_ref, iq_ref,
                ik_ref, full_ref, slot, total, send_sems, recv_sems, *sems):
    del full_in
    i = pl.program_id(0)
    me = lax.axis_index('tp')
    src = shard_ref if pick is None else shard_ref.at[pick]

    @pl.when(i == 0)
    def _():
        entry_barrier(me)
        sums = exchange(me, [s_ref], [slot], send_sems, recv_sems)
        start(sums)
        start(stage1(me, src, full_ref, sems, TOK // 2, TOK // 2))
        wait(sums)
        total[...] = lax.rsqrt(ordered_total(me, s_ref, slot) / DIM + EPS)

    cos, sin = cos_ref[...], sin_ref[...]
    for raw, dst, inv_ref, g_ref, row in ((q_ref, qo_ref, iq_ref, gq_ref, i), (k_ref, ko_ref, ik_ref, gk_ref, i + NB)):
        inv = as_column(total[pl.ds(row, 1), :])
        inv_ref[...] = inv
        g = g_ref[...].astype(F32)
        for h in range(LOC // HD):
            sl = slice(h * HD, (h + 1) * HD)
            hat = raw[:, sl] * inv * g[:, sl]
            dst[:, sl] = (hat * cos + pltpu.roll(hat, HD // 2, 1) * sin).astype(BF)

    @pl.when(i == NB - 1)
    def _():
        wait(stage1(me, src, full_ref, sems, TOK // 2, TOK // 2))


def norm_rope(q, k, s, gq, gk, cos, sin, shard, full, pick, cid):
    row = pl.BlockSpec((BLK, LOC), lambda i: (i, 0))
    half = pl.BlockSpec((BLK, HD), lambda i: (i, 0))
    gain = pl.BlockSpec((1, LOC), lambda i: (0, 0))
    return pl.pallas_call(
        functools.partial(norm_kernel, pick),
        grid=(NB,),
        in_specs=[row, row, pl.BlockSpec((2 * NB, BLK), lambda i: (0, 0)), gain, gain, half, half, ANYWHERE, ANYWHERE],
        out_specs=[row, row, half, half, ANYWHERE],
        out_shape=[sds((SEQ, LOC), BF), sds((SEQ, LOC), BF), sds((SEQ, HD), F32), sds((SEQ, HD), F32), sds((SEQ, DIM), BF)],
        input_output_aliases={8: 4},
        scratch_shapes=[pltpu.VMEM((NDEV - 1, 2 * NB, BLK), F32), pltpu.VMEM((2 * NB, BLK), F32),
                        DMA((1, NDEV - 1)), DMA((1, NDEV - 1))] + BG_SEMS,
        compiler_params=params(dimension_semantics=("arbitrary",), collective_id=cid, has_side_effects=True),
        cost_estimate=cost(2e9, 10e6),
        name="norm_rope",
    )(q, k, s, gq, gk, cos, sin, shard, full)


def causal_mask():
    keys = lax.broadcasted_iota(jnp.int32, (BLK, BLK), 0)
    queries = lax.broadcasted_iota(jnp.int32, (BLK, BLK), 1)
    return keys <= queries


def attn_kernel(q_ref, k_ref, v_ref, full_in, o_ref, lse_ref, recv_ref, full_ref, p_scr, vt_scr, acc_scr, o_scr, send_sems,
                recv_sems, own_sems, *sems):
    del full_in
    h, step = pl.program_id(0), pl.program_id(1)
    me = lax.axis_index('tp')
    qi = (me // 2 + 1 + step) % NB
    rows = pl.ds(pl.multiple_of(qi * BLK, BLK), BLK)

    @pl.when(jnp.logical_and(h == 0, step == 0))
    def _():
        entry_barrier(me)
        start(stage2(me, full_ref, sems))

    @pl.when(jnp.logical_and(h == 1, step == NB - 2))
    def _():
        wait(stage2(me, full_ref, sems))
        start(stage3(me, full_ref, sems, 4))

    @pl.when(step == 0)
    def _():
        vt_scr[...] = v_ref[...].T

    qb = q_ref[rows, :]

    def scores(j):
        return dot(k_ref[pl.ds(pl.multiple_of(j * BLK, BLK), BLK), :], qb, NT)

    def first(j, m):
        s = scores(j)
        p_scr[j] = s
        return jnp.maximum(m, jnp.max(s.reshape(BLK // 8, 8, BLK), axis=0))

    s = jnp.where(causal_mask(), scores(qi), -1e30)
    p_scr[qi] = s
    m = lax.fori_loop(0, qi, first, jnp.max(s.reshape(BLK // 8, 8, BLK), axis=0))
    m = jnp.max(m, axis=0, keepdims=True)

    def second(j, l):
        p = jnp.exp2((p_scr[j] - m) * C2)
        p_scr[j] = p
        return l + jnp.sum(p.reshape(BLK // 8, 8, BLK), axis=0)

    l = lax.fori_loop(0, qi + 1, second, jnp.zeros((8, BLK), F32))
    l = jnp.sum(l, axis=0, keepdims=True)
    rl = 1.0 / l
    lse_ref[pl.ds(h * NB + qi, 1), :] = m * C2 + jnp.log2(l)

    acc_scr[...] = jnp.zeros_like(acc_scr)

    def third(j, carry):
        p = (p_scr[j] * rl).astype(BF)
        acc_scr[...] += dot(vt_scr[:, pl.ds(pl.multiple_of(j * BLK, BLK), BLK)], p)
        return carry

    lax.fori_loop(0, qi + 1, third, 0)
    out = acc_scr[...].T.astype(BF)
    o_scr[h, step] = out
    o_ref[rows, :] = out

    def block_copy(hh, st, half, remote):
        dest = 2 * ((me // 2 + 1 + st) % NB) + half
        src = o_scr.at[hh, st, pl.ds(half * TOK, TOK), :]
        dst = recv_ref.at[:, pl.ds(pl.multiple_of(me * LOC + hh * HD, HD), HD)]
        if remote:
            return dest, pltpu.make_async_remote_copy(
                src_ref=src, dst_ref=dst, send_sem=send_sems.at[hh, st, half], recv_sem=recv_sems.at[hh, me],
                device_id=(dest,), device_id_type=MESH)
        return dest, pltpu.make_async_copy(src, dst, own_sems.at[hh])

    for half in range(2):
        dest, away = block_copy(h, step, half, True)
        _, here = block_copy(h, step, half, False)
        pl.when(dest != me)(away.start)
        pl.when(dest == me)(here.start)

    @pl.when(jnp.logical_and(h == 1, step == NB - 1))
    def _():
        wait(stage3(me, full_ref, sems, 4))
        for hh in range(2):
            for st in range(NB):
                for half in range(2):
                    dest, away = block_copy(hh, st, half, True)
                    _, here = block_copy(hh, st, half, False)
                    if st < NB - 1:
                        away.wait_send()
                    else:
                        pl.when(dest != me)(away.wait_send)
                        pl.when(dest == me)(here.wait)
            for mask in ORDER:
                peer = peer_of(me, mask)
                pltpu.make_async_remote_copy(
                    src_ref=o_scr.at[0, 0, pl.ds(0, TOK), :],
                    dst_ref=recv_ref.at[:, pl.ds(pl.multiple_of(peer * LOC + hh * HD, HD), HD)],
                    send_sem=send_sems.at[0, 0, 0], recv_sem=recv_sems.at[hh, peer],
                    device_id=(peer,), device_id_type=MESH).wait_recv()


def attention(q, k, v, gathered, cid):
    full = pl.BlockSpec((SEQ, HD), lambda h, i: (0, h))
    return pl.pallas_call(
        attn_kernel,
        grid=(2, NB),
        in_specs=[full, full, full, ANYWHERE],
        out_specs=[full, pl.BlockSpec((2 * NB, BLK), lambda h, i: (0, 0)), ANYWHERE, ANYWHERE],
        out_shape=[sds((SEQ, LOC), BF), sds((2 * NB, BLK), F32), sds((TOK, DIM), BF), sds((SEQ, DIM), BF)],
        input_output_aliases={3: 3},
        scratch_shapes=[pltpu.VMEM((NB, BLK, BLK), F32), pltpu.VMEM((HD, SEQ), BF), pltpu.VMEM((HD, BLK), F32),
                        pltpu.VMEM((2, NB, BLK, HD), BF), pltpu.SemaphoreType.DMA((2, NB, 2)),
                        DMA((2, NDEV)), DMA((2,))] + BG_SEMS,
        compiler_params=params(dimension_semantics=("arbitrary", "arbitrary"), collective_id=cid, has_side_effects=True),
        cost_estimate=cost(9e9, 6e6),
        name="attn_fwd",
    )(q, k, v, gathered)


def out_kernel(o_ref, wo_ref, x_ref, dy_ref, ga_ref, y_ref, da_ref, gga_ref, recv_ref, a_scr, dh_scr, send_sems, recv_sems, own_sem):
    me = lax.axis_index('tp')
    entry_barrier(me)
    step = DIM // NB
    o = o_ref[...]

    def fwd(j, carry):
        cols = pl.ds(pl.multiple_of(j * step, step), step)
        a_scr[:, cols] = dot(o, wo_ref[:, cols])
        return carry

    lax.fori_loop(0, NB, fwd, 0)
    a = a_scr[...]
    r = lax.rsqrt(jnp.mean(a * a, axis=-1, keepdims=True) + EPS)
    n = a * r
    ga = ga_ref[...].astype(F32)
    dy = dy_ref[0].astype(F32)
    y_ref[...] = (x_ref[0].astype(F32) + n * ga).astype(BF)
    col = jnp.sum(dy * n, axis=0, keepdims=True)
    for i in range(8):
        gga_ref[i:i + 1, :] = col[:, i * (DIM // 8):(i + 1) * (DIM // 8)]
    gn = dy * ga
    da_ref[...] = (r * (gn - n * jnp.mean(gn * n, axis=-1, keepdims=True))).astype(BF)
    da = da_ref[...]
    mine = recv_ref.at[pl.ds(pl.multiple_of(me * TOK, TOK), TOK), :]

    def block_copy(st, half):
        dest = 2 * ((me // 2 + 1 + st) % NB) + half
        src = dh_scr.at[st, :, pl.ds(half * LOC, LOC)]
        away = pltpu.make_async_remote_copy(
            src_ref=src, dst_ref=mine, send_sem=send_sems.at[st, half], recv_sem=recv_sems.at[me],
            device_id=(dest,), device_id_type=MESH)
        return dest, away, pltpu.make_async_copy(src, mine, own_sem)

    def bwd(st, carry):
        blk = (me // 2 + 1 + st) % NB
        dh_scr[st] = dot(da, wo_ref[pl.ds(pl.multiple_of(blk * step, step), step), :], NT).astype(BF)
        for half in range(2):
            dest, away, here = block_copy(st, half)
            pl.when(dest != me)(away.start)
            pl.when(dest == me)(here.start)
        return carry

    lax.fori_loop(0, NB, bwd, 0)
    for st in range(NB):
        for half in range(2):
            dest, away, here = block_copy(st, half)
            if st < NB - 1:
                away.wait_send()
            else:
                pl.when(dest != me)(away.wait_send)
                pl.when(dest == me)(here.wait)
    for mask in ORDER:
        peer = peer_of(me, mask)
        pltpu.make_async_remote_copy(
            src_ref=dh_scr.at[0, :, pl.ds(0, LOC)], dst_ref=recv_ref.at[pl.ds(pl.multiple_of(peer * TOK, TOK), TOK), :],
            send_sem=send_sems.at[0, 0], recv_sem=recv_sems.at[peer], device_id=(peer,), device_id_type=MESH).wait_recv()


def out_block(o, wo, x, dy, ga, b, cid):
    def whole(*shape):
        return pl.BlockSpec(shape, lambda i: (0,) * len(shape))

    batch = pl.BlockSpec((1, TOK, DIM), lambda i: (b, 0, 0))
    return pl.pallas_call(
        out_kernel,
        grid=(1,),
        in_specs=[whole(TOK, DIM), whole(DIM, DIM), batch, batch, whole(1, DIM)],
        out_specs=[whole(TOK, DIM), whole(TOK, DIM), whole(8, DIM // 8), ANYWHERE],
        out_shape=[sds((TOK, DIM), BF), sds((TOK, DIM), BF), sds((8, DIM // 8), F32), sds((SEQ, LOC), BF)],
        scratch_shapes=[pltpu.VMEM((TOK, DIM), F32), pltpu.VMEM((NB, TOK, DIM // NB), BF), pltpu.SemaphoreType.DMA((NB, 2)),
                        pltpu.SemaphoreType.DMA((NDEV,)), pltpu.SemaphoreType.DMA],
        compiler_params=params(dimension_semantics=("arbitrary",), collective_id=cid, has_side_effects=True),
        cost_estimate=cost(4 * TOK * DIM * DIM + 5e9, 14e6),
        name="out_block",
    )(o, wo, x, dy, ga)


def attn_bwd_kernel(older, q_ref, k_ref, v_ref, do_ref, lse_ref, qr_ref, kr_ref, iq_ref, ik_ref, gq_ref, gk_ref, cos_ref, sin_ref,
                    shard_ref, *rest):
    if older:
        _, dqu_ref, dku_ref, dv_ref, dots_ref, gg_ref, full_ref, old_ref, *rest = rest
    else:
        dqu_ref, dku_ref, dv_ref, dots_ref, gg_ref, full_ref, *rest = rest
    p_scr, dp_scr, kt_scr, dqt_scr, dq_scr, dk_scr, dv_scr, *sems = rest
    h, qi = pl.program_id(0), pl.program_id(1)
    me = lax.axis_index('tp')

    def moving():
        return (stage3(me, old_ref, sems, 4) if older else []) + stage1(me, shard_ref, full_ref, sems)

    @pl.when(jnp.logical_and(h == 0, qi == 0))
    def _():
        nbr_barrier(me)
        start(moving())

    @pl.when(jnp.logical_and(h == 1, qi == NB - 1))
    def _():
        wait(moving())

    @pl.when(qi == 0)
    def _():
        kt_scr[...] = k_ref[...].T
        dk_scr[...] = jnp.zeros_like(dk_scr)
        dv_scr[...] = jnp.zeros_like(dv_scr)

    qb = q_ref[...]
    dob = do_ref[...]
    lse = lse_ref[pl.ds(h * NB + qi, 1), :]

    def first(j, acc, diag=False):
        rows = pl.ds(pl.multiple_of(j * BLK, BLK), BLK)
        p = jnp.exp2(dot(k_ref[rows, :], qb, NT) * C2 - lse)
        if diag:
            p = jnp.where(causal_mask(), p, 0.0)
        dp = dot(v_ref[rows, :], dob, NT)
        p_scr[j] = p
        dp_scr[j] = dp
        dv_scr[rows, :] += dot(p.astype(BF), dob)
        return acc + jnp.sum((p * dp).reshape(BLK // 8, 8, BLK), axis=0)

    acc = first(qi, jnp.zeros((8, BLK), F32), True)
    acc = lax.fori_loop(0, qi, first, acc)
    delta = jnp.sum(acc, axis=0, keepdims=True)
    dqt_scr[...] = jnp.zeros_like(dqt_scr)

    def second(j, carry):
        rows = pl.ds(pl.multiple_of(j * BLK, BLK), BLK)
        ds = (p_scr[j] * (dp_scr[j] - delta) * SCALE).astype(BF)
        dk_scr[rows, :] += dot(ds, qb)
        dqt_scr[...] += dot(kt_scr[:, rows], ds)
        return carry

    lax.fori_loop(0, qi + 1, second, 0)
    dq_scr[pl.ds(pl.multiple_of(qi * BLK, BLK), BLK), :] = dqt_scr[...].T

    @pl.when(qi == NB - 1)
    def _():
        dv_ref[...] = dv_scr[...].astype(BF)

        @pl.when(h == 0)
        def _():
            dots_ref[...] = jnp.zeros_like(dots_ref)

        gg_ref[...] = jnp.zeros_like(gg_ref)

        def tail(i, carry):
            rows = pl.ds(pl.multiple_of(i * BLK, BLK), BLK)
            cos, sin = cos_ref[rows, :], sin_ref[rows, :]
            for n, (d_scr, raw_ref, inv_ref, g_ref, out_ref) in enumerate((
                    (dq_scr, qr_ref, iq_ref, gq_ref, dqu_ref), (dk_scr, kr_ref, ik_ref, gk_ref, dku_ref))):
                d = d_scr[rows, :]
                hat = d * cos - pltpu.roll(d, HD // 2, 1) * sin
                unit = raw_ref[rows, :] * inv_ref[rows, :]
                gg_ref[n:n + 1, :] += jnp.sum(hat * unit, axis=0, keepdims=True)
                du = hat * g_ref[...].astype(F32)
                out_ref[rows, :] = du
                dots_ref[pl.ds(i + n * NB, 1), :] += row_sums(du * unit)
            return carry

        lax.fori_loop(0, NB, tail, 0)


def attention_bwd(q, k, v, do, lse, qr, kr, iq, ik, gq, gk, cos, sin, shard, old, cid):
    blk = pl.BlockSpec((BLK, HD), lambda h, i: (i, h))
    full = pl.BlockSpec((SEQ, HD), lambda h, i: (0, h))
    shared = pl.BlockSpec((SEQ, HD), lambda h, i: (0, 0))
    gain = pl.BlockSpec((1, HD), lambda h, i: (0, h))
    rows = pl.BlockSpec((2 * NB, BLK), lambda h, i: (0, 0))
    return pl.pallas_call(
        functools.partial(attn_bwd_kernel, bool(old)),
        grid=(2, NB),
        in_specs=[blk, full, full, blk, rows, full, full, shared, shared, gain, gain, shared, shared, ANYWHERE] + [ANYWHERE] * len(old),
        out_specs=[full, full, full, rows, pl.BlockSpec((8, HD), lambda h, i: (0, h)), ANYWHERE] + [ANYWHERE] * len(old),
        out_shape=[sds((SEQ, LOC), F32), sds((SEQ, LOC), F32), sds((SEQ, LOC), BF), sds((2 * NB, BLK), F32),
                   sds((8, LOC), F32), sds((SEQ, DIM), BF)] + [sds((SEQ, DIM), BF)] * len(old),
        input_output_aliases={14: 6} if old else {},
        scratch_shapes=[pltpu.VMEM((NB, BLK, BLK), F32), pltpu.VMEM((NB, BLK, BLK), F32), pltpu.VMEM((HD, SEQ), BF),
                        pltpu.VMEM((HD, BLK), F32), pltpu.VMEM((SEQ, HD), F32), pltpu.VMEM((SEQ, HD), F32),
                        pltpu.VMEM((SEQ, HD), F32)] + BG_SEMS,
        compiler_params=params(dimension_semantics=("arbitrary", "arbitrary"), collective_id=cid, has_side_effects=True),
        cost_estimate=cost(16e9, 16e6),
        name="attn_bwd",
    )(q, k, v, do, lse, qr, kr, iq, ik, gq, gk, cos, sin, shard, *old)


def norm_bwd_kernel(dqu_ref, dku_ref, dv_ref, qr_ref, kr_ref, iq_ref, ik_ref, dots_ref, ga_ref, full_in, out_ref, gga_ref,
                    full_ref, slot, ga_slot, total, send_sems, recv_sems, *sems):
    del full_in
    i = pl.program_id(0)
    me = lax.axis_index('tp')

    @pl.when(i == 0)
    def _():
        entry_barrier(me)
        sums = exchange(me, [dots_ref, ga_ref], [slot, ga_slot], send_sems, recv_sems)
        start(sums)
        start(stage2(me, full_ref, sems))
        wait(sums)
        total[...] = ordered_total(me, dots_ref, slot) / DIM
        gga_ref[...] = ordered_total(me, ga_ref, ga_slot)

    for n, (du_ref, raw_ref, inv_ref) in enumerate(((dqu_ref, qr_ref, iq_ref), (dku_ref, kr_ref, ik_ref))):
        dots = as_column(total[pl.ds(i + n * NB, 1), :])
        inv = inv_ref[...]
        for h in range(LOC // HD):
            sl = slice(h * HD, (h + 1) * HD)
            unit = raw_ref[:, sl] * inv
            out_ref[:, n * LOC + h * HD:n * LOC + (h + 1) * HD] = (inv * (du_ref[:, sl] - unit * dots)).astype(BF)
    out_ref[:, 2 * LOC:] = dv_ref[...]

    @pl.when(i == NB - 1)
    def _():
        wait(stage2(me, full_ref, sems))


def norm_bwd(dqu, dku, dv, qr, kr, iq, ik, dots, gga, full, cid):
    row = pl.BlockSpec((BLK, LOC), lambda i: (i, 0))
    half = pl.BlockSpec((BLK, HD), lambda i: (i, 0))
    rows = pl.BlockSpec((2 * NB, BLK), lambda i: (0, 0))
    gsp = pl.BlockSpec((8, DIM // 8), lambda i: (0, 0))
    return pl.pallas_call(
        norm_bwd_kernel,
        grid=(NB,),
        in_specs=[row, row, row, row, row, half, half, rows, gsp, ANYWHERE],
        out_specs=[pl.BlockSpec((BLK, 3 * LOC), lambda i: (i, 0)), gsp, ANYWHERE],
        out_shape=[sds((SEQ, 3 * LOC), BF), sds((8, DIM // 8), F32), sds((SEQ, DIM), BF)],
        input_output_aliases={9: 2},
        scratch_shapes=[pltpu.VMEM((NDEV - 1, 2 * NB, BLK), F32), pltpu.VMEM((NDEV - 1, 8, DIM // 8), F32),
                        pltpu.VMEM((2 * NB, BLK), F32),
                        DMA((2, NDEV - 1)), DMA((2, NDEV - 1))] + BG_SEMS,
        compiler_params=params(dimension_semantics=("arbitrary",), collective_id=cid, has_side_effects=True),
        cost_estimate=cost(2e9, 14e6),
        name="norm_bwd",
    )(dqu, dku, dv, qr, kr, iq, ik, dots, gga, full)


HALF = DIM // 2
CH = 256


def grads_kernel(d0, d1, wq, wk, wv, x0, x1, o0, o1, da0, da1_in, dy_ref, dx_ref, gwq_ref, gwk_ref, gwv_ref, gwo_ref, da1,
                 d_all, w_all, sbuf, r1, r2, fin, acc, xbuf, obuf,
                 dl_sems, dsnd_sems, drcv_sems, w_sems, s1_sems, r1_sems, s2_sems, r2_sems, fs_sems, fr_sems, x_sems, o_sems, *sems):
    del da1_in
    me = lax.axis_index('tp')
    core, chip = me % 2, me // 2
    partner = peer_of(me, 1)
    first = peer_of(me, 2) * (1 - core) + peer_of(me, 4) * core
    second = peer_of(me, 4) * (1 - core) + peer_of(me, 2) * core
    diag_chip, first_chip, second_chip = peer_of(me, 6) // 2, first // 2, second // 2
    d_src = (d0, d1)

    barrier = pltpu.get_barrier_semaphore()
    for dev in (partner, first, second):
        pl.semaphore_signal(barrier, inc=1, device_id=(dev,), device_id_type=MESH)
    pl.semaphore_wait(barrier, 3)

    def rows_of(blk):
        return pl.ds(pl.multiple_of(blk * BLK, BLK), BLK)

    def half_rows(c):
        return pl.ds(pl.multiple_of(c * HALF, HALF), HALF)

    chips = (diag_chip, first_chip, second_chip, chip)
    w_copies = []
    for n, w in enumerate((wq, wk, wv)):
        part = pl.ds(n * LOC, LOC)
        w_copies.append(pltpu.make_async_remote_copy(
            src_ref=w.at[half_rows(1 - core), :], dst_ref=w_all.at[1, :, part], send_sem=w_sems.at[n],
            recv_sem=w_sems.at[3 + n], device_id=(partner,), device_id_type=MESH))
        w_copies.append(pltpu.make_async_copy(w.at[half_rows(core), :], w_all.at[0, :, part], w_sems.at[6 + n]))
    start(w_copies)
    swaps, loads = [], []
    for kind in range(4):
        for b in range(2):
            n = 2 * kind + b
            rows = rows_of(chips[kind])
            loads.append(pltpu.make_async_copy(d_src[b].at[rows, :], d_all.at[0, b, rows, :], dl_sems.at[n]))
            kp = {0: 0, 1: 2, 2: 1, 3: 3}[kind]
            prow = rows_of(chips[kp])
            swaps.append(pltpu.make_async_remote_copy(
                src_ref=d_src[b].at[prow, :], dst_ref=d_all.at[1, b, prow, :], send_sem=dsnd_sems.at[n],
                recv_sem=drcv_sems.at[n], device_id=(partner,), device_id_type=MESH))
    for load, swap in zip(loads, swaps):
        swap.start()
        load.start()
    last_stage = stage3(me, da1, sems)
    start(last_stage)
    wait(w_copies)

    def arrived(n, b, blk):
        rows = rows_of(blk)
        pltpu.make_async_copy(d0.at[rows, :], d_all.at[0, b, rows, :], dl_sems.at[n]).wait()
        pltpu.make_async_remote_copy(
            src_ref=d0.at[rows, :], dst_ref=d_all.at[1, b, rows, :], send_sem=dsnd_sems.at[n],
            recv_sem=drcv_sems.at[n], device_id=(partner,), device_id_type=MESH).wait()

    def partial(b, blk):
        rows = rows_of(blk)
        return dot(d_all[0, b, rows, :], w_all[0], NT) + dot(d_all[1, b, rows, :], w_all[1], NT)

    def to_first(n):
        return pltpu.make_async_remote_copy(
            src_ref=sbuf.at[n], dst_ref=r1.at[n], send_sem=s1_sems.at[n], recv_sem=r1_sems.at[n],
            device_id=(first,), device_id_type=MESH)

    def to_second(b):
        return pltpu.make_async_remote_copy(
            src_ref=r1.at[b], dst_ref=r2.at[b], send_sem=s2_sems.at[b], recv_sem=r2_sems.at[b],
            device_id=(second,), device_id_type=MESH)

    def to_partner(b):
        return pltpu.make_async_remote_copy(
            src_ref=r1.at[2 + b, pl.ds(pl.multiple_of((1 - core) * TOK, TOK), TOK), :], dst_ref=fin.at[b],
            send_sem=fs_sems.at[b], recv_sem=fr_sems.at[b], device_id=(partner,), device_id_type=MESH)

    def phase1(n, carry):
        kind, b = n // 2, n % 2
        blk = diag_chip * (1 - kind) + first_chip * kind
        arrived(n, b, blk)
        sbuf[n] = partial(b, blk)
        to_first(n).start()
        return carry

    lax.fori_loop(0, 4, phase1, 0)
    for n in range(4, 8):
        arrived(n, n % 2, chips[n // 2])

    steps = SEQ // CH

    def chunk(i):
        return pl.ds(pl.multiple_of(i * CH, CH), CH)

    def stream(pairs, body):
        def fetch(i):
            return [pltpu.make_async_copy(src.at[chunk(i), :], buf.at[i % 2], sems.at[i % 2]) for src, buf, sems in pairs]

        for c in fetch(0):
            c.start()

        def it(i, carry):
            @pl.when(i + 1 < steps)
            def _():
                for c in fetch(i + 1):
                    c.start()

            for c in fetch(i):
                c.wait()
            body(i)
            return carry

        lax.fori_loop(0, steps, it, 0)

    def wgrad(b, src):
        def body(i):
            left = d_all[0, b, chunk(i), :].T
            for c in range(3):
                part = slice(c * LOC, (c + 1) * LOC)
                acc[part, :] += dot(left[part, :], xbuf[i % 2])

        stream([(src, xbuf, x_sems)], body)

    def forward_second(b, carry):
        to_first(b).wait_recv()
        r1[b] += partial(b, second_chip)
        to_second(b).start()
        return carry

    acc[...] = jnp.zeros_like(acc)
    wgrad(0, x0)
    forward_second(0, 0)
    wgrad(1, x1)
    for n, ref in enumerate((gwq_ref, gwk_ref, gwv_ref)):
        ref[...] = acc[n * LOC:(n + 1) * LOC, :].T.astype(BF)
    forward_second(1, 0)
    acc[:LOC, :] = jnp.zeros((LOC, DIM), F32)

    def wo_body(i):
        acc[:LOC, :] += dot(obuf[i % 2].T, xbuf[i % 2])

    wait(last_stage)
    for o_src, da_src in ((o0, da0), (o1, da1)):
        stream([(da_src, xbuf, x_sems), (o_src, obuf, o_sems)], wo_body)
    gwo_ref[...] = acc[:LOC, :].astype(BF)

    def own_part(b, carry):
        r1_own = partial(b, chip)
        to_first(2 + b).wait_recv()
        to_second(b).wait_recv()
        r1[2 + b] += r1_own + r2[b]
        to_partner(b).start()
        cols = half_rows(core)
        rows = pl.ds(pl.multiple_of(core * TOK, TOK), TOK)
        dx_ref[b, :, cols] = (r1[2 + b, rows, :] + dy_ref[b, :, cols].astype(F32)).astype(BF)
        return carry

    lax.fori_loop(0, 2, own_part, 0)

    def finish(b, carry):
        to_partner(b).wait()
        cols = half_rows(1 - core)
        dx_ref[b, :, cols] = (fin[b] + dy_ref[b, :, cols].astype(F32)).astype(BF)
        to_second(b).wait_send()
        to_first(b).wait_send()
        to_first(2 + b).wait_send()
        return carry

    lax.fori_loop(0, 2, finish, 0)


def grads(d0, d1, wq, wk, wv, x0, x1, o0, o1, da0, da1, dy, cid):
    vm = pl.BlockSpec(memory_space=pltpu.VMEM)
    far = pl.BlockSpec(memory_space=pl.ANY)
    dma = pltpu.SemaphoreType.DMA
    return pl.pallas_call(
        grads_kernel,
        in_specs=[far] * 11 + [vm],
        out_specs=[vm] * 5 + [far],
        out_shape=[sds((2, TOK, DIM), BF)] + [sds((DIM, LOC), BF)] * 3 + [sds((LOC, DIM), BF), sds((SEQ, DIM), BF)],
        input_output_aliases={10: 5},
        scratch_shapes=[pltpu.VMEM((2, 2, SEQ, 3 * LOC), BF), pltpu.VMEM((2, HALF, 3 * LOC), BF),
                        pltpu.VMEM((4, BLK, HALF), F32), pltpu.VMEM((4, BLK, HALF), F32), pltpu.VMEM((2, BLK, HALF), F32),
                        pltpu.VMEM((2, TOK, HALF), F32), pltpu.VMEM((3 * LOC, DIM), F32),
                        pltpu.VMEM((2, CH, DIM), BF), pltpu.VMEM((2, CH, LOC), BF),
                        dma((8,)), dma((8,)), dma((8,)), dma((9,)), dma((4,)), dma((4,)), dma((2,)), dma((2,)),
                        dma((2,)), dma((2,)), dma((2,)), dma((2,))] + BG_SEMS,
        compiler_params=pltpu.CompilerParams(vmem_limit_bytes=67043328, collective_id=cid, has_side_effects=True),
        cost_estimate=cost(100e9, 40e6),
        name="grads",
    )(d0, d1, wq, wk, wv, x0, x1, o0, o1, da0, da1, dy)


def local_block(x_loc, wq, wk, wv, wo, gq, gk, ga, dy_loc):
    gq, gk, ga = gq[None, :], gk[None, :], ga[None, :]
    x_full, cos, sin = first_gather(x_loc, 0)
    gathered, fwd, o_recv = [x_full], [], []
    for b in range(2):
        shard, pick = (x_loc, 1) if b == 0 else (wo, None)
        q_raw, k_raw, v, s, full = project(gathered[b], wq, wk, wv, shard, pick, 1 + b)
        q_rot, k_rot, iq, ik, full = norm_rope(q_raw, k_raw, s, gq, gk, cos, sin, shard, full, pick, 3 + b)
        o, lse, recv, full = attention(q_rot, k_rot, v, full, 5 + b)
        gathered.append(full)
        o_recv.append(recv)
        fwd.append((q_raw, k_raw, v, q_rot, k_rot, iq, ik, o, lse))
    ys, das, dhs, ggas = [], [], [], []
    for b in range(2):
        y, da, gga, dh = out_block(o_recv[b], gathered[2], x_loc, dy_loc, ga, b, 7 + b)
        ys.append(y)
        das.append(da)
        dhs.append(dh)
        ggas.append(gga)
    ds, gga_sum, ggs, da_full = [], [], [], []
    for b in range(2):
        q_raw, k_raw, v, q_rot, k_rot, iq, ik, o, lse = fwd[b]
        dqu, dku, dv, dots, gg, full, *old = attention_bwd(
            q_rot, k_rot, v, dhs[b], lse, q_raw, k_raw, iq, ik, gq, gk, cos, sin, das[b], da_full, 9 + b)
        d, gsum, full = norm_bwd(dqu, dku, dv, q_raw, k_raw, iq, ik, dots, ggas[b], full, 11 + b)
        da_full = list(old) + [full]
        ds.append(d)
        gga_sum.append(gsum)
        ggs.append(gg)
    dx, gwq, gwk, gwv, gwo, _ = grads(ds[0], ds[1], wq, wk, wv, gathered[0], gathered[1], fwd[0][7], fwd[1][7],
                                      da_full[0], da_full[1], dy_loc, 13)
    gg = ggs[0] + ggs[1]
    grad_ga = (gga_sum[0] + gga_sum[1]).reshape(DIM).astype(BF)
    return (jnp.stack(ys), dx, gwq, gwk, gwv, gwo, gg[0].astype(BF), gg[1].astype(BF), grad_ga)


def solution(mesh):
    act, col, row, vec = P(None, 'tp', None), P(None, 'tp'), P('tp', None), P('tp')
    in_specs = (act, col, col, col, row, vec, vec, P(), act)
    out_specs = (act, act, col, col, col, row, vec, vec, P())
    return jax.shard_map(local_block, mesh=mesh, in_specs=in_specs, out_specs=out_specs, check_vma=False)
```

```python
import functools
import math

import jax
import jax.numpy as jnp
from jax import lax
from jax.experimental import pallas as pl
from jax.experimental.pallas import tpu as pltpu
from jax.sharding import PartitionSpec as P

HD = 128
ROPE_THETA = 500000.0
EPS = 1e-6
DIM = 2048
SEQ = 2048
LOC = 256
TOK = 256
BLK = 512
NB = SEQ // BLK
NDEV = 8
SCALE = HD ** -0.5
C2 = SCALE * math.log2(math.e)
MESH = pl.DeviceIdType.MESH
BF = jnp.bfloat16
F32 = jnp.float32
VMEM_MAX = 60 * 1024 * 1024

NT = (((1,), (1,)), ((), ()))
NN = (((1,), (0,)), ((), ()))


def dot(a, b, dims=NN):
    return lax.dot_general(a, b, dims, preferred_element_type=F32)


def sds(shape, dtype):
    return jax.ShapeDtypeStruct(shape, dtype)


def cost(flops, nbytes, trans=0):
    return pl.CostEstimate(flops=int(flops), bytes_accessed=int(nbytes), transcendentals=int(trans))


def params(**kw):
    return pltpu.CompilerParams(vmem_limit_bytes=VMEM_MAX, **kw)


def peer_of(me, mask):
    core, ax, ay = me % 2, (me // 2) % 2, me // 4
    core = 1 - core if mask & 1 else core
    ax = 1 - ax if mask & 2 else ax
    ay = 1 - ay if mask & 4 else ay
    return ay * 4 + ax * 2 + core


ORDER = (6, 7, 2, 4, 3, 5, 1)


def entry_barrier(me):
    barrier = pltpu.get_barrier_semaphore()
    for mask in ORDER:
        pl.semaphore_signal(barrier, inc=1, device_id=(peer_of(me, mask),), device_id_type=MESH)
    pl.semaphore_wait(barrier, NDEV - 1)


def nbr_barrier(me):
    barrier = pltpu.get_barrier_semaphore()
    for mask in (1, 2, 4):
        pl.semaphore_signal(barrier, inc=1, device_id=(peer_of(me, mask),), device_id_type=MESH)
    pl.semaphore_wait(barrier, 3)


DMA = pltpu.SemaphoreType.DMA
ANYWHERE = pl.BlockSpec(memory_space=pl.ANY)
BG_SEMS = [DMA((8,)), DMA((8,)), DMA((4,))]
BG = BG_SEMS + [pltpu.VMEM((2, TOK, DIM), BF)]


def shard_rows(dev, lo=0, count=TOK):
    return pl.ds(pl.multiple_of(dev * TOK + lo, HD), count)


class Stage:
    def __init__(self, loads, copies):
        self.loads, self.copies = loads, copies

    def load(self):
        start(self.loads)

    def send(self):
        wait(self.loads)
        start(self.copies)

    def wait(self):
        wait(self.copies)


def stage1(me, src, full, bg, lo=0, count=TOK):
    send, recv, own, buf = bg
    there = full.at[shard_rows(me, lo, count), :]
    part = buf.at[0, pl.ds(0, count), :]
    copies = [pltpu.make_async_remote_copy(
        src_ref=part, dst_ref=there, send_sem=send.at[k], recv_sem=recv.at[k],
        device_id=(peer_of(me, mask),), device_id_type=MESH) for k, mask in enumerate((2, 4, 1))]
    return Stage([pltpu.make_async_copy(src.at[pl.ds(lo, count), :], part, own.at[0])],
                 copies + [pltpu.make_async_copy(part, there, own.at[2])])


def stage2(me, full, bg):
    send, recv, own, buf = bg
    xn, yn = peer_of(me, 2), peer_of(me, 4)
    half = TOK // 2
    plan = ((1, half, half, yn, 2), (0, 0, half, xn, 4), (0, 0, TOK, xn, 1), (1, 0, TOK, yn, 1))
    return Stage(
        [pltpu.make_async_copy(full.at[shard_rows(dev), :], buf.at[n], own.at[n]) for n, dev in enumerate((xn, yn))],
        [pltpu.make_async_remote_copy(
            src_ref=buf.at[slot, pl.ds(lo, count), :], dst_ref=full.at[shard_rows(dev, lo, count), :],
            send_sem=send.at[3 + k], recv_sem=recv.at[3 + k], device_id=(peer_of(me, mask),), device_id_type=MESH)
         for k, (slot, lo, count, dev, mask) in enumerate(plan)])


def stage3(me, full, bg):
    send, recv, own, buf = bg
    rows = full.at[shard_rows(peer_of(me, 6)), :]
    return Stage([pltpu.make_async_copy(rows, buf.at[1], own.at[1])], [pltpu.make_async_remote_copy(
        src_ref=buf.at[1], dst_ref=rows, send_sem=send.at[7], recv_sem=recv.at[7],
        device_id=(peer_of(me, 1),), device_id_type=MESH)])


def start(copies):
    for c in copies:
        c.start()


def wait(copies):
    for c in copies:
        c.wait()


def gather_kernel(x_ref, freq_ref, full_ref, cos_ref, sin_ref, *bg):
    me = lax.axis_index('tp')
    first = stage1(me, x_ref.at[0], full_ref, bg)
    first.load()
    nbr_barrier(me)
    first.send()
    freq = freq_ref[...]
    sign = jnp.where(lax.broadcasted_iota(jnp.int32, (TOK, HD), 1) < HD // 2, -1.0, 1.0)

    def table(i, carry):
        rows = pl.ds(pl.multiple_of(i * TOK, TOK), TOK)
        pos = (lax.broadcasted_iota(jnp.int32, (TOK, HD), 0) + i * TOK).astype(F32)
        angle = pos * freq
        cos_ref[rows, :] = jnp.cos(angle)
        sin_ref[rows, :] = jnp.sin(angle) * sign
        return carry

    lax.fori_loop(0, SEQ // TOK, table, 0)
    first.wait()
    for stage in (stage2(me, full_ref, bg), stage3(me, full_ref, bg)):
        stage.load()
        stage.send()
        stage.wait()


def first_gather(x, cid):
    half = HD // 2
    inv_freq = 1.0 / (ROPE_THETA ** (jnp.arange(half, dtype=F32) / half))
    freq = jnp.concatenate([inv_freq, inv_freq])[None, :]
    vm = pl.BlockSpec(memory_space=pltpu.VMEM)
    return pl.pallas_call(
        gather_kernel,
        in_specs=[ANYWHERE, vm],
        out_specs=[ANYWHERE, vm, vm],
        out_shape=[sds((SEQ, DIM), BF), sds((SEQ, HD), F32), sds((SEQ, HD), F32)],
        scratch_shapes=BG,
        compiler_params=params(collective_id=cid, has_side_effects=True),
        cost_estimate=cost(20e9, 20e6),
        name="gather",
    )(x, freq)


def row_sums(vals):
    folded = vals[:, :HD]
    for start in range(HD, vals.shape[1], HD):
        folded = folded + vals[:, start:start + HD]
    return jnp.sum(folded.T, axis=0, keepdims=True)


def as_column(row):
    return jnp.broadcast_to(row, (HD, row.shape[1])).T


def proj_kernel(pick, x_ref, wq_ref, wk_ref, wv_ref, shard_ref, q_ref, k_ref, v_ref, s_ref, full_ref, *bg):
    i = pl.program_id(0)
    me = lax.axis_index('tp')
    src = shard_ref if pick is None else shard_ref.at[pick]

    @pl.when(i == 0)
    def _():
        stage = stage1(me, src, full_ref, bg, 0, TOK // 2)
        stage.load()
        nbr_barrier(me)
        stage.send()

    x = x_ref[...]
    q = dot(x, wq_ref[...])
    q_ref[...] = q
    s_ref[pl.ds(i, 1), :] = row_sums(q * q)
    k = dot(x, wk_ref[...])
    k_ref[...] = k
    s_ref[pl.ds(i + NB, 1), :] = row_sums(k * k)
    v_ref[...] = dot(x, wv_ref[...]).astype(BF)

    @pl.when(i == NB - 1)
    def _():
        stage1(me, src, full_ref, bg, 0, TOK // 2).wait()


def project(x, wq, wk, wv, shard, pick, cid):
    row = pl.BlockSpec((BLK, LOC), lambda i: (i, 0))
    wspec = pl.BlockSpec((DIM, LOC), lambda i: (0, 0))
    return pl.pallas_call(
        functools.partial(proj_kernel, pick),
        grid=(NB,),
        in_specs=[pl.BlockSpec((BLK, DIM), lambda i: (i, 0)), wspec, wspec, wspec, ANYWHERE],
        out_specs=[row, row, row, pl.BlockSpec((2 * NB, BLK), lambda i: (0, 0)), ANYWHERE],
        out_shape=[sds((SEQ, LOC), F32), sds((SEQ, LOC), F32), sds((SEQ, LOC), BF), sds((2 * NB, BLK), F32),
                   sds((SEQ, DIM), BF)],
        scratch_shapes=BG,
        compiler_params=params(dimension_semantics=("arbitrary",), collective_id=cid, has_side_effects=True),
        cost_estimate=cost(2 * SEQ * DIM * 3 * LOC, 16e6),
        name="proj",
    )(x, wq, wk, wv, shard)


def exchange(me, srcs, slots, send_sems, recv_sems):
    copies = []
    for n, (src, slot) in enumerate(zip(srcs, slots)):
        for p, mask in enumerate(ORDER):
            copies.append(pltpu.make_async_remote_copy(
                src_ref=src, dst_ref=slot.at[p], send_sem=send_sems.at[n, p], recv_sem=recv_sems.at[n, p],
                device_id=(peer_of(me, mask),), device_id_type=MESH))
    return copies


def ordered_total(me, src, slot):
    own = src[...]
    total = jnp.zeros_like(own)
    for dev in range(NDEV):
        term = jnp.where(me == dev, own, 0.0)
        for p, mask in enumerate(ORDER):
            term = term + jnp.where(peer_of(me, mask) == dev, slot[p], 0.0)
        total = total + term
    return total


def norm_kernel(pick, q_ref, k_ref, s_ref, gains_ref, cos_ref, sin_ref, shard_ref, full_in, qo_ref, ko_ref, iq_ref,
                ik_ref, full_ref, slot, total, send_sems, recv_sems, *bg):
    del full_in
    i = pl.program_id(0)
    me = lax.axis_index('tp')
    src = shard_ref if pick is None else shard_ref.at[pick]

    @pl.when(i == 0)
    def _():
        stage = stage1(me, src, full_ref, bg, TOK // 2, TOK // 2)
        stage.load()
        entry_barrier(me)
        sums = exchange(me, [s_ref], [slot], send_sems, recv_sems)
        start(sums)
        stage.send()
        wait(sums)
        total[...] = lax.rsqrt(ordered_total(me, s_ref, slot) / DIM + EPS)

    cos, sin = cos_ref[...], sin_ref[...]
    for n, (raw, dst, inv_ref) in enumerate(((q_ref, qo_ref, iq_ref), (k_ref, ko_ref, ik_ref))):
        row = i + n * NB
        inv = as_column(total[pl.ds(row, 1), :])
        inv_ref[...] = inv
        g = gains_ref[n:n + 1, :]
        for h in range(LOC // HD):
            sl = slice(h * HD, (h + 1) * HD)
            hat = raw[:, sl] * inv * g[:, sl]
            dst[:, sl] = (hat * cos + pltpu.roll(hat, HD // 2, 1) * sin).astype(BF)

    @pl.when(i == NB - 1)
    def _():
        stage1(me, src, full_ref, bg, TOK // 2, TOK // 2).wait()


def norm_rope(q, k, s, gains, cos, sin, shard, full, pick, cid):
    row = pl.BlockSpec((BLK, LOC), lambda i: (i, 0))
    half = pl.BlockSpec((BLK, HD), lambda i: (i, 0))
    gain = pl.BlockSpec((2 + DIM // LOC, LOC), lambda i: (0, 0))
    return pl.pallas_call(
        functools.partial(norm_kernel, pick),
        grid=(NB,),
        in_specs=[row, row, pl.BlockSpec((2 * NB, BLK), lambda i: (0, 0)), gain, half, half, ANYWHERE, ANYWHERE],
        out_specs=[row, row, half, half, ANYWHERE],
        out_shape=[sds((SEQ, LOC), BF), sds((SEQ, LOC), BF), sds((SEQ, HD), F32), sds((SEQ, HD), F32), sds((SEQ, DIM), BF)],
        input_output_aliases={7: 4},
        scratch_shapes=[pltpu.VMEM((NDEV - 1, 2 * NB, BLK), F32), pltpu.VMEM((2 * NB, BLK), F32),
                        DMA((1, NDEV - 1)), DMA((1, NDEV - 1))] + BG,
        compiler_params=params(dimension_semantics=("arbitrary",), collective_id=cid, has_side_effects=True),
        cost_estimate=cost(2e9, 10e6),
        name="norm_rope",
    )(q, k, s, gains, cos, sin, shard, full)


def causal_mask():
    keys = lax.broadcasted_iota(jnp.int32, (BLK, BLK), 0)
    queries = lax.broadcasted_iota(jnp.int32, (BLK, BLK), 1)
    return keys <= queries


def attn_kernel(b, q_ref, k_ref, v_ref, full_in, *rest):
    del full_in
    if b:
        _, *rest = rest
    o_ref, lse_ref, both_ref, full_ref, p_scr, vt_scr, acc_scr, o_scr, send_sems, recv_sems, own_sems, *bg = rest
    recv_ref = both_ref.at[b]
    h, step = pl.program_id(0), pl.program_id(1)
    me = lax.axis_index('tp')
    qi = (me // 2 + 1 + step) % NB
    rows = pl.ds(pl.multiple_of(qi * BLK, BLK), BLK)

    @pl.when(jnp.logical_and(h == 0, step == 0))
    def _():
        stage = stage2(me, full_ref, bg)
        stage.load()
        entry_barrier(me)
        stage.send()

    @pl.when(jnp.logical_and(h == 1, step == NB - 2))
    def _():
        stage2(me, full_ref, bg).wait()
        stage = stage3(me, full_ref, bg)
        stage.load()
        stage.send()

    @pl.when(step == 0)
    def _():
        vt_scr[...] = v_ref[...].T

    qb = q_ref[rows, :]

    def scores(j):
        return dot(k_ref[pl.ds(pl.multiple_of(j * BLK, BLK), BLK), :], qb, NT)

    def first(j, m):
        s = scores(j)
        p_scr[j] = s
        return jnp.maximum(m, jnp.max(s.reshape(BLK // 8, 8, BLK), axis=0))

    s = jnp.where(causal_mask(), scores(qi), -1e30)
    p_scr[qi] = s
    m = lax.fori_loop(0, qi, first, jnp.max(s.reshape(BLK // 8, 8, BLK), axis=0))
    m = jnp.max(m, axis=0, keepdims=True)

    def second(j, l):
        p = jnp.exp2((p_scr[j] - m) * C2)
        p_scr[j] = p
        return l + jnp.sum(p.reshape(BLK // 8, 8, BLK), axis=0)

    l = lax.fori_loop(0, qi + 1, second, jnp.zeros((8, BLK), F32))
    l = jnp.sum(l, axis=0, keepdims=True)
    rl = 1.0 / l
    lse_ref[pl.ds(h * NB + qi, 1), :] = m * C2 + jnp.log2(l)

    acc_scr[...] = jnp.zeros_like(acc_scr)

    def third(j, carry):
        p = (p_scr[j] * rl).astype(BF)
        acc_scr[...] += dot(vt_scr[:, pl.ds(pl.multiple_of(j * BLK, BLK), BLK)], p)
        return carry

    lax.fori_loop(0, qi + 1, third, 0)
    out = acc_scr[...].T.astype(BF)
    o_scr[h, step] = out
    o_ref[rows, :] = out

    def block_copy(hh, st, half, remote):
        dest = 2 * ((me // 2 + 1 + st) % NB) + half
        src = o_scr.at[hh, st, pl.ds(half * TOK, TOK), :]
        dst = recv_ref.at[:, pl.ds(pl.multiple_of(me * LOC + hh * HD, HD), HD)]
        if remote:
            return dest, pltpu.make_async_remote_copy(
                src_ref=src, dst_ref=dst, send_sem=send_sems.at[hh, st, half], recv_sem=recv_sems.at[hh, me],
                device_id=(dest,), device_id_type=MESH)
        return dest, pltpu.make_async_copy(src, dst, own_sems.at[hh])

    for half in range(2):
        dest, away = block_copy(h, step, half, True)
        _, here = block_copy(h, step, half, False)
        pl.when(dest != me)(away.start)
        pl.when(dest == me)(here.start)

    @pl.when(jnp.logical_and(h == 1, step == NB - 1))
    def _():
        stage3(me, full_ref, bg).wait()
        for hh in range(2):
            for st in range(NB):
                for half in range(2):
                    dest, away = block_copy(hh, st, half, True)
                    _, here = block_copy(hh, st, half, False)
                    if st < NB - 1:
                        away.wait_send()
                    else:
                        pl.when(dest != me)(away.wait_send)
                        pl.when(dest == me)(here.wait)
            for mask in ORDER:
                peer = peer_of(me, mask)
                pltpu.make_async_remote_copy(
                    src_ref=o_scr.at[0, 0, pl.ds(0, TOK), :],
                    dst_ref=recv_ref.at[:, pl.ds(pl.multiple_of(peer * LOC + hh * HD, HD), HD)],
                    send_sem=send_sems.at[0, 0, 0], recv_sem=recv_sems.at[hh, peer],
                    device_id=(peer,), device_id_type=MESH).wait_recv()


def attention(b, q, k, v, gathered, both, cid):
    full = pl.BlockSpec((SEQ, HD), lambda h, i: (0, h))
    return pl.pallas_call(
        functools.partial(attn_kernel, b),
        grid=(2, NB),
        in_specs=[full, full, full, ANYWHERE] + [ANYWHERE] * len(both),
        out_specs=[full, pl.BlockSpec((2 * NB, BLK), lambda h, i: (0, 0)), ANYWHERE, ANYWHERE],
        out_shape=[sds((SEQ, LOC), BF), sds((2 * NB, BLK), F32), sds((2, TOK, DIM), BF), sds((SEQ, DIM), BF)],
        input_output_aliases={3: 3, 4: 2} if both else {3: 3},
        scratch_shapes=[pltpu.VMEM((NB, BLK, BLK), F32), pltpu.VMEM((HD, SEQ), BF), pltpu.VMEM((HD, BLK), F32),
                        pltpu.VMEM((2, NB, BLK, HD), BF), pltpu.SemaphoreType.DMA((2, NB, 2)),
                        DMA((2, NDEV)), DMA((2,))] + BG,
        compiler_params=params(dimension_semantics=("arbitrary", "arbitrary"), collective_id=cid, has_side_effects=True),
        cost_estimate=cost(9e9, 6e6),
        name="attn_fwd",
    )(q, k, v, gathered, *both)


def out_kernel(o_ref, wo_ref, x_ref, dy_ref, gains_ref, y_ref, da_ref, gga_ref, both_ref, a_scr, dh_scr, send_sems, recv_sems,
               own_sems):
    b = pl.program_id(0)
    me = lax.axis_index('tp')

    @pl.when(b == 0)
    def _():
        entry_barrier(me)
        gga_ref[...] = jnp.zeros_like(gga_ref)

    step = DIM // NB
    o = o_ref[0]

    def fwd(j, carry):
        cols = pl.ds(pl.multiple_of(j * step, step), step)
        a_scr[:, cols] = dot(o, wo_ref[:, cols])
        return carry

    lax.fori_loop(0, NB, fwd, 0)
    a = a_scr[...]
    r = lax.rsqrt(jnp.mean(a * a, axis=-1, keepdims=True) + EPS)
    n = a * r
    ga = jnp.concatenate([gains_ref[2 + i:3 + i, :] for i in range(8)], axis=1)
    dy = dy_ref[0].astype(F32)
    y_ref[0] = (x_ref[0].astype(F32) + n * ga).astype(BF)
    col = jnp.sum(dy * n, axis=0, keepdims=True)
    for i in range(8):
        gga_ref[i:i + 1, :] += col[:, i * LOC:(i + 1) * LOC]
    gn = dy * ga
    da_ref[0] = (r * (gn - n * jnp.mean(gn * n, axis=-1, keepdims=True))).astype(BF)
    da = da_ref[0]

    def block_copy(bb, st, half):
        dest = 2 * ((me // 2 + 1 + st) % NB) + half
        src = dh_scr.at[bb, st, :, pl.ds(half * LOC, LOC)]
        mine = both_ref.at[bb, shard_rows(me), :]
        away = pltpu.make_async_remote_copy(
            src_ref=src, dst_ref=mine, send_sem=send_sems.at[bb, st, half], recv_sem=recv_sems.at[bb, me],
            device_id=(dest,), device_id_type=MESH)
        return dest, away, pltpu.make_async_copy(src, mine, own_sems.at[bb])

    def bwd(st, carry):
        blk = (me // 2 + 1 + st) % NB
        dh_scr[b, st] = dot(da, wo_ref[pl.ds(pl.multiple_of(blk * step, step), step), :], NT).astype(BF)
        for half in range(2):
            dest, away, here = block_copy(b, st, half)
            pl.when(dest != me)(away.start)
            pl.when(dest == me)(here.start)
        return carry

    lax.fori_loop(0, NB, bwd, 0)

    @pl.when(b == 1)
    def _():
        for bb in range(2):
            for st in range(NB):
                for half in range(2):
                    dest, away, here = block_copy(bb, st, half)
                    if st < NB - 1:
                        away.wait_send()
                    else:
                        pl.when(dest != me)(away.wait_send)
                        pl.when(dest == me)(here.wait)
            for mask in ORDER:
                peer = peer_of(me, mask)
                pltpu.make_async_remote_copy(
                    src_ref=dh_scr.at[0, 0, :, pl.ds(0, LOC)], dst_ref=both_ref.at[bb, shard_rows(peer), :],
                    send_sem=send_sems.at[0, 0, 0], recv_sem=recv_sems.at[bb, peer], device_id=(peer,),
                    device_id_type=MESH).wait_recv()


def out_block(o, wo, x, dy, gains, cid):
    def whole(*shape):
        return pl.BlockSpec(shape, lambda i: (0,) * len(shape))

    batch = pl.BlockSpec((1, TOK, DIM), lambda i: (i, 0, 0))
    return pl.pallas_call(
        out_kernel,
        grid=(2,),
        in_specs=[batch, whole(DIM, DIM), batch, batch, whole(2 + DIM // LOC, LOC)],
        out_specs=[batch, batch, whole(8, DIM // 8), ANYWHERE],
        out_shape=[sds((2, TOK, DIM), BF), sds((2, TOK, DIM), BF), sds((8, DIM // 8), F32), sds((2, SEQ, LOC), BF)],
        scratch_shapes=[pltpu.VMEM((TOK, DIM), F32), pltpu.VMEM((2, NB, TOK, DIM // NB), BF), DMA((2, NB, 2)),
                        DMA((2, NDEV)), DMA((2,))],
        compiler_params=params(dimension_semantics=("arbitrary",), collective_id=cid, has_side_effects=True),
        cost_estimate=cost(8 * TOK * DIM * DIM + 5e9, 18e6),
        name="out_block",
    )(o, wo, x, dy, gains)


def attn_bwd_kernel(b, older, q_ref, k_ref, v_ref, do_ref, lse_ref, qr_ref, kr_ref, iq_ref, ik_ref, gains_ref, cos_ref, sin_ref,
                    shard_ref, *rest):
    if older:
        _, dqu_ref, dku_ref, dv_ref, dots_ref, gg_ref, full_ref, old_ref, *rest = rest
    else:
        dqu_ref, dku_ref, dv_ref, dots_ref, gg_ref, full_ref, *rest = rest
    p_scr, dp_scr, kt_scr, dqt_scr, dq_scr, dk_scr, dv_scr, *bg = rest
    h, qi = pl.program_id(0), pl.program_id(1)
    me = lax.axis_index('tp')

    def moving():
        return ([stage3(me, old_ref, bg)] if older else []) + [stage1(me, shard_ref.at[b], full_ref, bg)]

    @pl.when(jnp.logical_and(h == 0, qi == 0))
    def _():
        stages = moving()
        for stage in stages:
            stage.load()
        nbr_barrier(me)
        for stage in stages:
            stage.send()

    @pl.when(jnp.logical_and(h == 1, qi == NB - 1))
    def _():
        for stage in moving():
            stage.wait()

    @pl.when(qi == 0)
    def _():
        kt_scr[...] = k_ref[...].T
        dk_scr[...] = jnp.zeros_like(dk_scr)
        dv_scr[...] = jnp.zeros_like(dv_scr)

    qb = q_ref[...]
    dob = do_ref[...]
    lse = lse_ref[pl.ds(h * NB + qi, 1), :]

    def first(j, acc, diag=False):
        rows = pl.ds(pl.multiple_of(j * BLK, BLK), BLK)
        p = jnp.exp2(dot(k_ref[rows, :], qb, NT) * C2 - lse)
        if diag:
            p = jnp.where(causal_mask(), p, 0.0)
        dp = dot(v_ref[rows, :], dob, NT)
        p_scr[j] = p
        dp_scr[j] = dp
        dv_scr[rows, :] += dot(p.astype(BF), dob)
        return acc + jnp.sum((p * dp).reshape(BLK // 8, 8, BLK), axis=0)

    acc = first(qi, jnp.zeros((8, BLK), F32), True)
    acc = lax.fori_loop(0, qi, first, acc)
    delta = jnp.sum(acc, axis=0, keepdims=True)
    dqt_scr[...] = jnp.zeros_like(dqt_scr)

    def second(j, carry):
        rows = pl.ds(pl.multiple_of(j * BLK, BLK), BLK)
        ds = (p_scr[j] * (dp_scr[j] - delta) * SCALE).astype(BF)
        dk_scr[rows, :] += dot(ds, qb)
        dqt_scr[...] += dot(kt_scr[:, rows], ds)
        return carry

    lax.fori_loop(0, qi + 1, second, 0)
    dq_scr[pl.ds(pl.multiple_of(qi * BLK, BLK), BLK), :] = dqt_scr[...].T

    @pl.when(qi == NB - 1)
    def _():
        dv_ref[...] = dv_scr[...].astype(BF)

        @pl.when(h == 0)
        def _():
            dots_ref[...] = jnp.zeros_like(dots_ref)

        gg_ref[...] = jnp.zeros_like(gg_ref)

        def tail(i, carry):
            rows = pl.ds(pl.multiple_of(i * BLK, BLK), BLK)
            cos, sin = cos_ref[rows, :], sin_ref[rows, :]
            for n, (d_scr, raw_ref, inv_ref, out_ref) in enumerate((
                    (dq_scr, qr_ref, iq_ref, dqu_ref), (dk_scr, kr_ref, ik_ref, dku_ref))):
                d = d_scr[rows, :]
                hat = d * cos - pltpu.roll(d, HD // 2, 1) * sin
                unit = raw_ref[rows, :] * inv_ref[rows, :]
                gg_ref[n:n + 1, :] += jnp.sum(hat * unit, axis=0, keepdims=True)
                du = hat * gains_ref[n:n + 1, :]
                out_ref[rows, :] = du
                dots_ref[pl.ds(i + n * NB, 1), :] += row_sums(du * unit)
            return carry

        lax.fori_loop(0, NB, tail, 0)


def attention_bwd(b, q, k, v, do, lse, qr, kr, iq, ik, gains, cos, sin, shard, old, cid):
    blk = pl.BlockSpec((BLK, HD), lambda h, i: (i, h))
    full = pl.BlockSpec((SEQ, HD), lambda h, i: (0, h))
    shared = pl.BlockSpec((SEQ, HD), lambda h, i: (0, 0))
    gain = pl.BlockSpec((2 + DIM // LOC, HD), lambda h, i: (0, h))
    do_blk = pl.BlockSpec((None, BLK, HD), lambda h, i: (b, i, h))
    rows = pl.BlockSpec((2 * NB, BLK), lambda h, i: (0, 0))
    return pl.pallas_call(
        functools.partial(attn_bwd_kernel, b, bool(old)),
        grid=(2, NB),
        in_specs=[blk, full, full, do_blk, rows, full, full, shared, shared, gain, shared, shared, ANYWHERE] + [ANYWHERE] * len(old),
        out_specs=[full, full, full, rows, pl.BlockSpec((8, HD), lambda h, i: (0, h)), ANYWHERE] + [ANYWHERE] * len(old),
        out_shape=[sds((SEQ, LOC), F32), sds((SEQ, LOC), F32), sds((SEQ, LOC), BF), sds((2 * NB, BLK), F32),
                   sds((8, LOC), F32), sds((SEQ, DIM), BF)] + [sds((SEQ, DIM), BF)] * len(old),
        input_output_aliases={13: 6} if old else {},
        scratch_shapes=[pltpu.VMEM((NB, BLK, BLK), F32), pltpu.VMEM((NB, BLK, BLK), F32), pltpu.VMEM((HD, SEQ), BF),
                        pltpu.VMEM((HD, BLK), F32), pltpu.VMEM((SEQ, HD), F32), pltpu.VMEM((SEQ, HD), F32),
                        pltpu.VMEM((SEQ, HD), F32)] + BG,
        compiler_params=params(dimension_semantics=("arbitrary", "arbitrary"), collective_id=cid, has_side_effects=True),
        cost_estimate=cost(16e9, 16e6),
        name="attn_bwd",
    )(q, k, v, do, lse, qr, kr, iq, ik, gains, cos, sin, shard, *old)


def norm_bwd_kernel(dqu_ref, dku_ref, dv_ref, qr_ref, kr_ref, iq_ref, ik_ref, dots_ref, ga_ref, full_in, out_ref, gga_ref,
                    full_ref, slot, ga_slot, total, send_sems, recv_sems, *bg):
    del full_in
    i = pl.program_id(0)
    me = lax.axis_index('tp')

    @pl.when(i == 0)
    def _():
        stage = stage2(me, full_ref, bg)
        stage.load()
        entry_barrier(me)
        sums = exchange(me, [dots_ref, ga_ref], [slot, ga_slot], send_sems, recv_sems)
        start(sums)
        stage.send()
        wait(sums)
        total[...] = ordered_total(me, dots_ref, slot) / DIM
        gga_ref[...] = ordered_total(me, ga_ref, ga_slot)

    for n, (du_ref, raw_ref, inv_ref) in enumerate(((dqu_ref, qr_ref, iq_ref), (dku_ref, kr_ref, ik_ref))):
        dots = as_column(total[pl.ds(i + n * NB, 1), :])
        inv = inv_ref[...]
        for h in range(LOC // HD):
            sl = slice(h * HD, (h + 1) * HD)
            unit = raw_ref[:, sl] * inv
            out_ref[:, n * LOC + h * HD:n * LOC + (h + 1) * HD] = (inv * (du_ref[:, sl] - unit * dots)).astype(BF)
    out_ref[:, 2 * LOC:] = dv_ref[...]

    @pl.when(i == NB - 1)
    def _():
        stage2(me, full_ref, bg).wait()


def norm_bwd(dqu, dku, dv, qr, kr, iq, ik, dots, gga, full, cid):
    row = pl.BlockSpec((BLK, LOC), lambda i: (i, 0))
    half = pl.BlockSpec((BLK, HD), lambda i: (i, 0))
    rows = pl.BlockSpec((2 * NB, BLK), lambda i: (0, 0))
    gsp = pl.BlockSpec((8, DIM // 8), lambda i: (0, 0))
    return pl.pallas_call(
        norm_bwd_kernel,
        grid=(NB,),
        in_specs=[row, row, row, row, row, half, half, rows, gsp, ANYWHERE],
        out_specs=[pl.BlockSpec((BLK, 3 * LOC), lambda i: (i, 0)), gsp, ANYWHERE],
        out_shape=[sds((SEQ, 3 * LOC), BF), sds((8, DIM // 8), F32), sds((SEQ, DIM), BF)],
        input_output_aliases={9: 2},
        scratch_shapes=[pltpu.VMEM((NDEV - 1, 2 * NB, BLK), F32), pltpu.VMEM((NDEV - 1, 8, DIM // 8), F32),
                        pltpu.VMEM((2 * NB, BLK), F32),
                        DMA((2, NDEV - 1)), DMA((2, NDEV - 1))] + BG,
        compiler_params=params(dimension_semantics=("arbitrary",), collective_id=cid, has_side_effects=True),
        cost_estimate=cost(2e9, 14e6),
        name="norm_bwd",
    )(dqu, dku, dv, qr, kr, iq, ik, dots, gga, full)


HALF = DIM // 2
CH = 256


def grads_kernel(d0, d1, wq, wk, wv, x0, x1, o0, o1, da0, da1_in, dy_ref, dx_ref, gwq_ref, gwk_ref, gwv_ref, gwo_ref, da1,
                 d_all, w_all, sbuf, r1, r2, fin, acc, xbuf, obuf,
                 dl_sems, dsnd_sems, drcv_sems, w_sems, s1_sems, r1_sems, s2_sems, r2_sems, fs_sems, fr_sems, x_sems, o_sems, *sems):
    del da1_in
    me = lax.axis_index('tp')
    core, chip = me % 2, me // 2
    partner = peer_of(me, 1)
    first = peer_of(me, 2) * (1 - core) + peer_of(me, 4) * core
    second = peer_of(me, 4) * (1 - core) + peer_of(me, 2) * core
    diag_chip, first_chip, second_chip = peer_of(me, 6) // 2, first // 2, second // 2
    d_src = (d0, d1)

    barrier = pltpu.get_barrier_semaphore()
    for dev in (partner, first, second):
        pl.semaphore_signal(barrier, inc=1, device_id=(dev,), device_id_type=MESH)
    pl.semaphore_wait(barrier, 3)

    def rows_of(blk):
        return pl.ds(pl.multiple_of(blk * BLK, BLK), BLK)

    def half_rows(c):
        return pl.ds(pl.multiple_of(c * HALF, HALF), HALF)

    chips = (diag_chip, first_chip, second_chip, chip)
    w_copies = []
    for n, w in enumerate((wq, wk, wv)):
        part = pl.ds(n * LOC, LOC)
        w_copies.append(pltpu.make_async_remote_copy(
            src_ref=w.at[half_rows(1 - core), :], dst_ref=w_all.at[1, :, part], send_sem=w_sems.at[n],
            recv_sem=w_sems.at[3 + n], device_id=(partner,), device_id_type=MESH))
        w_copies.append(pltpu.make_async_copy(w.at[half_rows(core), :], w_all.at[0, :, part], w_sems.at[6 + n]))
    start(w_copies)
    swaps, loads = [], []
    for kind in range(4):
        for b in range(2):
            n = 2 * kind + b
            rows = rows_of(chips[kind])
            loads.append(pltpu.make_async_copy(d_src[b].at[rows, :], d_all.at[0, b, rows, :], dl_sems.at[n]))
            kp = {0: 0, 1: 2, 2: 1, 3: 3}[kind]
            prow = rows_of(chips[kp])
            swaps.append(pltpu.make_async_remote_copy(
                src_ref=d_src[b].at[prow, :], dst_ref=d_all.at[1, b, prow, :], send_sem=dsnd_sems.at[n],
                recv_sem=drcv_sems.at[n], device_id=(partner,), device_id_type=MESH))
    for load, swap in zip(loads, swaps):
        swap.start()
        load.start()
    last_stage = stage3(me, da1, (*sems, xbuf))
    last_stage.load()
    last_stage.send()
    wait(w_copies)

    def arrived(n, b, blk):
        rows = rows_of(blk)
        pltpu.make_async_copy(d0.at[rows, :], d_all.at[0, b, rows, :], dl_sems.at[n]).wait()
        pltpu.make_async_remote_copy(
            src_ref=d0.at[rows, :], dst_ref=d_all.at[1, b, rows, :], send_sem=dsnd_sems.at[n],
            recv_sem=drcv_sems.at[n], device_id=(partner,), device_id_type=MESH).wait()

    def partial(b, blk):
        rows = rows_of(blk)
        return dot(d_all[0, b, rows, :], w_all[0], NT) + dot(d_all[1, b, rows, :], w_all[1], NT)

    def to_first(n):
        return pltpu.make_async_remote_copy(
            src_ref=sbuf.at[n], dst_ref=r1.at[n], send_sem=s1_sems.at[n], recv_sem=r1_sems.at[n],
            device_id=(first,), device_id_type=MESH)

    def to_second(b):
        return pltpu.make_async_remote_copy(
            src_ref=r1.at[b], dst_ref=r2.at[b], send_sem=s2_sems.at[b], recv_sem=r2_sems.at[b],
            device_id=(second,), device_id_type=MESH)

    def to_partner(b):
        return pltpu.make_async_remote_copy(
            src_ref=r1.at[2 + b, pl.ds(pl.multiple_of((1 - core) * TOK, TOK), TOK), :], dst_ref=fin.at[b],
            send_sem=fs_sems.at[b], recv_sem=fr_sems.at[b], device_id=(partner,), device_id_type=MESH)

    def phase1(n, carry):
        kind, b = n // 2, n % 2
        blk = diag_chip * (1 - kind) + first_chip * kind
        arrived(n, b, blk)
        sbuf[n] = partial(b, blk)
        to_first(n).start()
        return carry

    lax.fori_loop(0, 4, phase1, 0)
    for n in range(4, 8):
        arrived(n, n % 2, chips[n // 2])

    steps = SEQ // CH

    def chunk(i):
        return pl.ds(pl.multiple_of(i * CH, CH), CH)

    def stream(pairs, body):
        def fetch(i):
            return [pltpu.make_async_copy(src.at[chunk(i), :], buf.at[i % 2], sems.at[i % 2]) for src, buf, sems in pairs]

        for c in fetch(0):
            c.start()

        def it(i, carry):
            @pl.when(i + 1 < steps)
            def _():
                for c in fetch(i + 1):
                    c.start()

            for c in fetch(i):
                c.wait()
            body(i)
            return carry

        lax.fori_loop(0, steps, it, 0)

    def wgrad(b, src):
        def body(i):
            left = d_all[0, b, chunk(i), :].T
            for c in range(3):
                part = slice(c * LOC, (c + 1) * LOC)
                acc[part, :] += dot(left[part, :], xbuf[i % 2])

        stream([(src, xbuf, x_sems)], body)

    def forward_second(b, carry):
        to_first(b).wait_recv()
        r1[b] += partial(b, second_chip)
        to_second(b).start()
        return carry

    acc[...] = jnp.zeros_like(acc)
    last_stage.wait()
    wgrad(0, x0)
    forward_second(0, 0)
    wgrad(1, x1)
    for n, ref in enumerate((gwq_ref, gwk_ref, gwv_ref)):
        ref[...] = acc[n * LOC:(n + 1) * LOC, :].T.astype(BF)
    forward_second(1, 0)
    acc[:LOC, :] = jnp.zeros((LOC, DIM), F32)

    def wo_body(i):
        acc[:LOC, :] += dot(obuf[i % 2].T, xbuf[i % 2])

    for o_src, da_src in ((o0, da0), (o1, da1)):
        stream([(da_src, xbuf, x_sems), (o_src, obuf, o_sems)], wo_body)
    gwo_ref[...] = acc[:LOC, :].astype(BF)

    def own_part(b, carry):
        r1_own = partial(b, chip)
        to_first(2 + b).wait_recv()
        to_second(b).wait_recv()
        r1[2 + b] += r1_own + r2[b]
        to_partner(b).start()
        cols = half_rows(core)
        rows = pl.ds(pl.multiple_of(core * TOK, TOK), TOK)
        dx_ref[b, :, cols] = (r1[2 + b, rows, :] + dy_ref[b, :, cols].astype(F32)).astype(BF)
        return carry

    lax.fori_loop(0, 2, own_part, 0)

    def finish(b, carry):
        to_partner(b).wait()
        cols = half_rows(1 - core)
        dx_ref[b, :, cols] = (fin[b] + dy_ref[b, :, cols].astype(F32)).astype(BF)
        to_second(b).wait_send()
        to_first(b).wait_send()
        to_first(2 + b).wait_send()
        return carry

    lax.fori_loop(0, 2, finish, 0)


def grads(d0, d1, wq, wk, wv, x0, x1, o0, o1, da0, da1, dy, cid):
    vm = pl.BlockSpec(memory_space=pltpu.VMEM)
    far = pl.BlockSpec(memory_space=pl.ANY)
    dma = pltpu.SemaphoreType.DMA
    return pl.pallas_call(
        grads_kernel,
        in_specs=[far] * 11 + [vm],
        out_specs=[vm] * 5 + [far],
        out_shape=[sds((2, TOK, DIM), BF)] + [sds((DIM, LOC), BF)] * 3 + [sds((LOC, DIM), BF), sds((SEQ, DIM), BF)],
        input_output_aliases={10: 5},
        scratch_shapes=[pltpu.VMEM((2, 2, SEQ, 3 * LOC), BF), pltpu.VMEM((2, HALF, 3 * LOC), BF),
                        pltpu.VMEM((4, BLK, HALF), F32), pltpu.VMEM((4, BLK, HALF), F32), pltpu.VMEM((2, BLK, HALF), F32),
                        pltpu.VMEM((2, TOK, HALF), F32), pltpu.VMEM((3 * LOC, DIM), F32),
                        pltpu.VMEM((2, CH, DIM), BF), pltpu.VMEM((2, CH, LOC), BF),
                        dma((8,)), dma((8,)), dma((8,)), dma((9,)), dma((4,)), dma((4,)), dma((2,)), dma((2,)),
                        dma((2,)), dma((2,)), dma((2,)), dma((2,))] + BG_SEMS,
        compiler_params=pltpu.CompilerParams(vmem_limit_bytes=67043328, collective_id=cid, has_side_effects=True),
        cost_estimate=cost(100e9, 40e6),
        name="grads",
    )(d0, d1, wq, wk, wv, x0, x1, o0, o1, da0, da1, dy)


def local_block(x_loc, wq, wk, wv, wo, gq, gk, ga, dy_loc):
    gains = jnp.concatenate([gq, gk, ga]).astype(F32).reshape(2 + DIM // LOC, LOC)
    x_full, cos, sin = first_gather(x_loc, 0)
    gathered, fwd, o_recv = [x_full], [], []
    for b in range(2):
        shard, pick = (x_loc, 1) if b == 0 else (wo, None)
        q_raw, k_raw, v, s, full = project(gathered[b], wq, wk, wv, shard, pick, 1 + b)
        q_rot, k_rot, iq, ik, full = norm_rope(q_raw, k_raw, s, gains, cos, sin, shard, full, pick, 3 + b)
        o, lse, recv, full = attention(b, q_rot, k_rot, v, full, o_recv, 5 + b)
        gathered.append(full)
        o_recv = [recv]
        fwd.append((q_raw, k_raw, v, q_rot, k_rot, iq, ik, o, lse))
    y, da, gga, dh = out_block(o_recv[0], gathered[2], x_loc, dy_loc, gains, 7)
    ds, gga_sum, ggs, da_full = [], [], [], []
    for b in range(2):
        q_raw, k_raw, v, q_rot, k_rot, iq, ik, o, lse = fwd[b]
        dqu, dku, dv, dots, gg, full, *old = attention_bwd(
            b, q_rot, k_rot, v, dh, lse, q_raw, k_raw, iq, ik, gains, cos, sin, da, da_full, 9 + b)
        d, gsum, full = norm_bwd(dqu, dku, dv, q_raw, k_raw, iq, ik, dots, gga, full, 11 + b)
        da_full = list(old) + [full]
        ds.append(d)
        gga_sum.append(gsum)
        ggs.append(gg)
    dx, gwq, gwk, gwv, gwo, _ = grads(ds[0], ds[1], wq, wk, wv, gathered[0], gathered[1], fwd[0][7], fwd[1][7],
                                      da_full[0], da_full[1], dy_loc, 13)
    gg = ggs[0] + ggs[1]
    grad_ga = gga_sum[0].reshape(DIM).astype(BF)
    return (y, dx, gwq, gwk, gwv, gwo, gg[0].astype(BF), gg[1].astype(BF), grad_ga)


def solution(mesh):
    act, col, row, vec = P(None, 'tp', None), P(None, 'tp'), P('tp', None), P('tp')
    in_specs = (act, col, col, col, row, vec, vec, P(), act)
    out_specs = (act, act, col, col, col, row, vec, vec, P())
    return jax.shard_map(local_block, mesh=mesh, in_specs=in_specs, out_specs=out_specs, check_vma=False)
```

```python
import functools
import math

import jax
import jax.numpy as jnp
from jax import lax
from jax.experimental import pallas as pl
from jax.experimental.pallas import tpu as pltpu
from jax.sharding import PartitionSpec as P

HD = 128
ROPE_THETA = 500000.0
EPS = 1e-6
DIM = 2048
SEQ = 2048
LOC = 256
TOK = 256
BLK = 512
NB = SEQ // BLK
NDEV = 8
SCALE = HD ** -0.5
C2 = SCALE * math.log2(math.e)
MESH = pl.DeviceIdType.MESH
BF = jnp.bfloat16
F32 = jnp.float32
VMEM_MAX = 60 * 1024 * 1024

NT = (((1,), (1,)), ((), ()))
NN = (((1,), (0,)), ((), ()))


def dot(a, b, dims=NN):
    return lax.dot_general(a, b, dims, preferred_element_type=F32)


def sds(shape, dtype):
    return jax.ShapeDtypeStruct(shape, dtype)


def cost(flops, nbytes, trans=0):
    return pl.CostEstimate(flops=int(flops), bytes_accessed=int(nbytes), transcendentals=int(trans))


def params(**kw):
    return pltpu.CompilerParams(vmem_limit_bytes=VMEM_MAX, **kw)


def peer_of(me, mask):
    core, ax, ay = me % 2, (me // 2) % 2, me // 4
    core = 1 - core if mask & 1 else core
    ax = 1 - ax if mask & 2 else ax
    ay = 1 - ay if mask & 4 else ay
    return ay * 4 + ax * 2 + core


ORDER = (6, 7, 2, 4, 3, 5, 1)


def entry_barrier(me):
    barrier = pltpu.get_barrier_semaphore()
    for mask in ORDER:
        pl.semaphore_signal(barrier, inc=1, device_id=(peer_of(me, mask),), device_id_type=MESH)
    pl.semaphore_wait(barrier, NDEV - 1)


def nbr_barrier(me):
    barrier = pltpu.get_barrier_semaphore()
    for mask in (1, 2, 4):
        pl.semaphore_signal(barrier, inc=1, device_id=(peer_of(me, mask),), device_id_type=MESH)
    pl.semaphore_wait(barrier, 3)


DMA = pltpu.SemaphoreType.DMA
ANYWHERE = pl.BlockSpec(memory_space=pl.ANY)
BG_SEMS = [DMA((8,)), DMA((8,)), DMA((4,))]
BG = BG_SEMS + [pltpu.VMEM((2, TOK, DIM), BF)]


def shard_rows(dev, lo=0, count=TOK):
    return pl.ds(pl.multiple_of(dev * TOK + lo, HD), count)


class Stage:
    def __init__(self, loads, copies):
        self.loads, self.copies = loads, copies

    def load(self):
        start(self.loads)

    def send(self):
        wait(self.loads)
        start(self.copies)

    def wait(self):
        wait(self.copies)


def stage1(me, src, full, bg, lo=0, count=TOK):
    send, recv, own, buf = bg
    there = full.at[shard_rows(me, lo, count), :]
    part = buf.at[0, pl.ds(0, count), :]
    copies = [pltpu.make_async_remote_copy(
        src_ref=part, dst_ref=there, send_sem=send.at[k], recv_sem=recv.at[k],
        device_id=(peer_of(me, mask),), device_id_type=MESH) for k, mask in enumerate((2, 4, 1))]
    return Stage([pltpu.make_async_copy(src.at[pl.ds(lo, count), :], part, own.at[0])],
                 copies + [pltpu.make_async_copy(part, there, own.at[2])])


def stage2(me, full, bg):
    send, recv, own, buf = bg
    xn, yn = peer_of(me, 2), peer_of(me, 4)
    half = TOK // 2
    plan = ((1, half, half, yn, 2), (0, 0, half, xn, 4), (0, 0, TOK, xn, 1), (1, 0, TOK, yn, 1))
    return Stage(
        [pltpu.make_async_copy(full.at[shard_rows(dev), :], buf.at[n], own.at[n]) for n, dev in enumerate((xn, yn))],
        [pltpu.make_async_remote_copy(
            src_ref=buf.at[slot, pl.ds(lo, count), :], dst_ref=full.at[shard_rows(dev, lo, count), :],
            send_sem=send.at[3 + k], recv_sem=recv.at[3 + k], device_id=(peer_of(me, mask),), device_id_type=MESH)
         for k, (slot, lo, count, dev, mask) in enumerate(plan)])


def stage3(me, full, bg):
    send, recv, own, buf = bg
    rows = full.at[shard_rows(peer_of(me, 6)), :]
    return Stage([pltpu.make_async_copy(rows, buf.at[1], own.at[1])], [pltpu.make_async_remote_copy(
        src_ref=buf.at[1], dst_ref=rows, send_sem=send.at[7], recv_sem=recv.at[7],
        device_id=(peer_of(me, 1),), device_id_type=MESH)])


def start(copies):
    for c in copies:
        c.start()


def wait(copies):
    for c in copies:
        c.wait()


def gather_kernel(x_ref, freq_ref, full_ref, cos_ref, sin_ref, *bg):
    me = lax.axis_index('tp')
    first = stage1(me, x_ref.at[0], full_ref, bg)
    first.load()
    nbr_barrier(me)
    first.send()
    freq = freq_ref[...]
    sign = jnp.where(lax.broadcasted_iota(jnp.int32, (TOK, HD), 1) < HD // 2, -1.0, 1.0)

    def table(i, carry):
        rows = pl.ds(pl.multiple_of(i * TOK, TOK), TOK)
        pos = (lax.broadcasted_iota(jnp.int32, (TOK, HD), 0) + i * TOK).astype(F32)
        angle = pos * freq
        cos_ref[rows, :] = jnp.cos(angle)
        sin_ref[rows, :] = jnp.sin(angle) * sign
        return carry

    lax.fori_loop(0, SEQ // TOK, table, 0)
    first.wait()
    for stage in (stage2(me, full_ref, bg), stage3(me, full_ref, bg)):
        stage.load()
        stage.send()
        stage.wait()


def first_gather(x, cid):
    half = HD // 2
    inv_freq = 1.0 / (ROPE_THETA ** (jnp.arange(half, dtype=F32) / half))
    freq = jnp.concatenate([inv_freq, inv_freq])[None, :]
    vm = pl.BlockSpec(memory_space=pltpu.VMEM)
    return pl.pallas_call(
        gather_kernel,
        in_specs=[ANYWHERE, vm],
        out_specs=[ANYWHERE, vm, vm],
        out_shape=[sds((SEQ, DIM), BF), sds((SEQ, HD), F32), sds((SEQ, HD), F32)],
        scratch_shapes=BG,
        compiler_params=params(collective_id=cid, has_side_effects=True),
        cost_estimate=cost(20e9, 20e6),
        name="gather",
    )(x, freq)


def row_sums(vals):
    folded = vals[:, :HD]
    for start in range(HD, vals.shape[1], HD):
        folded = folded + vals[:, start:start + HD]
    return jnp.sum(folded.T, axis=0, keepdims=True)


def as_column(row):
    return jnp.broadcast_to(row, (HD, row.shape[1])).T


def exchange(me, srcs, slots, send_sems, recv_sems):
    copies = []
    for n, (src, slot) in enumerate(zip(srcs, slots)):
        for p, mask in enumerate(ORDER):
            copies.append(pltpu.make_async_remote_copy(
                src_ref=src, dst_ref=slot.at[p], send_sem=send_sems.at[n, p], recv_sem=recv_sems.at[n, p],
                device_id=(peer_of(me, mask),), device_id_type=MESH))
    return copies


def ordered_total(me, src, slot):
    own = src[...]
    total = jnp.zeros_like(own)
    for dev in range(NDEV):
        term = jnp.where(me == dev, own, 0.0)
        for p, mask in enumerate(ORDER):
            term = term + jnp.where(peer_of(me, mask) == dev, slot[p], 0.0)
        total = total + term
    return total


def causal_mask():
    keys = lax.broadcasted_iota(jnp.int32, (BLK, BLK), 0)
    queries = lax.broadcasted_iota(jnp.int32, (BLK, BLK), 1)
    return keys <= queries


def block_rows(i):
    return pl.ds(pl.multiple_of(i * BLK, BLK), BLK)


def head_cols(h):
    return pl.ds(pl.multiple_of(h * HD, HD), HD)


def forward_kernel(b, pick, x_ref, wq_ref, wk_ref, wv_ref, gains_ref, cos_ref, sin_ref, shard_ref, *rest):
    if b:
        _, *rest = rest
    (raw_ref, qkv_ref, inv_ref, o_ref, lse_ref, both_ref, full_ref,
     raw, qkv, sums_scr, slot, p_scr, vt_scr, acc_scr, o_scr,
     ex_send, ex_recv, out_sems, send_sems, recv_sems, own_sems, *bg) = rest
    recv_ref = both_ref.at[b]
    t = pl.program_id(0)
    me = lax.axis_index('tp')
    src = shard_ref if pick is None else shard_ref.at[pick]

    def keep(n):
        return (pltpu.make_async_copy(raw, raw_ref, out_sems.at[0]), pltpu.make_async_copy(qkv, qkv_ref, out_sems.at[1]))[n]

    def sums():
        return exchange(me, [sums_scr], [slot], ex_send, ex_recv)

    def block_copy(hh, st, half):
        dest = 2 * ((me // 2 + 1 + st) % NB) + half
        part = o_scr.at[hh, st, pl.ds(half * TOK, TOK), :]
        dst = recv_ref.at[:, pl.ds(pl.multiple_of(me * LOC + hh * HD, HD), HD)]
        away = pltpu.make_async_remote_copy(
            src_ref=part, dst_ref=dst, send_sem=send_sems.at[hh, st, half], recv_sem=recv_sems.at[hh, me],
            device_id=(dest,), device_id_type=MESH)
        return dest, away, pltpu.make_async_copy(part, dst, own_sems.at[hh])

    @pl.when(t == 0)
    def _():
        stage = stage1(me, src, full_ref, bg)
        stage.load()
        entry_barrier(me)
        stage.send()

    @pl.when(t < NB)
    def _():
        rows = block_rows(t)
        x = x_ref[...]
        for n, w_ref in enumerate((wq_ref, wk_ref)):
            val = dot(x, w_ref[...])
            raw[n, rows, :] = val
            sums_scr[pl.ds(t + n * NB, 1), :] = row_sums(val * val)
        qkv[2, rows, :] = dot(x, wv_ref[...]).astype(BF)

    @pl.when(t == NB)
    def _():
        start(sums())
        keep(0).start()
        wait(sums())
        inv_ref[...] = lax.rsqrt(ordered_total(me, sums_scr, slot) / DIM + EPS)

    @pl.when(jnp.logical_and(t >= NB, t < 2 * NB))
    def _():
        i = t - NB
        rows = block_rows(i)
        cos, sin = cos_ref[rows, :], sin_ref[rows, :]
        for n in range(2):
            inv = as_column(inv_ref[pl.ds(i + n * NB, 1), :])
            g = gains_ref[n:n + 1, :]
            for h in range(LOC // HD):
                sl = slice(h * HD, (h + 1) * HD)
                hat = raw[n, rows, sl] * inv * g[:, sl]
                qkv[n, rows, sl] = (hat * cos + pltpu.roll(hat, HD // 2, 1) * sin).astype(BF)

    @pl.when(t == 2 * NB)
    def _():
        keep(1).start()
        stage1(me, src, full_ref, bg).wait()
        stage = stage2(me, full_ref, bg)
        stage.load()
        stage.send()

    @pl.when(t == 4 * NB - 2)
    def _():
        stage2(me, full_ref, bg).wait()
        stage = stage3(me, full_ref, bg)
        stage.load()
        stage.send()

    @pl.when(t >= 2 * NB)
    def _():
        h, step = t // NB - 2, t % NB
        qi = (me // 2 + 1 + step) % NB
        cols = head_cols(h)

        @pl.when(step == 0)
        def _():
            vt_scr[...] = qkv[2, :, cols].T

        qb = qkv[0, block_rows(qi), cols]

        def scores(j):
            return dot(qkv[1, block_rows(j), cols], qb, NT)

        def first(j, m):
            s = scores(j)
            p_scr[j] = s
            return jnp.maximum(m, jnp.max(s.reshape(BLK // 8, 8, BLK), axis=0))

        s = jnp.where(causal_mask(), scores(qi), -1e30)
        p_scr[qi] = s
        m = lax.fori_loop(0, qi, first, jnp.max(s.reshape(BLK // 8, 8, BLK), axis=0))
        m = jnp.max(m, axis=0, keepdims=True)

        def second(j, l):
            p = jnp.exp2((p_scr[j] - m) * C2)
            p_scr[j] = p
            return l + jnp.sum(p.reshape(BLK // 8, 8, BLK), axis=0)

        l = lax.fori_loop(0, qi + 1, second, jnp.zeros((8, BLK), F32))
        l = jnp.sum(l, axis=0, keepdims=True)
        rl = 1.0 / l
        lse_ref[pl.ds(h * NB + qi, 1), :] = m * C2 + jnp.log2(l)

        acc_scr[...] = jnp.zeros_like(acc_scr)

        def third(j, carry):
            p = (p_scr[j] * rl).astype(BF)
            acc_scr[...] += dot(vt_scr[:, block_rows(j)], p)
            return carry

        lax.fori_loop(0, qi + 1, third, 0)
        out = acc_scr[...].T.astype(BF)
        o_scr[h, step] = out
        o_ref[block_rows(qi), cols] = out

        for half in range(2):
            dest, away, here = block_copy(h, step, half)
            pl.when(dest != me)(away.start)
            pl.when(dest == me)(here.start)

    @pl.when(t == 4 * NB - 1)
    def _():
        keep(0).wait()
        keep(1).wait()
        stage3(me, full_ref, bg).wait()
        for hh in range(2):
            for st in range(NB):
                for half in range(2):
                    dest, away, here = block_copy(hh, st, half)
                    if st < NB - 1:
                        away.wait_send()
                    else:
                        pl.when(dest != me)(away.wait_send)
                        pl.when(dest == me)(here.wait)
            for mask in ORDER:
                peer = peer_of(me, mask)
                pltpu.make_async_remote_copy(
                    src_ref=o_scr.at[0, 0, pl.ds(0, TOK), :],
                    dst_ref=recv_ref.at[:, pl.ds(pl.multiple_of(peer * LOC + hh * HD, HD), HD)],
                    send_sem=send_sems.at[0, 0, 0], recv_sem=recv_sems.at[hh, peer],
                    device_id=(peer,), device_id_type=MESH).wait_recv()


def forward(b, x, wq, wk, wv, gains, cos, sin, shard, pick, both, cid):
    def whole(*shape):
        return pl.BlockSpec(shape, lambda t: (0,) * len(shape))

    wspec = whole(DIM, LOC)
    return pl.pallas_call(
        functools.partial(forward_kernel, b, pick),
        grid=(4 * NB,),
        in_specs=[pl.BlockSpec((BLK, DIM), lambda t: (jnp.minimum(t, NB - 1), 0)), wspec, wspec, wspec,
                  whole(2 + DIM // LOC, LOC), whole(SEQ, HD), whole(SEQ, HD), ANYWHERE] + [ANYWHERE] * len(both),
        out_specs=[ANYWHERE, ANYWHERE, whole(2 * NB, BLK), whole(SEQ, LOC), whole(2 * NB, BLK), ANYWHERE, ANYWHERE],
        out_shape=[sds((2, SEQ, LOC), F32), sds((3, SEQ, LOC), BF), sds((2 * NB, BLK), F32), sds((SEQ, LOC), BF),
                   sds((2 * NB, BLK), F32), sds((2, TOK, DIM), BF), sds((SEQ, DIM), BF)],
        input_output_aliases={8: 5} if both else {},
        scratch_shapes=[pltpu.VMEM((2, SEQ, LOC), F32), pltpu.VMEM((3, SEQ, LOC), BF), pltpu.VMEM((2 * NB, BLK), F32),
                        pltpu.VMEM((NDEV - 1, 2 * NB, BLK), F32),
                        pltpu.VMEM((NB, BLK, BLK), F32), pltpu.VMEM((HD, SEQ), BF), pltpu.VMEM((HD, BLK), F32),
                        pltpu.VMEM((2, NB, BLK, HD), BF), DMA((1, NDEV - 1)), DMA((1, NDEV - 1)), DMA((2,)),
                        DMA((2, NB, 2)), DMA((2, NDEV)), DMA((2,))] + BG,
        compiler_params=params(dimension_semantics=("arbitrary",), collective_id=cid, has_side_effects=True),
        cost_estimate=cost(30e9, 30e6),
        name="forward",
    )(x, wq, wk, wv, gains, cos, sin, shard, *both)


def out_kernel(o_ref, wo_ref, x_ref, dy_ref, gains_ref, y_ref, da_ref, gga_ref, both_ref, a_scr, dh_scr, send_sems, recv_sems,
               own_sems):
    b = pl.program_id(0)
    me = lax.axis_index('tp')

    @pl.when(b == 0)
    def _():
        entry_barrier(me)
        gga_ref[...] = jnp.zeros_like(gga_ref)

    step = DIM // NB
    o = o_ref[0]

    def fwd(j, carry):
        cols = pl.ds(pl.multiple_of(j * step, step), step)
        a_scr[:, cols] = dot(o, wo_ref[:, cols])
        return carry

    lax.fori_loop(0, NB, fwd, 0)
    a = a_scr[...]
    r = lax.rsqrt(jnp.mean(a * a, axis=-1, keepdims=True) + EPS)
    n = a * r
    ga = jnp.concatenate([gains_ref[2 + i:3 + i, :] for i in range(8)], axis=1)
    dy = dy_ref[0].astype(F32)
    y_ref[0] = (x_ref[0].astype(F32) + n * ga).astype(BF)
    col = jnp.sum(dy * n, axis=0, keepdims=True)
    for i in range(8):
        gga_ref[i:i + 1, :] += col[:, i * LOC:(i + 1) * LOC]
    gn = dy * ga
    da_ref[0] = (r * (gn - n * jnp.mean(gn * n, axis=-1, keepdims=True))).astype(BF)
    da = da_ref[0]

    def block_copy(bb, st, half):
        dest = 2 * ((me // 2 + 1 + st) % NB) + half
        src = dh_scr.at[bb, st, :, pl.ds(half * LOC, LOC)]
        mine = both_ref.at[bb, shard_rows(me), :]
        away = pltpu.make_async_remote_copy(
            src_ref=src, dst_ref=mine, send_sem=send_sems.at[bb, st, half], recv_sem=recv_sems.at[bb, me],
            device_id=(dest,), device_id_type=MESH)
        return dest, away, pltpu.make_async_copy(src, mine, own_sems.at[bb])

    def bwd(st, carry):
        blk = (me // 2 + 1 + st) % NB
        dh_scr[b, st] = dot(da, wo_ref[pl.ds(pl.multiple_of(blk * step, step), step), :], NT).astype(BF)
        for half in range(2):
            dest, away, here = block_copy(b, st, half)
            pl.when(dest != me)(away.start)
            pl.when(dest == me)(here.start)
        return carry

    lax.fori_loop(0, NB, bwd, 0)

    @pl.when(b == 1)
    def _():
        for bb in range(2):
            for st in range(NB):
                for half in range(2):
                    dest, away, here = block_copy(bb, st, half)
                    if st < NB - 1:
                        away.wait_send()
                    else:
                        pl.when(dest != me)(away.wait_send)
                        pl.when(dest == me)(here.wait)
            for mask in ORDER:
                peer = peer_of(me, mask)
                pltpu.make_async_remote_copy(
                    src_ref=dh_scr.at[0, 0, :, pl.ds(0, LOC)], dst_ref=both_ref.at[bb, shard_rows(peer), :],
                    send_sem=send_sems.at[0, 0, 0], recv_sem=recv_sems.at[bb, peer], device_id=(peer,),
                    device_id_type=MESH).wait_recv()


def out_block(o, wo, x, dy, gains, cid):
    def whole(*shape):
        return pl.BlockSpec(shape, lambda i: (0,) * len(shape))

    batch = pl.BlockSpec((1, TOK, DIM), lambda i: (i, 0, 0))
    return pl.pallas_call(
        out_kernel,
        grid=(2,),
        in_specs=[batch, whole(DIM, DIM), batch, batch, whole(2 + DIM // LOC, LOC)],
        out_specs=[batch, batch, whole(8, DIM // 8), ANYWHERE],
        out_shape=[sds((2, TOK, DIM), BF), sds((2, TOK, DIM), BF), sds((8, DIM // 8), F32), sds((2, SEQ, LOC), BF)],
        scratch_shapes=[pltpu.VMEM((TOK, DIM), F32), pltpu.VMEM((2, NB, TOK, DIM // NB), BF), DMA((2, NB, 2)),
                        DMA((2, NDEV)), DMA((2,))],
        compiler_params=params(dimension_semantics=("arbitrary",), collective_id=cid, has_side_effects=True),
        cost_estimate=cost(8 * TOK * DIM * DIM + 5e9, 18e6),
        name="out_block",
    )(o, wo, x, dy, gains)


def backward_kernel(b, qkv_ref, do_ref, lse_ref, raw_ref, inv_ref, gains_ref, cos_ref, sin_ref, gga_ref, shard_ref, *rest):
    if b:
        _, d_ref, pd_ref, gg_ref, gout_ref, full_ref, old_ref, *rest = rest
    else:
        d_ref, pd_ref, gg_ref, gout_ref, full_ref, *rest = rest
    (p_scr, dp_scr, kt_scr, dqt_scr, dq_scr, dk_scr, dv_scr, du_scr, d_scr, dots_scr, total, slot, ga_slot,
     ex_send, ex_recv, pd_send, pd_recv, d_sems, *bg) = rest
    h, qi = pl.program_id(0), pl.program_id(1)
    me = lax.axis_index('tp')
    gather = stage1(me, shard_ref.at[b], full_ref, bg)

    @pl.when(jnp.logical_and(h == 0, qi == 0))
    def _():
        stages = ([stage3(me, old_ref, bg)] if b else []) + [gather]
        for stage in stages:
            stage.load()
        entry_barrier(me)
        for stage in stages:
            stage.send()
        dots_scr[...] = jnp.zeros_like(dots_scr)

    @pl.when(qi == 0)
    def _():
        kt_scr[...] = qkv_ref[1].T
        dk_scr[...] = jnp.zeros_like(dk_scr)
        dv_scr[...] = jnp.zeros_like(dv_scr)

    qb = qkv_ref[0, block_rows(qi), :]
    dob = do_ref[...]
    lse = lse_ref[pl.ds(h * NB + qi, 1), :]

    def first(j, acc, diag=False):
        rows = block_rows(j)
        p = jnp.exp2(dot(qkv_ref[1, rows, :], qb, NT) * C2 - lse)
        if diag:
            p = jnp.where(causal_mask(), p, 0.0)
        dp = dot(qkv_ref[2, rows, :], dob, NT)
        p_scr[j] = p
        dp_scr[j] = dp
        dv_scr[rows, :] += dot(p.astype(BF), dob)
        return acc + jnp.sum((p * dp).reshape(BLK // 8, 8, BLK), axis=0)

    acc = first(qi, jnp.zeros((8, BLK), F32), True)
    acc = lax.fori_loop(0, qi, first, acc)
    delta = jnp.sum(acc, axis=0, keepdims=True)
    dqt_scr[...] = jnp.zeros_like(dqt_scr)

    def second(j, carry):
        rows = block_rows(j)
        ds = (p_scr[j] * (dp_scr[j] - delta) * SCALE).astype(BF)
        dk_scr[rows, :] += dot(ds, qb)
        dqt_scr[...] += dot(kt_scr[:, rows], ds)
        return carry

    lax.fori_loop(0, qi + 1, second, 0)
    dq_scr[block_rows(qi), :] = dqt_scr[...].T

    @pl.when(qi == NB - 1)
    def _():
        d_scr[:, pl.ds(pl.multiple_of(2 * LOC + h * HD, HD), HD)] = dv_scr[...].astype(BF)
        gg_ref[...] = jnp.zeros_like(gg_ref)
        cols = head_cols(h)

        def tail(i, carry):
            rows = block_rows(i)
            cos, sin = cos_ref[rows, :], sin_ref[rows, :]
            for n, from_scr in enumerate((dq_scr, dk_scr)):
                d = from_scr[rows, :]
                hat = d * cos - pltpu.roll(d, HD // 2, 1) * sin
                unit = raw_ref[n, rows, cols] * as_column(inv_ref[pl.ds(i + n * NB, 1), :])
                gg_ref[n:n + 1, :] += jnp.sum(hat * unit, axis=0, keepdims=True)
                du = hat * gains_ref[n:n + 1, :]
                du_scr[n, h, rows, :] = du
                dots_scr[pl.ds(i + n * NB, 1), :] += row_sums(du * unit)
            return carry

        lax.fori_loop(0, NB, tail, 0)

    @pl.when(jnp.logical_and(h == 1, qi == NB - 1))
    def _():
        gather.wait()
        if b:
            stage3(me, old_ref, bg).wait()
        sums = exchange(me, [dots_scr, gga_ref], [slot, ga_slot], ex_send, ex_recv)
        start(sums)
        more = stage2(me, full_ref, bg)
        more.load()
        more.send()
        wait(sums)
        total[...] = ordered_total(me, dots_scr, slot) / DIM
        gout_ref[...] = ordered_total(me, gga_ref, ga_slot)

        def copies(i):
            rows = block_rows(i)
            return [pltpu.make_async_copy(d_scr.at[rows, :], d_ref.at[rows, :], d_sems.at[i]),
                    pltpu.make_async_remote_copy(
                        src_ref=d_scr.at[rows, :], dst_ref=pd_ref.at[rows, :], send_sem=pd_send.at[i],
                        recv_sem=pd_recv.at[i], device_id=(peer_of(me, 1),), device_id_type=MESH)]

        def last(i, carry):
            rows = block_rows(i)
            for n in range(2):
                dots = as_column(total[pl.ds(i + n * NB, 1), :])
                inv = as_column(inv_ref[pl.ds(i + n * NB, 1), :])
                for hh in range(LOC // HD):
                    sl = slice(hh * HD, (hh + 1) * HD)
                    unit = raw_ref[n, rows, sl] * inv
                    val = inv * (du_scr[n, hh, rows, :] - unit * dots)
                    d_scr[rows, n * LOC + hh * HD:n * LOC + (hh + 1) * HD] = val.astype(BF)
            start(copies(i))
            return carry

        lax.fori_loop(0, NB, last, 0)
        for i in range(NB):
            wait(copies(i))
        more.wait()


def backward(b, qkv, do, lse, raw, inv, gains, cos, sin, gga, shard, old, cid):
    def whole(*shape):
        return pl.BlockSpec(shape, lambda h, i: (0,) * len(shape))

    gsp = whole(8, DIM // 8)
    return pl.pallas_call(
        functools.partial(backward_kernel, b),
        grid=(2, NB),
        in_specs=[pl.BlockSpec((3, SEQ, HD), lambda h, i: (0, 0, h)), pl.BlockSpec((None, BLK, HD), lambda h, i: (b, i, h)),
                  whole(2 * NB, BLK), whole(2, SEQ, LOC), whole(2 * NB, BLK),
                  pl.BlockSpec((2 + DIM // LOC, HD), lambda h, i: (0, h)), whole(SEQ, HD), whole(SEQ, HD), gsp, ANYWHERE]
        + [ANYWHERE] * len(old),
        out_specs=[ANYWHERE, ANYWHERE, pl.BlockSpec((8, HD), lambda h, i: (0, h)), gsp, ANYWHERE] + [ANYWHERE] * len(old),
        out_shape=[sds((SEQ, 3 * LOC), BF), sds((SEQ, 3 * LOC), BF), sds((8, LOC), F32), sds((8, DIM // 8), F32),
                   sds((SEQ, DIM), BF)] + [sds((SEQ, DIM), BF)] * len(old),
        input_output_aliases={10: 5} if old else {},
        scratch_shapes=[pltpu.VMEM((NB, BLK, BLK), F32), pltpu.VMEM((NB, BLK, BLK), F32), pltpu.VMEM((HD, SEQ), BF),
                        pltpu.VMEM((HD, BLK), F32), pltpu.VMEM((SEQ, HD), F32), pltpu.VMEM((SEQ, HD), F32),
                        pltpu.VMEM((SEQ, HD), F32), pltpu.VMEM((2, 2, SEQ, HD), F32), pltpu.VMEM((SEQ, 3 * LOC), BF),
                        pltpu.VMEM((2 * NB, BLK), F32), pltpu.VMEM((2 * NB, BLK), F32),
                        pltpu.VMEM((NDEV - 1, 2 * NB, BLK), F32), pltpu.VMEM((NDEV - 1, 8, DIM // 8), F32),
                        DMA((2, NDEV - 1)), DMA((2, NDEV - 1)), DMA((NB,)), DMA((NB,)), DMA((NB,))] + BG,
        compiler_params=params(dimension_semantics=("arbitrary", "arbitrary"), collective_id=cid, has_side_effects=True),
        cost_estimate=cost(20e9, 20e6),
        name="backward",
    )(qkv, do, lse, raw, inv, gains, cos, sin, gga, shard, *old)


HALF = DIM // 2
CH = 256


def grads_kernel(d0, d1, pd0, pd1, wq, wk, wv, x0, x1, o0, o1, da0, da1_in, dy_ref, dx_ref, gwq_ref, gwk_ref, gwv_ref, gwo_ref, da1,
                 d_all, w_all, sbuf, r1, r2, fin, acc, xbuf, obuf,
                 dl_sems, w_sems, s1_sems, r1_sems, s2_sems, r2_sems, fs_sems, fr_sems, x_sems, o_sems, *sems):
    del da1_in
    me = lax.axis_index('tp')
    core, chip = me % 2, me // 2
    partner = peer_of(me, 1)
    first = peer_of(me, 2) * (1 - core) + peer_of(me, 4) * core
    second = peer_of(me, 4) * (1 - core) + peer_of(me, 2) * core
    diag_chip, first_chip, second_chip = peer_of(me, 6) // 2, first // 2, second // 2

    barrier = pltpu.get_barrier_semaphore()
    for dev in (partner, first, second):
        pl.semaphore_signal(barrier, inc=1, device_id=(dev,), device_id_type=MESH)
    pl.semaphore_wait(barrier, 3)

    def rows_of(blk):
        return pl.ds(pl.multiple_of(blk * BLK, BLK), BLK)

    def half_rows(c):
        return pl.ds(pl.multiple_of(c * HALF, HALF), HALF)

    chips = (diag_chip, first_chip, second_chip, chip)
    w_copies = []
    for n, w in enumerate((wq, wk, wv)):
        part = pl.ds(n * LOC, LOC)
        w_copies.append(pltpu.make_async_remote_copy(
            src_ref=w.at[half_rows(1 - core), :], dst_ref=w_all.at[1, :, part], send_sem=w_sems.at[n],
            recv_sem=w_sems.at[3 + n], device_id=(partner,), device_id_type=MESH))
        w_copies.append(pltpu.make_async_copy(w.at[half_rows(core), :], w_all.at[0, :, part], w_sems.at[6 + n]))
    start(w_copies)
    loads = []
    for kind in range(4):
        for b in range(2):
            n = 2 * kind + b
            rows = rows_of(chips[kind])
            for side, d in enumerate(((d0, d1)[b], (pd0, pd1)[b])):
                loads.append(pltpu.make_async_copy(d.at[rows, :], d_all.at[side, b, rows, :], dl_sems.at[side, n]))
    start(loads)
    last_stage = stage3(me, da1, (*sems, xbuf))
    last_stage.load()
    last_stage.send()
    wait(w_copies)

    def arrived(n, b, blk):
        rows = rows_of(blk)
        for side in range(2):
            pltpu.make_async_copy(d0.at[rows, :], d_all.at[side, b, rows, :], dl_sems.at[side, n]).wait()

    def partial(b, blk):
        rows = rows_of(blk)
        return dot(d_all[0, b, rows, :], w_all[0], NT) + dot(d_all[1, b, rows, :], w_all[1], NT)

    def to_first(n):
        return pltpu.make_async_remote_copy(
            src_ref=sbuf.at[n], dst_ref=r1.at[n], send_sem=s1_sems.at[n], recv_sem=r1_sems.at[n],
            device_id=(first,), device_id_type=MESH)

    def to_second(b):
        return pltpu.make_async_remote_copy(
            src_ref=r1.at[b], dst_ref=r2.at[b], send_sem=s2_sems.at[b], recv_sem=r2_sems.at[b],
            device_id=(second,), device_id_type=MESH)

    def to_partner(b):
        return pltpu.make_async_remote_copy(
            src_ref=r1.at[2 + b, pl.ds(pl.multiple_of((1 - core) * TOK, TOK), TOK), :], dst_ref=fin.at[b],
            send_sem=fs_sems.at[b], recv_sem=fr_sems.at[b], device_id=(partner,), device_id_type=MESH)

    def phase1(n, carry):
        kind, b = n // 2, n % 2
        blk = diag_chip * (1 - kind) + first_chip * kind
        arrived(n, b, blk)
        sbuf[n] = partial(b, blk)
        to_first(n).start()
        return carry

    lax.fori_loop(0, 4, phase1, 0)
    for n in range(4, 8):
        arrived(n, n % 2, chips[n // 2])

    steps = SEQ // CH

    def chunk(i):
        return pl.ds(pl.multiple_of(i * CH, CH), CH)

    def stream(pairs, body):
        def fetch(i):
            return [pltpu.make_async_copy(src.at[chunk(i), :], buf.at[i % 2], sems.at[i % 2]) for src, buf, sems in pairs]

        for c in fetch(0):
            c.start()

        def it(i, carry):
            @pl.when(i + 1 < steps)
            def _():
                for c in fetch(i + 1):
                    c.start()

            for c in fetch(i):
                c.wait()
            body(i)
            return carry

        lax.fori_loop(0, steps, it, 0)

    def wgrad(b, src):
        def body(i):
            left = d_all[0, b, chunk(i), :].T
            for c in range(3):
                part = slice(c * LOC, (c + 1) * LOC)
                acc[part, :] += dot(left[part, :], xbuf[i % 2])

        stream([(src, xbuf, x_sems)], body)

    def forward_second(b, carry):
        to_first(b).wait_recv()
        r1[b] += partial(b, second_chip)
        to_second(b).start()
        return carry

    acc[...] = jnp.zeros_like(acc)
    last_stage.wait()
    wgrad(0, x0)
    forward_second(0, 0)
    wgrad(1, x1)
    for n, ref in enumerate((gwq_ref, gwk_ref, gwv_ref)):
        ref[...] = acc[n * LOC:(n + 1) * LOC, :].T.astype(BF)
    forward_second(1, 0)
    acc[:LOC, :] = jnp.zeros((LOC, DIM), F32)

    def wo_body(i):
        acc[:LOC, :] += dot(obuf[i % 2].T, xbuf[i % 2])

    for o_src, da_src in ((o0, da0), (o1, da1)):
        stream([(da_src, xbuf, x_sems), (o_src, obuf, o_sems)], wo_body)
    gwo_ref[...] = acc[:LOC, :].astype(BF)

    def own_part(b, carry):
        r1_own = partial(b, chip)
        to_first(2 + b).wait_recv()
        to_second(b).wait_recv()
        r1[2 + b] += r1_own + r2[b]
        to_partner(b).start()
        cols = half_rows(core)
        rows = pl.ds(pl.multiple_of(core * TOK, TOK), TOK)
        dx_ref[b, :, cols] = (r1[2 + b, rows, :] + dy_ref[b, :, cols].astype(F32)).astype(BF)
        return carry

    lax.fori_loop(0, 2, own_part, 0)

    def finish(b, carry):
        to_partner(b).wait()
        cols = half_rows(1 - core)
        dx_ref[b, :, cols] = (fin[b] + dy_ref[b, :, cols].astype(F32)).astype(BF)
        to_second(b).wait_send()
        to_first(b).wait_send()
        to_first(2 + b).wait_send()
        return carry

    lax.fori_loop(0, 2, finish, 0)


def grads(d0, d1, pd0, pd1, wq, wk, wv, x0, x1, o0, o1, da0, da1, dy, cid):
    vm = pl.BlockSpec(memory_space=pltpu.VMEM)
    far = pl.BlockSpec(memory_space=pl.ANY)
    dma = pltpu.SemaphoreType.DMA
    return pl.pallas_call(
        grads_kernel,
        in_specs=[far] * 13 + [vm],
        out_specs=[vm] * 5 + [far],
        out_shape=[sds((2, TOK, DIM), BF)] + [sds((DIM, LOC), BF)] * 3 + [sds((LOC, DIM), BF), sds((SEQ, DIM), BF)],
        input_output_aliases={12: 5},
        scratch_shapes=[pltpu.VMEM((2, 2, SEQ, 3 * LOC), BF), pltpu.VMEM((2, HALF, 3 * LOC), BF),
                        pltpu.VMEM((4, BLK, HALF), F32), pltpu.VMEM((4, BLK, HALF), F32), pltpu.VMEM((2, BLK, HALF), F32),
                        pltpu.VMEM((2, TOK, HALF), F32), pltpu.VMEM((3 * LOC, DIM), F32),
                        pltpu.VMEM((2, CH, DIM), BF), pltpu.VMEM((2, CH, LOC), BF),
                        dma((2, 8)), dma((9,)), dma((4,)), dma((4,)), dma((2,)), dma((2,)),
                        dma((2,)), dma((2,)), dma((2,)), dma((2,))] + BG_SEMS,
        compiler_params=pltpu.CompilerParams(vmem_limit_bytes=67043328, collective_id=cid, has_side_effects=True),
        cost_estimate=cost(100e9, 40e6),
        name="grads",
    )(d0, d1, pd0, pd1, wq, wk, wv, x0, x1, o0, o1, da0, da1, dy)


def local_block(x_loc, wq, wk, wv, wo, gq, gk, ga, dy_loc):
    gains = jnp.concatenate([gq, gk, ga]).astype(F32).reshape(2 + DIM // LOC, LOC)
    x_full, cos, sin = first_gather(x_loc, 0)
    gathered, fwd, o_recv = [x_full], [], []
    for b in range(2):
        shard, pick = (x_loc, 1) if b == 0 else (wo, None)
        raw, qkv, inv, o, lse, recv, full = forward(b, gathered[b], wq, wk, wv, gains, cos, sin, shard, pick, o_recv, 1 + b)
        gathered.append(full)
        o_recv = [recv]
        fwd.append((raw, qkv, inv, o, lse))
    y, da, gga, dh = out_block(o_recv[0], gathered[2], x_loc, dy_loc, gains, 3)
    ds, ggs, da_full = [], [], []
    for b in range(2):
        raw, qkv, inv, o, lse = fwd[b]
        d, pd, gg, gout, full, *old = backward(b, qkv, dh, lse, raw, inv, gains, cos, sin, gga, da, da_full, 4 + b)
        da_full = list(old) + [full]
        ds.append((d, pd))
        ggs.append(gg)
        if b == 0:
            grad_ga = gout.reshape(DIM).astype(BF)
    dx, gwq, gwk, gwv, gwo, _ = grads(ds[0][0], ds[1][0], ds[0][1], ds[1][1], wq, wk, wv, gathered[0], gathered[1],
                                      fwd[0][3], fwd[1][3], da_full[0], da_full[1], dy_loc, 6)
    gg = ggs[0] + ggs[1]
    return (y, dx, gwq, gwk, gwv, gwo, gg[0].astype(BF), gg[1].astype(BF), grad_ga)


def solution(mesh):
    act, col, row, vec = P(None, 'tp', None), P(None, 'tp'), P('tp', None), P('tp')
    in_specs = (act, col, col, col, row, vec, vec, P(), act)
    out_specs = (act, act, col, col, col, row, vec, vec, P())
    return jax.shard_map(local_block, mesh=mesh, in_specs=in_specs, out_specs=out_specs, check_vma=False)
```

```python
import functools
import math

import jax
import jax.numpy as jnp
from jax import lax
from jax.experimental import pallas as pl
from jax.experimental.pallas import tpu as pltpu
from jax.sharding import PartitionSpec as P

HD = 128
ROPE_THETA = 500000.0
EPS = 1e-6
DIM = 2048
SEQ = 2048
LOC = 256
TOK = 256
BLK = 512
NB = SEQ // BLK
NDEV = 8
SCALE = HD ** -0.5
C2 = SCALE * math.log2(math.e)
MESH = pl.DeviceIdType.MESH
BF = jnp.bfloat16
F32 = jnp.float32
VMEM_MAX = 60 * 1024 * 1024

NT = (((1,), (1,)), ((), ()))
NN = (((1,), (0,)), ((), ()))


def dot(a, b, dims=NN):
    return lax.dot_general(a, b, dims, preferred_element_type=F32)


def sds(shape, dtype):
    return jax.ShapeDtypeStruct(shape, dtype)


def cost(flops, nbytes, trans=0):
    return pl.CostEstimate(flops=int(flops), bytes_accessed=int(nbytes), transcendentals=int(trans))


def params(**kw):
    return pltpu.CompilerParams(vmem_limit_bytes=VMEM_MAX, **kw)


def peer_of(me, mask):
    core, ax, ay = me % 2, (me // 2) % 2, me // 4
    core = 1 - core if mask & 1 else core
    ax = 1 - ax if mask & 2 else ax
    ay = 1 - ay if mask & 4 else ay
    return ay * 4 + ax * 2 + core


ORDER = (6, 7, 2, 4, 3, 5, 1)


def entry_barrier(me):
    barrier = pltpu.get_barrier_semaphore()
    for mask in ORDER:
        pl.semaphore_signal(barrier, inc=1, device_id=(peer_of(me, mask),), device_id_type=MESH)
    pl.semaphore_wait(barrier, NDEV - 1)


def nbr_barrier(me):
    barrier = pltpu.get_barrier_semaphore()
    for mask in (1, 2, 4):
        pl.semaphore_signal(barrier, inc=1, device_id=(peer_of(me, mask),), device_id_type=MESH)
    pl.semaphore_wait(barrier, 3)


DMA = pltpu.SemaphoreType.DMA
ANYWHERE = pl.BlockSpec(memory_space=pl.ANY)
BG_SEMS = [DMA((11,)), DMA((11,)), DMA((5,))]
BG = BG_SEMS + [pltpu.VMEM((2, TOK, DIM), BF)]


def shard_rows(dev, lo=0, count=TOK):
    return pl.ds(pl.multiple_of(dev * TOK + lo, HD), count)


class Stage:
    def __init__(self, loads, copies):
        self.loads, self.copies = loads, copies

    def load(self):
        start(self.loads)

    def send(self):
        wait(self.loads)
        start(self.copies)

    def wait(self):
        wait(self.copies)


def stage1(me, src, full, bg, part=None):
    send, recv, own, buf = bg
    lo, count, at = (0, TOK, 0) if part is None else (part * (TOK // 2), TOK // 2, 8 * part)
    there = full.at[shard_rows(me, lo, count), :]
    mine = buf.at[0, pl.ds(lo, count), :]
    copies = [pltpu.make_async_remote_copy(
        src_ref=mine, dst_ref=there, send_sem=send.at[at + k], recv_sem=recv.at[at + k],
        device_id=(peer_of(me, mask),), device_id_type=MESH) for k, mask in enumerate((2, 4, 1))]
    loads = [] if part == 1 else [pltpu.make_async_copy(src, buf.at[0], own.at[0])]
    return Stage(loads, copies + [pltpu.make_async_copy(mine, there, own.at[3 if part == 1 else 2])])


def stage2(me, full, bg):
    send, recv, own, buf = bg
    xn, yn = peer_of(me, 2), peer_of(me, 4)
    half = TOK // 2
    plan = ((1, half, half, yn, 2), (0, 0, half, xn, 4), (0, 0, TOK, xn, 1), (1, 0, TOK, yn, 1))
    return Stage(
        [pltpu.make_async_copy(full.at[shard_rows(dev), :], buf.at[n], own.at[n]) for n, dev in enumerate((xn, yn))],
        [pltpu.make_async_remote_copy(
            src_ref=buf.at[slot, pl.ds(lo, count), :], dst_ref=full.at[shard_rows(dev, lo, count), :],
            send_sem=send.at[3 + k], recv_sem=recv.at[3 + k], device_id=(peer_of(me, mask),), device_id_type=MESH)
         for k, (slot, lo, count, dev, mask) in enumerate(plan)])


def stage3(me, full, bg):
    send, recv, own, buf = bg
    rows = full.at[shard_rows(peer_of(me, 6)), :]
    return Stage([pltpu.make_async_copy(rows, buf.at[1], own.at[1])], [pltpu.make_async_remote_copy(
        src_ref=buf.at[1], dst_ref=rows, send_sem=send.at[7], recv_sem=recv.at[7],
        device_id=(peer_of(me, 1),), device_id_type=MESH)])


def start(copies):
    for c in copies:
        c.start()


def wait(copies):
    for c in copies:
        c.wait()


def row_sums(vals):
    folded = vals[:, :HD]
    for start in range(HD, vals.shape[1], HD):
        folded = folded + vals[:, start:start + HD]
    return jnp.sum(folded.T, axis=0, keepdims=True)


def as_column(row):
    return jnp.broadcast_to(row, (HD, row.shape[1])).T


def exchange(me, srcs, slots, send_sems, recv_sems):
    copies = []
    for n, (src, slot) in enumerate(zip(srcs, slots)):
        for p, mask in enumerate(ORDER):
            copies.append(pltpu.make_async_remote_copy(
                src_ref=src, dst_ref=slot.at[p], send_sem=send_sems.at[n, p], recv_sem=recv_sems.at[n, p],
                device_id=(peer_of(me, mask),), device_id_type=MESH))
    return copies


def ordered_total(me, src, slot):
    own = src[...]
    total = jnp.zeros_like(own)
    for dev in range(NDEV):
        term = jnp.where(me == dev, own, 0.0)
        for p, mask in enumerate(ORDER):
            term = term + jnp.where(peer_of(me, mask) == dev, slot[p], 0.0)
        total = total + term
    return total


def causal_mask():
    keys = lax.broadcasted_iota(jnp.int32, (BLK, BLK), 0)
    queries = lax.broadcasted_iota(jnp.int32, (BLK, BLK), 1)
    return keys <= queries


def block_rows(i):
    return pl.ds(pl.multiple_of(i * BLK, BLK), BLK)


def head_cols(h):
    return pl.ds(pl.multiple_of(h * HD, HD), HD)


def forward_kernel(freq_ref, wq_ref, wk_ref, wv_ref, gains_ref, x_ref, wo_ref,
                   cos_ref, sin_ref, inv_ref, o_ref, lse_ref, raw_ref, qkv_ref, both_ref, full_ref, wof_ref,
                   raw, qkv, xbuf, sums_scr, slot, p_scr, vt_scr, acc_scr, o_scr, buf0, buf1,
                   ex_send, ex_recv, out_sems, send_sems, recv_sems, own_sems, x_sems, *bg_sems):
    g = pl.program_id(0)
    b, t = g // (4 * NB), g % (4 * NB)
    me = lax.axis_index('tp')
    bg0, bg1, bg2 = (*bg_sems[:3], buf0), (*bg_sems[3:6], buf1), (*bg_sems[6:], buf0)
    x0f, x1f = full_ref.at[0], full_ref.at[1]

    def x_gather(part=None):
        return stage1(me, x_ref.at[1], x1f, bg1, part)

    def wo_gather(part=None):
        return stage1(me, wo_ref, wof_ref, bg2, part)

    def keep(bb):
        return [pltpu.make_async_copy(raw, raw_ref.at[bb], out_sems.at[0]),
                pltpu.make_async_copy(qkv, qkv_ref.at[bb], out_sems.at[1])]

    def sums(bb):
        return exchange(me, [sums_scr.at[bb]], [slot.at[bb]], ex_send.at[bb], ex_recv.at[bb])

    def fetch(bb, i):
        return pltpu.make_async_copy(full_ref.at[bb, block_rows(i), :], xbuf.at[i % 2], x_sems.at[i % 2])

    def block_copy(bb, hh, st, half):
        dest = 2 * ((me // 2 + 1 + st) % NB) + half
        part = o_scr.at[bb, hh, st, pl.ds(half * TOK, TOK), :]
        dst = both_ref.at[bb, :, pl.ds(pl.multiple_of(me * LOC + hh * HD, HD), HD)]
        away = pltpu.make_async_remote_copy(
            src_ref=part, dst_ref=dst, send_sem=send_sems.at[bb, hh, st, half], recv_sem=recv_sems.at[bb, hh, me],
            device_id=(dest,), device_id_type=MESH)
        return dest, away, pltpu.make_async_copy(part, dst, own_sems.at[bb, hh])

    def run(stage):
        stage.load()
        stage.send()

    @pl.when(g == 0)
    def _():
        first = stage1(me, x_ref.at[0], x0f, bg0)
        first.load()
        entry_barrier(me)
        first.send()
        x_gather(0).load()
        freq = freq_ref[...]
        sign = jnp.where(lax.broadcasted_iota(jnp.int32, (TOK, HD), 1) < HD // 2, -1.0, 1.0)

        def table(i, carry):
            rows = pl.ds(pl.multiple_of(i * TOK, TOK), TOK)
            pos = (lax.broadcasted_iota(jnp.int32, (TOK, HD), 0) + i * TOK).astype(F32)
            angle = pos * freq
            cos_ref[rows, :] = jnp.cos(angle)
            sin_ref[rows, :] = jnp.sin(angle) * sign
            return carry

        lax.fori_loop(0, SEQ // TOK, table, 0)
        first.wait()
        second, third = stage2(me, x0f, bg0), stage3(me, x0f, bg0)
        run(second)
        x_gather(0).send()
        second.wait()
        run(third)
        third.wait()
        fetch(0, 0).start()

    @pl.when(g == 2 * NB + 2)
    def _():
        x_gather(0).wait()
        x_gather(1).wait()
        run(stage2(me, x1f, bg1))
        run(wo_gather(0))

    @pl.when(g == 4 * NB)
    def _():
        stage2(me, x1f, bg1).wait()
        third = stage3(me, x1f, bg1)
        run(third)
        for c in keep(0):
            c.wait()
        third.wait()
        fetch(1, 0).start()

    @pl.when(g == 6 * NB + 2)
    def _():
        wo_gather(0).wait()
        wo_gather(1).wait()
        run(stage2(me, wof_ref, bg2))

    @pl.when(t < NB)
    def _():
        rows = block_rows(t)

        @pl.when(t < NB - 1)
        def _():
            fetch(b, t + 1).start()

        fetch(b, t).wait()
        x = xbuf[t % 2]
        for n, w_ref in enumerate((wq_ref, wk_ref)):
            val = dot(x, w_ref[...])
            raw[n, rows, :] = val
            sums_scr[b, pl.ds(t + n * NB, 1), :] = row_sums(val * val)
        qkv[2, rows, :] = dot(x, wv_ref[...]).astype(BF)

    @pl.when(t == NB)
    def _():
        start(sums(b))
        keep(b)[0].start()
        pl.when(b == 0)(x_gather(1).send)
        pl.when(b == 1)(wo_gather(1).send)
        wait(sums(b))
        inv_ref[...] = lax.rsqrt(ordered_total(me, sums_scr.at[b], slot.at[b]) / DIM + EPS)

    @pl.when(jnp.logical_and(t >= NB, t < 2 * NB))
    def _():
        i = t - NB
        rows = block_rows(i)
        cos, sin = cos_ref[rows, :], sin_ref[rows, :]
        for n in range(2):
            inv = as_column(inv_ref[pl.ds(i + n * NB, 1), :])
            gain = gains_ref[n:n + 1, :]
            for h in range(LOC // HD):
                sl = slice(h * HD, (h + 1) * HD)
                hat = raw[n, rows, sl] * inv * gain[:, sl]
                qkv[n, rows, sl] = (hat * cos + pltpu.roll(hat, HD // 2, 1) * sin).astype(BF)

    @pl.when(t == 2 * NB)
    def _():
        keep(b)[1].start()

    @pl.when(t >= 2 * NB)
    def _():
        h, step = t // NB - 2, t % NB
        qi = (me // 2 + 1 + step) % NB
        cols = head_cols(h)

        @pl.when(step == 0)
        def _():
            vt_scr[...] = qkv[2, :, cols].T

        qb = qkv[0, block_rows(qi), cols]

        def scores(j):
            return dot(qkv[1, block_rows(j), cols], qb, NT)

        def first(j, m):
            s = scores(j)
            p_scr[j] = s
            return jnp.maximum(m, jnp.max(s.reshape(BLK // 8, 8, BLK), axis=0))

        s = jnp.where(causal_mask(), scores(qi), -1e30)
        p_scr[qi] = s
        m = lax.fori_loop(0, qi, first, jnp.max(s.reshape(BLK // 8, 8, BLK), axis=0))
        m = jnp.max(m, axis=0, keepdims=True)

        def second(j, l):
            p = jnp.exp2((p_scr[j] - m) * C2)
            p_scr[j] = p
            return l + jnp.sum(p.reshape(BLK // 8, 8, BLK), axis=0)

        l = lax.fori_loop(0, qi + 1, second, jnp.zeros((8, BLK), F32))
        l = jnp.sum(l, axis=0, keepdims=True)
        rl = 1.0 / l
        lse_ref[pl.ds(h * NB + qi, 1), :] = m * C2 + jnp.log2(l)

        acc_scr[...] = jnp.zeros_like(acc_scr)

        def third(j, carry):
            p = (p_scr[j] * rl).astype(BF)
            acc_scr[...] += dot(vt_scr[:, block_rows(j)], p)
            return carry

        lax.fori_loop(0, qi + 1, third, 0)
        out = acc_scr[...].T.astype(BF)
        o_scr[b, h, step] = out
        o_ref[block_rows(qi), cols] = out

        for half in range(2):
            dest, away, here = block_copy(b, h, step, half)
            pl.when(dest != me)(away.start)
            pl.when(dest == me)(here.start)

    @pl.when(g == 8 * NB - 1)
    def _():
        stage2(me, wof_ref, bg2).wait()
        third = stage3(me, wof_ref, bg2)
        run(third)
        for c in keep(1):
            c.wait()

        def drain(n, carry):
            bb, hh = n // 2, n % 2
            for st in range(NB):
                for half in range(2):
                    dest, away, here = block_copy(bb, hh, st, half)
                    if st < NB - 1:
                        away.wait_send()
                    else:
                        pl.when(dest != me)(away.wait_send)
                        pl.when(dest == me)(here.wait)
            for mask in ORDER:
                peer = peer_of(me, mask)
                pltpu.make_async_remote_copy(
                    src_ref=o_scr.at[0, 0, 0, pl.ds(0, TOK), :],
                    dst_ref=both_ref.at[bb, :, pl.ds(pl.multiple_of(peer * LOC + hh * HD, HD), HD)],
                    send_sem=send_sems.at[0, 0, 0, 0], recv_sem=recv_sems.at[bb, hh, peer],
                    device_id=(peer,), device_id_type=MESH).wait_recv()
            return carry

        lax.fori_loop(0, 4, drain, 0)
        third.wait()


def forward(x, wq, wk, wv, wo, gains, cid):
    half = HD // 2
    inv_freq = 1.0 / (ROPE_THETA ** (jnp.arange(half, dtype=F32) / half))
    freq = jnp.concatenate([inv_freq, inv_freq])[None, :]

    def whole(*shape):
        return pl.BlockSpec(shape, lambda g: (0,) * len(shape))

    def per_batch(*shape):
        return pl.BlockSpec((None,) + shape, lambda g: (g // (4 * NB),) + (0,) * len(shape))

    wspec, rows = whole(DIM, LOC), per_batch(2 * NB, BLK)
    return pl.pallas_call(
        forward_kernel,
        grid=(8 * NB,),
        in_specs=[whole(1, HD), wspec, wspec, wspec, whole(2 + DIM // LOC, LOC), ANYWHERE, ANYWHERE],
        out_specs=[whole(SEQ, HD), whole(SEQ, HD), rows, per_batch(SEQ, LOC), rows] + [ANYWHERE] * 5,
        out_shape=[sds((SEQ, HD), F32), sds((SEQ, HD), F32), sds((2, 2 * NB, BLK), F32), sds((2, SEQ, LOC), BF),
                   sds((2, 2 * NB, BLK), F32), sds((2, 2, SEQ, LOC), F32), sds((2, 3, SEQ, LOC), BF),
                   sds((2, TOK, DIM), BF), sds((2, SEQ, DIM), BF), sds((SEQ, DIM), BF)],
        scratch_shapes=[pltpu.VMEM((2, SEQ, LOC), F32), pltpu.VMEM((3, SEQ, LOC), BF), pltpu.VMEM((2, BLK, DIM), BF),
                        pltpu.VMEM((2, 2 * NB, BLK), F32), pltpu.VMEM((2, NDEV - 1, 2 * NB, BLK), F32),
                        pltpu.VMEM((NB, BLK, BLK), F32), pltpu.VMEM((HD, SEQ), BF), pltpu.VMEM((HD, BLK), F32),
                        pltpu.VMEM((2, 2, NB, BLK, HD), BF), pltpu.VMEM((2, TOK, DIM), BF), pltpu.VMEM((2, TOK, DIM), BF),
                        DMA((2, 1, NDEV - 1)), DMA((2, 1, NDEV - 1)), DMA((2,)),
                        DMA((2, 2, NB, 2)), DMA((2, 2, NDEV)), DMA((2, 2)), DMA((2,))] + BG_SEMS * 3,
        compiler_params=params(dimension_semantics=("arbitrary",), collective_id=cid, has_side_effects=True),
        cost_estimate=cost(60e9, 60e6),
        name="forward",
    )(freq, wq, wk, wv, gains, x, wo)


def out_kernel(o_ref, wo_ref, x_ref, dy_ref, gains_ref, y_ref, da_ref, gga_ref, both_ref, a_scr, dh_scr, send_sems, recv_sems,
               own_sems):
    b = pl.program_id(0)
    me = lax.axis_index('tp')

    @pl.when(b == 0)
    def _():
        entry_barrier(me)
        gga_ref[...] = jnp.zeros_like(gga_ref)

    step = DIM // NB
    o = o_ref[0]

    def fwd(j, carry):
        cols = pl.ds(pl.multiple_of(j * step, step), step)
        a_scr[:, cols] = dot(o, wo_ref[:, cols])
        return carry

    lax.fori_loop(0, NB, fwd, 0)
    a = a_scr[...]
    r = lax.rsqrt(jnp.mean(a * a, axis=-1, keepdims=True) + EPS)
    n = a * r
    ga = jnp.concatenate([gains_ref[2 + i:3 + i, :] for i in range(8)], axis=1)
    dy = dy_ref[0].astype(F32)
    y_ref[0] = (x_ref[0].astype(F32) + n * ga).astype(BF)
    col = jnp.sum(dy * n, axis=0, keepdims=True)
    for i in range(8):
        gga_ref[i:i + 1, :] += col[:, i * LOC:(i + 1) * LOC]
    gn = dy * ga
    da_ref[0] = (r * (gn - n * jnp.mean(gn * n, axis=-1, keepdims=True))).astype(BF)
    da = da_ref[0]

    def block_copy(bb, st, half):
        dest = 2 * ((me // 2 + 1 + st) % NB) + half
        src = dh_scr.at[bb, st, :, pl.ds(half * LOC, LOC)]
        mine = both_ref.at[bb, shard_rows(me), :]
        away = pltpu.make_async_remote_copy(
            src_ref=src, dst_ref=mine, send_sem=send_sems.at[bb, st, half], recv_sem=recv_sems.at[bb, me],
            device_id=(dest,), device_id_type=MESH)
        return dest, away, pltpu.make_async_copy(src, mine, own_sems.at[bb])

    def bwd(st, carry):
        blk = (me // 2 + 1 + st) % NB
        dh_scr[b, st] = dot(da, wo_ref[pl.ds(pl.multiple_of(blk * step, step), step), :], NT).astype(BF)
        for half in range(2):
            dest, away, here = block_copy(b, st, half)
            pl.when(dest != me)(away.start)
            pl.when(dest == me)(here.start)
        return carry

    lax.fori_loop(0, NB, bwd, 0)

    @pl.when(b == 1)
    def _():
        for bb in range(2):
            for st in range(NB):
                for half in range(2):
                    dest, away, here = block_copy(bb, st, half)
                    if st < NB - 1:
                        away.wait_send()
                    else:
                        pl.when(dest != me)(away.wait_send)
                        pl.when(dest == me)(here.wait)
            for mask in ORDER:
                peer = peer_of(me, mask)
                pltpu.make_async_remote_copy(
                    src_ref=dh_scr.at[0, 0, :, pl.ds(0, LOC)], dst_ref=both_ref.at[bb, shard_rows(peer), :],
                    send_sem=send_sems.at[0, 0, 0], recv_sem=recv_sems.at[bb, peer], device_id=(peer,),
                    device_id_type=MESH).wait_recv()


def out_block(o, wo, x, dy, gains, cid):
    def whole(*shape):
        return pl.BlockSpec(shape, lambda i: (0,) * len(shape))

    batch = pl.BlockSpec((1, TOK, DIM), lambda i: (i, 0, 0))
    return pl.pallas_call(
        out_kernel,
        grid=(2,),
        in_specs=[batch, whole(DIM, DIM), batch, batch, whole(2 + DIM // LOC, LOC)],
        out_specs=[batch, batch, whole(8, DIM // 8), ANYWHERE],
        out_shape=[sds((2, TOK, DIM), BF), sds((2, TOK, DIM), BF), sds((8, DIM // 8), F32), sds((2, SEQ, LOC), BF)],
        scratch_shapes=[pltpu.VMEM((TOK, DIM), F32), pltpu.VMEM((2, NB, TOK, DIM // NB), BF), DMA((2, NB, 2)),
                        DMA((2, NDEV)), DMA((2,))],
        compiler_params=params(dimension_semantics=("arbitrary",), collective_id=cid, has_side_effects=True),
        cost_estimate=cost(8 * TOK * DIM * DIM + 5e9, 18e6),
        name="out_block",
    )(o, wo, x, dy, gains)


def backward_kernel(b, qkv_ref, do_ref, lse_ref, raw_ref, inv_ref, gains_ref, cos_ref, sin_ref, gga_ref, shard_ref, *rest):
    if b:
        _, d_ref, pd_ref, gg_ref, gout_ref, full_ref, old_ref, *rest = rest
    else:
        d_ref, pd_ref, gg_ref, gout_ref, full_ref, *rest = rest
    (p_scr, dp_scr, kt_scr, dqt_scr, dq_scr, dk_scr, dv_scr, du_scr, d_scr, dots_scr, total, slot, ga_slot,
     ex_send, ex_recv, pd_send, pd_recv, d_sems, *bg) = rest
    h, qi = pl.program_id(0), pl.program_id(1)
    me = lax.axis_index('tp')
    gather = stage1(me, shard_ref.at[b], full_ref, bg)

    @pl.when(jnp.logical_and(h == 0, qi == 0))
    def _():
        stages = ([stage3(me, old_ref, bg)] if b else []) + [gather]
        for stage in stages:
            stage.load()
        entry_barrier(me)
        for stage in stages:
            stage.send()
        dots_scr[...] = jnp.zeros_like(dots_scr)

    @pl.when(qi == 0)
    def _():
        kt_scr[...] = qkv_ref[1].T
        dk_scr[...] = jnp.zeros_like(dk_scr)
        dv_scr[...] = jnp.zeros_like(dv_scr)

    qb = qkv_ref[0, block_rows(qi), :]
    dob = do_ref[...]
    lse = lse_ref[pl.ds(h * NB + qi, 1), :]

    def first(j, acc, diag=False):
        rows = block_rows(j)
        p = jnp.exp2(dot(qkv_ref[1, rows, :], qb, NT) * C2 - lse)
        if diag:
            p = jnp.where(causal_mask(), p, 0.0)
        dp = dot(qkv_ref[2, rows, :], dob, NT)
        p_scr[j] = p
        dp_scr[j] = dp
        dv_scr[rows, :] += dot(p.astype(BF), dob)
        return acc + jnp.sum((p * dp).reshape(BLK // 8, 8, BLK), axis=0)

    acc = first(qi, jnp.zeros((8, BLK), F32), True)
    acc = lax.fori_loop(0, qi, first, acc)
    delta = jnp.sum(acc, axis=0, keepdims=True)
    dqt_scr[...] = jnp.zeros_like(dqt_scr)

    def second(j, carry):
        rows = block_rows(j)
        ds = (p_scr[j] * (dp_scr[j] - delta) * SCALE).astype(BF)
        dk_scr[rows, :] += dot(ds, qb)
        dqt_scr[...] += dot(kt_scr[:, rows], ds)
        return carry

    lax.fori_loop(0, qi + 1, second, 0)
    dq_scr[block_rows(qi), :] = dqt_scr[...].T

    @pl.when(qi == NB - 1)
    def _():
        d_scr[:, pl.ds(pl.multiple_of(2 * LOC + h * HD, HD), HD)] = dv_scr[...].astype(BF)
        gg_ref[...] = jnp.zeros_like(gg_ref)
        cols = head_cols(h)

        def tail(i, carry):
            rows = block_rows(i)
            cos, sin = cos_ref[rows, :], sin_ref[rows, :]
            for n, from_scr in enumerate((dq_scr, dk_scr)):
                d = from_scr[rows, :]
                hat = d * cos - pltpu.roll(d, HD // 2, 1) * sin
                unit = raw_ref[n, rows, cols] * as_column(inv_ref[pl.ds(i + n * NB, 1), :])
                gg_ref[n:n + 1, :] += jnp.sum(hat * unit, axis=0, keepdims=True)
                du = hat * gains_ref[n:n + 1, :]
                du_scr[n, h, rows, :] = du
                dots_scr[pl.ds(i + n * NB, 1), :] += row_sums(du * unit)
            return carry

        lax.fori_loop(0, NB, tail, 0)

    @pl.when(jnp.logical_and(h == 1, qi == NB - 1))
    def _():
        gather.wait()
        if b:
            stage3(me, old_ref, bg).wait()
        sums = exchange(me, [dots_scr, gga_ref], [slot, ga_slot], ex_send, ex_recv)
        start(sums)
        more = stage2(me, full_ref, bg)
        more.load()
        more.send()
        wait(sums)
        total[...] = ordered_total(me, dots_scr, slot) / DIM
        gout_ref[...] = ordered_total(me, gga_ref, ga_slot)

        def copies(i):
            rows = block_rows(i)
            return [pltpu.make_async_copy(d_scr.at[rows, :], d_ref.at[rows, :], d_sems.at[i]),
                    pltpu.make_async_remote_copy(
                        src_ref=d_scr.at[rows, :], dst_ref=pd_ref.at[rows, :], send_sem=pd_send.at[i],
                        recv_sem=pd_recv.at[i], device_id=(peer_of(me, 1),), device_id_type=MESH)]

        def last(i, carry):
            rows = block_rows(i)
            for n in range(2):
                dots = as_column(total[pl.ds(i + n * NB, 1), :])
                inv = as_column(inv_ref[pl.ds(i + n * NB, 1), :])
                for hh in range(LOC // HD):
                    sl = slice(hh * HD, (hh + 1) * HD)
                    unit = raw_ref[n, rows, sl] * inv
                    val = inv * (du_scr[n, hh, rows, :] - unit * dots)
                    d_scr[rows, n * LOC + hh * HD:n * LOC + (hh + 1) * HD] = val.astype(BF)
            start(copies(i))
            return carry

        lax.fori_loop(0, NB, last, 0)
        for i in range(NB):
            wait(copies(i))
        more.wait()


def backward(b, qkv, do, lse, raw, inv, gains, cos, sin, gga, shard, old, cid):
    def whole(*shape):
        return pl.BlockSpec(shape, lambda h, i: (0,) * len(shape))

    def picked(*shape):
        return pl.BlockSpec((None,) + shape, lambda h, i: (b,) + (0,) * len(shape))

    gsp = whole(8, DIM // 8)
    return pl.pallas_call(
        functools.partial(backward_kernel, b),
        grid=(2, NB),
        in_specs=[pl.BlockSpec((None, 3, SEQ, HD), lambda h, i: (b, 0, 0, h)), pl.BlockSpec((None, BLK, HD), lambda h, i: (b, i, h)),
                  picked(2 * NB, BLK), picked(2, SEQ, LOC), picked(2 * NB, BLK),
                  pl.BlockSpec((2 + DIM // LOC, HD), lambda h, i: (0, h)), whole(SEQ, HD), whole(SEQ, HD), gsp, ANYWHERE]
        + [ANYWHERE] * len(old),
        out_specs=[ANYWHERE, ANYWHERE, pl.BlockSpec((8, HD), lambda h, i: (0, h)), gsp, ANYWHERE] + [ANYWHERE] * len(old),
        out_shape=[sds((SEQ, 3 * LOC), BF), sds((SEQ, 3 * LOC), BF), sds((8, LOC), F32), sds((8, DIM // 8), F32),
                   sds((SEQ, DIM), BF)] + [sds((SEQ, DIM), BF)] * len(old),
        input_output_aliases={10: 5} if old else {},
        scratch_shapes=[pltpu.VMEM((NB, BLK, BLK), F32), pltpu.VMEM((NB, BLK, BLK), F32), pltpu.VMEM((HD, SEQ), BF),
                        pltpu.VMEM((HD, BLK), F32), pltpu.VMEM((SEQ, HD), F32), pltpu.VMEM((SEQ, HD), F32),
                        pltpu.VMEM((SEQ, HD), F32), pltpu.VMEM((2, 2, SEQ, HD), F32), pltpu.VMEM((SEQ, 3 * LOC), BF),
                        pltpu.VMEM((2 * NB, BLK), F32), pltpu.VMEM((2 * NB, BLK), F32),
                        pltpu.VMEM((NDEV - 1, 2 * NB, BLK), F32), pltpu.VMEM((NDEV - 1, 8, DIM // 8), F32),
                        DMA((2, NDEV - 1)), DMA((2, NDEV - 1)), DMA((NB,)), DMA((NB,)), DMA((NB,))] + BG,
        compiler_params=params(dimension_semantics=("arbitrary", "arbitrary"), collective_id=cid, has_side_effects=True),
        cost_estimate=cost(20e9, 20e6),
        name="backward",
    )(qkv, do, lse, raw, inv, gains, cos, sin, gga, shard, *old)


HALF = DIM // 2
CH = 256


def grads_kernel(d0, d1, pd0, pd1, wq, wk, wv, x_full, o_all, da0, da1_in, dy_ref, dx_ref, gwq_ref, gwk_ref, gwv_ref, gwo_ref, da1,
                 d_all, w_all, sbuf, r1, r2, fin, acc, xbuf, obuf,
                 dl_sems, w_sems, s1_sems, r1_sems, s2_sems, r2_sems, fs_sems, fr_sems, x_sems, o_sems, *sems):
    del da1_in
    me = lax.axis_index('tp')
    core, chip = me % 2, me // 2
    partner = peer_of(me, 1)
    first = peer_of(me, 2) * (1 - core) + peer_of(me, 4) * core
    second = peer_of(me, 4) * (1 - core) + peer_of(me, 2) * core
    diag_chip, first_chip, second_chip = peer_of(me, 6) // 2, first // 2, second // 2

    barrier = pltpu.get_barrier_semaphore()
    for dev in (partner, first, second):
        pl.semaphore_signal(barrier, inc=1, device_id=(dev,), device_id_type=MESH)
    pl.semaphore_wait(barrier, 3)

    def rows_of(blk):
        return pl.ds(pl.multiple_of(blk * BLK, BLK), BLK)

    def half_rows(c):
        return pl.ds(pl.multiple_of(c * HALF, HALF), HALF)

    chips = (diag_chip, first_chip, second_chip, chip)
    w_copies = []
    for n, w in enumerate((wq, wk, wv)):
        part = pl.ds(n * LOC, LOC)
        w_copies.append(pltpu.make_async_remote_copy(
            src_ref=w.at[half_rows(1 - core), :], dst_ref=w_all.at[1, :, part], send_sem=w_sems.at[n],
            recv_sem=w_sems.at[3 + n], device_id=(partner,), device_id_type=MESH))
        w_copies.append(pltpu.make_async_copy(w.at[half_rows(core), :], w_all.at[0, :, part], w_sems.at[6 + n]))
    start(w_copies)
    loads = []
    for kind in range(4):
        for b in range(2):
            n = 2 * kind + b
            rows = rows_of(chips[kind])
            for side, d in enumerate(((d0, d1)[b], (pd0, pd1)[b])):
                loads.append(pltpu.make_async_copy(d.at[rows, :], d_all.at[side, b, rows, :], dl_sems.at[side, n]))
    start(loads)
    last_stage = stage3(me, da1, (*sems, xbuf))
    last_stage.load()
    last_stage.send()
    wait(w_copies)

    def arrived(n, b, blk):
        rows = rows_of(blk)
        for side in range(2):
            pltpu.make_async_copy(d0.at[rows, :], d_all.at[side, b, rows, :], dl_sems.at[side, n]).wait()

    def partial(b, blk):
        rows = rows_of(blk)
        return dot(d_all[0, b, rows, :], w_all[0], NT) + dot(d_all[1, b, rows, :], w_all[1], NT)

    def to_first(n):
        return pltpu.make_async_remote_copy(
            src_ref=sbuf.at[n], dst_ref=r1.at[n], send_sem=s1_sems.at[n], recv_sem=r1_sems.at[n],
            device_id=(first,), device_id_type=MESH)

    def to_second(b):
        return pltpu.make_async_remote_copy(
            src_ref=r1.at[b], dst_ref=r2.at[b], send_sem=s2_sems.at[b], recv_sem=r2_sems.at[b],
            device_id=(second,), device_id_type=MESH)

    def to_partner(b):
        return pltpu.make_async_remote_copy(
            src_ref=r1.at[2 + b, pl.ds(pl.multiple_of((1 - core) * TOK, TOK), TOK), :], dst_ref=fin.at[b],
            send_sem=fs_sems.at[b], recv_sem=fr_sems.at[b], device_id=(partner,), device_id_type=MESH)

    def phase1(n, carry):
        kind, b = n // 2, n % 2
        blk = diag_chip * (1 - kind) + first_chip * kind
        arrived(n, b, blk)
        sbuf[n] = partial(b, blk)
        to_first(n).start()
        return carry

    lax.fori_loop(0, 4, phase1, 0)
    for n in range(4, 8):
        arrived(n, n % 2, chips[n // 2])

    steps = SEQ // CH

    def chunk(i):
        return pl.ds(pl.multiple_of(i * CH, CH), CH)

    def stream(pairs, body):
        def fetch(i):
            return [pltpu.make_async_copy(src.at[chunk(i), :], buf.at[i % 2], sems.at[i % 2]) for src, buf, sems in pairs]

        for c in fetch(0):
            c.start()

        def it(i, carry):
            @pl.when(i + 1 < steps)
            def _():
                for c in fetch(i + 1):
                    c.start()

            for c in fetch(i):
                c.wait()
            body(i)
            return carry

        lax.fori_loop(0, steps, it, 0)

    def wgrad(b, src):
        def body(i):
            left = d_all[0, b, chunk(i), :].T
            for c in range(3):
                part = slice(c * LOC, (c + 1) * LOC)
                acc[part, :] += dot(left[part, :], xbuf[i % 2])

        stream([(src, xbuf, x_sems)], body)

    def forward_second(b, carry):
        to_first(b).wait_recv()
        r1[b] += partial(b, second_chip)
        to_second(b).start()
        return carry

    acc[...] = jnp.zeros_like(acc)
    last_stage.wait()
    wgrad(0, x_full.at[0])
    forward_second(0, 0)
    wgrad(1, x_full.at[1])
    for n, ref in enumerate((gwq_ref, gwk_ref, gwv_ref)):
        ref[...] = acc[n * LOC:(n + 1) * LOC, :].T.astype(BF)
    forward_second(1, 0)
    acc[:LOC, :] = jnp.zeros((LOC, DIM), F32)

    def wo_body(i):
        acc[:LOC, :] += dot(obuf[i % 2].T, xbuf[i % 2])

    for o_src, da_src in ((o_all.at[0], da0), (o_all.at[1], da1)):
        stream([(da_src, xbuf, x_sems), (o_src, obuf, o_sems)], wo_body)
    gwo_ref[...] = acc[:LOC, :].astype(BF)

    def own_part(b, carry):
        r1_own = partial(b, chip)
        to_first(2 + b).wait_recv()
        to_second(b).wait_recv()
        r1[2 + b] += r1_own + r2[b]
        to_partner(b).start()
        cols = half_rows(core)
        rows = pl.ds(pl.multiple_of(core * TOK, TOK), TOK)
        dx_ref[b, :, cols] = (r1[2 + b, rows, :] + dy_ref[b, :, cols].astype(F32)).astype(BF)
        return carry

    lax.fori_loop(0, 2, own_part, 0)

    def finish(b, carry):
        to_partner(b).wait()
        cols = half_rows(1 - core)
        dx_ref[b, :, cols] = (fin[b] + dy_ref[b, :, cols].astype(F32)).astype(BF)
        to_second(b).wait_send()
        to_first(b).wait_send()
        to_first(2 + b).wait_send()
        return carry

    lax.fori_loop(0, 2, finish, 0)


def grads(d0, d1, pd0, pd1, wq, wk, wv, x_full, o_all, da0, da1, dy, cid):
    vm = pl.BlockSpec(memory_space=pltpu.VMEM)
    far = pl.BlockSpec(memory_space=pl.ANY)
    dma = pltpu.SemaphoreType.DMA
    return pl.pallas_call(
        grads_kernel,
        in_specs=[far] * 11 + [vm],
        out_specs=[vm] * 5 + [far],
        out_shape=[sds((2, TOK, DIM), BF)] + [sds((DIM, LOC), BF)] * 3 + [sds((LOC, DIM), BF), sds((SEQ, DIM), BF)],
        input_output_aliases={10: 5},
        scratch_shapes=[pltpu.VMEM((2, 2, SEQ, 3 * LOC), BF), pltpu.VMEM((2, HALF, 3 * LOC), BF),
                        pltpu.VMEM((4, BLK, HALF), F32), pltpu.VMEM((4, BLK, HALF), F32), pltpu.VMEM((2, BLK, HALF), F32),
                        pltpu.VMEM((2, TOK, HALF), F32), pltpu.VMEM((3 * LOC, DIM), F32),
                        pltpu.VMEM((2, CH, DIM), BF), pltpu.VMEM((2, CH, LOC), BF),
                        dma((2, 8)), dma((9,)), dma((4,)), dma((4,)), dma((2,)), dma((2,)),
                        dma((2,)), dma((2,)), dma((2,)), dma((2,))] + BG_SEMS,
        compiler_params=pltpu.CompilerParams(vmem_limit_bytes=67043328, collective_id=cid, has_side_effects=True),
        cost_estimate=cost(100e9, 40e6),
        name="grads",
    )(d0, d1, pd0, pd1, wq, wk, wv, x_full, o_all, da0, da1, dy)


def local_block(x_loc, wq, wk, wv, wo, gq, gk, ga, dy_loc):
    gains = jnp.concatenate([gq, gk, ga]).astype(F32).reshape(2 + DIM // LOC, LOC)
    cos, sin, inv, o, lse, raw, qkv, o_recv, x_full, wo_full = forward(x_loc, wq, wk, wv, wo, gains, 0)
    y, da, gga, dh = out_block(o_recv, wo_full, x_loc, dy_loc, gains, 1)
    ds, ggs, da_full = [], [], []
    for b in range(2):
        d, pd, gg, gout, full, *old = backward(b, qkv, dh, lse, raw, inv, gains, cos, sin, gga, da, da_full, 2 + b)
        da_full = list(old) + [full]
        ds.append((d, pd))
        ggs.append(gg)
        if b == 0:
            grad_ga = gout.reshape(DIM).astype(BF)
    dx, gwq, gwk, gwv, gwo, _ = grads(ds[0][0], ds[1][0], ds[0][1], ds[1][1], wq, wk, wv, x_full, o,
                                      da_full[0], da_full[1], dy_loc, 4)
    gg = ggs[0] + ggs[1]
    return (y, dx, gwq, gwk, gwv, gwo, gg[0].astype(BF), gg[1].astype(BF), grad_ga)


def solution(mesh):
    act, col, row, vec = P(None, 'tp', None), P(None, 'tp'), P('tp', None), P('tp')
    in_specs = (act, col, col, col, row, vec, vec, P(), act)
    out_specs = (act, act, col, col, col, row, vec, vec, P())
    return jax.shard_map(local_block, mesh=mesh, in_specs=in_specs, out_specs=out_specs, check_vma=False)
```

```python
import functools
import math

import jax
import jax.numpy as jnp
from jax import lax
from jax.experimental import pallas as pl
from jax.experimental.pallas import tpu as pltpu
from jax.sharding import PartitionSpec as P

HD = 128
ROPE_THETA = 500000.0
EPS = 1e-6
DIM = 2048
SEQ = 2048
LOC = 256
TOK = 256
BLK = 512
NB = SEQ // BLK
NDEV = 8
SCALE = HD ** -0.5
C2 = SCALE * math.log2(math.e)
MESH = pl.DeviceIdType.MESH
BF = jnp.bfloat16
F32 = jnp.float32
VMEM_MAX = 60 * 1024 * 1024

NT = (((1,), (1,)), ((), ()))
NN = (((1,), (0,)), ((), ()))


def dot(a, b, dims=NN):
    return lax.dot_general(a, b, dims, preferred_element_type=F32)


def sds(shape, dtype):
    return jax.ShapeDtypeStruct(shape, dtype)


def cost(flops, nbytes, trans=0):
    return pl.CostEstimate(flops=int(flops), bytes_accessed=int(nbytes), transcendentals=int(trans))


def params(**kw):
    return pltpu.CompilerParams(vmem_limit_bytes=VMEM_MAX, **kw)


def peer_of(me, mask):
    core, ax, ay = me % 2, (me // 2) % 2, me // 4
    core = 1 - core if mask & 1 else core
    ax = 1 - ax if mask & 2 else ax
    ay = 1 - ay if mask & 4 else ay
    return ay * 4 + ax * 2 + core


ORDER = (6, 7, 2, 4, 3, 5, 1)


def entry_barrier(me):
    barrier = pltpu.get_barrier_semaphore()
    for mask in ORDER:
        pl.semaphore_signal(barrier, inc=1, device_id=(peer_of(me, mask),), device_id_type=MESH)
    pl.semaphore_wait(barrier, NDEV - 1)


def nbr_barrier(me):
    barrier = pltpu.get_barrier_semaphore()
    for mask in (1, 2, 4):
        pl.semaphore_signal(barrier, inc=1, device_id=(peer_of(me, mask),), device_id_type=MESH)
    pl.semaphore_wait(barrier, 3)


DMA = pltpu.SemaphoreType.DMA
ANYWHERE = pl.BlockSpec(memory_space=pl.ANY)
BG_SEMS = [DMA((11,)), DMA((11,)), DMA((5,))]
BG = BG_SEMS + [pltpu.VMEM((2, TOK, DIM), BF)]


def shard_rows(dev, lo=0, count=TOK):
    return pl.ds(pl.multiple_of(dev * TOK + lo, HD), count)


class Stage:
    def __init__(self, loads, copies):
        self.loads, self.copies = loads, copies

    def load(self):
        start(self.loads)

    def send(self):
        wait(self.loads)
        start(self.copies)

    def wait(self):
        wait(self.copies)


def stage1(me, src, full, bg, part=None, fresh=False):
    send, recv, own, buf = bg
    lo, count, at = (0, TOK, 0) if part is None else (part * (TOK // 2), TOK // 2, 8 * part)
    there = full.at[shard_rows(me, lo, count), :]
    mine = buf.at[0, pl.ds(lo, count), :]
    copies = [pltpu.make_async_remote_copy(
        src_ref=mine, dst_ref=there, send_sem=send.at[at + k], recv_sem=recv.at[at + k],
        device_id=(peer_of(me, mask),), device_id_type=MESH) for k, mask in enumerate((2, 4, 1))]
    loads = [] if part == 1 and not fresh else [pltpu.make_async_copy(src, buf.at[0], own.at[0])]
    return Stage(loads, copies + [pltpu.make_async_copy(mine, there, own.at[3 if part == 1 else 2])])


def stage2(me, full, bg):
    send, recv, own, buf = bg
    xn, yn = peer_of(me, 2), peer_of(me, 4)
    half = TOK // 2
    plan = ((1, half, half, yn, 2), (0, 0, half, xn, 4), (0, 0, TOK, xn, 1), (1, 0, TOK, yn, 1))
    return Stage(
        [pltpu.make_async_copy(full.at[shard_rows(dev), :], buf.at[n], own.at[n]) for n, dev in enumerate((xn, yn))],
        [pltpu.make_async_remote_copy(
            src_ref=buf.at[slot, pl.ds(lo, count), :], dst_ref=full.at[shard_rows(dev, lo, count), :],
            send_sem=send.at[3 + k], recv_sem=recv.at[3 + k], device_id=(peer_of(me, mask),), device_id_type=MESH)
         for k, (slot, lo, count, dev, mask) in enumerate(plan)])


def stage3(me, full, bg):
    send, recv, own, buf = bg
    rows = full.at[shard_rows(peer_of(me, 6)), :]
    return Stage([pltpu.make_async_copy(rows, buf.at[1], own.at[1])], [pltpu.make_async_remote_copy(
        src_ref=buf.at[1], dst_ref=rows, send_sem=send.at[7], recv_sem=recv.at[7],
        device_id=(peer_of(me, 1),), device_id_type=MESH)])


def route(me):
    core = me % 2
    first = peer_of(me, 2) * (1 - core) + peer_of(me, 4) * core
    second = peer_of(me, 4) * (1 - core) + peer_of(me, 2) * core
    return core, peer_of(me, 1), first, second


def half_rows(c):
    return pl.ds(pl.multiple_of(c * (DIM // 2), DIM // 2), DIM // 2)


def start(copies):
    for c in copies:
        c.start()


def wait(copies):
    for c in copies:
        c.wait()


def row_sums(vals):
    folded = vals[:, :HD]
    for start in range(HD, vals.shape[1], HD):
        folded = folded + vals[:, start:start + HD]
    return jnp.sum(folded.T, axis=0, keepdims=True)


def as_column(row):
    return jnp.broadcast_to(row, (HD, row.shape[1])).T


def exchange(me, srcs, slots, send_sems, recv_sems):
    copies = []
    for n, (src, slot) in enumerate(zip(srcs, slots)):
        for p, mask in enumerate(ORDER):
            copies.append(pltpu.make_async_remote_copy(
                src_ref=src, dst_ref=slot.at[p], send_sem=send_sems.at[n, p], recv_sem=recv_sems.at[n, p],
                device_id=(peer_of(me, mask),), device_id_type=MESH))
    return copies


def ordered_total(me, src, slot):
    own = src[...]
    total = jnp.zeros_like(own)
    for dev in range(NDEV):
        term = jnp.where(me == dev, own, 0.0)
        for p, mask in enumerate(ORDER):
            term = term + jnp.where(peer_of(me, mask) == dev, slot[p], 0.0)
        total = total + term
    return total


def causal_mask():
    keys = lax.broadcasted_iota(jnp.int32, (BLK, BLK), 0)
    queries = lax.broadcasted_iota(jnp.int32, (BLK, BLK), 1)
    return keys <= queries


def block_rows(i):
    return pl.ds(pl.multiple_of(i * BLK, BLK), BLK)


def head_cols(h):
    return pl.ds(pl.multiple_of(h * HD, HD), HD)


def forward_kernel(freq_ref, wq_ref, wk_ref, wv_ref, gains_ref, x_ref, wo_ref,
                   cos_ref, sin_ref, inv_ref, o_ref, lse_ref, raw_ref, qkv_ref, both_ref, full_ref, wof_ref,
                   raw, qkv, xbuf, sums_scr, slot, p_scr, vt_scr, acc_scr, o_scr, buf0, buf1,
                   ex_send, ex_recv, out_sems, send_sems, recv_sems, own_sems, x_sems, *bg_sems):
    g = pl.program_id(0)
    b, t = g // (4 * NB), g % (4 * NB)
    me = lax.axis_index('tp')
    bg0, bg1, bg2 = (*bg_sems[:3], buf0), (*bg_sems[3:6], buf1), (*bg_sems[6:], buf0)
    x0f, x1f = full_ref.at[0], full_ref.at[1]

    def x_gather(part=None):
        return stage1(me, x_ref.at[1], x1f, bg1, part)

    def wo_gather(part=None):
        return stage1(me, wo_ref, wof_ref, bg2, part)

    def keep(bb):
        return [pltpu.make_async_copy(raw, raw_ref.at[bb], out_sems.at[0]),
                pltpu.make_async_copy(qkv, qkv_ref.at[bb], out_sems.at[1])]

    def sums(bb):
        return exchange(me, [sums_scr.at[bb]], [slot.at[bb]], ex_send.at[bb], ex_recv.at[bb])

    def fetch(bb, i):
        return pltpu.make_async_copy(full_ref.at[bb, block_rows(i), :], xbuf.at[i % 2], x_sems.at[i % 2])

    def block_copy(bb, hh, st, half):
        dest = 2 * ((me // 2 + 1 + st) % NB) + half
        part = o_scr.at[bb, hh, st, pl.ds(half * TOK, TOK), :]
        dst = both_ref.at[bb, :, pl.ds(pl.multiple_of(me * LOC + hh * HD, HD), HD)]
        away = pltpu.make_async_remote_copy(
            src_ref=part, dst_ref=dst, send_sem=send_sems.at[bb, hh, st, half], recv_sem=recv_sems.at[bb, hh, me],
            device_id=(dest,), device_id_type=MESH)
        return dest, away, pltpu.make_async_copy(part, dst, own_sems.at[bb, hh])

    def run(stage):
        stage.load()
        stage.send()

    @pl.when(g == 0)
    def _():
        first = stage1(me, x_ref.at[0], x0f, bg0)
        first.load()
        entry_barrier(me)
        first.send()
        x_gather(0).load()
        freq = freq_ref[...]
        sign = jnp.where(lax.broadcasted_iota(jnp.int32, (TOK, HD), 1) < HD // 2, -1.0, 1.0)

        def table(i, carry):
            rows = pl.ds(pl.multiple_of(i * TOK, TOK), TOK)
            pos = (lax.broadcasted_iota(jnp.int32, (TOK, HD), 0) + i * TOK).astype(F32)
            angle = pos * freq
            cos_ref[rows, :] = jnp.cos(angle)
            sin_ref[rows, :] = jnp.sin(angle) * sign
            return carry

        lax.fori_loop(0, SEQ // TOK, table, 0)
        first.wait()
        second, third = stage2(me, x0f, bg0), stage3(me, x0f, bg0)
        run(second)
        x_gather(0).send()
        second.wait()
        run(third)
        third.wait()
        fetch(0, 0).start()

    @pl.when(g == 2 * NB + 2)
    def _():
        x_gather(0).wait()
        x_gather(1).wait()
        run(stage2(me, x1f, bg1))
        run(wo_gather(0))

    @pl.when(g == 4 * NB)
    def _():
        stage2(me, x1f, bg1).wait()
        third = stage3(me, x1f, bg1)
        run(third)
        for c in keep(0):
            c.wait()
        third.wait()
        fetch(1, 0).start()

    @pl.when(g == 6 * NB + 2)
    def _():
        wo_gather(0).wait()
        wo_gather(1).wait()
        run(stage2(me, wof_ref, bg2))

    @pl.when(t < NB)
    def _():
        rows = block_rows(t)

        @pl.when(t < NB - 1)
        def _():
            fetch(b, t + 1).start()

        fetch(b, t).wait()
        x = xbuf[t % 2]
        for n, w_ref in enumerate((wq_ref, wk_ref)):
            val = dot(x, w_ref[...])
            raw[n, rows, :] = val
            sums_scr[b, pl.ds(t + n * NB, 1), :] = row_sums(val * val)
        qkv[2, rows, :] = dot(x, wv_ref[...]).astype(BF)

    @pl.when(t == NB)
    def _():
        start(sums(b))
        keep(b)[0].start()
        pl.when(b == 0)(x_gather(1).send)
        pl.when(b == 1)(wo_gather(1).send)
        wait(sums(b))
        inv_ref[...] = lax.rsqrt(ordered_total(me, sums_scr.at[b], slot.at[b]) / DIM + EPS)

    @pl.when(jnp.logical_and(t >= NB, t < 2 * NB))
    def _():
        i = t - NB
        rows = block_rows(i)
        cos, sin = cos_ref[rows, :], sin_ref[rows, :]
        for n in range(2):
            inv = as_column(inv_ref[pl.ds(i + n * NB, 1), :])
            gain = gains_ref[n:n + 1, :]
            for h in range(LOC // HD):
                sl = slice(h * HD, (h + 1) * HD)
                hat = raw[n, rows, sl] * inv * gain[:, sl]
                qkv[n, rows, sl] = (hat * cos + pltpu.roll(hat, HD // 2, 1) * sin).astype(BF)

    @pl.when(t == 2 * NB)
    def _():
        keep(b)[1].start()

    @pl.when(t >= 2 * NB)
    def _():
        h, step = t // NB - 2, t % NB
        qi = (me // 2 + 1 + step) % NB
        cols = head_cols(h)

        @pl.when(step == 0)
        def _():
            vt_scr[...] = qkv[2, :, cols].T

        qb = qkv[0, block_rows(qi), cols]

        def scores(j):
            return dot(qkv[1, block_rows(j), cols], qb, NT)

        def first(j, m):
            s = scores(j)
            p_scr[j] = s
            return jnp.maximum(m, jnp.max(s.reshape(BLK // 8, 8, BLK), axis=0))

        s = jnp.where(causal_mask(), scores(qi), -1e30)
        p_scr[qi] = s
        m = lax.fori_loop(0, qi, first, jnp.max(s.reshape(BLK // 8, 8, BLK), axis=0))
        m = jnp.max(m, axis=0, keepdims=True)

        def second(j, l):
            p = jnp.exp2((p_scr[j] - m) * C2)
            p_scr[j] = p
            return l + jnp.sum(p.reshape(BLK // 8, 8, BLK), axis=0)

        l = lax.fori_loop(0, qi + 1, second, jnp.zeros((8, BLK), F32))
        l = jnp.sum(l, axis=0, keepdims=True)
        rl = 1.0 / l
        lse_ref[pl.ds(h * NB + qi, 1), :] = m * C2 + jnp.log2(l)

        acc_scr[...] = jnp.zeros_like(acc_scr)

        def third(j, carry):
            p = (p_scr[j] * rl).astype(BF)
            acc_scr[...] += dot(vt_scr[:, block_rows(j)], p)
            return carry

        lax.fori_loop(0, qi + 1, third, 0)
        out = acc_scr[...].T.astype(BF)
        o_scr[b, h, step] = out
        o_ref[block_rows(qi), cols] = out

        for half in range(2):
            dest, away, here = block_copy(b, h, step, half)
            pl.when(dest != me)(away.start)
            pl.when(dest == me)(here.start)

    @pl.when(g == 8 * NB - 1)
    def _():
        stage2(me, wof_ref, bg2).wait()
        third = stage3(me, wof_ref, bg2)
        run(third)
        for c in keep(1):
            c.wait()

        def drain(n, carry):
            bb, hh = n // 2, n % 2
            for st in range(NB):
                for half in range(2):
                    dest, away, here = block_copy(bb, hh, st, half)
                    if st < NB - 1:
                        away.wait_send()
                    else:
                        pl.when(dest != me)(away.wait_send)
                        pl.when(dest == me)(here.wait)
            for mask in ORDER:
                peer = peer_of(me, mask)
                pltpu.make_async_remote_copy(
                    src_ref=o_scr.at[0, 0, 0, pl.ds(0, TOK), :],
                    dst_ref=both_ref.at[bb, :, pl.ds(pl.multiple_of(peer * LOC + hh * HD, HD), HD)],
                    send_sem=send_sems.at[0, 0, 0, 0], recv_sem=recv_sems.at[bb, hh, peer],
                    device_id=(peer,), device_id_type=MESH).wait_recv()
            return carry

        lax.fori_loop(0, 4, drain, 0)
        third.wait()


def forward(x, wq, wk, wv, wo, gains, cid):
    half = HD // 2
    inv_freq = 1.0 / (ROPE_THETA ** (jnp.arange(half, dtype=F32) / half))
    freq = jnp.concatenate([inv_freq, inv_freq])[None, :]

    def whole(*shape):
        return pl.BlockSpec(shape, lambda g: (0,) * len(shape))

    def per_batch(*shape):
        return pl.BlockSpec((None,) + shape, lambda g: (g // (4 * NB),) + (0,) * len(shape))

    wspec, rows = whole(DIM, LOC), per_batch(2 * NB, BLK)
    return pl.pallas_call(
        forward_kernel,
        grid=(8 * NB,),
        in_specs=[whole(1, HD), wspec, wspec, wspec, whole(2 + DIM // LOC, LOC), ANYWHERE, ANYWHERE],
        out_specs=[whole(SEQ, HD), whole(SEQ, HD), rows, per_batch(SEQ, LOC), rows] + [ANYWHERE] * 5,
        out_shape=[sds((SEQ, HD), F32), sds((SEQ, HD), F32), sds((2, 2 * NB, BLK), F32), sds((2, SEQ, LOC), BF),
                   sds((2, 2 * NB, BLK), F32), sds((2, 2, SEQ, LOC), F32), sds((2, 3, SEQ, LOC), BF),
                   sds((2, TOK, DIM), BF), sds((2, SEQ, DIM), BF), sds((SEQ, DIM), BF)],
        scratch_shapes=[pltpu.VMEM((2, SEQ, LOC), F32), pltpu.VMEM((3, SEQ, LOC), BF), pltpu.VMEM((2, BLK, DIM), BF),
                        pltpu.VMEM((2, 2 * NB, BLK), F32), pltpu.VMEM((2, NDEV - 1, 2 * NB, BLK), F32),
                        pltpu.VMEM((NB, BLK, BLK), F32), pltpu.VMEM((HD, SEQ), BF), pltpu.VMEM((HD, BLK), F32),
                        pltpu.VMEM((2, 2, NB, BLK, HD), BF), pltpu.VMEM((2, TOK, DIM), BF), pltpu.VMEM((2, TOK, DIM), BF),
                        DMA((2, 1, NDEV - 1)), DMA((2, 1, NDEV - 1)), DMA((2,)),
                        DMA((2, 2, NB, 2)), DMA((2, 2, NDEV)), DMA((2, 2)), DMA((2,))] + BG_SEMS * 3,
        compiler_params=params(dimension_semantics=("arbitrary",), collective_id=cid, has_side_effects=True),
        cost_estimate=cost(60e9, 60e6),
        name="forward",
    )(freq, wq, wk, wv, gains, x, wo)


def out_kernel(o_ref, wo_ref, x_ref, dy_ref, gains_ref, y_ref, da_ref, gga_ref, both_ref, a_scr, dh_scr, send_sems, recv_sems,
               own_sems):
    b = pl.program_id(0)
    me = lax.axis_index('tp')

    @pl.when(b == 0)
    def _():
        entry_barrier(me)
        gga_ref[...] = jnp.zeros_like(gga_ref)

    step = DIM // NB
    o = o_ref[0]

    def fwd(j, carry):
        cols = pl.ds(pl.multiple_of(j * step, step), step)
        a_scr[:, cols] = dot(o, wo_ref[:, cols])
        return carry

    lax.fori_loop(0, NB, fwd, 0)
    a = a_scr[...]
    r = lax.rsqrt(jnp.mean(a * a, axis=-1, keepdims=True) + EPS)
    n = a * r
    ga = jnp.concatenate([gains_ref[2 + i:3 + i, :] for i in range(8)], axis=1)
    dy = dy_ref[0].astype(F32)
    y_ref[0] = (x_ref[0].astype(F32) + n * ga).astype(BF)
    col = jnp.sum(dy * n, axis=0, keepdims=True)
    for i in range(8):
        gga_ref[i:i + 1, :] += col[:, i * LOC:(i + 1) * LOC]
    gn = dy * ga
    da_ref[0] = (r * (gn - n * jnp.mean(gn * n, axis=-1, keepdims=True))).astype(BF)
    da = da_ref[0]

    def block_copy(bb, st, half):
        dest = 2 * ((me // 2 + 1 + st) % NB) + half
        src = dh_scr.at[bb, st, :, pl.ds(half * LOC, LOC)]
        mine = both_ref.at[bb, shard_rows(me), :]
        away = pltpu.make_async_remote_copy(
            src_ref=src, dst_ref=mine, send_sem=send_sems.at[bb, st, half], recv_sem=recv_sems.at[bb, me],
            device_id=(dest,), device_id_type=MESH)
        return dest, away, pltpu.make_async_copy(src, mine, own_sems.at[bb])

    def bwd(st, carry):
        blk = (me // 2 + 1 + st) % NB
        dh_scr[b, st] = dot(da, wo_ref[pl.ds(pl.multiple_of(blk * step, step), step), :], NT).astype(BF)
        for half in range(2):
            dest, away, here = block_copy(b, st, half)
            pl.when(dest != me)(away.start)
            pl.when(dest == me)(here.start)
        return carry

    lax.fori_loop(0, NB, bwd, 0)

    @pl.when(b == 1)
    def _():
        for bb in range(2):
            for st in range(NB):
                for half in range(2):
                    dest, away, here = block_copy(bb, st, half)
                    if st < NB - 1:
                        away.wait_send()
                    else:
                        pl.when(dest != me)(away.wait_send)
                        pl.when(dest == me)(here.wait)
            for mask in ORDER:
                peer = peer_of(me, mask)
                pltpu.make_async_remote_copy(
                    src_ref=dh_scr.at[0, 0, :, pl.ds(0, LOC)], dst_ref=both_ref.at[bb, shard_rows(peer), :],
                    send_sem=send_sems.at[0, 0, 0], recv_sem=recv_sems.at[bb, peer], device_id=(peer,),
                    device_id_type=MESH).wait_recv()


def out_block(o, wo, x, dy, gains, cid):
    def whole(*shape):
        return pl.BlockSpec(shape, lambda i: (0,) * len(shape))

    batch = pl.BlockSpec((1, TOK, DIM), lambda i: (i, 0, 0))
    return pl.pallas_call(
        out_kernel,
        grid=(2,),
        in_specs=[batch, whole(DIM, DIM), batch, batch, whole(2 + DIM // LOC, LOC)],
        out_specs=[batch, batch, whole(8, DIM // 8), ANYWHERE],
        out_shape=[sds((2, TOK, DIM), BF), sds((2, TOK, DIM), BF), sds((8, DIM // 8), F32), sds((2, SEQ, LOC), BF)],
        scratch_shapes=[pltpu.VMEM((TOK, DIM), F32), pltpu.VMEM((2, NB, TOK, DIM // NB), BF), DMA((2, NB, 2)),
                        DMA((2, NDEV)), DMA((2,))],
        compiler_params=params(dimension_semantics=("arbitrary",), collective_id=cid, has_side_effects=True),
        cost_estimate=cost(8 * TOK * DIM * DIM + 5e9, 18e6),
        name="out_block",
    )(o, wo, x, dy, gains)


def backward_kernel(b, qkv_ref, do_ref, lse_ref, raw_ref, inv_ref, gains_ref, cos_ref, sin_ref, gga_ref, shard_ref,
                    wq_ref, wk_ref, wv_ref, *rest):
    if b:
        (d0_ref, pd0_ref, pw_ref, _, _, d_ref, pd_ref, gg_ref, gout_ref, full_ref, old_ref, first_ref,
         w_all, d_two, sbuf, *rest) = rest
    else:
        d_ref, pd_ref, gg_ref, gout_ref, full_ref, next_ref, pw_ref, *rest = rest
    (p_scr, dp_scr, kt_scr, dqt_scr, dq_scr, dk_scr, dv_scr, du_scr, d_scr, dots_scr, total, slot, ga_slot,
     ex_send, ex_recv, pd_send, pd_recv, d_sems, rs_sems, ld_sems, buf0, buf1, *bg_sems) = rest
    h, qi = pl.program_id(0), pl.program_id(1)
    me = lax.axis_index('tp')
    core, partner, first_dev, _ = route(me)
    bg0, bg1 = (*bg_sems[:3], buf0), (*bg_sems[3:], buf1)
    weights = (wq_ref, wk_ref, wv_ref)

    if b:
        gather = stage1(me, shard_ref.at[1], full_ref, bg0, 1, True)
        beside = [stage3(me, old_ref, bg1)]
        diag_rows = block_rows(peer_of(me, 6) // 2)
        operands = [pltpu.make_async_copy(d.at[diag_rows, :], d_two.at[n], ld_sems.at[n])
                    for n, d in enumerate((d0_ref, pd0_ref))]
        operands += [pltpu.make_async_copy(w.at[half_rows(core), :], w_all.at[0, :, pl.ds(n * LOC, LOC)], ld_sems.at[2 + n])
                     for n, w in enumerate(weights)]
        operands.append(pltpu.make_async_copy(pw_ref, w_all.at[1], ld_sems.at[5]))
        moved = [pltpu.make_async_remote_copy(
            src_ref=sbuf, dst_ref=first_ref, send_sem=rs_sems.at[0], recv_sem=rs_sems.at[1], device_id=(first_dev,),
            device_id_type=MESH)]
    else:
        gather = stage1(me, shard_ref.at[0], full_ref, bg0)
        beside = [stage1(me, shard_ref.at[1], next_ref, bg1, 0)]
        moved = [pltpu.make_async_remote_copy(
            src_ref=w.at[half_rows(1 - core), :], dst_ref=pw_ref.at[:, pl.ds(n * LOC, LOC)], send_sem=rs_sems.at[n],
            recv_sem=rs_sems.at[3 + n], device_id=(partner,), device_id_type=MESH) for n, w in enumerate(weights)]

    @pl.when(jnp.logical_and(h == 0, qi == 0))
    def _():
        stages = [gather] + beside
        for stage in stages:
            stage.load()
        if b:
            start(operands)
        entry_barrier(me)
        for stage in stages:
            stage.send()
        if b:
            wait(operands)
            sbuf[...] = dot(d_two[0], w_all[0], NT) + dot(d_two[1], w_all[1], NT)
        start(moved)
        dots_scr[...] = jnp.zeros_like(dots_scr)

    @pl.when(qi == 0)
    def _():
        kt_scr[...] = qkv_ref[1].T
        dk_scr[...] = jnp.zeros_like(dk_scr)
        dv_scr[...] = jnp.zeros_like(dv_scr)

    qb = qkv_ref[0, block_rows(qi), :]
    dob = do_ref[...]
    lse = lse_ref[pl.ds(h * NB + qi, 1), :]

    def first(j, acc, diag=False):
        rows = block_rows(j)
        p = jnp.exp2(dot(qkv_ref[1, rows, :], qb, NT) * C2 - lse)
        if diag:
            p = jnp.where(causal_mask(), p, 0.0)
        dp = dot(qkv_ref[2, rows, :], dob, NT)
        p_scr[j] = p
        dp_scr[j] = dp
        dv_scr[rows, :] += dot(p.astype(BF), dob)
        return acc + jnp.sum((p * dp).reshape(BLK // 8, 8, BLK), axis=0)

    acc = first(qi, jnp.zeros((8, BLK), F32), True)
    acc = lax.fori_loop(0, qi, first, acc)
    delta = jnp.sum(acc, axis=0, keepdims=True)
    dqt_scr[...] = jnp.zeros_like(dqt_scr)

    def second(j, carry):
        rows = block_rows(j)
        ds = (p_scr[j] * (dp_scr[j] - delta) * SCALE).astype(BF)
        dk_scr[rows, :] += dot(ds, qb)
        dqt_scr[...] += dot(kt_scr[:, rows], ds)
        return carry

    lax.fori_loop(0, qi + 1, second, 0)
    dq_scr[block_rows(qi), :] = dqt_scr[...].T

    @pl.when(qi == NB - 1)
    def _():
        d_scr[:, pl.ds(pl.multiple_of(2 * LOC + h * HD, HD), HD)] = dv_scr[...].astype(BF)
        gg_ref[...] = jnp.zeros_like(gg_ref)
        cols = head_cols(h)

        def tail(i, carry):
            rows = block_rows(i)
            cos, sin = cos_ref[rows, :], sin_ref[rows, :]
            for n, from_scr in enumerate((dq_scr, dk_scr)):
                d = from_scr[rows, :]
                hat = d * cos - pltpu.roll(d, HD // 2, 1) * sin
                unit = raw_ref[n, rows, cols] * as_column(inv_ref[pl.ds(i + n * NB, 1), :])
                gg_ref[n:n + 1, :] += jnp.sum(hat * unit, axis=0, keepdims=True)
                du = hat * gains_ref[n:n + 1, :]
                du_scr[n, h, rows, :] = du
                dots_scr[pl.ds(i + n * NB, 1), :] += row_sums(du * unit)
            return carry

        lax.fori_loop(0, NB, tail, 0)

    @pl.when(jnp.logical_and(h == 1, qi == NB - 1))
    def _():
        gather.wait()
        for stage in beside:
            stage.wait()
        sums = exchange(me, [dots_scr, gga_ref], [slot, ga_slot], ex_send, ex_recv)
        start(sums)
        more = stage2(me, full_ref, bg0)
        more.load()
        more.send()
        wait(sums)
        total[...] = ordered_total(me, dots_scr, slot) / DIM
        gout_ref[...] = ordered_total(me, gga_ref, ga_slot)

        def copies(i):
            rows = block_rows(i)
            return [pltpu.make_async_copy(d_scr.at[rows, :], d_ref.at[rows, :], d_sems.at[i]),
                    pltpu.make_async_remote_copy(
                        src_ref=d_scr.at[rows, :], dst_ref=pd_ref.at[rows, :], send_sem=pd_send.at[i],
                        recv_sem=pd_recv.at[i], device_id=(peer_of(me, 1),), device_id_type=MESH)]

        def last(i, carry):
            rows = block_rows(i)
            for n in range(2):
                dots = as_column(total[pl.ds(i + n * NB, 1), :])
                inv = as_column(inv_ref[pl.ds(i + n * NB, 1), :])
                for hh in range(LOC // HD):
                    sl = slice(hh * HD, (hh + 1) * HD)
                    unit = raw_ref[n, rows, sl] * inv
                    val = inv * (du_scr[n, hh, rows, :] - unit * dots)
                    d_scr[rows, n * LOC + hh * HD:n * LOC + (hh + 1) * HD] = val.astype(BF)
            start(copies(i))
            return carry

        lax.fori_loop(0, NB, last, 0)
        for i in range(NB):
            wait(copies(i))
        wait(moved)
        more.wait()


def backward(b, qkv, do, lse, raw, inv, gains, cos, sin, gga, shard, weights, older, cid):
    def whole(*shape):
        return pl.BlockSpec(shape, lambda h, i: (0,) * len(shape))

    def picked(*shape):
        return pl.BlockSpec((None,) + shape, lambda h, i: (b,) + (0,) * len(shape))

    gsp = whole(8, DIM // 8)
    half = (DIM // 2, 3 * LOC)
    extra = [sds((BLK, DIM // 2), F32)] if b else [sds(half, BF)]
    early = [pltpu.VMEM((2,) + half, BF), pltpu.VMEM((2, BLK, 3 * LOC), BF), pltpu.VMEM((BLK, DIM // 2), F32)] if b else []
    return pl.pallas_call(
        functools.partial(backward_kernel, b),
        grid=(2, NB),
        in_specs=[pl.BlockSpec((None, 3, SEQ, HD), lambda h, i: (b, 0, 0, h)), pl.BlockSpec((None, BLK, HD), lambda h, i: (b, i, h)),
                  picked(2 * NB, BLK), picked(2, SEQ, LOC), picked(2 * NB, BLK),
                  pl.BlockSpec((2 + DIM // LOC, HD), lambda h, i: (0, h)), whole(SEQ, HD), whole(SEQ, HD), gsp]
        + [ANYWHERE] * (4 + len(older)),
        out_specs=[ANYWHERE, ANYWHERE, pl.BlockSpec((8, HD), lambda h, i: (0, h)), gsp] + [ANYWHERE] * 3,
        out_shape=[sds((SEQ, 3 * LOC), BF), sds((SEQ, 3 * LOC), BF), sds((8, LOC), F32), sds((8, DIM // 8), F32),
                   sds((SEQ, DIM), BF), sds((SEQ, DIM), BF)] + extra,
        input_output_aliases={16: 4, 17: 5} if b else {},
        scratch_shapes=early + [
            pltpu.VMEM((NB, BLK, BLK), F32), pltpu.VMEM((NB, BLK, BLK), F32), pltpu.VMEM((HD, SEQ), BF),
            pltpu.VMEM((HD, BLK), F32), pltpu.VMEM((SEQ, HD), F32), pltpu.VMEM((SEQ, HD), F32),
            pltpu.VMEM((SEQ, HD), F32), pltpu.VMEM((2, 2, SEQ, HD), F32), pltpu.VMEM((SEQ, 3 * LOC), BF),
            pltpu.VMEM((2 * NB, BLK), F32), pltpu.VMEM((2 * NB, BLK), F32),
            pltpu.VMEM((NDEV - 1, 2 * NB, BLK), F32), pltpu.VMEM((NDEV - 1, 8, DIM // 8), F32),
            DMA((2, NDEV - 1)), DMA((2, NDEV - 1)), DMA((NB,)), DMA((NB,)), DMA((NB,)), DMA((6,)), DMA((6,)),
            pltpu.VMEM((2, TOK, DIM), BF), pltpu.VMEM((2, TOK, DIM), BF)] + BG_SEMS * 2,
        compiler_params=params(dimension_semantics=("arbitrary", "arbitrary"), collective_id=cid, has_side_effects=True),
        cost_estimate=cost(20e9, 20e6),
        name="backward",
    )(qkv, do, lse, raw, inv, gains, cos, sin, gga, shard, *weights, *older)


HALF = DIM // 2
CH = 256


def grads_kernel(d0, d1, pd0, pd1, wq, wk, wv, pw, got, x_full, o_all, da0, da1_in, dy_ref, dx_ref, gwq_ref, gwk_ref, gwv_ref, gwo_ref, da1,
                 d_all, w_all, sbuf, r1, r2, fin, acc, xbuf, obuf,
                 dl_sems, w_sems, s1_sems, r1_sems, s2_sems, r2_sems, fs_sems, fr_sems, x_sems, o_sems, *sems):
    del da1_in
    me = lax.axis_index('tp')
    core, partner, first, second = route(me)
    chip = me // 2
    diag_chip, first_chip, second_chip = peer_of(me, 6) // 2, first // 2, second // 2

    barrier = pltpu.get_barrier_semaphore()
    for dev in (partner, first, second):
        pl.semaphore_signal(barrier, inc=1, device_id=(dev,), device_id_type=MESH)
    pl.semaphore_wait(barrier, 3)

    def rows_of(blk):
        return pl.ds(pl.multiple_of(blk * BLK, BLK), BLK)

    chips = (diag_chip, first_chip, second_chip, chip)
    w_copies = [pltpu.make_async_copy(w.at[half_rows(core), :], w_all.at[0, :, pl.ds(n * LOC, LOC)], w_sems.at[n])
                for n, w in enumerate((wq, wk, wv))]
    w_copies.append(pltpu.make_async_copy(pw, w_all.at[1], w_sems.at[3]))
    loads = []
    for n in range(8):
        rows, b = rows_of(chips[n // 2]), n % 2
        loads.append([pltpu.make_async_copy(d.at[rows, :], d_all.at[side, b, rows, :], dl_sems.at[side, n])
                      for side, d in enumerate(((d0, d1)[b], (pd0, pd1)[b]))])
    start(w_copies)
    start(loads[1])
    wait(w_copies)

    def partial(b, blk):
        rows = rows_of(blk)
        return dot(d_all[0, b, rows, :], w_all[0], NT) + dot(d_all[1, b, rows, :], w_all[1], NT)

    def to_first(n):
        return pltpu.make_async_remote_copy(
            src_ref=sbuf.at[n - 1], dst_ref=r1.at[n], send_sem=s1_sems.at[n], recv_sem=r1_sems.at[n],
            device_id=(first,), device_id_type=MESH)

    def to_second(b):
        return pltpu.make_async_remote_copy(
            src_ref=r1.at[b], dst_ref=r2.at[b], send_sem=s2_sems.at[b], recv_sem=r2_sems.at[b],
            device_id=(second,), device_id_type=MESH)

    def to_partner(b):
        return pltpu.make_async_remote_copy(
            src_ref=r1.at[2 + b, pl.ds(pl.multiple_of((1 - core) * TOK, TOK), TOK), :], dst_ref=fin.at[b],
            send_sem=fs_sems.at[b], recv_sem=fr_sems.at[b], device_id=(partner,), device_id_type=MESH)

    taken = pltpu.make_async_copy(got, r1.at[0], w_sems.at[4])
    last_stage = stage3(me, da1, (*sems, xbuf))
    for n in range(1, 4):
        wait(loads[n])
        if n == 1:
            start(loads[2] + loads[3])
        sbuf[n - 1] = partial(n % 2, chips[n // 2])
        to_first(n).start()
        if n == 1:
            start([taken] + loads[0] + loads[4] + loads[5] + loads[6] + loads[7])
            last_stage.load()
            last_stage.send()
    for n in (0, 4, 5, 6, 7):
        wait(loads[n])
    taken.wait()

    steps = SEQ // CH

    def chunk(i):
        return pl.ds(pl.multiple_of(i * CH, CH), CH)

    def stream(pairs, body):
        def fetch(i):
            return [pltpu.make_async_copy(src.at[chunk(i), :], buf.at[i % 2], sems.at[i % 2]) for src, buf, sems in pairs]

        for c in fetch(0):
            c.start()

        def it(i, carry):
            @pl.when(i + 1 < steps)
            def _():
                for c in fetch(i + 1):
                    c.start()

            for c in fetch(i):
                c.wait()
            body(i)
            return carry

        lax.fori_loop(0, steps, it, 0)

    def wgrad(b, src):
        def body(i):
            left = d_all[0, b, chunk(i), :].T
            for c in range(3):
                part = slice(c * LOC, (c + 1) * LOC)
                acc[part, :] += dot(left[part, :], xbuf[i % 2])

        stream([(src, xbuf, x_sems)], body)

    def forward_second(b):
        if b:
            to_first(b).wait_recv()
        r1[b] += partial(b, second_chip)
        to_second(b).start()

    forward_second(0)
    acc[...] = jnp.zeros_like(acc)
    last_stage.wait()
    wgrad(0, x_full.at[0])
    wgrad(1, x_full.at[1])
    for n, ref in enumerate((gwq_ref, gwk_ref, gwv_ref)):
        ref[...] = acc[n * LOC:(n + 1) * LOC, :].T.astype(BF)
    forward_second(1)
    acc[:LOC, :] = jnp.zeros((LOC, DIM), F32)

    def wo_body(i):
        acc[:LOC, :] += dot(obuf[i % 2].T, xbuf[i % 2])

    for o_src, da_src in ((o_all.at[0], da0), (o_all.at[1], da1)):
        stream([(da_src, xbuf, x_sems), (o_src, obuf, o_sems)], wo_body)
    gwo_ref[...] = acc[:LOC, :].astype(BF)

    def own_part(b, carry):
        r1_own = partial(b, chip)
        to_first(2 + b).wait_recv()
        to_second(b).wait_recv()
        r1[2 + b] += r1_own + r2[b]
        to_partner(b).start()
        cols = half_rows(core)
        rows = pl.ds(pl.multiple_of(core * TOK, TOK), TOK)
        dx_ref[b, :, cols] = (r1[2 + b, rows, :] + dy_ref[b, :, cols].astype(F32)).astype(BF)
        return carry

    lax.fori_loop(0, 2, own_part, 0)

    def finish(b, carry):
        to_partner(b).wait()
        cols = half_rows(1 - core)
        dx_ref[b, :, cols] = (fin[b] + dy_ref[b, :, cols].astype(F32)).astype(BF)
        to_second(b).wait_send()
        to_first(2 + b).wait_send()
        return carry

    to_first(1).wait_send()
    lax.fori_loop(0, 2, finish, 0)


def grads(d0, d1, pd0, pd1, wq, wk, wv, pw, got, x_full, o_all, da0, da1, dy, cid):
    vm = pl.BlockSpec(memory_space=pltpu.VMEM)
    far = pl.BlockSpec(memory_space=pl.ANY)
    dma = pltpu.SemaphoreType.DMA
    return pl.pallas_call(
        grads_kernel,
        in_specs=[far] * 13 + [vm],
        out_specs=[vm] * 5 + [far],
        out_shape=[sds((2, TOK, DIM), BF)] + [sds((DIM, LOC), BF)] * 3 + [sds((LOC, DIM), BF), sds((SEQ, DIM), BF)],
        input_output_aliases={12: 5},
        scratch_shapes=[pltpu.VMEM((2, 2, SEQ, 3 * LOC), BF), pltpu.VMEM((2, HALF, 3 * LOC), BF),
                        pltpu.VMEM((3, BLK, HALF), F32), pltpu.VMEM((4, BLK, HALF), F32), pltpu.VMEM((2, BLK, HALF), F32),
                        pltpu.VMEM((2, TOK, HALF), F32), pltpu.VMEM((3 * LOC, DIM), F32),
                        pltpu.VMEM((2, CH, DIM), BF), pltpu.VMEM((2, CH, LOC), BF),
                        dma((2, 8)), dma((9,)), dma((4,)), dma((4,)), dma((2,)), dma((2,)),
                        dma((2,)), dma((2,)), dma((2,)), dma((2,))] + BG_SEMS,
        compiler_params=pltpu.CompilerParams(vmem_limit_bytes=67043328, collective_id=cid, has_side_effects=True),
        cost_estimate=cost(100e9, 40e6),
        name="grads",
    )(d0, d1, pd0, pd1, wq, wk, wv, pw, got, x_full, o_all, da0, da1, dy)


def local_block(x_loc, wq, wk, wv, wo, gq, gk, ga, dy_loc):
    gains = jnp.concatenate([gq, gk, ga]).astype(F32).reshape(2 + DIM // LOC, LOC)
    cos, sin, inv, o, lse, raw, qkv, o_recv, x_full, wo_full = forward(x_loc, wq, wk, wv, wo, gains, 0)
    y, da, gga, dh = out_block(o_recv, wo_full, x_loc, dy_loc, gains, 1)
    weights = (wq, wk, wv)
    state = (qkv, dh, lse, raw, inv, gains, cos, sin, gga, da, weights)
    d0, pd0, gg0, gout, da0, da1, pw = backward(0, *state, (), 2)
    d1, pd1, gg1, _, da1, da0, got = backward(1, *state, (d0, pd0, pw, da1, da0), 3)
    grad_ga = gout.reshape(DIM).astype(BF)
    dx, gwq, gwk, gwv, gwo, _ = grads(d0, d1, pd0, pd1, *weights, pw, got, x_full, o, da0, da1, dy_loc, 4)
    gg = gg0 + gg1
    return (y, dx, gwq, gwk, gwv, gwo, gg[0].astype(BF), gg[1].astype(BF), grad_ga)


def solution(mesh):
    act, col, row, vec = P(None, 'tp', None), P(None, 'tp'), P('tp', None), P('tp')
    in_specs = (act, col, col, col, row, vec, vec, P(), act)
    out_specs = (act, act, col, col, col, row, vec, vec, P())
    return jax.shard_map(local_block, mesh=mesh, in_specs=in_specs, out_specs=out_specs, check_vma=False)
```

```python
import functools
import math

import jax
import jax.numpy as jnp
import numpy as np
from jax import lax
from jax.experimental import pallas as pl
from jax.experimental.pallas import tpu as pltpu
from jax.sharding import PartitionSpec as P

HD = 128
ROPE_THETA = 500000.0
EPS = 1e-6
DIM = 2048
SEQ = 2048
LOC = 256
TOK = 256
BLK = 512
NB = SEQ // BLK
NDEV = 8
SCALE = HD ** -0.5
C2 = SCALE * math.log2(math.e)
MESH = pl.DeviceIdType.MESH
BF = jnp.bfloat16
F32 = jnp.float32
VMEM_MAX = 60 * 1024 * 1024

NT = (((1,), (1,)), ((), ()))
NN = (((1,), (0,)), ((), ()))


def dot(a, b, dims=NN):
    return lax.dot_general(a, b, dims, preferred_element_type=F32)


def sds(shape, dtype):
    return jax.ShapeDtypeStruct(shape, dtype)


def cost(flops, nbytes, trans=0):
    return pl.CostEstimate(flops=int(flops), bytes_accessed=int(nbytes), transcendentals=int(trans))


def params(**kw):
    return pltpu.CompilerParams(vmem_limit_bytes=VMEM_MAX, **kw)


def peer_of(me, mask):
    core, ax, ay = me % 2, (me // 2) % 2, me // 4
    core = 1 - core if mask & 1 else core
    ax = 1 - ax if mask & 2 else ax
    ay = 1 - ay if mask & 4 else ay
    return ay * 4 + ax * 2 + core


ORDER = (6, 7, 2, 4, 3, 5, 1)


def entry_barrier(me):
    barrier = pltpu.get_barrier_semaphore()
    for mask in ORDER:
        pl.semaphore_signal(barrier, inc=1, device_id=(peer_of(me, mask),), device_id_type=MESH)
    pl.semaphore_wait(barrier, NDEV - 1)


def nbr_signal(me):
    for mask in (1, 2, 4):
        pl.semaphore_signal(pltpu.get_barrier_semaphore(), inc=1, device_id=(peer_of(me, mask),), device_id_type=MESH)


def nbr_wait():
    pl.semaphore_wait(pltpu.get_barrier_semaphore(), 3)


DMA = pltpu.SemaphoreType.DMA
ANYWHERE = pl.BlockSpec(memory_space=pl.ANY)
BG_SEMS = [DMA((11,)), DMA((11,)), DMA((5,))]
BG = BG_SEMS + [pltpu.VMEM((2, TOK, DIM), BF)]


def shard_rows(dev, lo=0, count=TOK):
    return pl.ds(pl.multiple_of(dev * TOK + lo, HD), count)


class Stage:
    def __init__(self, loads, copies):
        self.loads, self.copies = loads, copies

    def load(self):
        start(self.loads)

    def send(self):
        wait(self.loads)
        start(self.copies)

    def wait(self):
        wait(self.copies)


def stage1(me, src, full, bg, part=None):
    send, recv, own, buf = bg
    lo, count, at = (0, TOK, 0) if part is None else (part * (TOK // 2), TOK // 2, 8 * part)
    there = full.at[shard_rows(me, lo, count), :]
    mine = buf.at[0, pl.ds(lo, count), :]
    copies = [pltpu.make_async_remote_copy(
        src_ref=mine, dst_ref=there, send_sem=send.at[at + k], recv_sem=recv.at[at + k],
        device_id=(peer_of(me, mask),), device_id_type=MESH) for k, mask in enumerate((2, 4, 1))]
    loads = [] if part == 1 or src is None else [pltpu.make_async_copy(src, buf.at[0], own.at[0])]
    return Stage(loads, copies + [pltpu.make_async_copy(mine, there, own.at[3 if part == 1 else 2])])


def stage2(me, full, bg):
    send, recv, own, buf = bg
    xn, yn = peer_of(me, 2), peer_of(me, 4)
    half = TOK // 2
    plan = ((1, half, half, yn, 2), (0, 0, half, xn, 4), (0, 0, TOK, xn, 1), (1, 0, TOK, yn, 1))
    return Stage(
        [pltpu.make_async_copy(full.at[shard_rows(dev), :], buf.at[n], own.at[n]) for n, dev in enumerate((xn, yn))],
        [pltpu.make_async_remote_copy(
            src_ref=buf.at[slot, pl.ds(lo, count), :], dst_ref=full.at[shard_rows(dev, lo, count), :],
            send_sem=send.at[3 + k], recv_sem=recv.at[3 + k], device_id=(peer_of(me, mask),), device_id_type=MESH)
         for k, (slot, lo, count, dev, mask) in enumerate(plan)])


def stage3(me, full, bg):
    send, recv, own, buf = bg
    rows = full.at[shard_rows(peer_of(me, 6)), :]
    return Stage([pltpu.make_async_copy(rows, buf.at[1], own.at[1])], [pltpu.make_async_remote_copy(
        src_ref=buf.at[1], dst_ref=rows, send_sem=send.at[7], recv_sem=recv.at[7],
        device_id=(peer_of(me, 1),), device_id_type=MESH)])


def route(me):
    core = me % 2
    first = peer_of(me, 2) * (1 - core) + peer_of(me, 4) * core
    second = peer_of(me, 4) * (1 - core) + peer_of(me, 2) * core
    return core, peer_of(me, 1), first, second


def half_rows(c):
    return pl.ds(pl.multiple_of(c * (DIM // 2), DIM // 2), DIM // 2)


def start(copies):
    for c in copies:
        c.start()


def wait(copies):
    for c in copies:
        c.wait()


def row_sums(vals):
    folded = vals[:, :HD]
    for start in range(HD, vals.shape[1], HD):
        folded = folded + vals[:, start:start + HD]
    return jnp.sum(folded.T, axis=0, keepdims=True)


def as_column(row):
    return jnp.broadcast_to(row, (HD, row.shape[1])).T


def exchange(me, srcs, slots, send_sems, recv_sems):
    copies = []
    for n, (src, slot) in enumerate(zip(srcs, slots)):
        for p, mask in enumerate(ORDER):
            copies.append(pltpu.make_async_remote_copy(
                src_ref=src, dst_ref=slot.at[p], send_sem=send_sems.at[n, p], recv_sem=recv_sems.at[n, p],
                device_id=(peer_of(me, mask),), device_id_type=MESH))
    return copies


def ordered_total(me, src, slot):
    own = src[...]
    total = jnp.zeros_like(own)
    for dev in range(NDEV):
        term = jnp.where(me == dev, own, 0.0)
        for p, mask in enumerate(ORDER):
            term = term + jnp.where(peer_of(me, mask) == dev, slot[p], 0.0)
        total = total + term
    return total


def causal_mask():
    keys = lax.broadcasted_iota(jnp.int32, (BLK, BLK), 0)
    queries = lax.broadcasted_iota(jnp.int32, (BLK, BLK), 1)
    return keys <= queries


def block_rows(i):
    return pl.ds(pl.multiple_of(i * BLK, BLK), BLK)


def head_cols(h):
    return pl.ds(pl.multiple_of(h * HD, HD), HD)


def forward_kernel(freq_ref, wq_ref, wk_ref, wv_ref, gains_ref, x_ref, wo_ref,
                   cos_ref, sin_ref, inv_ref, o_ref, lse_ref, raw_ref, qkv_ref, both_ref, full_ref, wof_ref,
                   raw, qkv, xbuf, sums_scr, slot, p_scr, vt_scr, acc_scr, o_scr, buf0, buf1,
                   ex_send, ex_recv, out_sems, send_sems, recv_sems, own_sems, x_sems, *bg_sems):
    g = pl.program_id(0)
    b, t = g // (4 * NB), g % (4 * NB)
    me = lax.axis_index('tp')
    bg0, bg1, bg2 = (*bg_sems[:3], buf0), (*bg_sems[3:6], buf1), (*bg_sems[6:], buf0)
    x0f, x1f = full_ref.at[0], full_ref.at[1]

    def x_gather(part=None):
        return stage1(me, x_ref.at[1], x1f, bg1, part)

    def wo_gather(part=None):
        return stage1(me, wo_ref, wof_ref, bg2, part)

    def keep(bb):
        return [pltpu.make_async_copy(raw, raw_ref.at[bb], out_sems.at[0]),
                pltpu.make_async_copy(qkv, qkv_ref.at[bb], out_sems.at[1])]

    def sums(bb):
        return exchange(me, [sums_scr.at[bb]], [slot.at[bb]], ex_send.at[bb], ex_recv.at[bb])

    def fetch(bb, i):
        return pltpu.make_async_copy(full_ref.at[bb, block_rows(i), :], xbuf.at[i % 2], x_sems.at[i % 2])

    def block_copy(bb, hh, st, half):
        dest = 2 * ((me // 2 + 1 + st) % NB) + half
        part = o_scr.at[bb, hh, st, pl.ds(half * TOK, TOK), :]
        dst = both_ref.at[bb, :, pl.ds(pl.multiple_of(me * LOC + hh * HD, HD), HD)]
        away = pltpu.make_async_remote_copy(
            src_ref=part, dst_ref=dst, send_sem=send_sems.at[bb, hh, st, half], recv_sem=recv_sems.at[bb, hh, me],
            device_id=(dest,), device_id_type=MESH)
        return dest, away, pltpu.make_async_copy(part, dst, own_sems.at[bb, hh])

    def run(stage):
        stage.load()
        stage.send()

    @pl.when(g == 0)
    def _():
        first = stage1(me, x_ref.at[0], x0f, bg0)
        first.load()
        entry_barrier(me)
        first.send()
        x_gather(0).load()
        freq = freq_ref[...]
        sign = jnp.where(lax.broadcasted_iota(jnp.int32, (TOK, HD), 1) < HD // 2, -1.0, 1.0)

        def table(i, carry):
            rows = pl.ds(pl.multiple_of(i * TOK, TOK), TOK)
            pos = (lax.broadcasted_iota(jnp.int32, (TOK, HD), 0) + i * TOK).astype(F32)
            angle = pos * freq
            cos_ref[rows, :] = jnp.cos(angle)
            sin_ref[rows, :] = jnp.sin(angle) * sign
            return carry

        lax.fori_loop(0, SEQ // TOK, table, 0)
        first.wait()
        second, third = stage2(me, x0f, bg0), stage3(me, x0f, bg0)
        run(second)
        x_gather(0).send()
        second.wait()
        run(third)
        third.wait()
        fetch(0, 0).start()

    @pl.when(g == 2 * NB + 2)
    def _():
        x_gather(0).wait()
        x_gather(1).wait()
        run(stage2(me, x1f, bg1))
        run(wo_gather(0))

    @pl.when(g == 4 * NB)
    def _():
        stage2(me, x1f, bg1).wait()
        third = stage3(me, x1f, bg1)
        run(third)
        for c in keep(0):
            c.wait()
        third.wait()
        fetch(1, 0).start()

    @pl.when(g == 6 * NB + 2)
    def _():
        wo_gather(0).wait()
        wo_gather(1).wait()
        run(stage2(me, wof_ref, bg2))

    @pl.when(t < NB)
    def _():
        rows = block_rows(t)

        @pl.when(t < NB - 1)
        def _():
            fetch(b, t + 1).start()

        fetch(b, t).wait()
        x = xbuf[t % 2]
        for n, w_ref in enumerate((wq_ref, wk_ref)):
            val = dot(x, w_ref[...])
            raw[n, rows, :] = val
            sums_scr[b, pl.ds(t + n * NB, 1), :] = row_sums(val * val)
        qkv[2, rows, :] = dot(x, wv_ref[...]).astype(BF)

    @pl.when(t == NB)
    def _():
        start(sums(b))
        keep(b)[0].start()
        pl.when(b == 0)(x_gather(1).send)
        pl.when(b == 1)(wo_gather(1).send)
        wait(sums(b))
        inv_ref[...] = lax.rsqrt(ordered_total(me, sums_scr.at[b], slot.at[b]) / DIM + EPS)

    @pl.when(jnp.logical_and(t >= NB, t < 2 * NB))
    def _():
        i = t - NB
        rows = block_rows(i)
        cos, sin = cos_ref[rows, :], sin_ref[rows, :]
        for n in range(2):
            inv = as_column(inv_ref[pl.ds(i + n * NB, 1), :])
            gain = gains_ref[n:n + 1, :]
            for h in range(LOC // HD):
                sl = slice(h * HD, (h + 1) * HD)
                hat = raw[n, rows, sl] * inv * gain[:, sl]
                qkv[n, rows, sl] = (hat * cos + pltpu.roll(hat, HD // 2, 1) * sin).astype(BF)

    @pl.when(t == 2 * NB)
    def _():
        keep(b)[1].start()

    @pl.when(t >= 2 * NB)
    def _():
        h, step = t // NB - 2, t % NB
        qi = (me // 2 + 1 + step) % NB
        cols = head_cols(h)

        @pl.when(step == 0)
        def _():
            vt_scr[...] = qkv[2, :, cols].T

        qb = qkv[0, block_rows(qi), cols]

        def scores(j):
            return dot(qkv[1, block_rows(j), cols], qb, NT)

        def first(j, m):
            s = scores(j)
            p_scr[j] = s
            return jnp.maximum(m, jnp.max(s.reshape(BLK // 8, 8, BLK), axis=0))

        s = jnp.where(causal_mask(), scores(qi), -1e30)
        p_scr[qi] = s
        m = lax.fori_loop(0, qi, first, jnp.max(s.reshape(BLK // 8, 8, BLK), axis=0))
        m = jnp.max(m, axis=0, keepdims=True)

        def second(j, l):
            p = jnp.exp2((p_scr[j] - m) * C2)
            p_scr[j] = p
            return l + jnp.sum(p.reshape(BLK // 8, 8, BLK), axis=0)

        l = lax.fori_loop(0, qi + 1, second, jnp.zeros((8, BLK), F32))
        l = jnp.sum(l, axis=0, keepdims=True)
        rl = 1.0 / l
        lse_ref[pl.ds(h * NB + qi, 1), :] = m * C2 + jnp.log2(l)

        acc_scr[...] = jnp.zeros_like(acc_scr)

        def third(j, carry):
            p = (p_scr[j] * rl).astype(BF)
            acc_scr[...] += dot(vt_scr[:, block_rows(j)], p)
            return carry

        lax.fori_loop(0, qi + 1, third, 0)
        out = acc_scr[...].T.astype(BF)
        o_scr[b, h, step] = out
        o_ref[block_rows(qi), cols] = out

        for half in range(2):
            dest, away, here = block_copy(b, h, step, half)
            pl.when(dest != me)(away.start)
            pl.when(dest == me)(here.start)

    @pl.when(g == 8 * NB - 1)
    def _():
        stage2(me, wof_ref, bg2).wait()
        third = stage3(me, wof_ref, bg2)
        run(third)
        for c in keep(1):
            c.wait()

        def drain(n, carry):
            bb, hh = n // 2, n % 2
            for st in range(NB):
                for half in range(2):
                    dest, away, here = block_copy(bb, hh, st, half)
                    if st < NB - 1:
                        away.wait_send()
                    else:
                        pl.when(dest != me)(away.wait_send)
                        pl.when(dest == me)(here.wait)
            for mask in ORDER:
                peer = peer_of(me, mask)
                pltpu.make_async_remote_copy(
                    src_ref=o_scr.at[0, 0, 0, pl.ds(0, TOK), :],
                    dst_ref=both_ref.at[bb, :, pl.ds(pl.multiple_of(peer * LOC + hh * HD, HD), HD)],
                    send_sem=send_sems.at[0, 0, 0, 0], recv_sem=recv_sems.at[bb, hh, peer],
                    device_id=(peer,), device_id_type=MESH).wait_recv()
            return carry

        lax.fori_loop(0, 4, drain, 0)
        third.wait()


def forward(x, wq, wk, wv, wo, gains, cid):
    inv_freq = np.float32(1.0) / np.float32(ROPE_THETA) ** (np.arange(HD // 2, dtype=np.float32) / np.float32(HD // 2))
    freq = jnp.asarray(np.concatenate([inv_freq, inv_freq])[None, :], F32)

    def whole(*shape):
        return pl.BlockSpec(shape, lambda g: (0,) * len(shape))

    def per_batch(*shape):
        return pl.BlockSpec((None,) + shape, lambda g: (g // (4 * NB),) + (0,) * len(shape))

    wspec, rows = whole(DIM, LOC), per_batch(2 * NB, BLK)
    return pl.pallas_call(
        forward_kernel,
        grid=(8 * NB,),
        in_specs=[whole(1, HD), wspec, wspec, wspec, whole(2 + DIM // LOC, LOC), ANYWHERE, ANYWHERE],
        out_specs=[whole(SEQ, HD), whole(SEQ, HD), rows, per_batch(SEQ, LOC), rows] + [ANYWHERE] * 5,
        out_shape=[sds((SEQ, HD), F32), sds((SEQ, HD), F32), sds((2, 2 * NB, BLK), F32), sds((2, SEQ, LOC), BF),
                   sds((2, 2 * NB, BLK), F32), sds((2, 2, SEQ, LOC), F32), sds((2, 3, SEQ, LOC), BF),
                   sds((2, TOK, DIM), BF), sds((2, SEQ, DIM), BF), sds((SEQ, DIM), BF)],
        scratch_shapes=[pltpu.VMEM((2, SEQ, LOC), F32), pltpu.VMEM((3, SEQ, LOC), BF), pltpu.VMEM((2, BLK, DIM), BF),
                        pltpu.VMEM((2, 2 * NB, BLK), F32), pltpu.VMEM((2, NDEV - 1, 2 * NB, BLK), F32),
                        pltpu.VMEM((NB, BLK, BLK), F32), pltpu.VMEM((HD, SEQ), BF), pltpu.VMEM((HD, BLK), F32),
                        pltpu.VMEM((2, 2, NB, BLK, HD), BF), pltpu.VMEM((2, TOK, DIM), BF), pltpu.VMEM((2, TOK, DIM), BF),
                        DMA((2, 1, NDEV - 1)), DMA((2, 1, NDEV - 1)), DMA((2,)),
                        DMA((2, 2, NB, 2)), DMA((2, 2, NDEV)), DMA((2, 2)), DMA((2,))] + BG_SEMS * 3,
        compiler_params=params(dimension_semantics=("arbitrary",), collective_id=cid, has_side_effects=True),
        cost_estimate=cost(60e9, 60e6),
        name="forward",
    )(freq, wq, wk, wv, gains, x, wo)


def out_kernel(o_ref, x_ref, dy_ref, gains_ref, wo_ref, y_ref, da_ref, gga_ref, full_ref, wo_scr, a_scr, wo_sems, buf, *bg_sems):
    b = pl.program_id(0)
    me = lax.axis_index('tp')
    bg = (*bg_sems, buf)
    step = DIM // NB

    def piece(j):
        cols = pl.ds(pl.multiple_of(j * step, step), step)
        return cols, pltpu.make_async_copy(wo_ref.at[:, cols], wo_scr.at[:, cols], wo_sems.at[j])

    @pl.when(b == 0)
    def _():
        nbr_signal(me)
        for j in range(NB):
            piece(j)[1].start()
        gga_ref[...] = jnp.zeros_like(gga_ref)

    o = o_ref[0]

    def fwd(j, carry):
        cols, load = piece(j)
        pl.when(b == 0)(load.wait)
        a_scr[:, cols] = dot(o, wo_scr[:, cols])
        return carry

    lax.fori_loop(0, NB, fwd, 0)
    a = a_scr[...]
    r = lax.rsqrt(jnp.mean(a * a, axis=-1, keepdims=True) + EPS)
    n = a * r
    ga = jnp.concatenate([gains_ref[2 + i:3 + i, :] for i in range(8)], axis=1)
    dy = dy_ref[0].astype(F32)
    gn = dy * ga
    da = (r * (gn - n * jnp.mean(gn * n, axis=-1, keepdims=True))).astype(BF)
    da_ref[0] = da

    @pl.when(b == 0)
    def _():
        buf[0] = da
        nbr_wait()
        stage1(me, None, full_ref, bg).send()

    y_ref[0] = (x_ref[0].astype(F32) + n * ga).astype(BF)
    col = jnp.sum(dy * n, axis=0, keepdims=True)
    for i in range(8):
        gga_ref[i:i + 1, :] += col[:, i * LOC:(i + 1) * LOC]

    @pl.when(b == 1)
    def _():
        stage1(me, None, full_ref, bg).wait()
        for stage in (stage2(me, full_ref, bg), stage3(me, full_ref, bg)):
            stage.load()
            stage.send()
            stage.wait()


def out_block(o, wo, x, dy, gains, cid):
    def whole(*shape):
        return pl.BlockSpec(shape, lambda i: (0,) * len(shape))

    batch = pl.BlockSpec((1, TOK, DIM), lambda i: (i, 0, 0))
    return pl.pallas_call(
        out_kernel,
        grid=(2,),
        in_specs=[batch, batch, batch, whole(2 + DIM // LOC, LOC), ANYWHERE],
        out_specs=[batch, batch, whole(8, DIM // 8), ANYWHERE],
        out_shape=[sds((2, TOK, DIM), BF), sds((2, TOK, DIM), BF), sds((8, DIM // 8), F32), sds((SEQ, DIM), BF)],
        scratch_shapes=[pltpu.VMEM((DIM, DIM), BF), pltpu.VMEM((TOK, DIM), F32), DMA((NB,)),
                        pltpu.VMEM((2, TOK, DIM), BF)] + BG_SEMS,
        compiler_params=params(dimension_semantics=("arbitrary",), collective_id=cid, has_side_effects=True),
        cost_estimate=cost(8 * TOK * DIM * DIM + 5e9, 18e6),
        name="out_block",
    )(o, x, dy, gains, wo)


def backward_kernel(b, qkv_ref, da_ref, wo_ref, lse_ref, raw_ref, inv_ref, gains_ref, cos_ref, sin_ref, gga_ref,
                    wq_ref, wk_ref, wv_ref, *rest):
    if b:
        d0_ref, pd0_ref, pw_ref, d_ref, pd_ref, gg_ref, gout_ref, got_ref, w_all, d_two, sbuf, *rest = rest
    else:
        shard_ref, d_ref, pd_ref, gg_ref, gout_ref, full_ref, pw_ref, buf, *rest = rest
    (p_scr, dp_scr, kt_scr, dqt_scr, dq_scr, dk_scr, dv_scr, du_scr, d_scr, dh_scr, dots_scr, total, slot, ga_slot,
     ex_send, ex_recv, pd_send, pd_recv, d_sems, rs_sems, ld_sems, *bg_sems) = rest
    h, qi = pl.program_id(0), pl.program_id(1)
    me = lax.axis_index('tp')
    core, partner, first_dev, _ = route(me)
    weights = (wq_ref, wk_ref, wv_ref)

    if b:
        operands = []
        for blk, chip in enumerate((peer_of(me, 6) // 2, first_dev // 2)):
            operands += [pltpu.make_async_copy(d.at[block_rows(chip), :], d_two.at[blk, n], ld_sems.at[2 * blk + n])
                         for n, d in enumerate((d0_ref, pd0_ref))]
        operands += [pltpu.make_async_copy(w.at[half_rows(core), :], w_all.at[0, :, pl.ds(n * LOC, LOC)], ld_sems.at[4 + n])
                     for n, w in enumerate(weights)]
        operands.append(pltpu.make_async_copy(pw_ref, w_all.at[1], ld_sems.at[7]))
        moved = [pltpu.make_async_remote_copy(
            src_ref=sbuf.at[blk, pl.ds(lo, count), :], dst_ref=got_ref.at[blk, pl.ds(lo, count), :], send_sem=rs_sems.at[n],
            recv_sem=rs_sems.at[3 + n], device_id=(first_dev,), device_id_type=MESH)
            for n, (blk, lo, count) in enumerate(((0, 0, BLK), (1, 0, BLK // 2), (1, BLK // 2, BLK // 2)))]
    else:
        bg = (*bg_sems, buf)
        gather = stage1(me, shard_ref.at[1], full_ref, bg)
        moved = [pltpu.make_async_remote_copy(
            src_ref=w.at[half_rows(1 - core), :], dst_ref=pw_ref.at[:, pl.ds(n * LOC, LOC)], send_sem=rs_sems.at[n],
            recv_sem=rs_sems.at[3 + n], device_id=(partner,), device_id_type=MESH) for n, w in enumerate(weights)]

    @pl.when(jnp.logical_and(h == 0, qi == 0))
    def _():
        if b:
            start(operands)
            entry_barrier(me)
            wait(operands)
            for blk in range(2):
                sbuf[blk] = dot(d_two[blk, 0], w_all[0], NT) + dot(d_two[blk, 1], w_all[1], NT)
                moved[blk].start()
        else:
            gather.load()
            entry_barrier(me)
            gather.send()
            start(moved)
        dots_scr[...] = jnp.zeros_like(dots_scr)

    if not b:
        @pl.when(jnp.logical_and(h == 1, qi == 1))
        def _():
            gather.wait()
            more = stage2(me, full_ref, bg)
            more.load()
            more.send()

    @pl.when(h == 0)
    def _():
        dh_scr[block_rows(qi), :] = dot(da_ref[...], wo_ref[...], NT).astype(BF)

    @pl.when(qi == 0)
    def _():
        kt_scr[...] = qkv_ref[1].T
        dk_scr[...] = jnp.zeros_like(dk_scr)
        dv_scr[...] = jnp.zeros_like(dv_scr)

    qb = qkv_ref[0, block_rows(qi), :]
    dob = dh_scr[block_rows(qi), head_cols(h)]
    lse = lse_ref[pl.ds(h * NB + qi, 1), :]

    def first(j, acc, diag=False):
        rows = block_rows(j)
        p = jnp.exp2(dot(qkv_ref[1, rows, :], qb, NT) * C2 - lse)
        if diag:
            p = jnp.where(causal_mask(), p, 0.0)
        dp = dot(qkv_ref[2, rows, :], dob, NT)
        p_scr[j] = p
        dp_scr[j] = dp
        dv_scr[rows, :] += dot(p.astype(BF), dob)
        return acc + jnp.sum((p * dp).reshape(BLK // 8, 8, BLK), axis=0)

    acc = first(qi, jnp.zeros((8, BLK), F32), True)
    acc = lax.fori_loop(0, qi, first, acc)
    delta = jnp.sum(acc, axis=0, keepdims=True)
    dqt_scr[...] = jnp.zeros_like(dqt_scr)

    def second(j, carry):
        rows = block_rows(j)
        ds = (p_scr[j] * (dp_scr[j] - delta) * SCALE).astype(BF)
        dk_scr[rows, :] += dot(ds, qb)
        dqt_scr[...] += dot(kt_scr[:, rows], ds)
        return carry

    lax.fori_loop(0, qi + 1, second, 0)
    dq_scr[block_rows(qi), :] = dqt_scr[...].T

    @pl.when(qi == NB - 1)
    def _():
        d_scr[:, pl.ds(pl.multiple_of(2 * LOC + h * HD, HD), HD)] = dv_scr[...].astype(BF)
        gg_ref[...] = jnp.zeros_like(gg_ref)
        cols = head_cols(h)

        def tail(i, carry):
            rows = block_rows(i)
            cos, sin = cos_ref[rows, :], sin_ref[rows, :]
            for n, from_scr in enumerate((dq_scr, dk_scr)):
                d = from_scr[rows, :]
                hat = d * cos - pltpu.roll(d, HD // 2, 1) * sin
                unit = raw_ref[n, rows, cols] * as_column(inv_ref[pl.ds(i + n * NB, 1), :])
                gg_ref[n:n + 1, :] += jnp.sum(hat * unit, axis=0, keepdims=True)
                du = hat * gains_ref[n:n + 1, :]
                du_scr[n, h, rows, :] = du
                dots_scr[pl.ds(i + n * NB, 1), :] += row_sums(du * unit)
            return carry

        lax.fori_loop(0, NB, tail, 0)

    @pl.when(jnp.logical_and(h == 1, qi == NB - 1))
    def _():
        sums = exchange(me, [dots_scr, gga_ref], [slot, ga_slot], ex_send, ex_recv)
        start(sums)
        if b:
            moved[2].start()
        wait(sums)
        if not b:
            stage2(me, full_ref, bg).wait()
            last_stage = stage3(me, full_ref, bg)
            last_stage.load()
            last_stage.send()
        total[...] = ordered_total(me, dots_scr, slot) / DIM
        gout_ref[...] = ordered_total(me, gga_ref, ga_slot)

        def copies(i):
            rows = block_rows(i)
            return [pltpu.make_async_copy(d_scr.at[rows, :], d_ref.at[rows, :], d_sems.at[i]),
                    pltpu.make_async_remote_copy(
                        src_ref=d_scr.at[rows, :], dst_ref=pd_ref.at[rows, :], send_sem=pd_send.at[i],
                        recv_sem=pd_recv.at[i], device_id=(peer_of(me, 1),), device_id_type=MESH)]

        def last(i, carry):
            rows = block_rows(i)
            for n in range(2):
                dots = as_column(total[pl.ds(i + n * NB, 1), :])
                inv = as_column(inv_ref[pl.ds(i + n * NB, 1), :])
                for hh in range(LOC // HD):
                    sl = slice(hh * HD, (hh + 1) * HD)
                    unit = raw_ref[n, rows, sl] * inv
                    val = inv * (du_scr[n, hh, rows, :] - unit * dots)
                    d_scr[rows, n * LOC + hh * HD:n * LOC + (hh + 1) * HD] = val.astype(BF)
            start(copies(i))
            return carry

        lax.fori_loop(0, NB, last, 0)
        for i in range(NB):
            wait(copies(i))
        wait(moved)
        if not b:
            last_stage.wait()


def backward(b, da, qkv, wo, lse, raw, inv, gains, cos, sin, gga, weights, others, cid):
    def whole(*shape):
        return pl.BlockSpec(shape, lambda h, i: (0,) * len(shape))

    def picked(*shape):
        return pl.BlockSpec((None,) + shape, lambda h, i: (b,) + (0,) * len(shape))

    gsp = whole(8, DIM // 8)
    half = (DIM // 2, 3 * LOC)
    if b:
        extra = [sds((2, BLK, DIM // 2), F32)]
        own = [pltpu.VMEM((2,) + half, BF), pltpu.VMEM((2, 2, BLK, 3 * LOC), BF), pltpu.VMEM((2, BLK, DIM // 2), F32)]
    else:
        extra = [sds((SEQ, DIM), BF), sds(half, BF)]
        own = [pltpu.VMEM((2, TOK, DIM), BF)]
    return pl.pallas_call(
        functools.partial(backward_kernel, b),
        grid=(2, NB),
        in_specs=[pl.BlockSpec((None, 3, SEQ, HD), lambda h, i: (b, 0, 0, h)),
                  pl.BlockSpec((BLK, DIM), lambda h, i: (jnp.where(h == 0, i, NB - 1), 0)), whole(LOC, DIM),
                  picked(2 * NB, BLK), picked(2, SEQ, LOC), picked(2 * NB, BLK),
                  pl.BlockSpec((2 + DIM // LOC, HD), lambda h, i: (0, h)), whole(SEQ, HD), whole(SEQ, HD), gsp]
        + [ANYWHERE] * (3 + len(others)),
        out_specs=[ANYWHERE, ANYWHERE, pl.BlockSpec((8, HD), lambda h, i: (0, h)), gsp] + [ANYWHERE] * len(extra),
        out_shape=[sds((SEQ, 3 * LOC), BF), sds((SEQ, 3 * LOC), BF), sds((8, LOC), F32), sds((8, DIM // 8), F32)] + extra,
        scratch_shapes=own + [
            pltpu.VMEM((NB, BLK, BLK), F32), pltpu.VMEM((NB, BLK, BLK), F32), pltpu.VMEM((HD, SEQ), BF),
            pltpu.VMEM((HD, BLK), F32), pltpu.VMEM((SEQ, HD), F32), pltpu.VMEM((SEQ, HD), F32),
            pltpu.VMEM((SEQ, HD), F32), pltpu.VMEM((2, 2, SEQ, HD), F32), pltpu.VMEM((SEQ, 3 * LOC), BF),
            pltpu.VMEM((SEQ, LOC), BF), pltpu.VMEM((2 * NB, BLK), F32), pltpu.VMEM((2 * NB, BLK), F32),
            pltpu.VMEM((NDEV - 1, 2 * NB, BLK), F32), pltpu.VMEM((NDEV - 1, 8, DIM // 8), F32),
            DMA((2, NDEV - 1)), DMA((2, NDEV - 1)), DMA((NB,)), DMA((NB,)), DMA((NB,)), DMA((6,)), DMA((8,))]
        + ([] if b else BG_SEMS),
        compiler_params=params(dimension_semantics=("arbitrary", "arbitrary"), collective_id=cid, has_side_effects=True),
        cost_estimate=cost(25e9, 30e6),
        name="backward",
    )(qkv, da, wo, lse, raw, inv, gains, cos, sin, gga, *weights, *others)


HALF = DIM // 2
CH = 256


def grads_kernel(d0, d1, pd0, pd1, wq, wk, wv, pw, got, x_full, o_all, da0, da1, dy_ref, dx_ref, gwq_ref, gwk_ref, gwv_ref, gwo_ref,
                 d_all, w_all, sbuf, r1, r2, fin, acc, xbuf, obuf,
                 dl_sems, w_sems, s1_sems, r1_sems, s2_sems, r2_sems, fs_sems, fr_sems, x_sems, o_sems):
    me = lax.axis_index('tp')
    core, partner, first, second = route(me)
    chip = me // 2
    diag_chip, first_chip, second_chip = peer_of(me, 6) // 2, first // 2, second // 2

    barrier = pltpu.get_barrier_semaphore()
    for dev in (partner, first, second):
        pl.semaphore_signal(barrier, inc=1, device_id=(dev,), device_id_type=MESH)
    pl.semaphore_wait(barrier, 3)

    def rows_of(blk):
        return pl.ds(pl.multiple_of(blk * BLK, BLK), BLK)

    chips = (diag_chip, first_chip, second_chip, chip)
    w_copies = [pltpu.make_async_copy(w.at[half_rows(core), :], w_all.at[0, :, pl.ds(n * LOC, LOC)], w_sems.at[n])
                for n, w in enumerate((wq, wk, wv))]
    w_copies.append(pltpu.make_async_copy(pw, w_all.at[1], w_sems.at[3]))
    loads = []
    for n in range(8):
        rows, b = rows_of(chips[n // 2]), n % 2
        loads.append([pltpu.make_async_copy(d.at[rows, :], d_all.at[side, b, rows, :], dl_sems.at[side, n])
                      for side, d in enumerate(((d0, d1)[b], (pd0, pd1)[b]))])
    start(w_copies)
    start(loads[1])
    wait(w_copies)

    def partial(b, blk):
        rows = rows_of(blk)
        return dot(d_all[0, b, rows, :], w_all[0], NT) + dot(d_all[1, b, rows, :], w_all[1], NT)

    def to_first(n):
        return pltpu.make_async_remote_copy(
            src_ref=sbuf.at[n // 2], dst_ref=r1.at[n], send_sem=s1_sems.at[n], recv_sem=r1_sems.at[n],
            device_id=(first,), device_id_type=MESH)

    def to_second(b):
        return pltpu.make_async_remote_copy(
            src_ref=r1.at[b], dst_ref=r2.at[b], send_sem=s2_sems.at[b], recv_sem=r2_sems.at[b],
            device_id=(second,), device_id_type=MESH)

    def to_partner(b):
        return pltpu.make_async_remote_copy(
            src_ref=r1.at[2 + b, pl.ds(pl.multiple_of((1 - core) * TOK, TOK), TOK), :], dst_ref=fin.at[b],
            send_sem=fs_sems.at[b], recv_sem=fr_sems.at[b], device_id=(partner,), device_id_type=MESH)

    taken = [pltpu.make_async_copy(got.at[n], r1.at[2 * n], w_sems.at[4 + n]) for n in range(2)]
    for n in (1, 3):
        wait(loads[n])
        if n == 1:
            start(loads[3])
        sbuf[n // 2] = partial(1, chips[n // 2])
        to_first(n).start()
        if n == 1:
            start(taken)
            for later in (4, 0, 2, 5, 6, 7):
                start(loads[later])
    for n in (0, 2, 4, 5, 6, 7):
        wait(loads[n])
    wait(taken)

    steps = SEQ // CH

    def chunk(i):
        return pl.ds(pl.multiple_of(i * CH, CH), CH)

    def stream(pairs, body):
        def fetch(i):
            return [pltpu.make_async_copy(src.at[chunk(i), :], buf.at[i % 2], sems.at[i % 2]) for src, buf, sems in pairs]

        for c in fetch(0):
            c.start()

        def it(i, carry):
            @pl.when(i + 1 < steps)
            def _():
                for c in fetch(i + 1):
                    c.start()

            for c in fetch(i):
                c.wait()
            body(i)
            return carry

        lax.fori_loop(0, steps, it, 0)

    def wgrad(b, src):
        def body(i):
            left = d_all[0, b, chunk(i), :].T
            for c in range(3):
                part = slice(c * LOC, (c + 1) * LOC)
                acc[part, :] += dot(left[part, :], xbuf[i % 2])

        stream([(src, xbuf, x_sems)], body)

    def forward_second(b):
        if b:
            to_first(b).wait_recv()
        r1[b] += partial(b, second_chip)
        to_second(b).start()

    forward_second(0)
    acc[...] = jnp.zeros_like(acc)
    wgrad(0, x_full.at[0])
    wgrad(1, x_full.at[1])
    for n, ref in enumerate((gwq_ref, gwk_ref, gwv_ref)):
        ref[...] = acc[n * LOC:(n + 1) * LOC, :].T.astype(BF)
    forward_second(1)
    acc[:LOC, :] = jnp.zeros((LOC, DIM), F32)

    def wo_body(i):
        acc[:LOC, :] += dot(obuf[i % 2].T, xbuf[i % 2])

    for o_src, da_src in ((o_all.at[0], da0), (o_all.at[1], da1)):
        stream([(da_src, xbuf, x_sems), (o_src, obuf, o_sems)], wo_body)
    gwo_ref[...] = acc[:LOC, :].astype(BF)

    def own_part(b, carry):
        r1_own = partial(b, chip)
        pl.when(b == 1)(to_first(3).wait_recv)
        to_second(b).wait_recv()
        r1[2 + b] += r1_own + r2[b]
        to_partner(b).start()
        cols = half_rows(core)
        rows = pl.ds(pl.multiple_of(core * TOK, TOK), TOK)
        dx_ref[b, :, cols] = (r1[2 + b, rows, :] + dy_ref[b, :, cols].astype(F32)).astype(BF)
        return carry

    lax.fori_loop(0, 2, own_part, 0)

    def finish(b, carry):
        to_partner(b).wait()
        cols = half_rows(1 - core)
        dx_ref[b, :, cols] = (fin[b] + dy_ref[b, :, cols].astype(F32)).astype(BF)
        to_second(b).wait_send()
        return carry

    to_first(1).wait_send()
    to_first(3).wait_send()
    lax.fori_loop(0, 2, finish, 0)


def grads(d0, d1, pd0, pd1, wq, wk, wv, pw, got, x_full, o_all, da0, da1, dy, cid):
    vm = pl.BlockSpec(memory_space=pltpu.VMEM)
    far = pl.BlockSpec(memory_space=pl.ANY)
    dma = pltpu.SemaphoreType.DMA
    return pl.pallas_call(
        grads_kernel,
        in_specs=[far] * 13 + [vm],
        out_specs=[vm] * 5,
        out_shape=[sds((2, TOK, DIM), BF)] + [sds((DIM, LOC), BF)] * 3 + [sds((LOC, DIM), BF)],
        scratch_shapes=[pltpu.VMEM((2, 2, SEQ, 3 * LOC), BF), pltpu.VMEM((2, HALF, 3 * LOC), BF),
                        pltpu.VMEM((2, BLK, HALF), F32), pltpu.VMEM((4, BLK, HALF), F32), pltpu.VMEM((2, BLK, HALF), F32),
                        pltpu.VMEM((2, TOK, HALF), F32), pltpu.VMEM((3 * LOC, DIM), F32),
                        pltpu.VMEM((2, CH, DIM), BF), pltpu.VMEM((2, CH, LOC), BF),
                        dma((2, 8)), dma((9,)), dma((4,)), dma((4,)), dma((2,)), dma((2,)),
                        dma((2,)), dma((2,)), dma((2,)), dma((2,))],
        compiler_params=pltpu.CompilerParams(vmem_limit_bytes=67043328, collective_id=cid, has_side_effects=True),
        cost_estimate=cost(100e9, 40e6),
        name="grads",
    )(d0, d1, pd0, pd1, wq, wk, wv, pw, got, x_full, o_all, da0, da1, dy)


def deliver_kernel(*refs):
    count = (len(refs) - 2) // 3
    srcs, dsts, bufs = refs[:count], refs[count:2 * count], refs[2 * count:3 * count]
    loads = [pltpu.make_async_copy(src, buf, refs[-2].at[n]) for n, (src, buf) in enumerate(zip(srcs, bufs))]
    stores = [pltpu.make_async_copy(buf, dst, refs[-1].at[n]) for n, (buf, dst) in enumerate(zip(bufs, dsts))]
    start(loads)
    for load, store in zip(loads, stores):
        load.wait()
        store.start()
    wait(stores)


def deliver(*arrays):
    return pl.pallas_call(
        deliver_kernel,
        in_specs=[ANYWHERE] * len(arrays),
        out_specs=[ANYWHERE] * len(arrays),
        out_shape=[sds(t.shape, t.dtype) for t in arrays],
        scratch_shapes=[pltpu.VMEM(t.shape, t.dtype) for t in arrays] + [DMA((len(arrays),)), DMA((len(arrays),))],
        compiler_params=params(),
        cost_estimate=cost(1e9, 16e6),
        name="deliver",
    )(*arrays)


def local_block(x_loc, wq, wk, wv, wo, gq, gk, ga, dy_loc):
    gains = jnp.concatenate([gq, gk, ga]).astype(F32).reshape(2 + DIM // LOC, LOC)
    weights = (wq, wk, wv)
    cos, sin, inv, o, lse, raw, qkv, o_recv, x_full, wo_full = forward(x_loc, wq, wk, wv, wo, gains, 0)
    y, da, gga, da0 = out_block(o_recv, wo_full, x_loc, dy_loc, gains, 1)
    state = (qkv, wo, lse, raw, inv, gains, cos, sin, gga, weights)
    d0, pd0, gg0, gout, da1, pw = backward(0, da0, *state, (da,), 2)
    d1, pd1, gg1, _, got = backward(1, da1, *state, (d0, pd0, pw), 3)
    grad_ga = gout.reshape(DIM).astype(BF)
    big = grads(d0, d1, pd0, pd1, *weights, pw, got, x_full, o, da0, da1, dy_loc, 4)
    y, dx, gwq, gwk, gwv, gwo = deliver(y, *big)
    gg = gg0 + gg1
    return (y, dx, gwq, gwk, gwv, gwo, gg[0].astype(BF), gg[1].astype(BF), grad_ga)


def solution(mesh):
    act, col, row, vec = P(None, 'tp', None), P(None, 'tp'), P('tp', None), P('tp')
    in_specs = (act, col, col, col, row, vec, vec, P(), act)
    out_specs = (act, act, col, col, col, row, vec, vec, P())
    return jax.shard_map(local_block, mesh=mesh, in_specs=in_specs, out_specs=out_specs, check_vma=False)
```

```python
import functools
import math

import jax
import jax.numpy as jnp
import numpy as np
from jax import lax
from jax.experimental import pallas as pl
from jax.experimental.pallas import tpu as pltpu
from jax.sharding import PartitionSpec as P

HD = 128
ROPE_THETA = 500000.0
EPS = 1e-6
DIM = 2048
SEQ = 2048
LOC = 256
TOK = 256
BLK = 512
NB = SEQ // BLK
NDEV = 8
SCALE = HD ** -0.5
C2 = SCALE * math.log2(math.e)
MESH = pl.DeviceIdType.MESH
BF = jnp.bfloat16
F32 = jnp.float32
VMEM_MAX = 60 * 1024 * 1024

NT = (((1,), (1,)), ((), ()))
NN = (((1,), (0,)), ((), ()))


def dot(a, b, dims=NN):
    return lax.dot_general(a, b, dims, preferred_element_type=F32)


def sds(shape, dtype):
    return jax.ShapeDtypeStruct(shape, dtype)


def cost(flops, nbytes, trans=0):
    return pl.CostEstimate(flops=int(flops), bytes_accessed=int(nbytes), transcendentals=int(trans))


def params(**kw):
    return pltpu.CompilerParams(vmem_limit_bytes=VMEM_MAX, **kw)


def peer_of(me, mask):
    core, ax, ay = me % 2, (me // 2) % 2, me // 4
    core = 1 - core if mask & 1 else core
    ax = 1 - ax if mask & 2 else ax
    ay = 1 - ay if mask & 4 else ay
    return ay * 4 + ax * 2 + core


ORDER = (6, 7, 2, 4, 3, 5, 1)


def entry_barrier(me):
    barrier = pltpu.get_barrier_semaphore()
    for mask in ORDER:
        pl.semaphore_signal(barrier, inc=1, device_id=(peer_of(me, mask),), device_id_type=MESH)
    pl.semaphore_wait(barrier, NDEV - 1)


def nbr_signal(me):
    for mask in (1, 2, 4):
        pl.semaphore_signal(pltpu.get_barrier_semaphore(), inc=1, device_id=(peer_of(me, mask),), device_id_type=MESH)


def nbr_wait():
    pl.semaphore_wait(pltpu.get_barrier_semaphore(), 3)


DMA = pltpu.SemaphoreType.DMA
ANYWHERE = pl.BlockSpec(memory_space=pl.ANY)
BG_SEMS = [DMA((11,)), DMA((11,)), DMA((5,))]
BG = BG_SEMS + [pltpu.VMEM((2, TOK, DIM), BF)]


def shard_rows(dev, lo=0, count=TOK):
    return pl.ds(pl.multiple_of(dev * TOK + lo, HD), count)


class Stage:
    def __init__(self, loads, copies):
        self.loads, self.copies = loads, copies

    def load(self):
        start(self.loads)

    def send(self):
        wait(self.loads)
        start(self.copies)

    def wait(self, *which):
        wait([self.copies[n] for n in which] or self.copies)


def stage1(me, src, full, bg, part=None):
    send, recv, own, buf = bg
    lo, count, at = (0, TOK, 0) if part is None else (part * (TOK // 2), TOK // 2, 8 * part)
    there = full.at[shard_rows(me, lo, count), :]
    mine = buf.at[0, pl.ds(lo, count), :]
    copies = [pltpu.make_async_remote_copy(
        src_ref=mine, dst_ref=there, send_sem=send.at[at + k], recv_sem=recv.at[at + k],
        device_id=(peer_of(me, mask),), device_id_type=MESH) for k, mask in enumerate((2, 4, 1))]
    loads = [] if part == 1 or src is None else [pltpu.make_async_copy(src, buf.at[0], own.at[0])]
    return Stage(loads, copies + [pltpu.make_async_copy(mine, there, own.at[3 if part == 1 else 2])])


def stage2(me, full, bg):
    send, recv, own, buf = bg
    xn, yn = peer_of(me, 2), peer_of(me, 4)
    half = TOK // 2
    plan = ((1, half, half, yn, 2), (0, 0, half, xn, 4), (0, 0, TOK, xn, 1), (1, 0, TOK, yn, 1))
    return Stage(
        [pltpu.make_async_copy(full.at[shard_rows(dev), :], buf.at[n], own.at[n]) for n, dev in enumerate((xn, yn))],
        [pltpu.make_async_remote_copy(
            src_ref=buf.at[slot, pl.ds(lo, count), :], dst_ref=full.at[shard_rows(dev, lo, count), :],
            send_sem=send.at[3 + k], recv_sem=recv.at[3 + k], device_id=(peer_of(me, mask),), device_id_type=MESH)
         for k, (slot, lo, count, dev, mask) in enumerate(plan)])


def stage3(me, full, bg):
    send, recv, own, buf = bg
    rows = full.at[shard_rows(peer_of(me, 6)), :]
    return Stage([pltpu.make_async_copy(rows, buf.at[1], own.at[1])], [pltpu.make_async_remote_copy(
        src_ref=buf.at[1], dst_ref=rows, send_sem=send.at[7], recv_sem=recv.at[7],
        device_id=(peer_of(me, 1),), device_id_type=MESH)])


def route(me):
    core = me % 2
    first = peer_of(me, 2) * (1 - core) + peer_of(me, 4) * core
    second = peer_of(me, 4) * (1 - core) + peer_of(me, 2) * core
    return core, peer_of(me, 1), first, second


def half_rows(c):
    return pl.ds(pl.multiple_of(c * (DIM // 2), DIM // 2), DIM // 2)


def start(copies):
    for c in copies:
        c.start()


def wait(copies):
    for c in copies:
        c.wait()


def row_sums(vals):
    folded = vals[:, :HD]
    for start in range(HD, vals.shape[1], HD):
        folded = folded + vals[:, start:start + HD]
    return jnp.sum(folded.T, axis=0, keepdims=True)


def as_column(row):
    return jnp.broadcast_to(row, (HD, row.shape[1])).T


def exchange(me, srcs, slots, send_sems, recv_sems):
    copies = []
    for n, (src, slot) in enumerate(zip(srcs, slots)):
        for p, mask in enumerate(ORDER):
            copies.append(pltpu.make_async_remote_copy(
                src_ref=src, dst_ref=slot.at[p], send_sem=send_sems.at[n, p], recv_sem=recv_sems.at[n, p],
                device_id=(peer_of(me, mask),), device_id_type=MESH))
    return copies


def ordered_total(me, src, slot):
    own = src[...]
    total = jnp.zeros_like(own)
    for dev in range(NDEV):
        term = jnp.where(me == dev, own, 0.0)
        for p, mask in enumerate(ORDER):
            term = term + jnp.where(peer_of(me, mask) == dev, slot[p], 0.0)
        total = total + term
    return total


def causal_mask():
    keys = lax.broadcasted_iota(jnp.int32, (BLK, BLK), 0)
    queries = lax.broadcasted_iota(jnp.int32, (BLK, BLK), 1)
    return keys <= queries


def block_rows(i):
    return pl.ds(pl.multiple_of(i * BLK, BLK), BLK)


def head_cols(h):
    return pl.ds(pl.multiple_of(h * HD, HD), HD)


def forward_kernel(freq_ref, wq_ref, wk_ref, wv_ref, gains_ref, x_ref, wo_ref,
                   cos_ref, sin_ref, inv_ref, o_ref, lse_ref, raw_ref, qkv_ref, both_ref, full_ref, wof_ref,
                   raw, qkv, xbuf, sums_scr, slot, p_scr, vt_scr, acc_scr, o_scr, buf0, buf1,
                   ex_send, ex_recv, out_sems, send_sems, recv_sems, own_sems, x_sems, *bg_sems):
    g = pl.program_id(0)
    b, t = g // (4 * NB), g % (4 * NB)
    me = lax.axis_index('tp')
    bg0, bg1, bg2 = (*bg_sems[:3], buf0), (*bg_sems[3:6], buf1), (*bg_sems[6:], buf0)
    x0f, x1f = full_ref.at[0], full_ref.at[1]

    def x_gather(part=None):
        return stage1(me, x_ref.at[1], x1f, bg1, part)

    def wo_gather(part=None):
        return stage1(me, wo_ref, wof_ref, bg2, part)

    def keep(bb):
        return [pltpu.make_async_copy(raw, raw_ref.at[bb], out_sems.at[0]),
                pltpu.make_async_copy(qkv, qkv_ref.at[bb], out_sems.at[1])]

    def sums(bb):
        return exchange(me, [sums_scr.at[bb]], [slot.at[bb]], ex_send.at[bb], ex_recv.at[bb])

    def fetch(bb, i):
        return pltpu.make_async_copy(full_ref.at[bb, block_rows(i), :], xbuf.at[i % 2], x_sems.at[i % 2])

    def block_copy(bb, hh, st, half):
        dest = 2 * ((me // 2 + 1 + st) % NB) + half
        part = o_scr.at[bb, hh, st, pl.ds(half * TOK, TOK), :]
        dst = both_ref.at[bb, :, pl.ds(pl.multiple_of(me * LOC + hh * HD, HD), HD)]
        away = pltpu.make_async_remote_copy(
            src_ref=part, dst_ref=dst, send_sem=send_sems.at[bb, hh, st, half], recv_sem=recv_sems.at[bb, hh, me],
            device_id=(dest,), device_id_type=MESH)
        return dest, away, pltpu.make_async_copy(part, dst, own_sems.at[bb, hh])

    def run(stage):
        stage.load()
        stage.send()

    @pl.when(g == 0)
    def _():
        first = stage1(me, x_ref.at[0], x0f, bg0)
        first.load()
        entry_barrier(me)
        first.send()
        x_gather(0).load()
        freq = freq_ref[...]
        sign = jnp.where(lax.broadcasted_iota(jnp.int32, (TOK, HD), 1) < HD // 2, -1.0, 1.0)

        def table(i, carry):
            rows = pl.ds(pl.multiple_of(i * TOK, TOK), TOK)
            pos = (lax.broadcasted_iota(jnp.int32, (TOK, HD), 0) + i * TOK).astype(F32)
            angle = pos * freq
            cos_ref[rows, :] = jnp.cos(angle)
            sin_ref[rows, :] = jnp.sin(angle) * sign
            return carry

        lax.fori_loop(0, SEQ // TOK, table, 0)
        first.wait()
        second, third = stage2(me, x0f, bg0), stage3(me, x0f, bg0)
        run(second)
        x_gather(0).send()
        second.wait()
        run(third)
        third.wait()
        fetch(0, 0).start()

    @pl.when(g == 2 * NB + 2)
    def _():
        x_gather(0).wait()
        x_gather(1).wait()
        run(stage2(me, x1f, bg1))
        run(wo_gather(0))

    @pl.when(g == 4 * NB)
    def _():
        stage2(me, x1f, bg1).wait()
        third = stage3(me, x1f, bg1)
        run(third)
        for c in keep(0):
            c.wait()
        third.wait()
        fetch(1, 0).start()

    @pl.when(g == 6 * NB + 2)
    def _():
        wo_gather(0).wait()
        wo_gather(1).wait()
        run(stage2(me, wof_ref, bg2))

    @pl.when(t < NB)
    def _():
        rows = block_rows(t)

        @pl.when(t < NB - 1)
        def _():
            fetch(b, t + 1).start()

        fetch(b, t).wait()
        x = xbuf[t % 2]
        for n, w_ref in enumerate((wq_ref, wk_ref)):
            val = dot(x, w_ref[...])
            raw[n, rows, :] = val
            sums_scr[b, pl.ds(t + n * NB, 1), :] = row_sums(val * val)
        qkv[2, rows, :] = dot(x, wv_ref[...]).astype(BF)

    @pl.when(t == NB)
    def _():
        start(sums(b))
        keep(b)[0].start()
        pl.when(b == 0)(x_gather(1).send)
        pl.when(b == 1)(wo_gather(1).send)
        wait(sums(b))
        inv_ref[...] = lax.rsqrt(ordered_total(me, sums_scr.at[b], slot.at[b]) / DIM + EPS)

    @pl.when(jnp.logical_and(t >= NB, t < 2 * NB))
    def _():
        i = t - NB
        rows = block_rows(i)
        cos, sin = cos_ref[rows, :], sin_ref[rows, :]
        for n in range(2):
            inv = as_column(inv_ref[pl.ds(i + n * NB, 1), :])
            gain = gains_ref[n:n + 1, :]
            for h in range(LOC // HD):
                sl = slice(h * HD, (h + 1) * HD)
                hat = raw[n, rows, sl] * inv * gain[:, sl]
                qkv[n, rows, sl] = (hat * cos + pltpu.roll(hat, HD // 2, 1) * sin).astype(BF)

    @pl.when(t == 2 * NB)
    def _():
        keep(b)[1].start()

    @pl.when(t >= 2 * NB)
    def _():
        h, step = t // NB - 2, t % NB
        qi = (me // 2 + 1 + step) % NB
        cols = head_cols(h)

        @pl.when(step == 0)
        def _():
            vt_scr[...] = qkv[2, :, cols].T

        qb = qkv[0, block_rows(qi), cols]

        def scores(j):
            return dot(qkv[1, block_rows(j), cols], qb, NT)

        def first(j, m):
            s = scores(j)
            p_scr[j] = s
            return jnp.maximum(m, jnp.max(s.reshape(BLK // 8, 8, BLK), axis=0))

        s = jnp.where(causal_mask(), scores(qi), -1e30)
        p_scr[qi] = s
        m = lax.fori_loop(0, qi, first, jnp.max(s.reshape(BLK // 8, 8, BLK), axis=0))
        m = jnp.max(m, axis=0, keepdims=True)

        def second(j, l):
            p = jnp.exp2((p_scr[j] - m) * C2)
            p_scr[j] = p
            return l + jnp.sum(p.reshape(BLK // 8, 8, BLK), axis=0)

        l = lax.fori_loop(0, qi + 1, second, jnp.zeros((8, BLK), F32))
        l = jnp.sum(l, axis=0, keepdims=True)
        rl = 1.0 / l
        lse_ref[pl.ds(h * NB + qi, 1), :] = m * C2 + jnp.log2(l)

        acc_scr[...] = jnp.zeros_like(acc_scr)

        def third(j, carry):
            p = (p_scr[j] * rl).astype(BF)
            acc_scr[...] += dot(vt_scr[:, block_rows(j)], p)
            return carry

        lax.fori_loop(0, qi + 1, third, 0)
        out = acc_scr[...].T.astype(BF)
        o_scr[b, h, step] = out
        o_ref[block_rows(qi), cols] = out

        for half in range(2):
            dest, away, here = block_copy(b, h, step, half)
            pl.when(dest != me)(away.start)
            pl.when(dest == me)(here.start)

    @pl.when(g == 8 * NB - 1)
    def _():
        stage2(me, wof_ref, bg2).wait()
        third = stage3(me, wof_ref, bg2)
        run(third)
        for c in keep(1):
            c.wait()

        def drain(n, carry):
            bb, hh = n // 2, n % 2
            for st in range(NB):
                for half in range(2):
                    dest, away, here = block_copy(bb, hh, st, half)
                    if st < NB - 1:
                        away.wait_send()
                    else:
                        pl.when(dest != me)(away.wait_send)
                        pl.when(dest == me)(here.wait)
            for mask in ORDER:
                peer = peer_of(me, mask)
                pltpu.make_async_remote_copy(
                    src_ref=o_scr.at[0, 0, 0, pl.ds(0, TOK), :],
                    dst_ref=both_ref.at[bb, :, pl.ds(pl.multiple_of(peer * LOC + hh * HD, HD), HD)],
                    send_sem=send_sems.at[0, 0, 0, 0], recv_sem=recv_sems.at[bb, hh, peer],
                    device_id=(peer,), device_id_type=MESH).wait_recv()
            return carry

        lax.fori_loop(0, 4, drain, 0)
        third.wait()


def forward(x, wq, wk, wv, wo, gains, cid):
    inv_freq = np.float32(1.0) / np.float32(ROPE_THETA) ** (np.arange(HD // 2, dtype=np.float32) / np.float32(HD // 2))
    freq = jnp.asarray(np.concatenate([inv_freq, inv_freq])[None, :], F32)

    def whole(*shape):
        return pl.BlockSpec(shape, lambda g: (0,) * len(shape))

    def per_batch(*shape):
        return pl.BlockSpec((None,) + shape, lambda g: (g // (4 * NB),) + (0,) * len(shape))

    wspec, rows = whole(DIM, LOC), per_batch(2 * NB, BLK)
    return pl.pallas_call(
        forward_kernel,
        grid=(8 * NB,),
        in_specs=[whole(1, HD), wspec, wspec, wspec, whole(2 + DIM // LOC, LOC), ANYWHERE, ANYWHERE],
        out_specs=[whole(SEQ, HD), whole(SEQ, HD), rows, per_batch(SEQ, LOC), rows] + [ANYWHERE] * 5,
        out_shape=[sds((SEQ, HD), F32), sds((SEQ, HD), F32), sds((2, 2 * NB, BLK), F32), sds((2, SEQ, LOC), BF),
                   sds((2, 2 * NB, BLK), F32), sds((2, 2, SEQ, LOC), F32), sds((2, 3, SEQ, LOC), BF),
                   sds((2, TOK, DIM), BF), sds((2, SEQ, DIM), BF), sds((SEQ, DIM), BF)],
        scratch_shapes=[pltpu.VMEM((2, SEQ, LOC), F32), pltpu.VMEM((3, SEQ, LOC), BF), pltpu.VMEM((2, BLK, DIM), BF),
                        pltpu.VMEM((2, 2 * NB, BLK), F32), pltpu.VMEM((2, NDEV - 1, 2 * NB, BLK), F32),
                        pltpu.VMEM((NB, BLK, BLK), F32), pltpu.VMEM((HD, SEQ), BF), pltpu.VMEM((HD, BLK), F32),
                        pltpu.VMEM((2, 2, NB, BLK, HD), BF), pltpu.VMEM((2, TOK, DIM), BF), pltpu.VMEM((2, TOK, DIM), BF),
                        DMA((2, 1, NDEV - 1)), DMA((2, 1, NDEV - 1)), DMA((2,)),
                        DMA((2, 2, NB, 2)), DMA((2, 2, NDEV)), DMA((2, 2)), DMA((2,))] + BG_SEMS * 3,
        compiler_params=params(dimension_semantics=("arbitrary",), collective_id=cid, has_side_effects=True),
        cost_estimate=cost(60e9, 60e6),
        name="forward",
    )(freq, wq, wk, wv, gains, x, wo)


def out_kernel(o_ref, x_ref, dy_ref, gains_ref, wo_ref, y_ref, da_ref, gga_ref, full_ref, wo_scr, a_scr, wo_sems, buf, *bg_sems):
    b = pl.program_id(0)
    me = lax.axis_index('tp')
    bg = (*bg_sems, buf)
    step = DIM // NB

    def piece(j):
        cols = pl.ds(pl.multiple_of(j * step, step), step)
        return cols, pltpu.make_async_copy(wo_ref.at[:, cols], wo_scr.at[:, cols], wo_sems.at[j])

    @pl.when(b == 0)
    def _():
        nbr_signal(me)
        for j in range(NB):
            piece(j)[1].start()
        gga_ref[...] = jnp.zeros_like(gga_ref)

    o = o_ref[0]

    def fwd(j, carry):
        cols, load = piece(j)
        pl.when(b == 0)(load.wait)
        a_scr[:, cols] = dot(o, wo_scr[:, cols])
        return carry

    lax.fori_loop(0, NB, fwd, 0)
    a = a_scr[...]
    r = lax.rsqrt(jnp.mean(a * a, axis=-1, keepdims=True) + EPS)
    n = a * r
    ga = jnp.concatenate([gains_ref[2 + i:3 + i, :] for i in range(8)], axis=1)
    dy = dy_ref[0].astype(F32)
    gn = dy * ga
    da = (r * (gn - n * jnp.mean(gn * n, axis=-1, keepdims=True))).astype(BF)
    da_ref[0] = da

    @pl.when(b == 0)
    def _():
        buf[0] = da
        nbr_wait()
        stage1(me, None, full_ref, bg).send()

    y_ref[0] = (x_ref[0].astype(F32) + n * ga).astype(BF)
    col = jnp.sum(dy * n, axis=0, keepdims=True)
    for i in range(8):
        gga_ref[i:i + 1, :] += col[:, i * LOC:(i + 1) * LOC]

    @pl.when(b == 1)
    def _():
        stage1(me, None, full_ref, bg).wait()


def out_block(o, wo, x, dy, gains, cid):
    def whole(*shape):
        return pl.BlockSpec(shape, lambda i: (0,) * len(shape))

    batch = pl.BlockSpec((1, TOK, DIM), lambda i: (i, 0, 0))
    return pl.pallas_call(
        out_kernel,
        grid=(2,),
        in_specs=[batch, batch, batch, whole(2 + DIM // LOC, LOC), ANYWHERE],
        out_specs=[batch, batch, whole(8, DIM // 8), ANYWHERE],
        out_shape=[sds((2, TOK, DIM), BF), sds((2, TOK, DIM), BF), sds((8, DIM // 8), F32), sds((SEQ, DIM), BF)],
        scratch_shapes=[pltpu.VMEM((DIM, DIM), BF), pltpu.VMEM((TOK, DIM), F32), DMA((NB,)),
                        pltpu.VMEM((2, TOK, DIM), BF)] + BG_SEMS,
        compiler_params=params(dimension_semantics=("arbitrary",), collective_id=cid, has_side_effects=True),
        cost_estimate=cost(8 * TOK * DIM * DIM + 5e9, 18e6),
        name="out_block",
    )(o, x, dy, gains, wo)


def backward_kernel(b, qkv_ref, wo_ref, lse_ref, raw_ref, inv_ref, gains_ref, cos_ref, sin_ref, gga_ref,
                    wq_ref, wk_ref, wv_ref, da_ref, *rest):
    if b:
        d0_ref, pd0_ref, pw_ref, d_ref, pd_ref, gg_ref, gout_ref, got_ref, w_all, d_two, sbuf, *rest = rest
    else:
        shard_ref, d_ref, pd_ref, gg_ref, gout_ref, full_ref, pw_ref, da_ref, buf0, buf1, *rest = rest
    (p_scr, dp_scr, kt_scr, dqt_scr, dq_scr, dk_scr, dv_scr, du_scr, d_scr, dh_scr, dbuf, dots_scr, total, slot, ga_slot,
     ex_send, ex_recv, pd_send, pd_recv, d_sems, rs_sems, ld_sems, db_sems, *bg_sems) = rest
    h, step = pl.program_id(0), pl.program_id(1)
    me = lax.axis_index('tp')

    def chip_at(n):
        ax, ay = (me // 2) % 2, me // 4
        return (ay + (n // 2) * (1 - 2 * ay)) * 2 + ax + (n % 2) * (1 - 2 * ax)

    def fetch(n):
        return pltpu.make_async_copy(da_ref.at[block_rows(chip_at(n)), :], dbuf.at[n % 2], db_sems.at[n % 2])

    qi = chip_at(step)
    core, partner, first_dev, _ = route(me)
    weights = (wq_ref, wk_ref, wv_ref)

    if b:
        operands = []
        for blk, chip in enumerate((peer_of(me, 6) // 2, first_dev // 2)):
            operands += [pltpu.make_async_copy(d.at[block_rows(chip), :], d_two.at[blk, n], ld_sems.at[2 * blk + n])
                         for n, d in enumerate((d0_ref, pd0_ref))]
        operands += [pltpu.make_async_copy(w.at[half_rows(core), :], w_all.at[0, :, pl.ds(n * LOC, LOC)], ld_sems.at[4 + n])
                     for n, w in enumerate(weights)]
        operands.append(pltpu.make_async_copy(pw_ref, w_all.at[1], ld_sems.at[7]))
        moved = [pltpu.make_async_remote_copy(
            src_ref=sbuf.at[blk, pl.ds(lo, count), :], dst_ref=got_ref.at[blk, pl.ds(lo, count), :], send_sem=rs_sems.at[n],
            recv_sem=rs_sems.at[3 + n], device_id=(first_dev,), device_id_type=MESH)
            for n, (blk, lo, count) in enumerate(((0, 0, BLK), (1, 0, BLK // 2), (1, BLK // 2, BLK // 2)))]
    else:
        bg0, bg = (*bg_sems[:3], buf0), (*bg_sems[3:], buf1)
        older2, older3 = stage2(me, da_ref, bg0), stage3(me, da_ref, bg0)
        gather = stage1(me, shard_ref.at[1], full_ref, bg)
        moved = [pltpu.make_async_remote_copy(
            src_ref=w.at[half_rows(1 - core), :], dst_ref=pw_ref.at[:, pl.ds(n * LOC, LOC)], send_sem=rs_sems.at[n],
            recv_sem=rs_sems.at[3 + n], device_id=(partner,), device_id_type=MESH) for n, w in enumerate(weights)]

    @pl.when(jnp.logical_and(h == 0, step == 0))
    def _():
        fetch(0).start()
        if b:
            start(operands)
            entry_barrier(me)
            wait(operands)
            for blk in range(2):
                sbuf[blk] = dot(d_two[blk, 0], w_all[0], NT) + dot(d_two[blk, 1], w_all[1], NT)
                moved[blk].start()
        else:
            older2.load()
            gather.load()
            entry_barrier(me)
            older2.send()
            gather.send()
            start(moved)
        dots_scr[...] = jnp.zeros_like(dots_scr)

    if not b:
        @pl.when(jnp.logical_and(h == 0, step == NB - 1))
        def _():
            older3.wait()
            fetch(NB - 1).start()

        @pl.when(jnp.logical_and(h == 1, step == 2))
        def _():
            gather.wait()
            more = stage2(me, full_ref, bg)
            more.load()
            more.send()

    @pl.when(h == 0)
    def _():
        fetch(step).wait()
        dh_scr[block_rows(qi), :] = dot(dbuf[step % 2], wo_ref[...], NT).astype(BF)
        if b:
            @pl.when(step < NB - 1)
            def _():
                fetch(step + 1).start()
        else:
            @pl.when(step == 0)
            def _():
                older2.wait(2, 3)

            @pl.when(step < NB - 2)
            def _():
                fetch(step + 1).start()

            @pl.when(step == NB - 2)
            def _():
                older2.wait(0, 1)
                older3.load()
                older3.send()

    @pl.when(step == 0)
    def _():
        kt_scr[...] = qkv_ref[1].T
        dk_scr[...] = jnp.zeros_like(dk_scr)
        dv_scr[...] = jnp.zeros_like(dv_scr)

    qb = qkv_ref[0, block_rows(qi), :]
    dob = dh_scr[block_rows(qi), head_cols(h)]
    lse = lse_ref[pl.ds(h * NB + qi, 1), :]

    def first(j, acc, diag=False):
        rows = block_rows(j)
        p = jnp.exp2(dot(qkv_ref[1, rows, :], qb, NT) * C2 - lse)
        if diag:
            p = jnp.where(causal_mask(), p, 0.0)
        dp = dot(qkv_ref[2, rows, :], dob, NT)
        p_scr[j] = p
        dp_scr[j] = dp
        dv_scr[rows, :] += dot(p.astype(BF), dob)
        return acc + jnp.sum((p * dp).reshape(BLK // 8, 8, BLK), axis=0)

    acc = first(qi, jnp.zeros((8, BLK), F32), True)
    acc = lax.fori_loop(0, qi, first, acc)
    delta = jnp.sum(acc, axis=0, keepdims=True)
    dqt_scr[...] = jnp.zeros_like(dqt_scr)

    def second(j, carry):
        rows = block_rows(j)
        ds = (p_scr[j] * (dp_scr[j] - delta) * SCALE).astype(BF)
        dk_scr[rows, :] += dot(ds, qb)
        dqt_scr[...] += dot(kt_scr[:, rows], ds)
        return carry

    lax.fori_loop(0, qi + 1, second, 0)
    dq_scr[block_rows(qi), :] = dqt_scr[...].T

    @pl.when(step == NB - 1)
    def _():
        d_scr[:, pl.ds(pl.multiple_of(2 * LOC + h * HD, HD), HD)] = dv_scr[...].astype(BF)
        gg_ref[...] = jnp.zeros_like(gg_ref)
        cols = head_cols(h)

        def tail(i, carry):
            rows = block_rows(i)
            cos, sin = cos_ref[rows, :], sin_ref[rows, :]
            for n, from_scr in enumerate((dq_scr, dk_scr)):
                d = from_scr[rows, :]
                hat = d * cos - pltpu.roll(d, HD // 2, 1) * sin
                unit = raw_ref[n, rows, cols] * as_column(inv_ref[pl.ds(i + n * NB, 1), :])
                gg_ref[n:n + 1, :] += jnp.sum(hat * unit, axis=0, keepdims=True)
                du = hat * gains_ref[n:n + 1, :]
                du_scr[n, h, rows, :] = du
                dots_scr[pl.ds(i + n * NB, 1), :] += row_sums(du * unit)
            return carry

        lax.fori_loop(0, NB, tail, 0)

    @pl.when(jnp.logical_and(h == 1, step == NB - 1))
    def _():
        sums = exchange(me, [dots_scr, gga_ref], [slot, ga_slot], ex_send, ex_recv)
        start(sums)
        if b:
            moved[2].start()
        wait(sums)
        if not b:
            stage2(me, full_ref, bg).wait()
            last_stage = stage3(me, full_ref, bg)
            last_stage.load()
            last_stage.send()
        total[...] = ordered_total(me, dots_scr, slot) / DIM
        gout_ref[...] = ordered_total(me, gga_ref, ga_slot)

        def copies(i):
            rows = block_rows(i)
            return [pltpu.make_async_copy(d_scr.at[rows, :], d_ref.at[rows, :], d_sems.at[i]),
                    pltpu.make_async_remote_copy(
                        src_ref=d_scr.at[rows, :], dst_ref=pd_ref.at[rows, :], send_sem=pd_send.at[i],
                        recv_sem=pd_recv.at[i], device_id=(peer_of(me, 1),), device_id_type=MESH)]

        def last(i, carry):
            rows = block_rows(i)
            for n in range(2):
                dots = as_column(total[pl.ds(i + n * NB, 1), :])
                inv = as_column(inv_ref[pl.ds(i + n * NB, 1), :])
                for hh in range(LOC // HD):
                    sl = slice(hh * HD, (hh + 1) * HD)
                    unit = raw_ref[n, rows, sl] * inv
                    val = inv * (du_scr[n, hh, rows, :] - unit * dots)
                    d_scr[rows, n * LOC + hh * HD:n * LOC + (hh + 1) * HD] = val.astype(BF)
            start(copies(i))
            return carry

        lax.fori_loop(0, NB, last, 0)
        for i in range(NB):
            wait(copies(i))
        wait(moved)
        if not b:
            last_stage.wait()


def backward(b, da, qkv, wo, lse, raw, inv, gains, cos, sin, gga, weights, others, cid):
    def whole(*shape):
        return pl.BlockSpec(shape, lambda h, i: (0,) * len(shape))

    def picked(*shape):
        return pl.BlockSpec((None,) + shape, lambda h, i: (b,) + (0,) * len(shape))

    gsp = whole(8, DIM // 8)
    half = (DIM // 2, 3 * LOC)
    if b:
        extra = [sds((2, BLK, DIM // 2), F32)]
        own = [pltpu.VMEM((2,) + half, BF), pltpu.VMEM((2, 2, BLK, 3 * LOC), BF), pltpu.VMEM((2, BLK, DIM // 2), F32)]
    else:
        extra = [sds((SEQ, DIM), BF), sds(half, BF), sds((SEQ, DIM), BF)]
        own = [pltpu.VMEM((2, TOK, DIM), BF), pltpu.VMEM((2, TOK, DIM), BF)]
    return pl.pallas_call(
        functools.partial(backward_kernel, b),
        grid=(2, NB),
        in_specs=[pl.BlockSpec((None, 3, SEQ, HD), lambda h, i: (b, 0, 0, h)),
                  whole(LOC, DIM),
                  picked(2 * NB, BLK), picked(2, SEQ, LOC), picked(2 * NB, BLK),
                  pl.BlockSpec((2 + DIM // LOC, HD), lambda h, i: (0, h)), whole(SEQ, HD), whole(SEQ, HD), gsp]
        + [ANYWHERE] * (4 + len(others)),
        out_specs=[ANYWHERE, ANYWHERE, pl.BlockSpec((8, HD), lambda h, i: (0, h)), gsp] + [ANYWHERE] * len(extra),
        out_shape=[sds((SEQ, 3 * LOC), BF), sds((SEQ, 3 * LOC), BF), sds((8, LOC), F32), sds((8, DIM // 8), F32)] + extra,
        input_output_aliases={} if b else {12: 6},
        scratch_shapes=own + [
            pltpu.VMEM((NB, BLK, BLK), F32), pltpu.VMEM((NB, BLK, BLK), F32), pltpu.VMEM((HD, SEQ), BF),
            pltpu.VMEM((HD, BLK), F32), pltpu.VMEM((SEQ, HD), F32), pltpu.VMEM((SEQ, HD), F32),
            pltpu.VMEM((SEQ, HD), F32), pltpu.VMEM((2, 2, SEQ, HD), F32), pltpu.VMEM((SEQ, 3 * LOC), BF),
            pltpu.VMEM((SEQ, LOC), BF), pltpu.VMEM((2, BLK, DIM), BF), pltpu.VMEM((2 * NB, BLK), F32), pltpu.VMEM((2 * NB, BLK), F32),
            pltpu.VMEM((NDEV - 1, 2 * NB, BLK), F32), pltpu.VMEM((NDEV - 1, 8, DIM // 8), F32),
            DMA((2, NDEV - 1)), DMA((2, NDEV - 1)), DMA((NB,)), DMA((NB,)), DMA((NB,)), DMA((6,)), DMA((8,)), DMA((2,))]
        + ([] if b else BG_SEMS * 2),
        compiler_params=params(dimension_semantics=("arbitrary", "arbitrary"), collective_id=cid, has_side_effects=True),
        cost_estimate=cost(25e9, 30e6),
        name="backward",
    )(qkv, wo, lse, raw, inv, gains, cos, sin, gga, *weights, da, *others)


HALF = DIM // 2
CH = 256


def grads_kernel(d0, d1, pd0, pd1, wq, wk, wv, pw, got, x_full, o_all, da0, da1, dy_ref, dx_ref, gwq_ref, gwk_ref, gwv_ref, gwo_ref,
                 d_all, w_all, sbuf, r1, r2, fin, acc, xbuf, obuf,
                 dl_sems, w_sems, s1_sems, r1_sems, s2_sems, r2_sems, fs_sems, fr_sems, x_sems, o_sems):
    me = lax.axis_index('tp')
    core, partner, first, second = route(me)
    chip = me // 2
    diag_chip, first_chip, second_chip = peer_of(me, 6) // 2, first // 2, second // 2

    barrier = pltpu.get_barrier_semaphore()
    for dev in (partner, first, second):
        pl.semaphore_signal(barrier, inc=1, device_id=(dev,), device_id_type=MESH)
    pl.semaphore_wait(barrier, 3)

    def rows_of(blk):
        return pl.ds(pl.multiple_of(blk * BLK, BLK), BLK)

    chips = (diag_chip, first_chip, second_chip, chip)
    w_copies = [pltpu.make_async_copy(w.at[half_rows(core), :], w_all.at[0, :, pl.ds(n * LOC, LOC)], w_sems.at[n])
                for n, w in enumerate((wq, wk, wv))]
    w_copies.append(pltpu.make_async_copy(pw, w_all.at[1], w_sems.at[3]))
    loads = []
    for n in range(8):
        rows, b = rows_of(chips[n // 2]), n % 2
        loads.append([pltpu.make_async_copy(d.at[rows, :], d_all.at[side, b, rows, :], dl_sems.at[side, n])
                      for side, d in enumerate(((d0, d1)[b], (pd0, pd1)[b]))])
    start(w_copies)
    start(loads[1])
    wait(w_copies)

    def partial(b, blk):
        rows = rows_of(blk)
        return dot(d_all[0, b, rows, :], w_all[0], NT) + dot(d_all[1, b, rows, :], w_all[1], NT)

    def to_first(n):
        return pltpu.make_async_remote_copy(
            src_ref=sbuf.at[n // 2], dst_ref=r1.at[n], send_sem=s1_sems.at[n], recv_sem=r1_sems.at[n],
            device_id=(first,), device_id_type=MESH)

    def to_second(b):
        return pltpu.make_async_remote_copy(
            src_ref=r1.at[b], dst_ref=r2.at[b], send_sem=s2_sems.at[b], recv_sem=r2_sems.at[b],
            device_id=(second,), device_id_type=MESH)

    def to_partner(b):
        return pltpu.make_async_remote_copy(
            src_ref=r1.at[2 + b, pl.ds(pl.multiple_of((1 - core) * TOK, TOK), TOK), :], dst_ref=fin.at[b],
            send_sem=fs_sems.at[b], recv_sem=fr_sems.at[b], device_id=(partner,), device_id_type=MESH)

    taken = [pltpu.make_async_copy(got.at[n], r1.at[2 * n], w_sems.at[4 + n]) for n in range(2)]
    for n in (1, 3):
        wait(loads[n])
        if n == 1:
            start(loads[3])
        sbuf[n // 2] = partial(1, chips[n // 2])
        to_first(n).start()
        if n == 1:
            start(taken)
            for later in (4, 0, 2, 5, 6, 7):
                start(loads[later])
    for n in (0, 2, 4, 5, 6, 7):
        wait(loads[n])
    wait(taken)

    steps = SEQ // CH

    def chunk(i):
        return pl.ds(pl.multiple_of(i * CH, CH), CH)

    def stream(pairs, body):
        def fetch(i):
            return [pltpu.make_async_copy(src.at[chunk(i), :], buf.at[i % 2], sems.at[i % 2]) for src, buf, sems in pairs]

        for c in fetch(0):
            c.start()

        def it(i, carry):
            @pl.when(i + 1 < steps)
            def _():
                for c in fetch(i + 1):
                    c.start()

            for c in fetch(i):
                c.wait()
            body(i)
            return carry

        lax.fori_loop(0, steps, it, 0)

    def wgrad(b, src):
        def body(i):
            left = d_all[0, b, chunk(i), :].T
            for c in range(3):
                part = slice(c * LOC, (c + 1) * LOC)
                acc[part, :] += dot(left[part, :], xbuf[i % 2])

        stream([(src, xbuf, x_sems)], body)

    def forward_second(b):
        if b:
            to_first(b).wait_recv()
        r1[b] += partial(b, second_chip)
        to_second(b).start()

    forward_second(0)
    acc[...] = jnp.zeros_like(acc)
    wgrad(0, x_full.at[0])
    wgrad(1, x_full.at[1])
    for n, ref in enumerate((gwq_ref, gwk_ref, gwv_ref)):
        ref[...] = acc[n * LOC:(n + 1) * LOC, :].T.astype(BF)
    forward_second(1)
    acc[:LOC, :] = jnp.zeros((LOC, DIM), F32)

    def wo_body(i):
        acc[:LOC, :] += dot(obuf[i % 2].T, xbuf[i % 2])

    for o_src, da_src in ((o_all.at[0], da0), (o_all.at[1], da1)):
        stream([(da_src, xbuf, x_sems), (o_src, obuf, o_sems)], wo_body)
    gwo_ref[...] = acc[:LOC, :].astype(BF)

    def own_part(b, carry):
        r1_own = partial(b, chip)
        pl.when(b == 1)(to_first(3).wait_recv)
        to_second(b).wait_recv()
        r1[2 + b] += r1_own + r2[b]
        to_partner(b).start()
        cols = half_rows(core)
        rows = pl.ds(pl.multiple_of(core * TOK, TOK), TOK)
        dx_ref[b, :, cols] = (r1[2 + b, rows, :] + dy_ref[b, :, cols].astype(F32)).astype(BF)
        return carry

    lax.fori_loop(0, 2, own_part, 0)

    def finish(b, carry):
        to_partner(b).wait()
        cols = half_rows(1 - core)
        dx_ref[b, :, cols] = (fin[b] + dy_ref[b, :, cols].astype(F32)).astype(BF)
        to_second(b).wait_send()
        return carry

    to_first(1).wait_send()
    to_first(3).wait_send()
    lax.fori_loop(0, 2, finish, 0)


def grads(d0, d1, pd0, pd1, wq, wk, wv, pw, got, x_full, o_all, da0, da1, dy, cid):
    vm = pl.BlockSpec(memory_space=pltpu.VMEM)
    far = pl.BlockSpec(memory_space=pl.ANY)
    dma = pltpu.SemaphoreType.DMA
    return pl.pallas_call(
        grads_kernel,
        in_specs=[far] * 13 + [vm],
        out_specs=[vm] * 5,
        out_shape=[sds((2, TOK, DIM), BF)] + [sds((DIM, LOC), BF)] * 3 + [sds((LOC, DIM), BF)],
        scratch_shapes=[pltpu.VMEM((2, 2, SEQ, 3 * LOC), BF), pltpu.VMEM((2, HALF, 3 * LOC), BF),
                        pltpu.VMEM((2, BLK, HALF), F32), pltpu.VMEM((4, BLK, HALF), F32), pltpu.VMEM((2, BLK, HALF), F32),
                        pltpu.VMEM((2, TOK, HALF), F32), pltpu.VMEM((3 * LOC, DIM), F32),
                        pltpu.VMEM((2, CH, DIM), BF), pltpu.VMEM((2, CH, LOC), BF),
                        dma((2, 8)), dma((9,)), dma((4,)), dma((4,)), dma((2,)), dma((2,)),
                        dma((2,)), dma((2,)), dma((2,)), dma((2,))],
        compiler_params=pltpu.CompilerParams(vmem_limit_bytes=67043328, collective_id=cid, has_side_effects=True),
        cost_estimate=cost(100e9, 40e6),
        name="grads",
    )(d0, d1, pd0, pd1, wq, wk, wv, pw, got, x_full, o_all, da0, da1, dy)


def deliver_kernel(*refs):
    count = (len(refs) - 2) // 3
    srcs, dsts, bufs = refs[:count], refs[count:2 * count], refs[2 * count:3 * count]
    loads = [pltpu.make_async_copy(src, buf, refs[-2].at[n]) for n, (src, buf) in enumerate(zip(srcs, bufs))]
    stores = [pltpu.make_async_copy(buf, dst, refs[-1].at[n]) for n, (buf, dst) in enumerate(zip(bufs, dsts))]
    start(loads)
    for load, store in zip(loads, stores):
        load.wait()
        store.start()
    wait(stores)


def deliver(*arrays):
    return pl.pallas_call(
        deliver_kernel,
        in_specs=[ANYWHERE] * len(arrays),
        out_specs=[ANYWHERE] * len(arrays),
        out_shape=[sds(t.shape, t.dtype) for t in arrays],
        scratch_shapes=[pltpu.VMEM(t.shape, t.dtype) for t in arrays] + [DMA((len(arrays),)), DMA((len(arrays),))],
        compiler_params=params(),
        cost_estimate=cost(1e9, 16e6),
        name="deliver",
    )(*arrays)


def local_block(x_loc, wq, wk, wv, wo, gq, gk, ga, dy_loc):
    gains = jnp.concatenate([gq, gk, ga]).astype(F32).reshape(2 + DIM // LOC, LOC)
    weights = (wq, wk, wv)
    cos, sin, inv, o, lse, raw, qkv, o_recv, x_full, wo_full = forward(x_loc, wq, wk, wv, wo, gains, 0)
    y, da, gga, da0 = out_block(o_recv, wo_full, x_loc, dy_loc, gains, 1)
    state = (qkv, wo, lse, raw, inv, gains, cos, sin, gga, weights)
    d0, pd0, gg0, gout, da1, pw, da0 = backward(0, da0, *state, (da,), 2)
    d1, pd1, gg1, _, got = backward(1, da1, *state, (d0, pd0, pw), 3)
    grad_ga = gout.reshape(DIM).astype(BF)
    big = grads(d0, d1, pd0, pd1, *weights, pw, got, x_full, o, da0, da1, dy_loc, 4)
    y, dx, gwq, gwk, gwv, gwo = deliver(y, *big)
    gg = gg0 + gg1
    return (y, dx, gwq, gwk, gwv, gwo, gg[0].astype(BF), gg[1].astype(BF), grad_ga)


def solution(mesh):
    act, col, row, vec = P(None, 'tp', None), P(None, 'tp'), P('tp', None), P('tp')
    in_specs = (act, col, col, col, row, vec, vec, P(), act)
    out_specs = (act, act, col, col, col, row, vec, vec, P())
    return jax.shard_map(local_block, mesh=mesh, in_specs=in_specs, out_specs=out_specs, check_vma=False)
```

```python
import functools
import math

import jax
import jax.numpy as jnp
import numpy as np
from jax import lax
from jax.experimental import pallas as pl
from jax.experimental.pallas import tpu as pltpu
from jax.sharding import PartitionSpec as P

HD = 128
ROPE_THETA = 500000.0
EPS = 1e-6
DIM = 2048
SEQ = 2048
LOC = 256
TOK = 256
BLK = 512
NB = SEQ // BLK
NDEV = 8
SCALE = HD ** -0.5
C2 = SCALE * math.log2(math.e)
MESH = pl.DeviceIdType.MESH
BF = jnp.bfloat16
F32 = jnp.float32
VMEM_MAX = 60 * 1024 * 1024

NT = (((1,), (1,)), ((), ()))
NN = (((1,), (0,)), ((), ()))


def dot(a, b, dims=NN):
    return lax.dot_general(a, b, dims, preferred_element_type=F32)


def sds(shape, dtype):
    return jax.ShapeDtypeStruct(shape, dtype)


def cost(flops, nbytes, trans=0):
    return pl.CostEstimate(flops=int(flops), bytes_accessed=int(nbytes), transcendentals=int(trans))


def params(**kw):
    return pltpu.CompilerParams(vmem_limit_bytes=VMEM_MAX, **kw)


def peer_of(me, mask):
    core, ax, ay = me % 2, (me // 2) % 2, me // 4
    core = 1 - core if mask & 1 else core
    ax = 1 - ax if mask & 2 else ax
    ay = 1 - ay if mask & 4 else ay
    return ay * 4 + ax * 2 + core


ORDER = (6, 7, 2, 4, 3, 5, 1)


def entry_barrier(me):
    barrier = pltpu.get_barrier_semaphore()
    for mask in ORDER:
        pl.semaphore_signal(barrier, inc=1, device_id=(peer_of(me, mask),), device_id_type=MESH)
    pl.semaphore_wait(barrier, NDEV - 1)


def nbr_signal(me):
    for mask in (1, 2, 4):
        pl.semaphore_signal(pltpu.get_barrier_semaphore(), inc=1, device_id=(peer_of(me, mask),), device_id_type=MESH)


def nbr_wait():
    pl.semaphore_wait(pltpu.get_barrier_semaphore(), 3)


DMA = pltpu.SemaphoreType.DMA
ANYWHERE = pl.BlockSpec(memory_space=pl.ANY)
BG_SEMS = [DMA((11,)), DMA((11,)), DMA((5,))]
BG = BG_SEMS + [pltpu.VMEM((2, TOK, DIM), BF)]


def shard_rows(dev, lo=0, count=TOK):
    return pl.ds(pl.multiple_of(dev * TOK + lo, HD), count)


class Stage:
    def __init__(self, loads, copies):
        self.loads, self.copies = loads, copies

    def load(self):
        start(self.loads)

    def send(self):
        wait(self.loads)
        start(self.copies)

    def wait(self, *which):
        wait([self.copies[n] for n in which] or self.copies)


def stage1(me, src, full, bg, part=None):
    send, recv, own, buf = bg
    lo, count, at = (0, TOK, 0) if part is None else (part * (TOK // 2), TOK // 2, 8 * part)
    there = full.at[shard_rows(me, lo, count), :]
    mine = buf.at[0, pl.ds(lo, count), :]
    copies = [pltpu.make_async_remote_copy(
        src_ref=mine, dst_ref=there, send_sem=send.at[at + k], recv_sem=recv.at[at + k],
        device_id=(peer_of(me, mask),), device_id_type=MESH) for k, mask in enumerate((2, 4, 1))]
    loads = [] if part == 1 or src is None else [pltpu.make_async_copy(src, buf.at[0], own.at[0])]
    return Stage(loads, copies + [pltpu.make_async_copy(mine, there, own.at[3 if part == 1 else 2])])


def stage2(me, full, bg):
    send, recv, own, buf = bg
    xn, yn = peer_of(me, 2), peer_of(me, 4)
    half = TOK // 2
    plan = ((1, half, half, yn, 2), (0, 0, half, xn, 4), (0, 0, TOK, xn, 1), (1, 0, TOK, yn, 1))
    return Stage(
        [pltpu.make_async_copy(full.at[shard_rows(dev), :], buf.at[n], own.at[n]) for n, dev in enumerate((xn, yn))],
        [pltpu.make_async_remote_copy(
            src_ref=buf.at[slot, pl.ds(lo, count), :], dst_ref=full.at[shard_rows(dev, lo, count), :],
            send_sem=send.at[3 + k], recv_sem=recv.at[3 + k], device_id=(peer_of(me, mask),), device_id_type=MESH)
         for k, (slot, lo, count, dev, mask) in enumerate(plan)])


def stage3(me, full, bg):
    send, recv, own, buf = bg
    rows = full.at[shard_rows(peer_of(me, 6)), :]
    return Stage([pltpu.make_async_copy(rows, buf.at[1], own.at[1])], [pltpu.make_async_remote_copy(
        src_ref=buf.at[1], dst_ref=rows, send_sem=send.at[7], recv_sem=recv.at[7],
        device_id=(peer_of(me, 1),), device_id_type=MESH)])


def route(me):
    core = me % 2
    first = peer_of(me, 2) * (1 - core) + peer_of(me, 4) * core
    second = peer_of(me, 4) * (1 - core) + peer_of(me, 2) * core
    return core, peer_of(me, 1), first, second


def half_rows(c):
    return pl.ds(pl.multiple_of(c * (DIM // 2), DIM // 2), DIM // 2)


def start(copies):
    for c in copies:
        c.start()


def wait(copies):
    for c in copies:
        c.wait()


def row_sums(vals):
    folded = vals[:, :HD]
    for start in range(HD, vals.shape[1], HD):
        folded = folded + vals[:, start:start + HD]
    return jnp.sum(folded.T, axis=0, keepdims=True)


def as_column(row):
    return jnp.broadcast_to(row, (HD, row.shape[1])).T


def exchange(me, srcs, slots, send_sems, recv_sems):
    copies = []
    for n, (src, slot) in enumerate(zip(srcs, slots)):
        for p, mask in enumerate(ORDER):
            copies.append(pltpu.make_async_remote_copy(
                src_ref=src, dst_ref=slot.at[p], send_sem=send_sems.at[n, p], recv_sem=recv_sems.at[n, p],
                device_id=(peer_of(me, mask),), device_id_type=MESH))
    return copies


def ordered_total(me, src, slot):
    own = src[...]
    total = jnp.zeros_like(own)
    for dev in range(NDEV):
        term = jnp.where(me == dev, own, 0.0)
        for p, mask in enumerate(ORDER):
            term = term + jnp.where(peer_of(me, mask) == dev, slot[p], 0.0)
        total = total + term
    return total


def causal_mask():
    keys = lax.broadcasted_iota(jnp.int32, (BLK, BLK), 0)
    queries = lax.broadcasted_iota(jnp.int32, (BLK, BLK), 1)
    return keys <= queries


def block_rows(i):
    return pl.ds(pl.multiple_of(i * BLK, BLK), BLK)


def head_cols(h):
    return pl.ds(pl.multiple_of(h * HD, HD), HD)


def forward_kernel(freq_ref, wq_ref, wk_ref, wv_ref, gains_ref, x_ref, wo_ref,
                   cos_ref, sin_ref, inv_ref, o_ref, lse_ref, raw_ref, qkv_ref, both_ref, full_ref, wof_ref,
                   raw, qkv, xbuf, sums_scr, slot, p_scr, vt_scr, acc_scr, o_scr, buf0, buf1,
                   ex_send, ex_recv, out_sems, send_sems, recv_sems, own_sems, x_sems, *bg_sems):
    g = pl.program_id(0)
    b, t = g // (4 * NB), g % (4 * NB)
    me = lax.axis_index('tp')
    bg0, bg1, bg2 = (*bg_sems[:3], buf0), (*bg_sems[3:6], buf1), (*bg_sems[6:], buf0)
    x0f, x1f = full_ref.at[0], full_ref.at[1]

    def x_gather(part=None):
        return stage1(me, x_ref.at[1], x1f, bg1, part)

    def wo_gather(part=None):
        return stage1(me, wo_ref, wof_ref, bg2, part)

    def keep(bb):
        return [pltpu.make_async_copy(raw, raw_ref.at[bb], out_sems.at[0]),
                pltpu.make_async_copy(qkv, qkv_ref.at[bb], out_sems.at[1])]

    def sums(bb):
        return exchange(me, [sums_scr.at[bb]], [slot.at[bb]], ex_send.at[bb], ex_recv.at[bb])

    def fetch(bb, i):
        return pltpu.make_async_copy(full_ref.at[bb, block_rows(i), :], xbuf.at[i % 2], x_sems.at[i % 2])

    def block_copy(bb, hh, st, half):
        dest = 2 * ((me // 2 + 1 + st) % NB) + half
        part = o_scr.at[bb, hh, st, pl.ds(half * TOK, TOK), :]
        dst = both_ref.at[bb, :, pl.ds(pl.multiple_of(me * LOC + hh * HD, HD), HD)]
        away = pltpu.make_async_remote_copy(
            src_ref=part, dst_ref=dst, send_sem=send_sems.at[bb, hh, st, half], recv_sem=recv_sems.at[bb, hh, me],
            device_id=(dest,), device_id_type=MESH)
        return dest, away, pltpu.make_async_copy(part, dst, own_sems.at[bb, hh])

    def run(stage):
        stage.load()
        stage.send()

    @pl.when(g == 0)
    def _():
        first = stage1(me, x_ref.at[0], x0f, bg0)
        first.load()
        entry_barrier(me)
        first.send()
        x_gather(0).load()
        freq = freq_ref[...]
        sign = jnp.where(lax.broadcasted_iota(jnp.int32, (TOK, HD), 1) < HD // 2, -1.0, 1.0)

        def table(i, carry):
            rows = pl.ds(pl.multiple_of(i * TOK, TOK), TOK)
            pos = (lax.broadcasted_iota(jnp.int32, (TOK, HD), 0) + i * TOK).astype(F32)
            angle = pos * freq
            cos_ref[rows, :] = jnp.cos(angle)
            sin_ref[rows, :] = jnp.sin(angle) * sign
            return carry

        lax.fori_loop(0, SEQ // TOK, table, 0)
        first.wait()
        second, third = stage2(me, x0f, bg0), stage3(me, x0f, bg0)
        run(second)
        x_gather(0).send()
        second.wait()
        run(third)
        third.wait()
        fetch(0, 0).start()

    @pl.when(g == 2 * NB + 2)
    def _():
        x_gather(0).wait()
        x_gather(1).wait()
        run(stage2(me, x1f, bg1))
        run(wo_gather(0))

    @pl.when(g == 4 * NB)
    def _():
        stage2(me, x1f, bg1).wait()
        third = stage3(me, x1f, bg1)
        run(third)
        for c in keep(0):
            c.wait()
        third.wait()
        fetch(1, 0).start()

    @pl.when(g == 6 * NB + 2)
    def _():
        wo_gather(0).wait()
        wo_gather(1).wait()
        run(stage2(me, wof_ref, bg2))

    @pl.when(t < NB)
    def _():
        rows = block_rows(t)

        @pl.when(t < NB - 1)
        def _():
            fetch(b, t + 1).start()

        fetch(b, t).wait()
        x = xbuf[t % 2]
        for n, w_ref in enumerate((wq_ref, wk_ref)):
            val = dot(x, w_ref[...])
            raw[n, rows, :] = val
            sums_scr[b, pl.ds(t + n * NB, 1), :] = row_sums(val * val)
        qkv[2, rows, :] = dot(x, wv_ref[...]).astype(BF)

    @pl.when(t == NB)
    def _():
        start(sums(b))
        keep(b)[0].start()
        pl.when(b == 0)(x_gather(1).send)
        pl.when(b == 1)(wo_gather(1).send)
        wait(sums(b))
        inv_ref[...] = lax.rsqrt(ordered_total(me, sums_scr.at[b], slot.at[b]) / DIM + EPS)

    @pl.when(jnp.logical_and(t >= NB, t < 2 * NB))
    def _():
        i = t - NB
        rows = block_rows(i)
        cos, sin = cos_ref[rows, :], sin_ref[rows, :]
        for n in range(2):
            inv = as_column(inv_ref[pl.ds(i + n * NB, 1), :])
            gain = gains_ref[n:n + 1, :]
            for h in range(LOC // HD):
                sl = slice(h * HD, (h + 1) * HD)
                hat = raw[n, rows, sl] * inv * gain[:, sl]
                qkv[n, rows, sl] = (hat * cos + pltpu.roll(hat, HD // 2, 1) * sin).astype(BF)

    @pl.when(t == 2 * NB)
    def _():
        keep(b)[1].start()

    @pl.when(t >= 2 * NB)
    def _():
        h, step = t // NB - 2, t % NB
        qi = (me // 2 + 1 + step) % NB
        cols = head_cols(h)

        @pl.when(step == 0)
        def _():
            vt_scr[...] = qkv[2, :, cols].T

        qb = qkv[0, block_rows(qi), cols]

        def scores(j):
            return dot(qkv[1, block_rows(j), cols], qb, NT)

        def first(j, m):
            s = scores(j)
            p_scr[j] = s
            return jnp.maximum(m, jnp.max(s.reshape(BLK // 8, 8, BLK), axis=0))

        s = jnp.where(causal_mask(), scores(qi), -1e30)
        p_scr[qi] = s
        m = lax.fori_loop(0, qi, first, jnp.max(s.reshape(BLK // 8, 8, BLK), axis=0))
        m = jnp.max(m, axis=0, keepdims=True)

        def second(j, l):
            p = jnp.exp2((p_scr[j] - m) * C2)
            p_scr[j] = p
            return l + jnp.sum(p.reshape(BLK // 8, 8, BLK), axis=0)

        l = lax.fori_loop(0, qi + 1, second, jnp.zeros((8, BLK), F32))
        l = jnp.sum(l, axis=0, keepdims=True)
        rl = 1.0 / l
        lse_ref[pl.ds(h * NB + qi, 1), :] = m * C2 + jnp.log2(l)

        acc_scr[...] = jnp.zeros_like(acc_scr)

        def third(j, carry):
            p = (p_scr[j] * rl).astype(BF)
            acc_scr[...] += dot(vt_scr[:, block_rows(j)], p)
            return carry

        lax.fori_loop(0, qi + 1, third, 0)
        out = acc_scr[...].T.astype(BF)
        o_scr[b, h, step] = out
        o_ref[block_rows(qi), cols] = out

        for half in range(2):
            dest, away, here = block_copy(b, h, step, half)
            pl.when(dest != me)(away.start)
            pl.when(dest == me)(here.start)

    @pl.when(g == 8 * NB - 1)
    def _():
        stage2(me, wof_ref, bg2).wait()
        third = stage3(me, wof_ref, bg2)
        run(third)
        for c in keep(1):
            c.wait()

        def drain(n, carry):
            bb, hh = n // 2, n % 2
            for st in range(NB):
                for half in range(2):
                    dest, away, here = block_copy(bb, hh, st, half)
                    if st < NB - 1:
                        away.wait_send()
                    else:
                        pl.when(dest != me)(away.wait_send)
                        pl.when(dest == me)(here.wait)
            for mask in ORDER:
                peer = peer_of(me, mask)
                pltpu.make_async_remote_copy(
                    src_ref=o_scr.at[0, 0, 0, pl.ds(0, TOK), :],
                    dst_ref=both_ref.at[bb, :, pl.ds(pl.multiple_of(peer * LOC + hh * HD, HD), HD)],
                    send_sem=send_sems.at[0, 0, 0, 0], recv_sem=recv_sems.at[bb, hh, peer],
                    device_id=(peer,), device_id_type=MESH).wait_recv()
            return carry

        lax.fori_loop(0, 4, drain, 0)
        third.wait()


def forward(x, wq, wk, wv, wo, gains, cid):
    inv_freq = np.float32(1.0) / np.float32(ROPE_THETA) ** (np.arange(HD // 2, dtype=np.float32) / np.float32(HD // 2))
    freq = jnp.asarray(np.concatenate([inv_freq, inv_freq])[None, :], F32)

    def whole(*shape):
        return pl.BlockSpec(shape, lambda g: (0,) * len(shape))

    def per_batch(*shape):
        return pl.BlockSpec((None,) + shape, lambda g: (g // (4 * NB),) + (0,) * len(shape))

    wspec, rows = whole(DIM, LOC), per_batch(2 * NB, BLK)
    return pl.pallas_call(
        forward_kernel,
        grid=(8 * NB,),
        in_specs=[whole(1, HD), wspec, wspec, wspec, whole(2 + DIM // LOC, LOC), ANYWHERE, ANYWHERE],
        out_specs=[whole(SEQ, HD), whole(SEQ, HD), rows, per_batch(SEQ, LOC), rows] + [ANYWHERE] * 5,
        out_shape=[sds((SEQ, HD), F32), sds((SEQ, HD), F32), sds((2, 2 * NB, BLK), F32), sds((2, SEQ, LOC), BF),
                   sds((2, 2 * NB, BLK), F32), sds((2, 2, SEQ, LOC), F32), sds((2, 3, SEQ, LOC), BF),
                   sds((2, TOK, DIM), BF), sds((2, SEQ, DIM), BF), sds((SEQ, DIM), BF)],
        scratch_shapes=[pltpu.VMEM((2, SEQ, LOC), F32), pltpu.VMEM((3, SEQ, LOC), BF), pltpu.VMEM((2, BLK, DIM), BF),
                        pltpu.VMEM((2, 2 * NB, BLK), F32), pltpu.VMEM((2, NDEV - 1, 2 * NB, BLK), F32),
                        pltpu.VMEM((NB, BLK, BLK), F32), pltpu.VMEM((HD, SEQ), BF), pltpu.VMEM((HD, BLK), F32),
                        pltpu.VMEM((2, 2, NB, BLK, HD), BF), pltpu.VMEM((2, TOK, DIM), BF), pltpu.VMEM((2, TOK, DIM), BF),
                        DMA((2, 1, NDEV - 1)), DMA((2, 1, NDEV - 1)), DMA((2,)),
                        DMA((2, 2, NB, 2)), DMA((2, 2, NDEV)), DMA((2, 2)), DMA((2,))] + BG_SEMS * 3,
        compiler_params=params(dimension_semantics=("arbitrary",), collective_id=cid, has_side_effects=True),
        cost_estimate=cost(60e9, 60e6),
        name="forward",
    )(freq, wq, wk, wv, gains, x, wo)


def out_kernel(o_ref, x_ref, dy_ref, gains_ref, wo_ref, y_ref, da_ref, gga_ref, full_ref, wo_scr, a_scr, wo_sems, buf, *bg_sems):
    b = pl.program_id(0)
    me = lax.axis_index('tp')
    bg = (*bg_sems, buf)
    step = DIM // NB

    def piece(j):
        cols = pl.ds(pl.multiple_of(j * step, step), step)
        return cols, pltpu.make_async_copy(wo_ref.at[:, cols], wo_scr.at[:, cols], wo_sems.at[j])

    @pl.when(b == 0)
    def _():
        nbr_signal(me)
        for j in range(NB):
            piece(j)[1].start()
        gga_ref[...] = jnp.zeros_like(gga_ref)

    o = o_ref[0]

    def fwd(j, carry):
        cols, load = piece(j)
        pl.when(b == 0)(load.wait)
        a_scr[:, cols] = dot(o, wo_scr[:, cols])
        return carry

    lax.fori_loop(0, NB, fwd, 0)
    a = a_scr[...]
    r = lax.rsqrt(jnp.mean(a * a, axis=-1, keepdims=True) + EPS)
    n = a * r
    ga = jnp.concatenate([gains_ref[2 + i:3 + i, :] for i in range(8)], axis=1)
    dy = dy_ref[0].astype(F32)
    gn = dy * ga
    da = (r * (gn - n * jnp.mean(gn * n, axis=-1, keepdims=True))).astype(BF)
    da_ref[0] = da

    @pl.when(b == 0)
    def _():
        buf[0] = da
        nbr_wait()
        stage1(me, None, full_ref, bg).send()

    y_ref[0] = (x_ref[0].astype(F32) + n * ga).astype(BF)
    col = jnp.sum(dy * n, axis=0, keepdims=True)
    for i in range(8):
        gga_ref[i:i + 1, :] += col[:, i * LOC:(i + 1) * LOC]

    @pl.when(b == 1)
    def _():
        stage1(me, None, full_ref, bg).wait()


def out_block(o, wo, x, dy, gains, cid):
    def whole(*shape):
        return pl.BlockSpec(shape, lambda i: (0,) * len(shape))

    batch = pl.BlockSpec((1, TOK, DIM), lambda i: (i, 0, 0))
    return pl.pallas_call(
        out_kernel,
        grid=(2,),
        in_specs=[batch, batch, batch, whole(2 + DIM // LOC, LOC), ANYWHERE],
        out_specs=[batch, batch, whole(8, DIM // 8), ANYWHERE],
        out_shape=[sds((2, TOK, DIM), BF), sds((2, TOK, DIM), BF), sds((8, DIM // 8), F32), sds((SEQ, DIM), BF)],
        scratch_shapes=[pltpu.VMEM((DIM, DIM), BF), pltpu.VMEM((TOK, DIM), F32), DMA((NB,)),
                        pltpu.VMEM((2, TOK, DIM), BF)] + BG_SEMS,
        compiler_params=params(dimension_semantics=("arbitrary",), collective_id=cid, has_side_effects=True),
        cost_estimate=cost(8 * TOK * DIM * DIM + 5e9, 18e6),
        name="out_block",
    )(o, x, dy, gains, wo)


def backward_kernel(b, qkv_ref, wo_ref, lse_ref, raw_hbm, inv_ref, gains_ref, cos_hbm, sin_hbm, gga_ref,
                    wq_ref, wk_ref, wv_ref, da_ref, *rest):
    if b:
        d0_ref, pd0_ref, pw_ref, d_ref, pd_ref, gg_ref, gout_ref, got_ref, w_all, d_two, sbuf, *rest = rest
    else:
        shard_ref, d_ref, pd_ref, gg_ref, gout_ref, full_ref, pw_ref, da_ref, buf0, buf1, w_half, *rest = rest
    (p_scr, dp_scr, kt_scr, dqt_scr, dq_scr, dk_scr, dv_scr, du_scr, d_scr, dh_scr, dbuf, dots_scr, total, slot, ga_slot,
     ex_send, ex_recv, pd_send, pd_recv, d_sems, rs_sems, ld_sems, db_sems, raw_ref, cos_ref, sin_ref, tb_sems, *bg_sems) = rest
    h, step = pl.program_id(0), pl.program_id(1)
    me = lax.axis_index('tp')

    def chip_at(n):
        ax, ay = (me // 2) % 2, me // 4
        return (ay + (n // 2) * (1 - 2 * ay)) * 2 + ax + (n % 2) * (1 - 2 * ax)

    def fetch(n):
        return pltpu.make_async_copy(da_ref.at[block_rows(chip_at(n)), :], dbuf.at[n % 2], db_sems.at[n % 2])

    qi = chip_at(step)
    tables = [pltpu.make_async_copy(src, dst, tb_sems.at[n]) for n, (src, dst) in enumerate(
        ((raw_hbm.at[b], raw_ref), (cos_hbm, cos_ref), (sin_hbm, sin_ref)))]
    core, partner, first_dev, _ = route(me)
    weights = (wq_ref, wk_ref, wv_ref)

    if b:
        operands = []
        for blk, chip in enumerate((peer_of(me, 6) // 2, first_dev // 2)):
            operands += [pltpu.make_async_copy(d.at[block_rows(chip), :], d_two.at[blk, n], ld_sems.at[2 * blk + n])
                         for n, d in enumerate((d0_ref, pd0_ref))]
        operands += [pltpu.make_async_copy(w.at[half_rows(core), :], w_all.at[0, :, pl.ds(n * LOC, LOC)], ld_sems.at[4 + n])
                     for n, w in enumerate(weights)]
        operands.append(pltpu.make_async_copy(pw_ref, w_all.at[1], ld_sems.at[7]))
        moved = [pltpu.make_async_remote_copy(
            src_ref=sbuf.at[blk, pl.ds(lo, count), :], dst_ref=got_ref.at[blk, pl.ds(lo, count), :], send_sem=rs_sems.at[n],
            recv_sem=rs_sems.at[3 + n], device_id=(first_dev,), device_id_type=MESH)
            for n, (blk, lo, count) in enumerate(((0, 0, BLK), (1, 0, BLK // 2), (1, BLK // 2, BLK // 2)))]
    else:
        bg0, bg = (*bg_sems[:3], buf0), (*bg_sems[3:], buf1)
        older2, older3 = stage2(me, da_ref, bg0), stage3(me, da_ref, bg0)
        gather = stage1(me, shard_ref.at[1], full_ref, bg)
        operands = [pltpu.make_async_copy(w.at[half_rows(1 - core), :], w_half.at[:, pl.ds(n * LOC, LOC)], ld_sems.at[n])
                    for n, w in enumerate(weights)]
        moved = [pltpu.make_async_remote_copy(
            src_ref=w_half, dst_ref=pw_ref, send_sem=rs_sems.at[0], recv_sem=rs_sems.at[3], device_id=(partner,),
            device_id_type=MESH)]

    @pl.when(jnp.logical_and(h == 0, step == 0))
    def _():
        if b:
            start(operands)
            fetch(0).start()
            start(tables)
            entry_barrier(me)
            wait(operands)
            for blk in range(2):
                sbuf[blk] = dot(d_two[blk, 0], w_all[0], NT) + dot(d_two[blk, 1], w_all[1], NT)
                moved[blk].start()
        else:
            older2.load()
            fetch(0).start()
            gather.load()
            start(operands)
            start(tables)
            entry_barrier(me)
            older2.send()
            gather.send()
            wait(operands)
            start(moved)
        dots_scr[...] = jnp.zeros_like(dots_scr)

    if not b:
        @pl.when(jnp.logical_and(h == 0, step == NB - 1))
        def _():
            older3.wait()
            fetch(NB - 1).start()

        @pl.when(jnp.logical_and(h == 1, step == 2))
        def _():
            gather.wait()
            more = stage2(me, full_ref, bg)
            more.load()
            more.send()

    @pl.when(h == 0)
    def _():
        fetch(step).wait()
        dh_scr[block_rows(qi), :] = dot(dbuf[step % 2], wo_ref[...], NT).astype(BF)
        if b:
            @pl.when(step < NB - 1)
            def _():
                fetch(step + 1).start()
        else:
            @pl.when(step == 0)
            def _():
                older2.wait(2, 3)

            @pl.when(step < NB - 2)
            def _():
                fetch(step + 1).start()

            @pl.when(step == NB - 2)
            def _():
                older2.wait(0, 1)
                older3.load()
                older3.send()

    @pl.when(step == 0)
    def _():
        kt_scr[...] = qkv_ref[1].T
        dk_scr[...] = jnp.zeros_like(dk_scr)
        dv_scr[...] = jnp.zeros_like(dv_scr)

    qb = qkv_ref[0, block_rows(qi), :]
    dob = dh_scr[block_rows(qi), head_cols(h)]
    lse = lse_ref[pl.ds(h * NB + qi, 1), :]

    def first(j, acc, diag=False):
        rows = block_rows(j)
        p = jnp.exp2(dot(qkv_ref[1, rows, :], qb, NT) * C2 - lse)
        if diag:
            p = jnp.where(causal_mask(), p, 0.0)
        dp = dot(qkv_ref[2, rows, :], dob, NT)
        p_scr[j] = p
        dp_scr[j] = dp
        dv_scr[rows, :] += dot(p.astype(BF), dob)
        return acc + jnp.sum((p * dp).reshape(BLK // 8, 8, BLK), axis=0)

    acc = first(qi, jnp.zeros((8, BLK), F32), True)
    acc = lax.fori_loop(0, qi, first, acc)
    delta = jnp.sum(acc, axis=0, keepdims=True)
    dqt_scr[...] = jnp.zeros_like(dqt_scr)

    def second(j, carry):
        rows = block_rows(j)
        ds = (p_scr[j] * (dp_scr[j] - delta) * SCALE).astype(BF)
        dk_scr[rows, :] += dot(ds, qb)
        dqt_scr[...] += dot(kt_scr[:, rows], ds)
        return carry

    lax.fori_loop(0, qi + 1, second, 0)
    dq_scr[block_rows(qi), :] = dqt_scr[...].T

    @pl.when(step == NB - 1)
    def _():
        d_scr[:, pl.ds(pl.multiple_of(2 * LOC + h * HD, HD), HD)] = dv_scr[...].astype(BF)
        gg_ref[...] = jnp.zeros_like(gg_ref)
        cols = head_cols(h)

        @pl.when(h == 0)
        def _():
            wait(tables)


        def tail(i, carry):
            rows = block_rows(i)
            cos, sin = cos_ref[rows, :], sin_ref[rows, :]
            for n, from_scr in enumerate((dq_scr, dk_scr)):
                d = from_scr[rows, :]
                hat = d * cos - pltpu.roll(d, HD // 2, 1) * sin
                unit = raw_ref[n, rows, cols] * as_column(inv_ref[pl.ds(i + n * NB, 1), :])
                gg_ref[n:n + 1, :] += jnp.sum(hat * unit, axis=0, keepdims=True)
                du = hat * gains_ref[n:n + 1, :]
                du_scr[n, h, rows, :] = du
                dots_scr[pl.ds(i + n * NB, 1), :] += row_sums(du * unit)
            return carry

        lax.fori_loop(0, NB, tail, 0)

    @pl.when(jnp.logical_and(h == 1, step == NB - 1))
    def _():
        sums = exchange(me, [dots_scr, gga_ref], [slot, ga_slot], ex_send, ex_recv)
        start(sums)
        if b:
            moved[2].start()
        wait(sums)
        if not b:
            stage2(me, full_ref, bg).wait()
            last_stage = stage3(me, full_ref, bg)
            last_stage.load()
            last_stage.send()
        total[...] = ordered_total(me, dots_scr, slot) / DIM
        gout_ref[...] = ordered_total(me, gga_ref, ga_slot)

        def copies(i):
            rows = block_rows(i)
            return [pltpu.make_async_copy(d_scr.at[rows, :], d_ref.at[rows, :], d_sems.at[i]),
                    pltpu.make_async_remote_copy(
                        src_ref=d_scr.at[rows, :], dst_ref=pd_ref.at[rows, :], send_sem=pd_send.at[i],
                        recv_sem=pd_recv.at[i], device_id=(peer_of(me, 1),), device_id_type=MESH)]

        def last(i, carry):
            rows = block_rows(i)
            for n in range(2):
                dots = as_column(total[pl.ds(i + n * NB, 1), :])
                inv = as_column(inv_ref[pl.ds(i + n * NB, 1), :])
                for hh in range(LOC // HD):
                    sl = slice(hh * HD, (hh + 1) * HD)
                    unit = raw_ref[n, rows, sl] * inv
                    val = inv * (du_scr[n, hh, rows, :] - unit * dots)
                    d_scr[rows, n * LOC + hh * HD:n * LOC + (hh + 1) * HD] = val.astype(BF)
            start(copies(i))
            return carry

        lax.fori_loop(0, NB, last, 0)
        for i in range(NB):
            wait(copies(i))
        wait(moved)
        if not b:
            last_stage.wait()


def backward(b, da, qkv, wo, lse, raw, inv, gains, cos, sin, gga, weights, others, cid):
    def whole(*shape):
        return pl.BlockSpec(shape, lambda h, i: (0,) * len(shape))

    def picked(*shape):
        return pl.BlockSpec((None,) + shape, lambda h, i: (b,) + (0,) * len(shape))

    gsp = whole(8, DIM // 8)
    half = (DIM // 2, 3 * LOC)
    if b:
        extra = [sds((2, BLK, DIM // 2), F32)]
        own = [pltpu.VMEM((2,) + half, BF), pltpu.VMEM((2, 2, BLK, 3 * LOC), BF), pltpu.VMEM((2, BLK, DIM // 2), F32)]
    else:
        extra = [sds((SEQ, DIM), BF), sds(half, BF), sds((SEQ, DIM), BF)]
        own = [pltpu.VMEM((2, TOK, DIM), BF), pltpu.VMEM((2, TOK, DIM), BF), pltpu.VMEM(half, BF)]
    return pl.pallas_call(
        functools.partial(backward_kernel, b),
        grid=(2, NB),
        in_specs=[pl.BlockSpec((None, 3, SEQ, HD), lambda h, i: (b, 0, 0, h)),
                  whole(LOC, DIM),
                  picked(2 * NB, BLK), ANYWHERE, picked(2 * NB, BLK),
                  pl.BlockSpec((2 + DIM // LOC, HD), lambda h, i: (0, h)), ANYWHERE, ANYWHERE, gsp]
        + [ANYWHERE] * (4 + len(others)),
        out_specs=[ANYWHERE, ANYWHERE, pl.BlockSpec((8, HD), lambda h, i: (0, h)), gsp] + [ANYWHERE] * len(extra),
        out_shape=[sds((SEQ, 3 * LOC), BF), sds((SEQ, 3 * LOC), BF), sds((8, LOC), F32), sds((8, DIM // 8), F32)] + extra,
        input_output_aliases={} if b else {12: 6},
        scratch_shapes=own + [
            pltpu.VMEM((NB, BLK, BLK), F32), pltpu.VMEM((NB, BLK, BLK), F32), pltpu.VMEM((HD, SEQ), BF),
            pltpu.VMEM((HD, BLK), F32), pltpu.VMEM((SEQ, HD), F32), pltpu.VMEM((SEQ, HD), F32),
            pltpu.VMEM((SEQ, HD), F32), pltpu.VMEM((2, 2, SEQ, HD), F32), pltpu.VMEM((SEQ, 3 * LOC), BF),
            pltpu.VMEM((SEQ, LOC), BF), pltpu.VMEM((2, BLK, DIM), BF), pltpu.VMEM((2 * NB, BLK), F32), pltpu.VMEM((2 * NB, BLK), F32),
            pltpu.VMEM((NDEV - 1, 2 * NB, BLK), F32), pltpu.VMEM((NDEV - 1, 8, DIM // 8), F32),
            DMA((2, NDEV - 1)), DMA((2, NDEV - 1)), DMA((NB,)), DMA((NB,)), DMA((NB,)), DMA((6,)), DMA((8,)), DMA((2,)),
            pltpu.VMEM((2, SEQ, LOC), F32), pltpu.VMEM((SEQ, HD), F32), pltpu.VMEM((SEQ, HD), F32), DMA((3,))]
        + ([] if b else BG_SEMS * 2),
        compiler_params=params(dimension_semantics=("arbitrary", "arbitrary"), collective_id=cid, has_side_effects=True),
        cost_estimate=cost(25e9, 30e6),
        name="backward",
    )(qkv, wo, lse, raw, inv, gains, cos, sin, gga, *weights, da, *others)


HALF = DIM // 2
CH = 256


def grads_kernel(d0, d1, pd0, pd1, wq, wk, wv, pw, got, x_full, o_all, da0, da1, dy_ref, dx_out, gwq_out, gwk_out, gwv_out, gwo_out,
                 d_all, w_all, sbuf, r1, r2, fin, acc, xbuf, obuf,
                 dl_sems, w_sems, s1_sems, r1_sems, s2_sems, r2_sems, fs_sems, fr_sems, x_sems, o_sems, dx_ref, gwq_ref, gwk_ref, gwv_ref, gwo_ref, out_sems):
    me = lax.axis_index('tp')
    core, partner, first, second = route(me)
    chip = me // 2
    diag_chip, first_chip, second_chip = peer_of(me, 6) // 2, first // 2, second // 2

    barrier = pltpu.get_barrier_semaphore()
    for dev in (partner, first, second):
        pl.semaphore_signal(barrier, inc=1, device_id=(dev,), device_id_type=MESH)

    def rows_of(blk):
        return pl.ds(pl.multiple_of(blk * BLK, BLK), BLK)

    results = [pltpu.make_async_copy(src, dst, out_sems.at[n]) for n, (src, dst) in enumerate((
        (gwq_ref, gwq_out), (gwk_ref, gwk_out), (gwv_ref, gwv_out), (gwo_ref, gwo_out)))]
    chips = (diag_chip, first_chip, second_chip, chip)
    w_copies = [pltpu.make_async_copy(w.at[half_rows(core), :], w_all.at[0, :, pl.ds(n * LOC, LOC)], w_sems.at[n])
                for n, w in enumerate((wq, wk, wv))]
    w_copies.append(pltpu.make_async_copy(pw, w_all.at[1], w_sems.at[3]))
    loads = []
    for n in range(8):
        rows, b = rows_of(chips[n // 2]), n % 2
        loads.append([pltpu.make_async_copy(d.at[rows, :], d_all.at[side, b, rows, :], dl_sems.at[side, n])
                      for side, d in enumerate(((d0, d1)[b], (pd0, pd1)[b]))])
    start(w_copies)
    start(loads[1])
    pl.semaphore_wait(barrier, 3)
    wait(w_copies)

    def partial(b, blk):
        rows = rows_of(blk)
        return dot(d_all[0, b, rows, :], w_all[0], NT) + dot(d_all[1, b, rows, :], w_all[1], NT)

    def to_first(n):
        return pltpu.make_async_remote_copy(
            src_ref=sbuf.at[n // 2], dst_ref=r1.at[n], send_sem=s1_sems.at[n], recv_sem=r1_sems.at[n],
            device_id=(first,), device_id_type=MESH)

    def to_second(b):
        return pltpu.make_async_remote_copy(
            src_ref=r1.at[b], dst_ref=r2.at[b], send_sem=s2_sems.at[b], recv_sem=r2_sems.at[b],
            device_id=(second,), device_id_type=MESH)

    def to_partner(b):
        return pltpu.make_async_remote_copy(
            src_ref=r1.at[2 + b, pl.ds(pl.multiple_of((1 - core) * TOK, TOK), TOK), :], dst_ref=fin.at[b],
            send_sem=fs_sems.at[b], recv_sem=fr_sems.at[b], device_id=(partner,), device_id_type=MESH)

    taken = [pltpu.make_async_copy(got.at[n], r1.at[2 * n], w_sems.at[4 + n]) for n in range(2)]
    for n in (1, 3):
        wait(loads[n])
        if n == 1:
            start(loads[3])
        sbuf[n // 2] = partial(1, chips[n // 2])
        to_first(n).start()
        if n == 1:
            start(taken)
            for later in (4, 0, 2, 5, 6, 7):
                start(loads[later])
    for n in (0, 2, 4, 5, 6, 7):
        wait(loads[n])
    wait(taken)

    steps = SEQ // CH

    def chunk(i):
        return pl.ds(pl.multiple_of(i * CH, CH), CH)

    def stream(pairs, body):
        def fetch(i):
            return [pltpu.make_async_copy(src.at[chunk(i), :], buf.at[i % 2], sems.at[i % 2]) for src, buf, sems in pairs]

        for c in fetch(0):
            c.start()

        def it(i, carry):
            @pl.when(i + 1 < steps)
            def _():
                for c in fetch(i + 1):
                    c.start()

            for c in fetch(i):
                c.wait()
            body(i)
            return carry

        lax.fori_loop(0, steps, it, 0)

    def wgrad(b, src):
        def body(i):
            left = d_all[0, b, chunk(i), :].T
            for c in range(3):
                part = slice(c * LOC, (c + 1) * LOC)
                acc[part, :] += dot(left[part, :], xbuf[i % 2])

        stream([(src, xbuf, x_sems)], body)

    def forward_second(b):
        if b:
            to_first(b).wait_recv()
        r1[b] += partial(b, second_chip)
        to_second(b).start()

    forward_second(0)
    acc[...] = jnp.zeros_like(acc)
    wgrad(0, x_full.at[0])
    wgrad(1, x_full.at[1])
    for n, ref in enumerate((gwq_ref, gwk_ref, gwv_ref)):
        ref[...] = acc[n * LOC:(n + 1) * LOC, :].T.astype(BF)
        results[n].start()
    forward_second(1)
    acc[:LOC, :] = jnp.zeros((LOC, DIM), F32)

    def wo_body(i):
        acc[:LOC, :] += dot(obuf[i % 2].T, xbuf[i % 2])

    for o_src, da_src in ((o_all.at[0], da0), (o_all.at[1], da1)):
        stream([(da_src, xbuf, x_sems), (o_src, obuf, o_sems)], wo_body)
    gwo_ref[...] = acc[:LOC, :].astype(BF)
    results[3].start()

    def own_part(b, carry):
        r1_own = partial(b, chip)
        pl.when(b == 1)(to_first(3).wait_recv)
        to_second(b).wait_recv()
        r1[2 + b] += r1_own + r2[b]
        to_partner(b).start()
        cols = half_rows(core)
        rows = pl.ds(pl.multiple_of(core * TOK, TOK), TOK)
        dx_ref[b, :, cols] = (r1[2 + b, rows, :] + dy_ref[b, :, cols].astype(F32)).astype(BF)
        return carry

    lax.fori_loop(0, 2, own_part, 0)

    def finish(b, carry):
        to_partner(b).wait()
        cols = half_rows(1 - core)
        dx_ref[b, :, cols] = (fin[b] + dy_ref[b, :, cols].astype(F32)).astype(BF)
        pltpu.make_async_copy(dx_ref.at[b], dx_out.at[b], out_sems.at[4 + b]).start()
        to_second(b).wait_send()
        return carry

    to_first(1).wait_send()
    to_first(3).wait_send()
    lax.fori_loop(0, 2, finish, 0)
    wait(results)
    for b in range(2):
        pltpu.make_async_copy(dx_ref.at[b], dx_out.at[b], out_sems.at[4 + b]).wait()


def grads(d0, d1, pd0, pd1, wq, wk, wv, pw, got, x_full, o_all, da0, da1, dy, cid):
    vm = pl.BlockSpec(memory_space=pltpu.VMEM)
    far = pl.BlockSpec(memory_space=pl.ANY)
    dma = pltpu.SemaphoreType.DMA
    return pl.pallas_call(
        grads_kernel,
        in_specs=[far] * 13 + [vm],
        out_specs=[far] * 5,
        out_shape=[sds((2, TOK, DIM), BF)] + [sds((DIM, LOC), BF)] * 3 + [sds((LOC, DIM), BF)],
        scratch_shapes=[pltpu.VMEM((2, 2, SEQ, 3 * LOC), BF), pltpu.VMEM((2, HALF, 3 * LOC), BF),
                        pltpu.VMEM((2, BLK, HALF), F32), pltpu.VMEM((4, BLK, HALF), F32), pltpu.VMEM((2, BLK, HALF), F32),
                        pltpu.VMEM((2, TOK, HALF), F32), pltpu.VMEM((3 * LOC, DIM), F32),
                        pltpu.VMEM((2, CH, DIM), BF), pltpu.VMEM((2, CH, LOC), BF),
                        dma((2, 8)), dma((9,)), dma((4,)), dma((4,)), dma((2,)), dma((2,)),
                        dma((2,)), dma((2,)), dma((2,)), dma((2,)), pltpu.VMEM((2, TOK, DIM), BF),
                        pltpu.VMEM((DIM, LOC), BF), pltpu.VMEM((DIM, LOC), BF), pltpu.VMEM((DIM, LOC), BF),
                        pltpu.VMEM((LOC, DIM), BF), dma((6,))],
        compiler_params=pltpu.CompilerParams(vmem_limit_bytes=67043328, collective_id=cid, has_side_effects=True),
        cost_estimate=cost(100e9, 40e6),
        name="grads",
    )(d0, d1, pd0, pd1, wq, wk, wv, pw, got, x_full, o_all, da0, da1, dy)


def deliver_kernel(*refs):
    count = (len(refs) - 2) // 3
    loads, stores = [], []
    for src, dst, buf in zip(refs[:count], refs[count:2 * count], refs[2 * count:3 * count]):
        for part in range(2):
            piece = (part,) if len(src.shape) == 3 else (pl.ds(part * (src.shape[0] // 2), src.shape[0] // 2),)
            n = len(loads)
            loads.append(pltpu.make_async_copy(src.at[piece], buf.at[piece], refs[-2].at[n]))
            stores.append(pltpu.make_async_copy(buf.at[piece], dst.at[piece], refs[-1].at[n]))
    ahead = 4
    start(loads[:ahead])
    for n, (load, store) in enumerate(zip(loads, stores)):
        load.wait()
        store.start()
        start(loads[n + ahead:n + ahead + 1])
    wait(stores)


def deliver(*arrays):
    return pl.pallas_call(
        deliver_kernel,
        in_specs=[ANYWHERE] * len(arrays),
        out_specs=[ANYWHERE] * len(arrays),
        out_shape=[sds(t.shape, t.dtype) for t in arrays],
        scratch_shapes=[pltpu.VMEM(t.shape, t.dtype) for t in arrays] + [DMA((2 * len(arrays),)), DMA((2 * len(arrays),))],
        compiler_params=params(),
        cost_estimate=cost(1e9, 16e6),
        name="deliver",
    )(*arrays)


def local_block(x_loc, wq, wk, wv, wo, gq, gk, ga, dy_loc):
    gains = jnp.concatenate([gq, gk, ga]).astype(F32).reshape(2 + DIM // LOC, LOC)
    weights = (wq, wk, wv)
    cos, sin, inv, o, lse, raw, qkv, o_recv, x_full, wo_full = forward(x_loc, wq, wk, wv, wo, gains, 0)
    y, da, gga, da0 = out_block(o_recv, wo_full, x_loc, dy_loc, gains, 1)
    state = (qkv, wo, lse, raw, inv, gains, cos, sin, gga, weights)
    d0, pd0, gg0, gout, da1, pw, da0 = backward(0, da0, *state, (da,), 2)
    d1, pd1, gg1, _, got = backward(1, da1, *state, (d0, pd0, pw), 3)
    grad_ga = gout.reshape(DIM).astype(BF)
    big = grads(d0, d1, pd0, pd1, *weights, pw, got, x_full, o, da0, da1, dy_loc, 4)
    y, dx, gwq, gwk, gwv, gwo = deliver(y, *big)
    gg = gg0 + gg1
    return (y, dx, gwq, gwk, gwv, gwo, gg[0].astype(BF), gg[1].astype(BF), grad_ga)


def solution(mesh):
    act, col, row, vec = P(None, 'tp', None), P(None, 'tp'), P('tp', None), P('tp')
    in_specs = (act, col, col, col, row, vec, vec, P(), act)
    out_specs = (act, act, col, col, col, row, vec, vec, P())
    return jax.shard_map(local_block, mesh=mesh, in_specs=in_specs, out_specs=out_specs, check_vma=False)
```

```python
import functools
import math

import jax
import jax.numpy as jnp
import numpy as np
from jax import lax
from jax.experimental import pallas as pl
from jax.experimental.pallas import tpu as pltpu
from jax.sharding import PartitionSpec as P

HD = 128
ROPE_THETA = 500000.0
EPS = 1e-6
DIM = 2048
SEQ = 2048
LOC = 256
TOK = 256
BLK = 512
NB = SEQ // BLK
NDEV = 8
SCALE = HD ** -0.5
C2 = SCALE * math.log2(math.e)
MESH = pl.DeviceIdType.MESH
BF = jnp.bfloat16
F32 = jnp.float32
VMEM_MAX = 60 * 1024 * 1024

NT = (((1,), (1,)), ((), ()))
NN = (((1,), (0,)), ((), ()))


def dot(a, b, dims=NN):
    return lax.dot_general(a, b, dims, preferred_element_type=F32)


def sds(shape, dtype):
    return jax.ShapeDtypeStruct(shape, dtype)


def cost(flops, nbytes, trans=0):
    return pl.CostEstimate(flops=int(flops), bytes_accessed=int(nbytes), transcendentals=int(trans))


def params(**kw):
    return pltpu.CompilerParams(vmem_limit_bytes=VMEM_MAX, **kw)


def peer_of(me, mask):
    core, ax, ay = me % 2, (me // 2) % 2, me // 4
    core = 1 - core if mask & 1 else core
    ax = 1 - ax if mask & 2 else ax
    ay = 1 - ay if mask & 4 else ay
    return ay * 4 + ax * 2 + core


ORDER = (6, 7, 2, 4, 3, 5, 1)


def entry_barrier(me):
    barrier = pltpu.get_barrier_semaphore()
    for mask in ORDER:
        pl.semaphore_signal(barrier, inc=1, device_id=(peer_of(me, mask),), device_id_type=MESH)
    pl.semaphore_wait(barrier, NDEV - 1)


def nbr_signal(me):
    for mask in (1, 2, 4):
        pl.semaphore_signal(pltpu.get_barrier_semaphore(), inc=1, device_id=(peer_of(me, mask),), device_id_type=MESH)


def nbr_wait():
    pl.semaphore_wait(pltpu.get_barrier_semaphore(), 3)


DMA = pltpu.SemaphoreType.DMA
ANYWHERE = pl.BlockSpec(memory_space=pl.ANY)
BG_SEMS = [DMA((11,)), DMA((11,)), DMA((5,))]
BG = BG_SEMS + [pltpu.VMEM((2, TOK, DIM), BF)]


def shard_rows(dev, lo=0, count=TOK):
    return pl.ds(pl.multiple_of(dev * TOK + lo, HD), count)


class Stage:
    def __init__(self, loads, copies):
        self.loads, self.copies = loads, copies

    def load(self):
        start(self.loads)

    def send(self):
        wait(self.loads)
        start(self.copies)

    def wait(self, *which):
        wait([self.copies[n] for n in which] or self.copies)


def stage1(me, src, full, bg, part=None):
    send, recv, own, buf = bg
    lo, count, at = (0, TOK, 0) if part is None else (part * (TOK // 2), TOK // 2, 8 * part)
    there = full.at[shard_rows(me, lo, count), :]
    mine = buf.at[0, pl.ds(lo, count), :]
    copies = [pltpu.make_async_remote_copy(
        src_ref=mine, dst_ref=there, send_sem=send.at[at + k], recv_sem=recv.at[at + k],
        device_id=(peer_of(me, mask),), device_id_type=MESH) for k, mask in enumerate((2, 4, 1))]
    loads = [] if part == 1 or src is None else [pltpu.make_async_copy(src, buf.at[0], own.at[0])]
    return Stage(loads, copies + [pltpu.make_async_copy(mine, there, own.at[3 if part == 1 else 2])])


def stage2(me, full, bg):
    send, recv, own, buf = bg
    xn, yn = peer_of(me, 2), peer_of(me, 4)
    half = TOK // 2
    plan = ((1, half, half, yn, 2), (0, 0, half, xn, 4), (0, 0, TOK, xn, 1), (1, 0, TOK, yn, 1))
    return Stage(
        [pltpu.make_async_copy(full.at[shard_rows(dev), :], buf.at[n], own.at[n]) for n, dev in enumerate((xn, yn))],
        [pltpu.make_async_remote_copy(
            src_ref=buf.at[slot, pl.ds(lo, count), :], dst_ref=full.at[shard_rows(dev, lo, count), :],
            send_sem=send.at[3 + k], recv_sem=recv.at[3 + k], device_id=(peer_of(me, mask),), device_id_type=MESH)
         for k, (slot, lo, count, dev, mask) in enumerate(plan)])


def stage3(me, full, bg):
    send, recv, own, buf = bg
    rows = full.at[shard_rows(peer_of(me, 6)), :]
    return Stage([pltpu.make_async_copy(rows, buf.at[1], own.at[1])], [pltpu.make_async_remote_copy(
        src_ref=buf.at[1], dst_ref=rows, send_sem=send.at[7], recv_sem=recv.at[7],
        device_id=(peer_of(me, 1),), device_id_type=MESH)])


def route(me):
    core = me % 2
    first = peer_of(me, 2) * (1 - core) + peer_of(me, 4) * core
    second = peer_of(me, 4) * (1 - core) + peer_of(me, 2) * core
    return core, peer_of(me, 1), first, second


def half_rows(c):
    return pl.ds(pl.multiple_of(c * (DIM // 2), DIM // 2), DIM // 2)


def start(copies):
    for c in copies:
        c.start()


def wait(copies):
    for c in copies:
        c.wait()


def row_sums(vals):
    folded = vals[:, :HD]
    for start in range(HD, vals.shape[1], HD):
        folded = folded + vals[:, start:start + HD]
    return jnp.sum(folded.T, axis=0, keepdims=True)


def columns_of(rows):
    turned = rows.T
    return [jnp.broadcast_to(turned[:, c:c + 1], (rows.shape[1], HD)) for c in range(rows.shape[0])]


def as_column(row):
    return jnp.broadcast_to(row, (HD, row.shape[1])).T


def exchange(me, srcs, slots, send_sems, recv_sems):
    copies = []
    for n, (src, slot) in enumerate(zip(srcs, slots)):
        for p, mask in enumerate(ORDER):
            copies.append(pltpu.make_async_remote_copy(
                src_ref=src, dst_ref=slot.at[p], send_sem=send_sems.at[n, p], recv_sem=recv_sems.at[n, p],
                device_id=(peer_of(me, mask),), device_id_type=MESH))
    return copies


def ordered_total(me, src, slot):
    own = src[...]
    total = jnp.zeros_like(own)
    for dev in range(NDEV):
        term = jnp.where(me == dev, own, 0.0)
        for p, mask in enumerate(ORDER):
            term = term + jnp.where(peer_of(me, mask) == dev, slot[p], 0.0)
        total = total + term
    return total


def causal_mask():
    keys = lax.broadcasted_iota(jnp.int32, (BLK, BLK), 0)
    queries = lax.broadcasted_iota(jnp.int32, (BLK, BLK), 1)
    return keys <= queries


def block_rows(i):
    return pl.ds(pl.multiple_of(i * BLK, BLK), BLK)


def head_cols(h):
    return pl.ds(pl.multiple_of(h * HD, HD), HD)


def forward_kernel(freq_ref, wq_ref, wk_ref, wv_ref, gains_ref, x_ref, wo_ref,
                   cos_ref, sin_ref, inv_ref, o_ref, lse_ref, raw_ref, qkv_ref, both_ref, full_ref, wof_ref,
                   raw, qkv, xbuf, sums_scr, slot, p_scr, vt_scr, acc_scr, o_scr, buf0, buf1,
                   ex_send, ex_recv, out_sems, send_sems, recv_sems, own_sems, x_sems, *bg_sems):
    g = pl.program_id(0)
    b, t = g // (4 * NB), g % (4 * NB)
    me = lax.axis_index('tp')
    bg0, bg1, bg2 = (*bg_sems[:3], buf0), (*bg_sems[3:6], buf1), (*bg_sems[6:], buf0)
    x0f, x1f = full_ref.at[0], full_ref.at[1]

    def x_gather(part=None):
        return stage1(me, x_ref.at[1], x1f, bg1, part)

    def wo_gather(part=None):
        return stage1(me, wo_ref, wof_ref, bg2, part)

    def keep(bb):
        return [pltpu.make_async_copy(raw, raw_ref.at[bb], out_sems.at[0]),
                pltpu.make_async_copy(qkv, qkv_ref.at[bb], out_sems.at[1])]

    def sums(bb):
        return exchange(me, [sums_scr.at[bb]], [slot.at[bb]], ex_send.at[bb], ex_recv.at[bb])

    def fetch(bb, i):
        return pltpu.make_async_copy(full_ref.at[bb, block_rows(i), :], xbuf.at[i % 2], x_sems.at[i % 2])

    def block_copy(bb, hh, st, half):
        dest = 2 * ((me // 2 + 1 + st) % NB) + half
        part = o_scr.at[bb, hh, st, pl.ds(half * TOK, TOK), :]
        dst = both_ref.at[bb, :, pl.ds(pl.multiple_of(me * LOC + hh * HD, HD), HD)]
        away = pltpu.make_async_remote_copy(
            src_ref=part, dst_ref=dst, send_sem=send_sems.at[bb, hh, st, half], recv_sem=recv_sems.at[bb, hh, me],
            device_id=(dest,), device_id_type=MESH)
        return dest, away, pltpu.make_async_copy(part, dst, own_sems.at[bb, hh])

    def run(stage):
        stage.load()
        stage.send()

    @pl.when(g == 0)
    def _():
        first = stage1(me, x_ref.at[0], x0f, bg0)
        first.load()
        entry_barrier(me)
        first.send()
        x_gather(0).load()
        freq = freq_ref[...]
        sign = jnp.where(lax.broadcasted_iota(jnp.int32, (TOK, HD), 1) < HD // 2, -1.0, 1.0)

        def table(i, carry):
            rows = pl.ds(pl.multiple_of(i * TOK, TOK), TOK)
            pos = (lax.broadcasted_iota(jnp.int32, (TOK, HD), 0) + i * TOK).astype(F32)
            angle = pos * freq
            cos_ref[rows, :] = jnp.cos(angle)
            sin_ref[rows, :] = jnp.sin(angle) * sign
            return carry

        lax.fori_loop(0, SEQ // TOK, table, 0)
        first.wait()
        second, third = stage2(me, x0f, bg0), stage3(me, x0f, bg0)
        run(second)
        x_gather(0).send()
        second.wait()
        run(third)
        third.wait()
        fetch(0, 0).start()

    @pl.when(g == 2 * NB + 2)
    def _():
        x_gather(0).wait()
        x_gather(1).wait()
        run(stage2(me, x1f, bg1))
        run(wo_gather(0))

    @pl.when(g == 4 * NB)
    def _():
        stage2(me, x1f, bg1).wait()
        third = stage3(me, x1f, bg1)
        run(third)
        for c in keep(0):
            c.wait()
        third.wait()
        fetch(1, 0).start()

    @pl.when(g == 6 * NB + 2)
    def _():
        wo_gather(0).wait()
        wo_gather(1).wait()
        run(stage2(me, wof_ref, bg2))

    @pl.when(t < NB)
    def _():
        rows = block_rows(t)

        @pl.when(t < NB - 1)
        def _():
            fetch(b, t + 1).start()

        fetch(b, t).wait()
        x = xbuf[t % 2]
        for n, w_ref in enumerate((wq_ref, wk_ref)):
            val = dot(x, w_ref[...])
            raw[n, rows, :] = val
            sums_scr[b, pl.ds(t + n * NB, 1), :] = row_sums(val * val)
        qkv[2, rows, :] = dot(x, wv_ref[...]).astype(BF)

    @pl.when(t == NB)
    def _():
        start(sums(b))
        keep(b)[0].start()
        pl.when(b == 0)(x_gather(1).send)
        pl.when(b == 1)(wo_gather(1).send)
        wait(sums(b))
        inv_ref[...] = lax.rsqrt(ordered_total(me, sums_scr.at[b], slot.at[b]) / DIM + EPS)

    @pl.when(jnp.logical_and(t >= NB, t < 2 * NB))
    def _():
        i = t - NB
        rows = block_rows(i)
        cos, sin = cos_ref[rows, :], sin_ref[rows, :]
        for n in range(2):
            inv = as_column(inv_ref[pl.ds(i + n * NB, 1), :])
            gain = gains_ref[n:n + 1, :]
            for h in range(LOC // HD):
                sl = slice(h * HD, (h + 1) * HD)
                hat = raw[n, rows, sl] * inv * gain[:, sl]
                qkv[n, rows, sl] = (hat * cos + pltpu.roll(hat, HD // 2, 1) * sin).astype(BF)

    @pl.when(t == 2 * NB)
    def _():
        keep(b)[1].start()

    @pl.when(t >= 2 * NB)
    def _():
        h, step = t // NB - 2, t % NB
        qi = (me // 2 + 1 + step) % NB
        cols = head_cols(h)

        @pl.when(step == 0)
        def _():
            vt_scr[...] = qkv[2, :, cols].T

        qb = qkv[0, block_rows(qi), cols]

        def scores(j):
            return dot(qkv[1, block_rows(j), cols], qb, NT)

        def first(j, m):
            s = scores(j)
            p_scr[j] = s
            return jnp.maximum(m, jnp.max(s.reshape(BLK // 8, 8, BLK), axis=0))

        s = jnp.where(causal_mask(), scores(qi), -1e30)
        p_scr[qi] = s
        m = lax.fori_loop(0, qi, first, jnp.max(s.reshape(BLK // 8, 8, BLK), axis=0))
        m = jnp.max(m, axis=0, keepdims=True)

        def second(j, l):
            p = jnp.exp2((p_scr[j] - m) * C2)
            p_scr[j] = p
            return l + jnp.sum(p.reshape(BLK // 8, 8, BLK), axis=0)

        l = lax.fori_loop(0, qi + 1, second, jnp.zeros((8, BLK), F32))
        l = jnp.sum(l, axis=0, keepdims=True)
        rl = 1.0 / l
        lse_ref[pl.ds(h * NB + qi, 1), :] = m * C2 + jnp.log2(l)

        acc_scr[...] = jnp.zeros_like(acc_scr)

        def third(j, carry):
            p = (p_scr[j] * rl).astype(BF)
            acc_scr[...] += dot(vt_scr[:, block_rows(j)], p)
            return carry

        lax.fori_loop(0, qi + 1, third, 0)
        out = acc_scr[...].T.astype(BF)
        o_scr[b, h, step] = out
        o_ref[block_rows(qi), cols] = out

        for half in range(2):
            dest, away, here = block_copy(b, h, step, half)
            pl.when(dest != me)(away.start)
            pl.when(dest == me)(here.start)

    @pl.when(g == 8 * NB - 1)
    def _():
        stage2(me, wof_ref, bg2).wait()
        third = stage3(me, wof_ref, bg2)
        run(third)
        for c in keep(1):
            c.wait()

        def drain(n, carry):
            bb, hh = n // 2, n % 2
            for st in range(NB):
                for half in range(2):
                    dest, away, here = block_copy(bb, hh, st, half)
                    if st < NB - 1:
                        away.wait_send()
                    else:
                        pl.when(dest != me)(away.wait_send)
                        pl.when(dest == me)(here.wait)
            for mask in ORDER:
                peer = peer_of(me, mask)
                pltpu.make_async_remote_copy(
                    src_ref=o_scr.at[0, 0, 0, pl.ds(0, TOK), :],
                    dst_ref=both_ref.at[bb, :, pl.ds(pl.multiple_of(peer * LOC + hh * HD, HD), HD)],
                    send_sem=send_sems.at[0, 0, 0, 0], recv_sem=recv_sems.at[bb, hh, peer],
                    device_id=(peer,), device_id_type=MESH).wait_recv()
            return carry

        lax.fori_loop(0, 4, drain, 0)
        third.wait()


def forward(x, wq, wk, wv, wo, gains, cid):
    inv_freq = np.float32(1.0) / np.float32(ROPE_THETA) ** (np.arange(HD // 2, dtype=np.float32) / np.float32(HD // 2))
    freq = jnp.asarray(np.concatenate([inv_freq, inv_freq])[None, :], F32)

    def whole(*shape):
        return pl.BlockSpec(shape, lambda g: (0,) * len(shape))

    def per_batch(*shape):
        return pl.BlockSpec((None,) + shape, lambda g: (g // (4 * NB),) + (0,) * len(shape))

    wspec, rows = whole(DIM, LOC), per_batch(2 * NB, BLK)
    return pl.pallas_call(
        forward_kernel,
        grid=(8 * NB,),
        in_specs=[whole(1, HD), wspec, wspec, wspec, whole(2 + DIM // LOC, LOC), ANYWHERE, ANYWHERE],
        out_specs=[whole(SEQ, HD), whole(SEQ, HD), rows, per_batch(SEQ, LOC), rows] + [ANYWHERE] * 5,
        out_shape=[sds((SEQ, HD), F32), sds((SEQ, HD), F32), sds((2, 2 * NB, BLK), F32), sds((2, SEQ, LOC), BF),
                   sds((2, 2 * NB, BLK), F32), sds((2, 2, SEQ, LOC), F32), sds((2, 3, SEQ, LOC), BF),
                   sds((2, TOK, DIM), BF), sds((2, SEQ, DIM), BF), sds((SEQ, DIM), BF)],
        scratch_shapes=[pltpu.VMEM((2, SEQ, LOC), F32), pltpu.VMEM((3, SEQ, LOC), BF), pltpu.VMEM((2, BLK, DIM), BF),
                        pltpu.VMEM((2, 2 * NB, BLK), F32), pltpu.VMEM((2, NDEV - 1, 2 * NB, BLK), F32),
                        pltpu.VMEM((NB, BLK, BLK), F32), pltpu.VMEM((HD, SEQ), BF), pltpu.VMEM((HD, BLK), F32),
                        pltpu.VMEM((2, 2, NB, BLK, HD), BF), pltpu.VMEM((2, TOK, DIM), BF), pltpu.VMEM((2, TOK, DIM), BF),
                        DMA((2, 1, NDEV - 1)), DMA((2, 1, NDEV - 1)), DMA((2,)),
                        DMA((2, 2, NB, 2)), DMA((2, 2, NDEV)), DMA((2, 2)), DMA((2,))] + BG_SEMS * 3,
        compiler_params=params(dimension_semantics=("arbitrary",), collective_id=cid, has_side_effects=True),
        cost_estimate=cost(60e9, 60e6),
        name="forward",
    )(freq, wq, wk, wv, gains, x, wo)


def out_kernel(o_ref, x_ref, dy_ref, gains_ref, wo_ref, y_ref, da_ref, gga_ref, full_ref, wo_scr, a_scr, wo_sems, buf, *bg_sems):
    b = pl.program_id(0)
    me = lax.axis_index('tp')
    bg = (*bg_sems, buf)
    step = DIM // NB

    def piece(j):
        cols = pl.ds(pl.multiple_of(j * step, step), step)
        return cols, pltpu.make_async_copy(wo_ref.at[:, cols], wo_scr.at[:, cols], wo_sems.at[j])

    @pl.when(b == 0)
    def _():
        nbr_signal(me)
        for j in range(NB):
            piece(j)[1].start()
        gga_ref[...] = jnp.zeros_like(gga_ref)

    o = o_ref[0]

    def fwd(j, carry):
        cols, load = piece(j)
        pl.when(b == 0)(load.wait)
        a_scr[:, cols] = dot(o, wo_scr[:, cols])
        return carry

    lax.fori_loop(0, NB, fwd, 0)
    a = a_scr[...]
    r = lax.rsqrt(jnp.mean(a * a, axis=-1, keepdims=True) + EPS)
    n = a * r
    ga = jnp.concatenate([gains_ref[2 + i:3 + i, :] for i in range(8)], axis=1)
    dy = dy_ref[0].astype(F32)
    gn = dy * ga
    da = (r * (gn - n * jnp.mean(gn * n, axis=-1, keepdims=True))).astype(BF)
    da_ref[0] = da

    @pl.when(b == 0)
    def _():
        buf[0] = da
        nbr_wait()
        stage1(me, None, full_ref, bg).send()

    y_ref[0] = (x_ref[0].astype(F32) + n * ga).astype(BF)
    col = jnp.sum(dy * n, axis=0, keepdims=True)
    for i in range(8):
        gga_ref[i:i + 1, :] += col[:, i * LOC:(i + 1) * LOC]

    @pl.when(b == 1)
    def _():
        stage1(me, None, full_ref, bg).wait()


def out_block(o, wo, x, dy, gains, cid):
    def whole(*shape):
        return pl.BlockSpec(shape, lambda i: (0,) * len(shape))

    batch = pl.BlockSpec((1, TOK, DIM), lambda i: (i, 0, 0))
    return pl.pallas_call(
        out_kernel,
        grid=(2,),
        in_specs=[batch, batch, batch, whole(2 + DIM // LOC, LOC), ANYWHERE],
        out_specs=[batch, batch, whole(8, DIM // 8), ANYWHERE],
        out_shape=[sds((2, TOK, DIM), BF), sds((2, TOK, DIM), BF), sds((8, DIM // 8), F32), sds((SEQ, DIM), BF)],
        scratch_shapes=[pltpu.VMEM((DIM, DIM), BF), pltpu.VMEM((TOK, DIM), F32), DMA((NB,)),
                        pltpu.VMEM((2, TOK, DIM), BF)] + BG_SEMS,
        compiler_params=params(dimension_semantics=("arbitrary",), collective_id=cid, has_side_effects=True),
        cost_estimate=cost(8 * TOK * DIM * DIM + 5e9, 18e6),
        name="out_block",
    )(o, x, dy, gains, wo)


def backward_kernel(b, qkv_ref, wo_ref, lse_ref, raw_hbm, inv_ref, gains_ref, cos_hbm, sin_hbm, gga_ref,
                    wq_ref, wk_ref, wv_ref, da_ref, *rest):
    if b:
        d0_ref, pd0_ref, pw_ref, d_ref, pd_ref, gg_ref, gout_ref, got_ref, da_ref, buf0, w_all, d_two, sbuf, *rest = rest
    else:
        shard_ref, d_ref, pd_ref, gg_ref, gout_ref, full_ref, pw_ref, da_ref, buf0, buf1, w_half, *rest = rest
    (p_scr, dp_scr, kt_scr, dqt_scr, dq_scr, dk_scr, dv_scr, du_scr, d_scr, dh_scr, dbuf, dots_scr, total, slot, ga_slot,
     ex_send, ex_recv, pd_send, pd_recv, d_sems, rs_sems, ld_sems, db_sems, raw_ref, cos_ref, sin_ref, tb_sems, *bg_sems) = rest
    h, step = pl.program_id(0), pl.program_id(1)
    me = lax.axis_index('tp')

    def chip_at(n):
        ax, ay = (me // 2) % 2, me // 4
        return (ay + (n // 2) * (1 - 2 * ay)) * 2 + ax + (n % 2) * (1 - 2 * ax)

    def fetch(n):
        return pltpu.make_async_copy(da_ref.at[block_rows(chip_at(n)), :], dbuf.at[n % 2], db_sems.at[n % 2])

    qi = chip_at(step)
    tables = [pltpu.make_async_copy(src, dst, tb_sems.at[n]) for n, (src, dst) in enumerate(
        ((raw_hbm.at[b], raw_ref), (cos_hbm, cos_ref), (sin_hbm, sin_ref)))]
    core, partner, first_dev, _ = route(me)
    weights = (wq_ref, wk_ref, wv_ref)

    bg0 = (*bg_sems[:3], buf0)
    older3 = stage3(me, da_ref, bg0)
    if b:
        operands = []
        for blk, chip in enumerate((peer_of(me, 6) // 2, first_dev // 2)):
            operands += [pltpu.make_async_copy(d.at[block_rows(chip), :], d_two.at[blk, n], ld_sems.at[2 * blk + n])
                         for n, d in enumerate((d0_ref, pd0_ref))]
        operands += [pltpu.make_async_copy(w.at[half_rows(core), :], w_all.at[0, :, pl.ds(n * LOC, LOC)], ld_sems.at[4 + n])
                     for n, w in enumerate(weights)]
        operands.append(pltpu.make_async_copy(pw_ref, w_all.at[1], ld_sems.at[7]))
        moved = [pltpu.make_async_remote_copy(
            src_ref=sbuf.at[blk, pl.ds(lo, count), :], dst_ref=got_ref.at[blk, pl.ds(lo, count), :], send_sem=rs_sems.at[n],
            recv_sem=rs_sems.at[3 + n], device_id=(first_dev,), device_id_type=MESH)
            for n, (blk, lo, count) in enumerate(((0, 0, BLK), (1, 0, BLK // 2), (1, BLK // 2, BLK // 2)))]
    else:
        bg = (*bg_sems[3:], buf1)
        older2 = stage2(me, da_ref, bg0)
        gather = stage1(me, shard_ref.at[1], full_ref, bg)
        operands = [pltpu.make_async_copy(w.at[half_rows(1 - core), :], w_half.at[:, pl.ds(n * LOC, LOC)], ld_sems.at[n])
                    for n, w in enumerate(weights)]
        moved = [pltpu.make_async_remote_copy(
            src_ref=w_half, dst_ref=pw_ref, send_sem=rs_sems.at[0], recv_sem=rs_sems.at[3], device_id=(partner,),
            device_id_type=MESH)]

    @pl.when(jnp.logical_and(h == 0, step == 0))
    def _():
        if b:
            start(operands)
            fetch(0).start()
            older3.load()
            start(tables)
            entry_barrier(me)
            older3.send()
            wait(operands)
            for blk in range(2):
                sbuf[blk] = dot(d_two[blk, 0], w_all[0], NT) + dot(d_two[blk, 1], w_all[1], NT)
                moved[blk].start()
        else:
            older2.load()
            fetch(0).start()
            gather.load()
            start(operands)
            start(tables)
            entry_barrier(me)
            older2.send()
            gather.send()
            wait(operands)
            start(moved)
        dots_scr[...] = jnp.zeros_like(dots_scr)

    @pl.when(jnp.logical_and(h == 0, step == NB - 1))
    def _():
        older3.wait()
        fetch(NB - 1).start()

    @pl.when(h == 0)
    def _():
        fetch(step).wait()
        dh_scr[block_rows(qi), :] = dot(dbuf[step % 2], wo_ref[...], NT).astype(BF)
        if b:
            @pl.when(step < NB - 2)
            def _():
                fetch(step + 1).start()
        else:
            @pl.when(step == 0)
            def _():
                older2.wait(2, 3)

            @pl.when(step < NB - 2)
            def _():
                fetch(step + 1).start()

            @pl.when(step == NB - 2)
            def _():
                older2.wait(0, 1)
                older3.load()
                older3.send()

    @pl.when(step == 0)
    def _():
        kt_scr[...] = qkv_ref[1].T
        dk_scr[...] = jnp.zeros_like(dk_scr)
        dv_scr[...] = jnp.zeros_like(dv_scr)

    qb = qkv_ref[0, block_rows(qi), :]
    dob = dh_scr[block_rows(qi), head_cols(h)]
    lse = lse_ref[pl.ds(h * NB + qi, 1), :]

    def first(j, acc, diag=False):
        rows = block_rows(j)
        p = jnp.exp2(dot(qkv_ref[1, rows, :], qb, NT) * C2 - lse)
        if diag:
            p = jnp.where(causal_mask(), p, 0.0)
        dp = dot(qkv_ref[2, rows, :], dob, NT)
        p_scr[j] = p
        dp_scr[j] = dp
        dv_scr[rows, :] += dot(p.astype(BF), dob)
        return acc + jnp.sum((p * dp).reshape(BLK // 8, 8, BLK), axis=0)

    acc = first(qi, jnp.zeros((8, BLK), F32), True)
    acc = lax.fori_loop(0, qi, first, acc)
    delta = jnp.sum(acc, axis=0, keepdims=True)
    dqt_scr[...] = jnp.zeros_like(dqt_scr)

    def second(j, carry):
        rows = block_rows(j)
        ds = (p_scr[j] * (dp_scr[j] - delta) * SCALE).astype(BF)
        dk_scr[rows, :] += dot(ds, qb)
        dqt_scr[...] += dot(kt_scr[:, rows], ds)
        return carry

    lax.fori_loop(0, qi + 1, second, 0)
    dq_scr[block_rows(qi), :] = dqt_scr[...].T

    @pl.when(step == NB - 1)
    def _():
        d_scr[:, pl.ds(pl.multiple_of(2 * LOC + h * HD, HD), HD)] = dv_scr[...].astype(BF)
        gg_ref[...] = jnp.zeros_like(gg_ref)
        cols = head_cols(h)

        @pl.when(h == 0)
        def _():
            wait(tables)


        inverse = columns_of(inv_ref[...])
        for i in range(NB):
            rows = pl.ds(i * BLK, BLK)
            cos, sin = cos_ref[rows, :], sin_ref[rows, :]
            for n, from_scr in enumerate((dq_scr, dk_scr)):
                d = from_scr[rows, :]
                hat = d * cos - pltpu.roll(d, HD // 2, 1) * sin
                unit = raw_ref[n, rows, cols] * inverse[i + n * NB]
                gg_ref[n:n + 1, :] += jnp.sum(hat * unit, axis=0, keepdims=True)
                du = hat * gains_ref[n:n + 1, :]
                du_scr[n, h, rows, :] = du
                dots_scr[i + n * NB:i + n * NB + 1, :] += row_sums(du * unit)

    @pl.when(jnp.logical_and(h == 1, step == NB - 1))
    def _():
        sums = exchange(me, [dots_scr, gga_ref], [slot, ga_slot], ex_send, ex_recv)
        start(sums)
        if b:
            moved[2].start()
        else:
            gather.wait()
            more = stage2(me, full_ref, bg)
            more.load()
            more.send()
        wait(sums)
        total[...] = ordered_total(me, dots_scr, slot) / DIM
        gout_ref[...] = ordered_total(me, gga_ref, ga_slot)

        def copies(i):
            rows = block_rows(i)
            return [pltpu.make_async_copy(d_scr.at[rows, :], d_ref.at[rows, :], d_sems.at[i]),
                    pltpu.make_async_remote_copy(
                        src_ref=d_scr.at[rows, :], dst_ref=pd_ref.at[rows, :], send_sem=pd_send.at[i],
                        recv_sem=pd_recv.at[i], device_id=(peer_of(me, 1),), device_id_type=MESH)]

        inverse, dots = columns_of(inv_ref[...]), columns_of(total[...])
        for i in range(NB):
            rows = pl.ds(i * BLK, BLK)
            for n in range(2):
                inv = inverse[i + n * NB]
                for hh in range(LOC // HD):
                    sl = slice(hh * HD, (hh + 1) * HD)
                    unit = raw_ref[n, rows, sl] * inv
                    val = inv * (du_scr[n, hh, rows, :] - unit * dots[i + n * NB])
                    d_scr[rows, n * LOC + hh * HD:n * LOC + (hh + 1) * HD] = val.astype(BF)
            start(copies(i))
        for i in range(NB):
            wait(copies(i))
        wait(moved)
        if not b:
            more.wait()


def backward(b, da, qkv, wo, lse, raw, inv, gains, cos, sin, gga, weights, others, cid):
    def whole(*shape):
        return pl.BlockSpec(shape, lambda h, i: (0,) * len(shape))

    def picked(*shape):
        return pl.BlockSpec((None,) + shape, lambda h, i: (b,) + (0,) * len(shape))

    gsp = whole(8, DIM // 8)
    half = (DIM // 2, 3 * LOC)
    if b:
        extra = [sds((2, BLK, DIM // 2), F32), sds((SEQ, DIM), BF)]
        own = [pltpu.VMEM((2, TOK, DIM), BF), pltpu.VMEM((2,) + half, BF), pltpu.VMEM((2, 2, BLK, 3 * LOC), BF), pltpu.VMEM((2, BLK, DIM // 2), F32)]
    else:
        extra = [sds((SEQ, DIM), BF), sds(half, BF), sds((SEQ, DIM), BF)]
        own = [pltpu.VMEM((2, TOK, DIM), BF), pltpu.VMEM((2, TOK, DIM), BF), pltpu.VMEM(half, BF)]
    return pl.pallas_call(
        functools.partial(backward_kernel, b),
        grid=(2, NB),
        in_specs=[pl.BlockSpec((None, 3, SEQ, HD), lambda h, i: (b, 0, 0, h)),
                  whole(LOC, DIM),
                  picked(2 * NB, BLK), ANYWHERE, picked(2 * NB, BLK),
                  pl.BlockSpec((2 + DIM // LOC, HD), lambda h, i: (0, h)), ANYWHERE, ANYWHERE, gsp]
        + [ANYWHERE] * (4 + len(others)),
        out_specs=[ANYWHERE, ANYWHERE, pl.BlockSpec((8, HD), lambda h, i: (0, h)), gsp] + [ANYWHERE] * len(extra),
        out_shape=[sds((SEQ, 3 * LOC), BF), sds((SEQ, 3 * LOC), BF), sds((8, LOC), F32), sds((8, DIM // 8), F32)] + extra,
        input_output_aliases={12: 5 if b else 6},
        scratch_shapes=own + [
            pltpu.VMEM((NB, BLK, BLK), F32), pltpu.VMEM((NB, BLK, BLK), F32), pltpu.VMEM((HD, SEQ), BF),
            pltpu.VMEM((HD, BLK), F32), pltpu.VMEM((SEQ, HD), F32), pltpu.VMEM((SEQ, HD), F32),
            pltpu.VMEM((SEQ, HD), F32), pltpu.VMEM((2, 2, SEQ, HD), F32), pltpu.VMEM((SEQ, 3 * LOC), BF),
            pltpu.VMEM((SEQ, LOC), BF), pltpu.VMEM((2, BLK, DIM), BF), pltpu.VMEM((2 * NB, BLK), F32), pltpu.VMEM((2 * NB, BLK), F32),
            pltpu.VMEM((NDEV - 1, 2 * NB, BLK), F32), pltpu.VMEM((NDEV - 1, 8, DIM // 8), F32),
            DMA((2, NDEV - 1)), DMA((2, NDEV - 1)), DMA((NB,)), DMA((NB,)), DMA((NB,)), DMA((6,)), DMA((8,)), DMA((2,)),
            pltpu.VMEM((2, SEQ, LOC), F32), pltpu.VMEM((SEQ, HD), F32), pltpu.VMEM((SEQ, HD), F32), DMA((3,))]
        + BG_SEMS * (1 if b else 2),
        compiler_params=params(dimension_semantics=("arbitrary", "arbitrary"), collective_id=cid, has_side_effects=True),
        cost_estimate=cost(25e9, 30e6),
        name="backward",
    )(qkv, wo, lse, raw, inv, gains, cos, sin, gga, *weights, da, *others)


HALF = DIM // 2
CH = 256


def grads_kernel(d0, d1, pd0, pd1, wq, wk, wv, pw, got, x_full, o_all, da0, da1, dy_ref, dx_out, gwq_out, gwk_out, gwv_out, gwo_out,
                 d_all, w_all, sbuf, r1, r2, fin, acc, xbuf, obuf,
                 dl_sems, w_sems, s1_sems, r1_sems, s2_sems, r2_sems, fs_sems, fr_sems, x_sems, o_sems, dx_ref, gwq_ref, gwk_ref, gwv_ref, gwo_ref, out_sems):
    me = lax.axis_index('tp')
    core, partner, first, second = route(me)
    chip = me // 2
    diag_chip, first_chip, second_chip = peer_of(me, 6) // 2, first // 2, second // 2

    barrier = pltpu.get_barrier_semaphore()
    for dev in (partner, first, second):
        pl.semaphore_signal(barrier, inc=1, device_id=(dev,), device_id_type=MESH)

    def rows_of(blk):
        return pl.ds(pl.multiple_of(blk * BLK, BLK), BLK)

    results = [pltpu.make_async_copy(src, dst, out_sems.at[n]) for n, (src, dst) in enumerate((
        (gwq_ref, gwq_out), (gwk_ref, gwk_out), (gwv_ref, gwv_out), (gwo_ref, gwo_out)))]
    chips = (diag_chip, first_chip, second_chip, chip)
    w_copies = [pltpu.make_async_copy(w.at[half_rows(core), :], w_all.at[0, :, pl.ds(n * LOC, LOC)], w_sems.at[n])
                for n, w in enumerate((wq, wk, wv))]
    w_copies.append(pltpu.make_async_copy(pw, w_all.at[1], w_sems.at[3]))
    loads = []
    for n in range(8):
        rows, b = rows_of(chips[n // 2]), n % 2
        loads.append([pltpu.make_async_copy(d.at[rows, :], d_all.at[side, b, rows, :], dl_sems.at[side, n])
                      for side, d in enumerate(((d0, d1)[b], (pd0, pd1)[b]))])
    start(w_copies)
    start(loads[1])
    pl.semaphore_wait(barrier, 3)
    wait(w_copies)

    def partial(b, blk):
        rows = rows_of(blk)
        return dot(d_all[0, b, rows, :], w_all[0], NT) + dot(d_all[1, b, rows, :], w_all[1], NT)

    def to_first(n):
        return pltpu.make_async_remote_copy(
            src_ref=sbuf.at[n // 2], dst_ref=r1.at[n], send_sem=s1_sems.at[n], recv_sem=r1_sems.at[n],
            device_id=(first,), device_id_type=MESH)

    def to_second(b):
        return pltpu.make_async_remote_copy(
            src_ref=r1.at[b], dst_ref=r2.at[b], send_sem=s2_sems.at[b], recv_sem=r2_sems.at[b],
            device_id=(second,), device_id_type=MESH)

    def to_partner(b):
        return pltpu.make_async_remote_copy(
            src_ref=r1.at[2 + b, pl.ds(pl.multiple_of((1 - core) * TOK, TOK), TOK), :], dst_ref=fin.at[b],
            send_sem=fs_sems.at[b], recv_sem=fr_sems.at[b], device_id=(partner,), device_id_type=MESH)

    taken = [pltpu.make_async_copy(got.at[n], r1.at[2 * n], w_sems.at[4 + n]) for n in range(2)]
    for n in (1, 3):
        wait(loads[n])
        if n == 1:
            start(loads[3])
        sbuf[n // 2] = partial(1, chips[n // 2])
        to_first(n).start()
        if n == 1:
            start(taken)
            for later in (4, 0, 2, 5, 6, 7):
                start(loads[later])
    for n in (0, 2, 4, 5, 6, 7):
        wait(loads[n])
    wait(taken)

    steps = SEQ // CH

    def chunk(i):
        return pl.ds(pl.multiple_of(i * CH, CH), CH)

    def stream(pairs, body):
        def fetch(i):
            return [pltpu.make_async_copy(src.at[chunk(i), :], buf.at[i % 2], sems.at[i % 2]) for src, buf, sems in pairs]

        for c in fetch(0):
            c.start()

        def it(i, carry):
            @pl.when(i + 1 < steps)
            def _():
                for c in fetch(i + 1):
                    c.start()

            for c in fetch(i):
                c.wait()
            body(i)
            return carry

        lax.fori_loop(0, steps, it, 0)

    def wgrad(b, src):
        def body(i):
            left = d_all[0, b, chunk(i), :].T
            for c in range(3):
                part = slice(c * LOC, (c + 1) * LOC)
                acc[part, :] += dot(left[part, :], xbuf[i % 2])

        stream([(src, xbuf, x_sems)], body)

    def forward_second(b):
        if b:
            to_first(b).wait_recv()
        r1[b] += partial(b, second_chip)
        to_second(b).start()

    forward_second(0)
    acc[...] = jnp.zeros_like(acc)
    wgrad(0, x_full.at[0])
    wgrad(1, x_full.at[1])
    for n, ref in enumerate((gwq_ref, gwk_ref, gwv_ref)):
        ref[...] = acc[n * LOC:(n + 1) * LOC, :].T.astype(BF)
        results[n].start()
    forward_second(1)
    acc[:LOC, :] = jnp.zeros((LOC, DIM), F32)

    def wo_body(i):
        acc[:LOC, :] += dot(obuf[i % 2].T, xbuf[i % 2])

    for o_src, da_src in ((o_all.at[0], da0), (o_all.at[1], da1)):
        stream([(da_src, xbuf, x_sems), (o_src, obuf, o_sems)], wo_body)
    gwo_ref[...] = acc[:LOC, :].astype(BF)
    results[3].start()

    def own_part(b, carry):
        r1_own = partial(b, chip)
        pl.when(b == 1)(to_first(3).wait_recv)
        to_second(b).wait_recv()
        r1[2 + b] += r1_own + r2[b]
        to_partner(b).start()
        cols = half_rows(core)
        rows = pl.ds(pl.multiple_of(core * TOK, TOK), TOK)
        dx_ref[b, :, cols] = (r1[2 + b, rows, :] + dy_ref[b, :, cols].astype(F32)).astype(BF)
        return carry

    lax.fori_loop(0, 2, own_part, 0)

    def finish(b, carry):
        to_partner(b).wait()
        cols = half_rows(1 - core)
        dx_ref[b, :, cols] = (fin[b] + dy_ref[b, :, cols].astype(F32)).astype(BF)
        pltpu.make_async_copy(dx_ref.at[b], dx_out.at[b], out_sems.at[4 + b]).start()
        to_second(b).wait_send()
        return carry

    to_first(1).wait_send()
    to_first(3).wait_send()
    lax.fori_loop(0, 2, finish, 0)
    wait(results)
    for b in range(2):
        pltpu.make_async_copy(dx_ref.at[b], dx_out.at[b], out_sems.at[4 + b]).wait()


def grads(d0, d1, pd0, pd1, wq, wk, wv, pw, got, x_full, o_all, da0, da1, dy, cid):
    vm = pl.BlockSpec(memory_space=pltpu.VMEM)
    far = pl.BlockSpec(memory_space=pl.ANY)
    dma = pltpu.SemaphoreType.DMA
    return pl.pallas_call(
        grads_kernel,
        in_specs=[far] * 13 + [vm],
        out_specs=[far] * 5,
        out_shape=[sds((2, TOK, DIM), BF)] + [sds((DIM, LOC), BF)] * 3 + [sds((LOC, DIM), BF)],
        scratch_shapes=[pltpu.VMEM((2, 2, SEQ, 3 * LOC), BF), pltpu.VMEM((2, HALF, 3 * LOC), BF),
                        pltpu.VMEM((2, BLK, HALF), F32), pltpu.VMEM((4, BLK, HALF), F32), pltpu.VMEM((2, BLK, HALF), F32),
                        pltpu.VMEM((2, TOK, HALF), F32), pltpu.VMEM((3 * LOC, DIM), F32),
                        pltpu.VMEM((2, CH, DIM), BF), pltpu.VMEM((2, CH, LOC), BF),
                        dma((2, 8)), dma((9,)), dma((4,)), dma((4,)), dma((2,)), dma((2,)),
                        dma((2,)), dma((2,)), dma((2,)), dma((2,)), pltpu.VMEM((2, TOK, DIM), BF),
                        pltpu.VMEM((DIM, LOC), BF), pltpu.VMEM((DIM, LOC), BF), pltpu.VMEM((DIM, LOC), BF),
                        pltpu.VMEM((LOC, DIM), BF), dma((6,))],
        compiler_params=pltpu.CompilerParams(vmem_limit_bytes=67043328, collective_id=cid, has_side_effects=True),
        cost_estimate=cost(100e9, 40e6),
        name="grads",
    )(d0, d1, pd0, pd1, wq, wk, wv, pw, got, x_full, o_all, da0, da1, dy)


def deliver_kernel(*refs):
    count = (len(refs) - 2) // 3
    loads, stores = [], []
    for src, dst, buf in zip(refs[:count], refs[count:2 * count], refs[2 * count:3 * count]):
        for part in range(2):
            piece = (part,) if len(src.shape) == 3 else (pl.ds(part * (src.shape[0] // 2), src.shape[0] // 2),)
            n = len(loads)
            loads.append(pltpu.make_async_copy(src.at[piece], buf.at[piece], refs[-2].at[n]))
            stores.append(pltpu.make_async_copy(buf.at[piece], dst.at[piece], refs[-1].at[n]))
    ahead = 4
    start(loads[:ahead])
    for n, (load, store) in enumerate(zip(loads, stores)):
        load.wait()
        store.start()
        start(loads[n + ahead:n + ahead + 1])
    wait(stores)


def deliver(*arrays):
    return pl.pallas_call(
        deliver_kernel,
        in_specs=[ANYWHERE] * len(arrays),
        out_specs=[ANYWHERE] * len(arrays),
        out_shape=[sds(t.shape, t.dtype) for t in arrays],
        scratch_shapes=[pltpu.VMEM(t.shape, t.dtype) for t in arrays] + [DMA((2 * len(arrays),)), DMA((2 * len(arrays),))],
        compiler_params=params(),
        cost_estimate=cost(1e9, 16e6),
        name="deliver",
    )(*arrays)


def local_block(x_loc, wq, wk, wv, wo, gq, gk, ga, dy_loc):
    gains = jnp.concatenate([gq, gk, ga]).astype(F32).reshape(2 + DIM // LOC, LOC)
    weights = (wq, wk, wv)
    cos, sin, inv, o, lse, raw, qkv, o_recv, x_full, wo_full = forward(x_loc, wq, wk, wv, wo, gains, 0)
    y, da, gga, da0 = out_block(o_recv, wo_full, x_loc, dy_loc, gains, 1)
    state = (qkv, wo, lse, raw, inv, gains, cos, sin, gga, weights)
    d0, pd0, gg0, gout, da1, pw, da0 = backward(0, da0, *state, (da,), 2)
    d1, pd1, gg1, _, got, da1 = backward(1, da1, *state, (d0, pd0, pw), 3)
    grad_ga = gout.reshape(DIM).astype(BF)
    big = grads(d0, d1, pd0, pd1, *weights, pw, got, x_full, o, da0, da1, dy_loc, 4)
    y, dx, gwq, gwk, gwv, gwo = deliver(y, *big)
    gg = gg0 + gg1
    return (y, dx, gwq, gwk, gwv, gwo, gg[0].astype(BF), gg[1].astype(BF), grad_ga)


def solution(mesh):
    act, col, row, vec = P(None, 'tp', None), P(None, 'tp'), P('tp', None), P('tp')
    in_specs = (act, col, col, col, row, vec, vec, P(), act)
    out_specs = (act, act, col, col, col, row, vec, vec, P())
    return jax.shard_map(local_block, mesh=mesh, in_specs=in_specs, out_specs=out_specs, check_vma=False)
```

```python
import functools
import math

import jax
import jax.numpy as jnp
import numpy as np
from jax import lax
from jax.experimental import pallas as pl
from jax.experimental.pallas import tpu as pltpu
from jax.sharding import PartitionSpec as P

HD = 128
ROPE_THETA = 500000.0
EPS = 1e-6
DIM = 2048
SEQ = 2048
LOC = 256
TOK = 256
BLK = 512
NB = SEQ // BLK
NDEV = 8
SCALE = HD ** -0.5
C2 = SCALE * math.log2(math.e)
MESH = pl.DeviceIdType.MESH
BF = jnp.bfloat16
F32 = jnp.float32
VMEM_MAX = 60 * 1024 * 1024

NT = (((1,), (1,)), ((), ()))
NN = (((1,), (0,)), ((), ()))


def dot(a, b, dims=NN):
    return lax.dot_general(a, b, dims, preferred_element_type=F32)


def sds(shape, dtype):
    return jax.ShapeDtypeStruct(shape, dtype)


def cost(flops, nbytes, trans=0):
    return pl.CostEstimate(flops=int(flops), bytes_accessed=int(nbytes), transcendentals=int(trans))


def params(**kw):
    return pltpu.CompilerParams(vmem_limit_bytes=VMEM_MAX, **kw)


def peer_of(me, mask):
    core, ax, ay = me % 2, (me // 2) % 2, me // 4
    core = 1 - core if mask & 1 else core
    ax = 1 - ax if mask & 2 else ax
    ay = 1 - ay if mask & 4 else ay
    return ay * 4 + ax * 2 + core


ORDER = (6, 7, 2, 4, 3, 5, 1)


def entry_signal(me):
    for mask in ORDER:
        pl.semaphore_signal(pltpu.get_barrier_semaphore(), inc=1, device_id=(peer_of(me, mask),), device_id_type=MESH)


def entry_wait():
    pl.semaphore_wait(pltpu.get_barrier_semaphore(), NDEV - 1)


def nbr_signal(me):
    for mask in (1, 2, 4):
        pl.semaphore_signal(pltpu.get_barrier_semaphore(), inc=1, device_id=(peer_of(me, mask),), device_id_type=MESH)


def nbr_wait():
    pl.semaphore_wait(pltpu.get_barrier_semaphore(), 3)


DMA = pltpu.SemaphoreType.DMA
ANYWHERE = pl.BlockSpec(memory_space=pl.ANY)
BG_SEMS = [DMA((11,)), DMA((11,)), DMA((5,))]
BG = BG_SEMS + [pltpu.VMEM((2, TOK, DIM), BF)]


def shard_rows(dev, lo=0, count=TOK):
    return pl.ds(pl.multiple_of(dev * TOK + lo, HD), count)


class Stage:
    def __init__(self, loads, copies):
        self.loads, self.copies = loads, copies

    def load(self):
        start(self.loads)

    def send(self):
        wait(self.loads)
        start(self.copies)

    def wait(self, *which):
        wait([self.copies[n] for n in which] or self.copies)


def stage1(me, src, full, bg, part=None):
    send, recv, own, buf = bg
    lo, count, at = (0, TOK, 0) if part is None else (part * (TOK // 2), TOK // 2, 8 * part)
    there = full.at[shard_rows(me, lo, count), :]
    mine = buf.at[0, pl.ds(lo, count), :]
    copies = [pltpu.make_async_remote_copy(
        src_ref=mine, dst_ref=there, send_sem=send.at[at + k], recv_sem=recv.at[at + k],
        device_id=(peer_of(me, mask),), device_id_type=MESH) for k, mask in enumerate((2, 4, 1))]
    loads = [] if part == 1 or src is None else [pltpu.make_async_copy(src, buf.at[0], own.at[0])]
    return Stage(loads, copies + [pltpu.make_async_copy(mine, there, own.at[3 if part == 1 else 2])])


def stage2(me, full, bg):
    send, recv, own, buf = bg
    xn, yn = peer_of(me, 2), peer_of(me, 4)
    half = TOK // 2
    plan = ((1, half, half, yn, 2), (0, 0, half, xn, 4), (0, 0, TOK, xn, 1), (1, 0, TOK, yn, 1))
    return Stage(
        [pltpu.make_async_copy(full.at[shard_rows(dev), :], buf.at[n], own.at[n]) for n, dev in enumerate((xn, yn))],
        [pltpu.make_async_remote_copy(
            src_ref=buf.at[slot, pl.ds(lo, count), :], dst_ref=full.at[shard_rows(dev, lo, count), :],
            send_sem=send.at[3 + k], recv_sem=recv.at[3 + k], device_id=(peer_of(me, mask),), device_id_type=MESH)
         for k, (slot, lo, count, dev, mask) in enumerate(plan)])


def stage3(me, full, bg):
    send, recv, own, buf = bg
    rows = full.at[shard_rows(peer_of(me, 6)), :]
    return Stage([pltpu.make_async_copy(rows, buf.at[1], own.at[1])], [pltpu.make_async_remote_copy(
        src_ref=buf.at[1], dst_ref=rows, send_sem=send.at[7], recv_sem=recv.at[7],
        device_id=(peer_of(me, 1),), device_id_type=MESH)])


def route(me):
    core = me % 2
    first = peer_of(me, 2) * (1 - core) + peer_of(me, 4) * core
    second = peer_of(me, 4) * (1 - core) + peer_of(me, 2) * core
    return core, peer_of(me, 1), first, second


def half_rows(c):
    return pl.ds(pl.multiple_of(c * (DIM // 2), DIM // 2), DIM // 2)


def start(copies):
    for c in copies:
        c.start()


def wait(copies):
    for c in copies:
        c.wait()


def row_sums(vals):
    folded = vals[:, :HD]
    for start in range(HD, vals.shape[1], HD):
        folded = folded + vals[:, start:start + HD]
    return jnp.sum(folded.T, axis=0, keepdims=True)


def columns_of(rows):
    turned = rows.T
    return [jnp.broadcast_to(turned[:, c:c + 1], (rows.shape[1], HD)) for c in range(rows.shape[0])]


def as_column(row):
    return jnp.broadcast_to(row, (HD, row.shape[1])).T


def exchange(me, srcs, slots, send_sems, recv_sems):
    copies = []
    for n, (src, slot) in enumerate(zip(srcs, slots)):
        for p, mask in enumerate(ORDER):
            copies.append(pltpu.make_async_remote_copy(
                src_ref=src, dst_ref=slot.at[p], send_sem=send_sems.at[n, p], recv_sem=recv_sems.at[n, p],
                device_id=(peer_of(me, mask),), device_id_type=MESH))
    return copies


def ordered_total(me, src, slot):
    own = src[...]
    total = jnp.zeros_like(own)
    for dev in range(NDEV):
        term = jnp.where(me == dev, own, 0.0)
        for p, mask in enumerate(ORDER):
            term = term + jnp.where(peer_of(me, mask) == dev, slot[p], 0.0)
        total = total + term
    return total


def causal_mask():
    keys = lax.broadcasted_iota(jnp.int32, (BLK, BLK), 0)
    queries = lax.broadcasted_iota(jnp.int32, (BLK, BLK), 1)
    return keys <= queries


def block_rows(i):
    return pl.ds(pl.multiple_of(i * BLK, BLK), BLK)


def head_cols(h):
    return pl.ds(pl.multiple_of(h * HD, HD), HD)


def forward_kernel(freq_ref, wq_ref, wk_ref, wv_ref, gains_ref, x_ref, wo_ref,
                   cos_ref, sin_ref, inv_ref, o_ref, lse_ref, raw_ref, qkv_ref, both_ref, full_ref, wof_ref,
                   raw, qkv, xbuf, sums_scr, slot, p_scr, vt_scr, acc_scr, o_scr, buf0, buf1,
                   ex_send, ex_recv, out_sems, send_sems, recv_sems, own_sems, x_sems, *bg_sems):
    g = pl.program_id(0)
    b, t = g // (4 * NB), g % (4 * NB)
    me = lax.axis_index('tp')
    bg0, bg1, bg2 = (*bg_sems[:3], buf0), (*bg_sems[3:6], buf1), (*bg_sems[6:], buf0)
    x0f, x1f = full_ref.at[0], full_ref.at[1]

    def x_gather(part=None):
        return stage1(me, x_ref.at[1], x1f, bg1, part)

    def wo_gather(part=None):
        return stage1(me, wo_ref, wof_ref, bg2, part)

    def keep(bb):
        return [pltpu.make_async_copy(raw, raw_ref.at[bb], out_sems.at[0]),
                pltpu.make_async_copy(qkv, qkv_ref.at[bb], out_sems.at[1])]

    def sums(bb):
        return exchange(me, [sums_scr.at[bb]], [slot.at[bb]], ex_send.at[bb], ex_recv.at[bb])

    def fetch(bb, i):
        return pltpu.make_async_copy(full_ref.at[bb, block_rows(i), :], xbuf.at[i % 2], x_sems.at[i % 2])

    def block_copy(bb, hh, st, half):
        dest = 2 * ((me // 2 + 1 + st) % NB) + half
        part = o_scr.at[bb, hh, st, pl.ds(half * TOK, TOK), :]
        dst = both_ref.at[bb, :, pl.ds(pl.multiple_of(me * LOC + hh * HD, HD), HD)]
        away = pltpu.make_async_remote_copy(
            src_ref=part, dst_ref=dst, send_sem=send_sems.at[bb, hh, st, half], recv_sem=recv_sems.at[bb, hh, me],
            device_id=(dest,), device_id_type=MESH)
        return dest, away, pltpu.make_async_copy(part, dst, own_sems.at[bb, hh])

    def run(stage):
        stage.load()
        stage.send()

    @pl.when(g == 0)
    def _():
        first = stage1(me, x_ref.at[0], x0f, bg0)
        entry_signal(me)
        first.load()
        entry_wait()
        first.send()
        x_gather(0).load()
        freq = freq_ref[...]
        sign = jnp.where(lax.broadcasted_iota(jnp.int32, (TOK, HD), 1) < HD // 2, -1.0, 1.0)

        def table(i, carry):
            rows = pl.ds(pl.multiple_of(i * TOK, TOK), TOK)
            pos = (lax.broadcasted_iota(jnp.int32, (TOK, HD), 0) + i * TOK).astype(F32)
            angle = pos * freq
            cos_ref[rows, :] = jnp.cos(angle)
            sin_ref[rows, :] = jnp.sin(angle) * sign
            return carry

        lax.fori_loop(0, SEQ // TOK, table, 0)
        first.wait()
        second, third = stage2(me, x0f, bg0), stage3(me, x0f, bg0)
        run(second)
        x_gather(0).send()
        second.wait()
        run(third)
        third.wait()
        fetch(0, 0).start()

    @pl.when(g == 2 * NB + 2)
    def _():
        x_gather(0).wait()
        x_gather(1).wait()
        run(stage2(me, x1f, bg1))
        run(wo_gather(0))

    @pl.when(g == 4 * NB)
    def _():
        stage2(me, x1f, bg1).wait()
        third = stage3(me, x1f, bg1)
        run(third)
        for c in keep(0):
            c.wait()
        third.wait()
        fetch(1, 0).start()

    @pl.when(g == 6 * NB + 2)
    def _():
        wo_gather(0).wait()
        wo_gather(1).wait()
        run(stage2(me, wof_ref, bg2))

    @pl.when(t < NB)
    def _():
        rows = block_rows(t)

        @pl.when(t < NB - 1)
        def _():
            fetch(b, t + 1).start()

        fetch(b, t).wait()
        x = xbuf[t % 2]
        for n, w_ref in enumerate((wq_ref, wk_ref)):
            val = dot(x, w_ref[...])
            raw[n, rows, :] = val
            sums_scr[b, pl.ds(t + n * NB, 1), :] = row_sums(val * val)
        qkv[2, rows, :] = dot(x, wv_ref[...]).astype(BF)

    @pl.when(t == NB)
    def _():
        start(sums(b))
        keep(b)[0].start()
        pl.when(b == 0)(x_gather(1).send)
        pl.when(b == 1)(wo_gather(1).send)
        wait(sums(b))
        inv_ref[...] = lax.rsqrt(ordered_total(me, sums_scr.at[b], slot.at[b]) / DIM + EPS)

    @pl.when(jnp.logical_and(t >= NB, t < 2 * NB))
    def _():
        i = t - NB
        rows = block_rows(i)
        cos, sin = cos_ref[rows, :], sin_ref[rows, :]
        for n in range(2):
            inv = as_column(inv_ref[pl.ds(i + n * NB, 1), :])
            gain = gains_ref[n:n + 1, :]
            for h in range(LOC // HD):
                sl = slice(h * HD, (h + 1) * HD)
                hat = raw[n, rows, sl] * inv * gain[:, sl]
                qkv[n, rows, sl] = (hat * cos + pltpu.roll(hat, HD // 2, 1) * sin).astype(BF)

    @pl.when(t == 2 * NB)
    def _():
        keep(b)[1].start()

    @pl.when(t >= 2 * NB)
    def _():
        h, step = t // NB - 2, t % NB
        qi = (me // 2 + 1 + step) % NB
        cols = head_cols(h)

        @pl.when(step == 0)
        def _():
            vt_scr[...] = qkv[2, :, cols].T

        qb = qkv[0, block_rows(qi), cols]

        def scores(j):
            return dot(qkv[1, block_rows(j), cols], qb, NT)

        def first(j, m):
            s = scores(j)
            p_scr[j] = s
            return jnp.maximum(m, jnp.max(s.reshape(BLK // 8, 8, BLK), axis=0))

        s = jnp.where(causal_mask(), scores(qi), -1e30)
        p_scr[qi] = s
        m = lax.fori_loop(0, qi, first, jnp.max(s.reshape(BLK // 8, 8, BLK), axis=0))
        m = jnp.max(m, axis=0, keepdims=True)

        def second(j, l):
            p = jnp.exp2((p_scr[j] - m) * C2)
            p_scr[j] = p
            return l + jnp.sum(p.reshape(BLK // 8, 8, BLK), axis=0)

        l = lax.fori_loop(0, qi + 1, second, jnp.zeros((8, BLK), F32))
        l = jnp.sum(l, axis=0, keepdims=True)
        rl = 1.0 / l
        lse_ref[pl.ds(h * NB + qi, 1), :] = m * C2 + jnp.log2(l)

        acc_scr[...] = jnp.zeros_like(acc_scr)

        def third(j, carry):
            p = (p_scr[j] * rl).astype(BF)
            acc_scr[...] += dot(vt_scr[:, block_rows(j)], p)
            return carry

        lax.fori_loop(0, qi + 1, third, 0)
        out = acc_scr[...].T.astype(BF)
        o_scr[b, h, step] = out
        o_ref[block_rows(qi), cols] = out

        for half in range(2):
            dest, away, here = block_copy(b, h, step, half)
            pl.when(dest != me)(away.start)
            pl.when(dest == me)(here.start)

    @pl.when(g == 8 * NB - 1)
    def _():
        stage2(me, wof_ref, bg2).wait()
        third = stage3(me, wof_ref, bg2)
        run(third)
        for c in keep(1):
            c.wait()

        def drain(n, carry):
            bb, hh = n // 2, n % 2
            for st in range(NB):
                for half in range(2):
                    dest, away, here = block_copy(bb, hh, st, half)
                    if st < NB - 1:
                        away.wait_send()
                    else:
                        pl.when(dest != me)(away.wait_send)
                        pl.when(dest == me)(here.wait)
            for mask in ORDER:
                peer = peer_of(me, mask)
                pltpu.make_async_remote_copy(
                    src_ref=o_scr.at[0, 0, 0, pl.ds(0, TOK), :],
                    dst_ref=both_ref.at[bb, :, pl.ds(pl.multiple_of(peer * LOC + hh * HD, HD), HD)],
                    send_sem=send_sems.at[0, 0, 0, 0], recv_sem=recv_sems.at[bb, hh, peer],
                    device_id=(peer,), device_id_type=MESH).wait_recv()
            return carry

        lax.fori_loop(0, 4, drain, 0)
        third.wait()


def forward(x, wq, wk, wv, wo, gains, cid):
    inv_freq = np.float32(1.0) / np.float32(ROPE_THETA) ** (np.arange(HD // 2, dtype=np.float32) / np.float32(HD // 2))
    freq = jnp.asarray(np.concatenate([inv_freq, inv_freq])[None, :], F32)

    def whole(*shape):
        return pl.BlockSpec(shape, lambda g: (0,) * len(shape))

    def per_batch(*shape):
        return pl.BlockSpec((None,) + shape, lambda g: (g // (4 * NB),) + (0,) * len(shape))

    wspec, rows = whole(DIM, LOC), per_batch(2 * NB, BLK)
    return pl.pallas_call(
        forward_kernel,
        grid=(8 * NB,),
        in_specs=[whole(1, HD), wspec, wspec, wspec, whole(2 + DIM // LOC, LOC), ANYWHERE, ANYWHERE],
        out_specs=[whole(SEQ, HD), whole(SEQ, HD), rows, per_batch(SEQ, LOC), rows] + [ANYWHERE] * 5,
        out_shape=[sds((SEQ, HD), F32), sds((SEQ, HD), F32), sds((2, 2 * NB, BLK), F32), sds((2, SEQ, LOC), BF),
                   sds((2, 2 * NB, BLK), F32), sds((2, 2, SEQ, LOC), F32), sds((2, 3, SEQ, LOC), BF),
                   sds((2, TOK, DIM), BF), sds((2, SEQ, DIM), BF), sds((SEQ, DIM), BF)],
        scratch_shapes=[pltpu.VMEM((2, SEQ, LOC), F32), pltpu.VMEM((3, SEQ, LOC), BF), pltpu.VMEM((2, BLK, DIM), BF),
                        pltpu.VMEM((2, 2 * NB, BLK), F32), pltpu.VMEM((2, NDEV - 1, 2 * NB, BLK), F32),
                        pltpu.VMEM((NB, BLK, BLK), F32), pltpu.VMEM((HD, SEQ), BF), pltpu.VMEM((HD, BLK), F32),
                        pltpu.VMEM((2, 2, NB, BLK, HD), BF), pltpu.VMEM((2, TOK, DIM), BF), pltpu.VMEM((2, TOK, DIM), BF),
                        DMA((2, 1, NDEV - 1)), DMA((2, 1, NDEV - 1)), DMA((2,)),
                        DMA((2, 2, NB, 2)), DMA((2, 2, NDEV)), DMA((2, 2)), DMA((2,))] + BG_SEMS * 3,
        compiler_params=params(dimension_semantics=("arbitrary",), collective_id=cid, has_side_effects=True),
        cost_estimate=cost(60e9, 60e6),
        name="forward",
    )(freq, wq, wk, wv, gains, x, wo)


def out_kernel(o_ref, x_ref, dy_ref, gains_ref, wo_ref, y_ref, da_ref, gga_ref, full_ref, wo_scr, a_scr, wo_sems, buf, *bg_sems):
    b = pl.program_id(0)
    me = lax.axis_index('tp')
    bg = (*bg_sems, buf)
    step = DIM // NB

    def piece(j):
        cols = pl.ds(pl.multiple_of(j * step, step), step)
        return cols, pltpu.make_async_copy(wo_ref.at[:, cols], wo_scr.at[:, cols], wo_sems.at[j])

    @pl.when(b == 0)
    def _():
        nbr_signal(me)
        for j in range(NB):
            piece(j)[1].start()
        gga_ref[...] = jnp.zeros_like(gga_ref)

    o = o_ref[0]

    def fwd(j, carry):
        cols, load = piece(j)
        pl.when(b == 0)(load.wait)
        a_scr[:, cols] = dot(o, wo_scr[:, cols])
        return carry

    lax.fori_loop(0, NB, fwd, 0)
    a = a_scr[...]
    r = lax.rsqrt(jnp.mean(a * a, axis=-1, keepdims=True) + EPS)
    n = a * r
    ga = jnp.concatenate([gains_ref[2 + i:3 + i, :] for i in range(8)], axis=1)
    dy = dy_ref[0].astype(F32)
    gn = dy * ga
    da = (r * (gn - n * jnp.mean(gn * n, axis=-1, keepdims=True))).astype(BF)
    da_ref[0] = da

    @pl.when(b == 0)
    def _():
        buf[0] = da
        nbr_wait()
        stage1(me, None, full_ref, bg).send()

    y_ref[0] = (x_ref[0].astype(F32) + n * ga).astype(BF)
    col = jnp.sum(dy * n, axis=0, keepdims=True)
    for i in range(8):
        gga_ref[i:i + 1, :] += col[:, i * LOC:(i + 1) * LOC]

    @pl.when(b == 1)
    def _():
        stage1(me, None, full_ref, bg).wait()


def out_block(o, wo, x, dy, gains, cid):
    def whole(*shape):
        return pl.BlockSpec(shape, lambda i: (0,) * len(shape))

    batch = pl.BlockSpec((1, TOK, DIM), lambda i: (i, 0, 0))
    return pl.pallas_call(
        out_kernel,
        grid=(2,),
        in_specs=[batch, batch, batch, whole(2 + DIM // LOC, LOC), ANYWHERE],
        out_specs=[batch, batch, whole(8, DIM // 8), ANYWHERE],
        out_shape=[sds((2, TOK, DIM), BF), sds((2, TOK, DIM), BF), sds((8, DIM // 8), F32), sds((SEQ, DIM), BF)],
        scratch_shapes=[pltpu.VMEM((DIM, DIM), BF), pltpu.VMEM((TOK, DIM), F32), DMA((NB,)),
                        pltpu.VMEM((2, TOK, DIM), BF)] + BG_SEMS,
        compiler_params=params(dimension_semantics=("arbitrary",), collective_id=cid, has_side_effects=True),
        cost_estimate=cost(8 * TOK * DIM * DIM + 5e9, 18e6),
        name="out_block",
    )(o, x, dy, gains, wo)


def backward_kernel(b, qkv_ref, wo_ref, lse_ref, raw_hbm, inv_ref, gains_ref, cos_hbm, sin_hbm, gga_ref,
                    wq_ref, wk_ref, wv_ref, da_ref, *rest):
    if b:
        d0_ref, pd0_ref, pw_ref, d_ref, pd_ref, gg_ref, gout_ref, got_ref, da_ref, buf0, w_all, d_two, sbuf, *rest = rest
    else:
        shard_ref, d_ref, pd_ref, gg_ref, gout_ref, full_ref, pw_ref, da_ref, buf0, buf1, w_half, *rest = rest
    (p_scr, dp_scr, kt_scr, dqt_scr, dq_scr, dk_scr, dv_scr, du_scr, d_scr, dh_scr, dbuf, dots_scr, total, slot, ga_slot,
     ex_send, ex_recv, pd_send, pd_recv, d_sems, rs_sems, ld_sems, db_sems, raw_ref, cos_ref, sin_ref, tb_sems, *bg_sems) = rest
    h, step = pl.program_id(0), pl.program_id(1)
    me = lax.axis_index('tp')

    def chip_at(n):
        ax, ay = (me // 2) % 2, me // 4
        return (ay + (n // 2) * (1 - 2 * ay)) * 2 + ax + (n % 2) * (1 - 2 * ax)

    def fetch(n):
        return pltpu.make_async_copy(da_ref.at[block_rows(chip_at(n)), :], dbuf.at[n % 2], db_sems.at[n % 2])

    qi = chip_at(step)
    tables = [pltpu.make_async_copy(src, dst, tb_sems.at[n]) for n, (src, dst) in enumerate(
        ((raw_hbm.at[b], raw_ref), (cos_hbm, cos_ref), (sin_hbm, sin_ref)))]
    core, partner, first_dev, _ = route(me)
    weights = (wq_ref, wk_ref, wv_ref)

    bg0 = (*bg_sems[:3], buf0)
    older3 = stage3(me, da_ref, bg0)
    if b:
        operands = []
        for blk, chip in enumerate((peer_of(me, 6) // 2, first_dev // 2)):
            operands += [pltpu.make_async_copy(d.at[block_rows(chip), :], d_two.at[blk, n], ld_sems.at[2 * blk + n])
                         for n, d in enumerate((d0_ref, pd0_ref))]
        operands += [pltpu.make_async_copy(w.at[half_rows(core), :], w_all.at[0, :, pl.ds(n * LOC, LOC)], ld_sems.at[4 + n])
                     for n, w in enumerate(weights)]
        operands.append(pltpu.make_async_copy(pw_ref, w_all.at[1], ld_sems.at[7]))
        moved = [pltpu.make_async_remote_copy(
            src_ref=sbuf.at[blk, pl.ds(lo, count), :], dst_ref=got_ref.at[blk, pl.ds(lo, count), :], send_sem=rs_sems.at[n],
            recv_sem=rs_sems.at[3 + n], device_id=(first_dev,), device_id_type=MESH)
            for n, (blk, lo, count) in enumerate(((0, 0, BLK), (1, 0, BLK * 3 // 4), (1, BLK * 3 // 4, BLK // 4)))]
    else:
        bg = (*bg_sems[3:], buf1)
        older2 = stage2(me, da_ref, bg0)
        gather = stage1(me, shard_ref.at[1], full_ref, bg)
        operands = [pltpu.make_async_copy(w.at[half_rows(1 - core), :], w_half.at[:, pl.ds(n * LOC, LOC)], ld_sems.at[n])
                    for n, w in enumerate(weights)]
        moved = [pltpu.make_async_remote_copy(
            src_ref=w_half, dst_ref=pw_ref, send_sem=rs_sems.at[0], recv_sem=rs_sems.at[3], device_id=(partner,),
            device_id_type=MESH)]

    @pl.when(jnp.logical_and(h == 0, step == 0))
    def _():
        entry_signal(me)
        if b:
            needed, rest_of = operands[:2] + operands[4:], operands[2:4]
            start(needed)
            fetch(0).start()
            start(rest_of)
            older3.load()
            start(tables)
            wait(needed)
            sbuf[0] = dot(d_two[0, 0], w_all[0], NT) + dot(d_two[0, 1], w_all[1], NT)
            entry_wait()
            moved[0].start()
            older3.send()
            wait(rest_of)
            sbuf[1] = dot(d_two[1, 0], w_all[0], NT) + dot(d_two[1, 1], w_all[1], NT)
            moved[1].start()
        else:
            older2.load()
            fetch(0).start()
            gather.load()
            start(operands)
            start(tables)
            entry_wait()
            older2.send()
            gather.send()
            wait(operands)
            start(moved)
        dots_scr[...] = jnp.zeros_like(dots_scr)

    @pl.when(jnp.logical_and(h == 0, step == NB - 1))
    def _():
        older3.wait()
        fetch(NB - 1).start()

    @pl.when(h == 0)
    def _():
        fetch(step).wait()
        dh_scr[block_rows(qi), :] = dot(dbuf[step % 2], wo_ref[...], NT).astype(BF)
        if b:
            @pl.when(step < NB - 2)
            def _():
                fetch(step + 1).start()
        else:
            @pl.when(step == 0)
            def _():
                older2.wait(2, 3)

            @pl.when(step < NB - 2)
            def _():
                fetch(step + 1).start()

            @pl.when(step == NB - 2)
            def _():
                older2.wait(0, 1)
                older3.load()
                older3.send()

    @pl.when(step == 0)
    def _():
        kt_scr[...] = qkv_ref[1].T
        dk_scr[...] = jnp.zeros_like(dk_scr)
        dv_scr[...] = jnp.zeros_like(dv_scr)

    qb = qkv_ref[0, block_rows(qi), :]
    dob = dh_scr[block_rows(qi), head_cols(h)]
    lse = lse_ref[pl.ds(h * NB + qi, 1), :]

    def first(j, acc, diag=False):
        rows = block_rows(j)
        p = jnp.exp2(dot(qkv_ref[1, rows, :], qb, NT) * C2 - lse)
        if diag:
            p = jnp.where(causal_mask(), p, 0.0)
        dp = dot(qkv_ref[2, rows, :], dob, NT)
        p_scr[j] = p
        dp_scr[j] = dp
        dv_scr[rows, :] += dot(p.astype(BF), dob)
        return acc + jnp.sum((p * dp).reshape(BLK // 8, 8, BLK), axis=0)

    acc = first(qi, jnp.zeros((8, BLK), F32), True)
    acc = lax.fori_loop(0, qi, first, acc)
    delta = jnp.sum(acc, axis=0, keepdims=True)
    dqt_scr[...] = jnp.zeros_like(dqt_scr)

    def second(j, carry):
        rows = block_rows(j)
        ds = (p_scr[j] * (dp_scr[j] - delta) * SCALE).astype(BF)
        dk_scr[rows, :] += dot(ds, qb)
        dqt_scr[...] += dot(kt_scr[:, rows], ds)
        return carry

    lax.fori_loop(0, qi + 1, second, 0)
    dq_scr[block_rows(qi), :] = dqt_scr[...].T

    @pl.when(step == NB - 1)
    def _():
        d_scr[:, pl.ds(pl.multiple_of(2 * LOC + h * HD, HD), HD)] = dv_scr[...].astype(BF)
        gg_ref[...] = jnp.zeros_like(gg_ref)
        cols = head_cols(h)

        @pl.when(h == 0)
        def _():
            wait(tables)


        inverse = columns_of(inv_ref[...])
        for i in range(NB):
            rows = pl.ds(i * BLK, BLK)
            cos, sin = cos_ref[rows, :], sin_ref[rows, :]
            for n, from_scr in enumerate((dq_scr, dk_scr)):
                d = from_scr[rows, :]
                hat = d * cos - pltpu.roll(d, HD // 2, 1) * sin
                unit = raw_ref[n, rows, cols] * inverse[i + n * NB]
                gg_ref[n:n + 1, :] += jnp.sum(hat * unit, axis=0, keepdims=True)
                du = hat * gains_ref[n:n + 1, :]
                du_scr[n, h, rows, :] = du
                dots_scr[i + n * NB:i + n * NB + 1, :] += row_sums(du * unit)

    @pl.when(jnp.logical_and(h == 1, step == NB - 1))
    def _():
        srcs, slots = ([dots_scr], [slot]) if b else ([dots_scr, gga_ref], [slot, ga_slot])
        sums = exchange(me, srcs, slots, ex_send, ex_recv)
        start(sums)
        if b:
            moved[2].start()
        else:
            gather.wait()
            more = stage2(me, full_ref, bg)
            more.load()
            more.send()
        wait(sums)
        total[...] = ordered_total(me, dots_scr, slot) / DIM
        gout_ref[...] = gga_ref[...] if b else ordered_total(me, gga_ref, ga_slot)

        def copies(i):
            rows = block_rows(i)
            return [pltpu.make_async_copy(d_scr.at[rows, :], d_ref.at[rows, :], d_sems.at[i]),
                    pltpu.make_async_remote_copy(
                        src_ref=d_scr.at[rows, :], dst_ref=pd_ref.at[rows, :], send_sem=pd_send.at[i],
                        recv_sem=pd_recv.at[i], device_id=(peer_of(me, 1),), device_id_type=MESH)]

        inverse, dots = columns_of(inv_ref[...]), columns_of(total[...])
        for i in range(NB):
            rows = pl.ds(i * BLK, BLK)
            for n in range(2):
                inv = inverse[i + n * NB]
                for hh in range(LOC // HD):
                    sl = slice(hh * HD, (hh + 1) * HD)
                    unit = raw_ref[n, rows, sl] * inv
                    val = inv * (du_scr[n, hh, rows, :] - unit * dots[i + n * NB])
                    d_scr[rows, n * LOC + hh * HD:n * LOC + (hh + 1) * HD] = val.astype(BF)
            start(copies(i))
        for i in range(NB):
            wait(copies(i))
        wait(moved)
        if not b:
            more.wait()


def backward(b, da, qkv, wo, lse, raw, inv, gains, cos, sin, gga, weights, others, cid):
    def whole(*shape):
        return pl.BlockSpec(shape, lambda h, i: (0,) * len(shape))

    def picked(*shape):
        return pl.BlockSpec((None,) + shape, lambda h, i: (b,) + (0,) * len(shape))

    gsp = whole(8, DIM // 8)
    half = (DIM // 2, 3 * LOC)
    if b:
        extra = [sds((2, BLK, DIM // 2), F32), sds((SEQ, DIM), BF)]
        own = [pltpu.VMEM((2, TOK, DIM), BF), pltpu.VMEM((2,) + half, BF), pltpu.VMEM((2, 2, BLK, 3 * LOC), BF), pltpu.VMEM((2, BLK, DIM // 2), F32)]
    else:
        extra = [sds((SEQ, DIM), BF), sds(half, BF), sds((SEQ, DIM), BF)]
        own = [pltpu.VMEM((2, TOK, DIM), BF), pltpu.VMEM((2, TOK, DIM), BF), pltpu.VMEM(half, BF)]
    return pl.pallas_call(
        functools.partial(backward_kernel, b),
        grid=(2, NB),
        in_specs=[pl.BlockSpec((None, 3, SEQ, HD), lambda h, i: (b, 0, 0, h)),
                  whole(LOC, DIM),
                  picked(2 * NB, BLK), ANYWHERE, picked(2 * NB, BLK),
                  pl.BlockSpec((2 + DIM // LOC, HD), lambda h, i: (0, h)), ANYWHERE, ANYWHERE, gsp]
        + [ANYWHERE] * (4 + len(others)),
        out_specs=[ANYWHERE, ANYWHERE, pl.BlockSpec((8, HD), lambda h, i: (0, h)), gsp] + [ANYWHERE] * len(extra),
        out_shape=[sds((SEQ, 3 * LOC), BF), sds((SEQ, 3 * LOC), BF), sds((8, LOC), F32), sds((8, DIM // 8), F32)] + extra,
        input_output_aliases={12: 5 if b else 6},
        scratch_shapes=own + [
            pltpu.VMEM((NB, BLK, BLK), F32), pltpu.VMEM((NB, BLK, BLK), F32), pltpu.VMEM((HD, SEQ), BF),
            pltpu.VMEM((HD, BLK), F32), pltpu.VMEM((SEQ, HD), F32), pltpu.VMEM((SEQ, HD), F32),
            pltpu.VMEM((SEQ, HD), F32), pltpu.VMEM((2, 2, SEQ, HD), F32), pltpu.VMEM((SEQ, 3 * LOC), BF),
            pltpu.VMEM((SEQ, LOC), BF), pltpu.VMEM((2, BLK, DIM), BF), pltpu.VMEM((2 * NB, BLK), F32), pltpu.VMEM((2 * NB, BLK), F32),
            pltpu.VMEM((NDEV - 1, 2 * NB, BLK), F32), pltpu.VMEM((NDEV - 1, 8, DIM // 8), F32),
            DMA((2, NDEV - 1)), DMA((2, NDEV - 1)), DMA((NB,)), DMA((NB,)), DMA((NB,)), DMA((6,)), DMA((8,)), DMA((2,)),
            pltpu.VMEM((2, SEQ, LOC), F32), pltpu.VMEM((SEQ, HD), F32), pltpu.VMEM((SEQ, HD), F32), DMA((3,))]
        + BG_SEMS * (1 if b else 2),
        compiler_params=params(dimension_semantics=("arbitrary", "arbitrary"), collective_id=cid, has_side_effects=True),
        cost_estimate=cost(25e9, 30e6),
        name="backward",
    )(qkv, wo, lse, raw, inv, gains, cos, sin, gga, *weights, da, *others)


HALF = DIM // 2
CH = 256


def grads_kernel(d0, d1, pd0, pd1, wq, wk, wv, pw, got, x_full, o_all, da0, da1, dy_ref, dx_out, gwq_out, gwk_out, gwv_out, gwo_out,
                 d_all, w_all, sbuf, r1, r2, fin, acc, xbuf, obuf,
                 dl_sems, w_sems, s1_sems, r1_sems, s2_sems, r2_sems, fs_sems, fr_sems, x_sems, o_sems, dx_ref, gwq_ref, gwk_ref, gwv_ref, gwo_ref, out_sems):
    me = lax.axis_index('tp')
    core, partner, first, second = route(me)
    chip = me // 2
    diag_chip, first_chip, second_chip = peer_of(me, 6) // 2, first // 2, second // 2

    barrier = pltpu.get_barrier_semaphore()
    for dev in (partner, first, second):
        pl.semaphore_signal(barrier, inc=1, device_id=(dev,), device_id_type=MESH)

    def rows_of(blk):
        return pl.ds(pl.multiple_of(blk * BLK, BLK), BLK)

    results = [pltpu.make_async_copy(src, dst, out_sems.at[n]) for n, (src, dst) in enumerate((
        (gwq_ref, gwq_out), (gwk_ref, gwk_out), (gwv_ref, gwv_out), (gwo_ref, gwo_out)))]
    chips = (diag_chip, first_chip, second_chip, chip)
    w_copies = [pltpu.make_async_copy(w.at[half_rows(core), :], w_all.at[0, :, pl.ds(n * LOC, LOC)], w_sems.at[n])
                for n, w in enumerate((wq, wk, wv))]
    w_copies.append(pltpu.make_async_copy(pw, w_all.at[1], w_sems.at[3]))
    loads = []
    for n in range(8):
        rows, b = rows_of(chips[n // 2]), n % 2
        loads.append([pltpu.make_async_copy(d.at[rows, :], d_all.at[side, b, rows, :], dl_sems.at[side, n])
                      for side, d in enumerate(((d0, d1)[b], (pd0, pd1)[b]))])
    start(w_copies)
    start(loads[1])
    pl.semaphore_wait(barrier, 3)
    wait(w_copies)

    def partial(b, blk):
        rows = rows_of(blk)
        return dot(d_all[0, b, rows, :], w_all[0], NT) + dot(d_all[1, b, rows, :], w_all[1], NT)

    def to_first(n):
        return pltpu.make_async_remote_copy(
            src_ref=sbuf.at[n // 2], dst_ref=r1.at[n], send_sem=s1_sems.at[n], recv_sem=r1_sems.at[n],
            device_id=(first,), device_id_type=MESH)

    def to_second(b):
        return pltpu.make_async_remote_copy(
            src_ref=r1.at[b], dst_ref=r2.at[b], send_sem=s2_sems.at[b], recv_sem=r2_sems.at[b],
            device_id=(second,), device_id_type=MESH)

    def to_partner(b):
        return pltpu.make_async_remote_copy(
            src_ref=r1.at[2 + b, pl.ds(pl.multiple_of((1 - core) * TOK, TOK), TOK), :], dst_ref=fin.at[b],
            send_sem=fs_sems.at[b], recv_sem=fr_sems.at[b], device_id=(partner,), device_id_type=MESH)

    taken = [pltpu.make_async_copy(got.at[n], r1.at[2 * n], w_sems.at[4 + n]) for n in range(2)]
    for n in (1, 3):
        wait(loads[n])
        if n == 1:
            start(loads[3])
        sbuf[n // 2] = partial(1, chips[n // 2])
        to_first(n).start()
        if n == 1:
            start(taken)
            for later in (4, 0, 2, 5, 6, 7):
                start(loads[later])
    for n in (0, 2, 4, 5, 6, 7):
        wait(loads[n])
    wait(taken)

    steps = SEQ // CH

    def chunk(i):
        return pl.ds(pl.multiple_of(i * CH, CH), CH)

    def stream(pairs, body):
        def fetch(i):
            return [pltpu.make_async_copy(src.at[chunk(i), :], buf.at[i % 2], sems.at[i % 2]) for src, buf, sems in pairs]

        for c in fetch(0):
            c.start()

        def it(i, carry):
            @pl.when(i + 1 < steps)
            def _():
                for c in fetch(i + 1):
                    c.start()

            for c in fetch(i):
                c.wait()
            body(i)
            return carry

        lax.fori_loop(0, steps, it, 0)

    def wgrad(b, src):
        def body(i):
            left = d_all[0, b, chunk(i), :].T
            for c in range(3):
                part = slice(c * LOC, (c + 1) * LOC)
                acc[part, :] += dot(left[part, :], xbuf[i % 2])

        stream([(src, xbuf, x_sems)], body)

    def forward_second(b):
        if b:
            to_first(b).wait_recv()
        r1[b] += partial(b, second_chip)
        to_second(b).start()

    forward_second(0)
    acc[...] = jnp.zeros_like(acc)
    wgrad(0, x_full.at[0])
    wgrad(1, x_full.at[1])
    for n, ref in enumerate((gwq_ref, gwk_ref, gwv_ref)):
        ref[...] = acc[n * LOC:(n + 1) * LOC, :].T.astype(BF)
        results[n].start()
    forward_second(1)
    acc[:LOC, :] = jnp.zeros((LOC, DIM), F32)

    def wo_body(i):
        acc[:LOC, :] += dot(obuf[i % 2].T, xbuf[i % 2])

    for o_src, da_src in ((o_all.at[0], da0), (o_all.at[1], da1)):
        stream([(da_src, xbuf, x_sems), (o_src, obuf, o_sems)], wo_body)
    gwo_ref[...] = acc[:LOC, :].astype(BF)
    results[3].start()

    def own_part(b, carry):
        r1_own = partial(b, chip)
        pl.when(b == 1)(to_first(3).wait_recv)
        to_second(b).wait_recv()
        r1[2 + b] += r1_own + r2[b]
        to_partner(b).start()
        cols = half_rows(core)
        rows = pl.ds(pl.multiple_of(core * TOK, TOK), TOK)
        dx_ref[b, :, cols] = (r1[2 + b, rows, :] + dy_ref[b, :, cols].astype(F32)).astype(BF)
        return carry

    lax.fori_loop(0, 2, own_part, 0)

    def finish(b, carry):
        to_partner(b).wait()
        cols = half_rows(1 - core)
        dx_ref[b, :, cols] = (fin[b] + dy_ref[b, :, cols].astype(F32)).astype(BF)
        pltpu.make_async_copy(dx_ref.at[b], dx_out.at[b], out_sems.at[4 + b]).start()
        to_second(b).wait_send()
        return carry

    to_first(1).wait_send()
    to_first(3).wait_send()
    lax.fori_loop(0, 2, finish, 0)
    wait(results)
    for b in range(2):
        pltpu.make_async_copy(dx_ref.at[b], dx_out.at[b], out_sems.at[4 + b]).wait()


def grads(d0, d1, pd0, pd1, wq, wk, wv, pw, got, x_full, o_all, da0, da1, dy, cid):
    vm = pl.BlockSpec(memory_space=pltpu.VMEM)
    far = pl.BlockSpec(memory_space=pl.ANY)
    dma = pltpu.SemaphoreType.DMA
    return pl.pallas_call(
        grads_kernel,
        in_specs=[far] * 13 + [vm],
        out_specs=[far] * 5,
        out_shape=[sds((2, TOK, DIM), BF)] + [sds((DIM, LOC), BF)] * 3 + [sds((LOC, DIM), BF)],
        scratch_shapes=[pltpu.VMEM((2, 2, SEQ, 3 * LOC), BF), pltpu.VMEM((2, HALF, 3 * LOC), BF),
                        pltpu.VMEM((2, BLK, HALF), F32), pltpu.VMEM((4, BLK, HALF), F32), pltpu.VMEM((2, BLK, HALF), F32),
                        pltpu.VMEM((2, TOK, HALF), F32), pltpu.VMEM((3 * LOC, DIM), F32),
                        pltpu.VMEM((2, CH, DIM), BF), pltpu.VMEM((2, CH, LOC), BF),
                        dma((2, 8)), dma((9,)), dma((4,)), dma((4,)), dma((2,)), dma((2,)),
                        dma((2,)), dma((2,)), dma((2,)), dma((2,)), pltpu.VMEM((2, TOK, DIM), BF),
                        pltpu.VMEM((DIM, LOC), BF), pltpu.VMEM((DIM, LOC), BF), pltpu.VMEM((DIM, LOC), BF),
                        pltpu.VMEM((LOC, DIM), BF), dma((6,))],
        compiler_params=pltpu.CompilerParams(vmem_limit_bytes=67043328, collective_id=cid, has_side_effects=True),
        cost_estimate=cost(100e9, 40e6),
        name="grads",
    )(d0, d1, pd0, pd1, wq, wk, wv, pw, got, x_full, o_all, da0, da1, dy)


def deliver_kernel(*refs):
    count = (len(refs) - 2) // 3
    loads, stores = [], []
    for src, dst, buf in zip(refs[:count], refs[count:2 * count], refs[2 * count:3 * count]):
        for part in range(2):
            piece = (part,) if len(src.shape) == 3 else (pl.ds(part * (src.shape[0] // 2), src.shape[0] // 2),)
            n = len(loads)
            loads.append(pltpu.make_async_copy(src.at[piece], buf.at[piece], refs[-2].at[n]))
            stores.append(pltpu.make_async_copy(buf.at[piece], dst.at[piece], refs[-1].at[n]))
    ahead = 4
    start(loads[:ahead])
    for n, (load, store) in enumerate(zip(loads, stores)):
        load.wait()
        store.start()
        start(loads[n + ahead:n + ahead + 1])
    wait(stores)


def deliver(*arrays):
    return pl.pallas_call(
        deliver_kernel,
        in_specs=[ANYWHERE] * len(arrays),
        out_specs=[ANYWHERE] * len(arrays),
        out_shape=[sds(t.shape, t.dtype) for t in arrays],
        scratch_shapes=[pltpu.VMEM(t.shape, t.dtype) for t in arrays] + [DMA((2 * len(arrays),)), DMA((2 * len(arrays),))],
        compiler_params=params(),
        cost_estimate=cost(1e9, 16e6),
        name="deliver",
    )(*arrays)


def local_block(x_loc, wq, wk, wv, wo, gq, gk, ga, dy_loc):
    gains = jnp.concatenate([gq, gk, ga]).astype(F32).reshape(2 + DIM // LOC, LOC)
    weights = (wq, wk, wv)
    cos, sin, inv, o, lse, raw, qkv, o_recv, x_full, wo_full = forward(x_loc, wq, wk, wv, wo, gains, 0)
    y, da, gga, da0 = out_block(o_recv, wo_full, x_loc, dy_loc, gains, 1)
    state = (qkv, wo, lse, raw, inv, gains, cos, sin, gga, weights)
    d0, pd0, gg0, gout, da1, pw, da0 = backward(0, da0, *state, (da,), 2)
    d1, pd1, gg1, _, got, da1 = backward(1, da1, *state, (d0, pd0, pw), 3)
    grad_ga = gout.reshape(DIM).astype(BF)
    big = grads(d0, d1, pd0, pd1, *weights, pw, got, x_full, o, da0, da1, dy_loc, 4)
    y, dx, gwq, gwk, gwv, gwo = deliver(y, *big)
    gg = gg0 + gg1
    return (y, dx, gwq, gwk, gwv, gwo, gg[0].astype(BF), gg[1].astype(BF), grad_ga)


def solution(mesh):
    act, col, row, vec = P(None, 'tp', None), P(None, 'tp'), P('tp', None), P('tp')
    in_specs = (act, col, col, col, row, vec, vec, P(), act)
    out_specs = (act, act, col, col, col, row, vec, vec, P())
    return jax.shard_map(local_block, mesh=mesh, in_specs=in_specs, out_specs=out_specs, check_vma=False)
```

```python
import functools
import math

import jax
import jax.numpy as jnp
import numpy as np
from jax import lax
from jax.experimental import pallas as pl
from jax.experimental.pallas import tpu as pltpu
from jax.sharding import PartitionSpec as P

HD = 128
ROPE_THETA = 500000.0
EPS = 1e-6
DIM = 2048
SEQ = 2048
LOC = 256
TOK = 256
BLK = 512
NB = SEQ // BLK
NDEV = 8
SCALE = HD ** -0.5
C2 = SCALE * math.log2(math.e)
MESH = pl.DeviceIdType.MESH
BF = jnp.bfloat16
F32 = jnp.float32
VMEM_MAX = 60 * 1024 * 1024

NT = (((1,), (1,)), ((), ()))
NN = (((1,), (0,)), ((), ()))


def dot(a, b, dims=NN):
    return lax.dot_general(a, b, dims, preferred_element_type=F32)


def sds(shape, dtype):
    return jax.ShapeDtypeStruct(shape, dtype)


def cost(flops, nbytes, trans=0):
    return pl.CostEstimate(flops=int(flops), bytes_accessed=int(nbytes), transcendentals=int(trans))


def params(**kw):
    return pltpu.CompilerParams(vmem_limit_bytes=VMEM_MAX, **kw)


def peer_of(me, mask):
    core, ax, ay = me % 2, (me // 2) % 2, me // 4
    core = 1 - core if mask & 1 else core
    ax = 1 - ax if mask & 2 else ax
    ay = 1 - ay if mask & 4 else ay
    return ay * 4 + ax * 2 + core


ORDER = (6, 7, 2, 4, 3, 5, 1)


def entry_signal(me):
    for mask in ORDER:
        pl.semaphore_signal(pltpu.get_barrier_semaphore(), inc=1, device_id=(peer_of(me, mask),), device_id_type=MESH)


def entry_wait():
    pl.semaphore_wait(pltpu.get_barrier_semaphore(), NDEV - 1)


def nbr_signal(me):
    for mask in (1, 2, 4):
        pl.semaphore_signal(pltpu.get_barrier_semaphore(), inc=1, device_id=(peer_of(me, mask),), device_id_type=MESH)


def nbr_wait():
    pl.semaphore_wait(pltpu.get_barrier_semaphore(), 3)


DMA = pltpu.SemaphoreType.DMA
ANYWHERE = pl.BlockSpec(memory_space=pl.ANY)
BG_SEMS = [DMA((11,)), DMA((11,)), DMA((5,))]
BG = BG_SEMS + [pltpu.VMEM((2, TOK, DIM), BF)]


def shard_rows(dev, lo=0, count=TOK):
    return pl.ds(pl.multiple_of(dev * TOK + lo, TOK // 4), count)


class Stage:
    def __init__(self, loads, copies):
        self.loads, self.copies = loads, copies

    def load(self):
        start(self.loads)

    def send(self):
        wait(self.loads)
        start(self.copies)

    def wait(self, *which):
        wait([self.copies[n] for n in which] or self.copies)


def stage1(me, src, full, bg, part=None):
    send, recv, own, buf = bg
    lo, count, at = (0, TOK, 0) if part is None else (part * (TOK // 2), TOK // 2, 8 * part)
    there = full.at[shard_rows(me, lo, count), :]
    mine = buf.at[0, pl.ds(lo, count), :]
    copies = [pltpu.make_async_remote_copy(
        src_ref=mine, dst_ref=there, send_sem=send.at[at + k], recv_sem=recv.at[at + k],
        device_id=(peer_of(me, mask),), device_id_type=MESH) for k, mask in enumerate((2, 4, 1))]
    loads = [] if part == 1 or src is None else [pltpu.make_async_copy(src, buf.at[0], own.at[0])]
    return Stage(loads, copies + [pltpu.make_async_copy(mine, there, own.at[3 if part == 1 else 2])])


def stage2(me, full, bg, part=None):
    send, recv, own, buf = bg
    xn, yn = peer_of(me, 2), peer_of(me, 4)
    half = TOK // 2
    lo, count = (0, half) if part is None else (part * (half // 2), half // 2)
    at = 8 if part == 1 else 3
    plan = [(1, half + lo, count, yn, 2, at), (0, lo, count, xn, 4, at + 1)]
    if part != 0:
        plan += [(0, 0, TOK, xn, 1, 5), (1, 0, TOK, yn, 1, 6)]
    loads = [pltpu.make_async_copy(full.at[shard_rows(dev), :], buf.at[n], own.at[n]) for n, dev in enumerate((xn, yn))]
    return Stage([] if part == 1 else loads, [pltpu.make_async_remote_copy(
        src_ref=buf.at[slot, pl.ds(first, rows), :], dst_ref=full.at[shard_rows(dev, first, rows), :],
        send_sem=send.at[sem], recv_sem=recv.at[sem], device_id=(peer_of(me, mask),), device_id_type=MESH)
        for slot, first, rows, dev, mask, sem in plan])


def stage3(me, full, bg):
    send, recv, own, buf = bg
    rows = full.at[shard_rows(peer_of(me, 6)), :]
    return Stage([pltpu.make_async_copy(rows, buf.at[1], own.at[1])], [pltpu.make_async_remote_copy(
        src_ref=buf.at[1], dst_ref=rows, send_sem=send.at[7], recv_sem=recv.at[7],
        device_id=(peer_of(me, 1),), device_id_type=MESH)])


def route(me):
    core = me % 2
    first = peer_of(me, 2) * (1 - core) + peer_of(me, 4) * core
    second = peer_of(me, 4) * (1 - core) + peer_of(me, 2) * core
    return core, peer_of(me, 1), first, second


def half_rows(c):
    return pl.ds(pl.multiple_of(c * (DIM // 2), DIM // 2), DIM // 2)


def start(copies):
    for c in copies:
        c.start()


def wait(copies):
    for c in copies:
        c.wait()


def row_sums(vals):
    folded = vals[:, :HD]
    for start in range(HD, vals.shape[1], HD):
        folded = folded + vals[:, start:start + HD]
    return jnp.sum(folded.T, axis=0, keepdims=True)


def columns_of(rows):
    turned = rows.T
    return [jnp.broadcast_to(turned[:, c:c + 1], (rows.shape[1], HD)) for c in range(rows.shape[0])]


def as_column(row):
    return jnp.broadcast_to(row, (HD, row.shape[1])).T


def exchange(me, srcs, slots, send_sems, recv_sems):
    copies = []
    for n, (src, slot) in enumerate(zip(srcs, slots)):
        for p, mask in enumerate(ORDER):
            copies.append(pltpu.make_async_remote_copy(
                src_ref=src, dst_ref=slot.at[p], send_sem=send_sems.at[n, p], recv_sem=recv_sems.at[n, p],
                device_id=(peer_of(me, mask),), device_id_type=MESH))
    return copies


def ordered_total(me, src, slot):
    own = src[...]
    total = jnp.zeros_like(own)
    for dev in range(NDEV):
        term = jnp.where(me == dev, own, 0.0)
        for p, mask in enumerate(ORDER):
            term = term + jnp.where(peer_of(me, mask) == dev, slot[p], 0.0)
        total = total + term
    return total


def causal_mask():
    keys = lax.broadcasted_iota(jnp.int32, (BLK, BLK), 0)
    queries = lax.broadcasted_iota(jnp.int32, (BLK, BLK), 1)
    return keys <= queries


def block_rows(i):
    return pl.ds(pl.multiple_of(i * BLK, BLK), BLK)


def head_cols(h):
    return pl.ds(pl.multiple_of(h * HD, HD), HD)


def forward_kernel(freq_ref, wq_ref, wk_ref, wv_ref, gains_ref, x_ref, wo_ref,
                   cos_ref, sin_ref, inv_ref, o_ref, lse_ref, raw_ref, qkv_ref, both_ref, full_ref, wof_ref,
                   raw, qkv, xbuf, sums_scr, slot, p_scr, vt_scr, acc_scr, o_scr, buf0, buf1,
                   ex_send, ex_recv, out_sems, send_sems, recv_sems, own_sems, x_sems, *bg_sems):
    g = pl.program_id(0)
    b, t = g // (4 * NB), g % (4 * NB)
    me = lax.axis_index('tp')
    bg0, bg1, bg2 = (*bg_sems[:3], buf0), (*bg_sems[3:6], buf1), (*bg_sems[6:], buf0)
    x0f, x1f = full_ref.at[0], full_ref.at[1]

    def x_gather(part=None):
        return stage1(me, x_ref.at[1], x1f, bg1, part)

    def wo_gather(part=None):
        return stage1(me, wo_ref, wof_ref, bg2, part)

    def keep(bb):
        return [pltpu.make_async_copy(raw, raw_ref.at[bb], out_sems.at[0]),
                pltpu.make_async_copy(qkv, qkv_ref.at[bb], out_sems.at[1])]

    def sums(bb):
        return exchange(me, [sums_scr.at[bb]], [slot.at[bb]], ex_send.at[bb], ex_recv.at[bb])

    def fetch(bb, i):
        return pltpu.make_async_copy(full_ref.at[bb, block_rows(i), :], xbuf.at[i % 2], x_sems.at[i % 2])

    def block_copy(bb, hh, st, half):
        dest = 2 * ((me // 2 + 1 + st) % NB) + half
        part = o_scr.at[bb, hh, st, pl.ds(half * TOK, TOK), :]
        dst = both_ref.at[bb, :, pl.ds(pl.multiple_of(me * LOC + hh * HD, HD), HD)]
        away = pltpu.make_async_remote_copy(
            src_ref=part, dst_ref=dst, send_sem=send_sems.at[bb, hh, st, half], recv_sem=recv_sems.at[bb, hh, me],
            device_id=(dest,), device_id_type=MESH)
        return dest, away, pltpu.make_async_copy(part, dst, own_sems.at[bb, hh])

    def run(stage):
        stage.load()
        stage.send()

    @pl.when(g == 0)
    def _():
        first = stage1(me, x_ref.at[0], x0f, bg0)
        entry_signal(me)
        first.load()
        entry_wait()
        first.send()
        x_gather(0).load()
        freq = freq_ref[...]
        sign = jnp.where(lax.broadcasted_iota(jnp.int32, (TOK, HD), 1) < HD // 2, -1.0, 1.0)

        def table(i, carry):
            rows = pl.ds(pl.multiple_of(i * TOK, TOK), TOK)
            pos = (lax.broadcasted_iota(jnp.int32, (TOK, HD), 0) + i * TOK).astype(F32)
            angle = pos * freq
            cos_ref[rows, :] = jnp.cos(angle)
            sin_ref[rows, :] = jnp.sin(angle) * sign
            return carry

        lax.fori_loop(0, SEQ // TOK, table, 0)
        first.wait()
        second, third = stage2(me, x0f, bg0), stage3(me, x0f, bg0)
        run(second)
        x_gather(0).send()
        second.wait()
        run(third)
        third.wait()
        fetch(0, 0).start()

    @pl.when(g == 2 * NB + 2)
    def _():
        x_gather(0).wait()
        x_gather(1).wait()
        run(stage2(me, x1f, bg1))
        run(wo_gather(0))

    @pl.when(g == 4 * NB)
    def _():
        stage2(me, x1f, bg1).wait()
        third = stage3(me, x1f, bg1)
        run(third)
        for c in keep(0):
            c.wait()
        third.wait()
        fetch(1, 0).start()

    @pl.when(g == 6 * NB + 2)
    def _():
        wo_gather(0).wait()
        wo_gather(1).wait()
        run(stage2(me, wof_ref, bg2))

    @pl.when(t < NB)
    def _():
        rows = block_rows(t)

        @pl.when(t < NB - 1)
        def _():
            fetch(b, t + 1).start()

        fetch(b, t).wait()
        x = xbuf[t % 2]
        for n, w_ref in enumerate((wq_ref, wk_ref)):
            val = dot(x, w_ref[...])
            raw[n, rows, :] = val
            sums_scr[b, pl.ds(t + n * NB, 1), :] = row_sums(val * val)
        qkv[2, rows, :] = dot(x, wv_ref[...]).astype(BF)

    @pl.when(t == NB)
    def _():
        start(sums(b))
        keep(b)[0].start()
        pl.when(b == 0)(x_gather(1).send)
        pl.when(b == 1)(wo_gather(1).send)
        wait(sums(b))
        inv_ref[...] = lax.rsqrt(ordered_total(me, sums_scr.at[b], slot.at[b]) / DIM + EPS)

    @pl.when(jnp.logical_and(t >= NB, t < 2 * NB))
    def _():
        i = t - NB
        rows = block_rows(i)
        cos, sin = cos_ref[rows, :], sin_ref[rows, :]
        for n in range(2):
            inv = as_column(inv_ref[pl.ds(i + n * NB, 1), :])
            gain = gains_ref[n:n + 1, :]
            for h in range(LOC // HD):
                sl = slice(h * HD, (h + 1) * HD)
                hat = raw[n, rows, sl] * inv * gain[:, sl]
                qkv[n, rows, sl] = (hat * cos + pltpu.roll(hat, HD // 2, 1) * sin).astype(BF)

    @pl.when(t == 2 * NB)
    def _():
        keep(b)[1].start()

    @pl.when(t >= 2 * NB)
    def _():
        h, step = t // NB - 2, t % NB
        qi = (me // 2 + 1 + step) % NB
        cols = head_cols(h)

        @pl.when(step == 0)
        def _():
            vt_scr[...] = qkv[2, :, cols].T

        qb = qkv[0, block_rows(qi), cols]

        def scores(j):
            return dot(qkv[1, block_rows(j), cols], qb, NT)

        def first(j, m):
            s = scores(j)
            p_scr[j] = s
            return jnp.maximum(m, jnp.max(s.reshape(BLK // 8, 8, BLK), axis=0))

        s = jnp.where(causal_mask(), scores(qi), -1e30)
        p_scr[qi] = s
        m = lax.fori_loop(0, qi, first, jnp.max(s.reshape(BLK // 8, 8, BLK), axis=0))
        m = jnp.max(m, axis=0, keepdims=True)

        def second(j, l):
            p = jnp.exp2((p_scr[j] - m) * C2)
            p_scr[j] = p
            return l + jnp.sum(p.reshape(BLK // 8, 8, BLK), axis=0)

        l = lax.fori_loop(0, qi + 1, second, jnp.zeros((8, BLK), F32))
        l = jnp.sum(l, axis=0, keepdims=True)
        rl = 1.0 / l
        lse_ref[pl.ds(h * NB + qi, 1), :] = m * C2 + jnp.log2(l)

        acc_scr[...] = jnp.zeros_like(acc_scr)

        def third(j, carry):
            p = (p_scr[j] * rl).astype(BF)
            acc_scr[...] += dot(vt_scr[:, block_rows(j)], p)
            return carry

        lax.fori_loop(0, qi + 1, third, 0)
        out = acc_scr[...].T.astype(BF)
        o_scr[b, h, step] = out
        o_ref[block_rows(qi), cols] = out

        for half in range(2):
            dest, away, here = block_copy(b, h, step, half)
            pl.when(dest != me)(away.start)
            pl.when(dest == me)(here.start)

    @pl.when(g == 8 * NB - 1)
    def _():
        stage2(me, wof_ref, bg2).wait()
        third = stage3(me, wof_ref, bg2)
        run(third)
        for c in keep(1):
            c.wait()

        def drain(n, carry):
            bb, hh = n // 2, n % 2
            for st in range(NB):
                for half in range(2):
                    dest, away, here = block_copy(bb, hh, st, half)
                    if st < NB - 1:
                        away.wait_send()
                    else:
                        pl.when(dest != me)(away.wait_send)
                        pl.when(dest == me)(here.wait)
            for mask in ORDER:
                peer = peer_of(me, mask)
                pltpu.make_async_remote_copy(
                    src_ref=o_scr.at[0, 0, 0, pl.ds(0, TOK), :],
                    dst_ref=both_ref.at[bb, :, pl.ds(pl.multiple_of(peer * LOC + hh * HD, HD), HD)],
                    send_sem=send_sems.at[0, 0, 0, 0], recv_sem=recv_sems.at[bb, hh, peer],
                    device_id=(peer,), device_id_type=MESH).wait_recv()
            return carry

        lax.fori_loop(0, 4, drain, 0)
        third.wait()


def forward(x, wq, wk, wv, wo, gains, cid):
    inv_freq = np.float32(1.0) / np.float32(ROPE_THETA) ** (np.arange(HD // 2, dtype=np.float32) / np.float32(HD // 2))
    freq = jnp.asarray(np.concatenate([inv_freq, inv_freq])[None, :], F32)

    def whole(*shape):
        return pl.BlockSpec(shape, lambda g: (0,) * len(shape))

    def per_batch(*shape):
        return pl.BlockSpec((None,) + shape, lambda g: (g // (4 * NB),) + (0,) * len(shape))

    wspec, rows = whole(DIM, LOC), per_batch(2 * NB, BLK)
    return pl.pallas_call(
        forward_kernel,
        grid=(8 * NB,),
        in_specs=[whole(1, HD), wspec, wspec, wspec, whole(2 + DIM // LOC, LOC), ANYWHERE, ANYWHERE],
        out_specs=[whole(SEQ, HD), whole(SEQ, HD), rows, per_batch(SEQ, LOC), rows] + [ANYWHERE] * 5,
        out_shape=[sds((SEQ, HD), F32), sds((SEQ, HD), F32), sds((2, 2 * NB, BLK), F32), sds((2, SEQ, LOC), BF),
                   sds((2, 2 * NB, BLK), F32), sds((2, 2, SEQ, LOC), F32), sds((2, 3, SEQ, LOC), BF),
                   sds((2, TOK, DIM), BF), sds((2, SEQ, DIM), BF), sds((SEQ, DIM), BF)],
        scratch_shapes=[pltpu.VMEM((2, SEQ, LOC), F32), pltpu.VMEM((3, SEQ, LOC), BF), pltpu.VMEM((2, BLK, DIM), BF),
                        pltpu.VMEM((2, 2 * NB, BLK), F32), pltpu.VMEM((2, NDEV - 1, 2 * NB, BLK), F32),
                        pltpu.VMEM((NB, BLK, BLK), F32), pltpu.VMEM((HD, SEQ), BF), pltpu.VMEM((HD, BLK), F32),
                        pltpu.VMEM((2, 2, NB, BLK, HD), BF), pltpu.VMEM((2, TOK, DIM), BF), pltpu.VMEM((2, TOK, DIM), BF),
                        DMA((2, 1, NDEV - 1)), DMA((2, 1, NDEV - 1)), DMA((2,)),
                        DMA((2, 2, NB, 2)), DMA((2, 2, NDEV)), DMA((2, 2)), DMA((2,))] + BG_SEMS * 3,
        compiler_params=params(dimension_semantics=("arbitrary",), collective_id=cid, has_side_effects=True),
        cost_estimate=cost(60e9, 60e6),
        name="forward",
    )(freq, wq, wk, wv, gains, x, wo)


def out_kernel(o_ref, x_ref, dy_ref, gains_ref, wo_ref, y_ref, da_ref, gga_ref, full_ref, wo_scr, a_scr, wo_sems, buf, *bg_sems):
    b = pl.program_id(0)
    me = lax.axis_index('tp')
    bg = (*bg_sems, buf)
    step = DIM // NB

    def piece(j):
        cols = pl.ds(pl.multiple_of(j * step, step), step)
        return cols, pltpu.make_async_copy(wo_ref.at[:, cols], wo_scr.at[:, cols], wo_sems.at[j])

    @pl.when(b == 0)
    def _():
        nbr_signal(me)
        for j in range(NB):
            piece(j)[1].start()
        gga_ref[...] = jnp.zeros_like(gga_ref)

    o = o_ref[0]

    def fwd(j, carry):
        cols, load = piece(j)
        pl.when(b == 0)(load.wait)
        a_scr[:, cols] = dot(o, wo_scr[:, cols])
        return carry

    lax.fori_loop(0, NB, fwd, 0)
    a = a_scr[...]
    r = lax.rsqrt(jnp.mean(a * a, axis=-1, keepdims=True) + EPS)
    n = a * r
    ga = jnp.concatenate([gains_ref[2 + i:3 + i, :] for i in range(8)], axis=1)
    dy = dy_ref[0].astype(F32)
    gn = dy * ga
    da = (r * (gn - n * jnp.mean(gn * n, axis=-1, keepdims=True))).astype(BF)
    da_ref[0] = da

    @pl.when(b == 0)
    def _():
        buf[0] = da
        nbr_wait()
        stage1(me, None, full_ref, bg).send()

    y_ref[0] = (x_ref[0].astype(F32) + n * ga).astype(BF)
    col = jnp.sum(dy * n, axis=0, keepdims=True)
    for i in range(8):
        gga_ref[i:i + 1, :] += col[:, i * LOC:(i + 1) * LOC]

    @pl.when(b == 1)
    def _():
        stage1(me, None, full_ref, bg).wait()


def out_block(o, wo, x, dy, gains, cid):
    def whole(*shape):
        return pl.BlockSpec(shape, lambda i: (0,) * len(shape))

    batch = pl.BlockSpec((1, TOK, DIM), lambda i: (i, 0, 0))
    return pl.pallas_call(
        out_kernel,
        grid=(2,),
        in_specs=[batch, batch, batch, whole(2 + DIM // LOC, LOC), ANYWHERE],
        out_specs=[batch, batch, whole(8, DIM // 8), ANYWHERE],
        out_shape=[sds((2, TOK, DIM), BF), sds((2, TOK, DIM), BF), sds((8, DIM // 8), F32), sds((SEQ, DIM), BF)],
        scratch_shapes=[pltpu.VMEM((DIM, DIM), BF), pltpu.VMEM((TOK, DIM), F32), DMA((NB,)),
                        pltpu.VMEM((2, TOK, DIM), BF)] + BG_SEMS,
        compiler_params=params(dimension_semantics=("arbitrary",), collective_id=cid, has_side_effects=True),
        cost_estimate=cost(8 * TOK * DIM * DIM + 5e9, 18e6),
        name="out_block",
    )(o, x, dy, gains, wo)


def backward_kernel(b, qkv_ref, wo_ref, lse_ref, raw_hbm, inv_ref, gains_ref, cos_hbm, sin_hbm, gga_ref,
                    wq_ref, wk_ref, wv_ref, da_ref, *rest):
    if b:
        d0_ref, pd0_ref, pw_ref, d_ref, pd_ref, gg_ref, gout_ref, got_ref, da_ref, buf0, w_all, d_two, sbuf, *rest = rest
    else:
        shard_ref, d_ref, pd_ref, gg_ref, gout_ref, full_ref, pw_ref, da_ref, buf0, buf1, w_half, *rest = rest
    (p_scr, dp_scr, kt_scr, dqt_scr, dq_scr, dk_scr, dv_scr, du_scr, d_scr, dh_scr, dbuf, dots_scr, total, slot, ga_slot,
     ex_send, ex_recv, pd_send, pd_recv, d_sems, rs_sems, ld_sems, db_sems, raw_ref, cos_ref, sin_ref, tb_sems, *bg_sems) = rest
    h, step = pl.program_id(0), pl.program_id(1)
    me = lax.axis_index('tp')

    def chip_at(n):
        ax, ay = (me // 2) % 2, me // 4
        return (ay + (n // 2) * (1 - 2 * ay)) * 2 + ax + (n % 2) * (1 - 2 * ax)

    def fetch(n):
        return pltpu.make_async_copy(da_ref.at[block_rows(chip_at(n)), :], dbuf.at[n % 2], db_sems.at[n % 2])

    qi = chip_at(step)
    tables = [pltpu.make_async_copy(src, dst, tb_sems.at[n]) for n, (src, dst) in enumerate(
        ((raw_hbm.at[b], raw_ref), (cos_hbm, cos_ref), (sin_hbm, sin_ref)))]
    core, partner, first_dev, _ = route(me)
    weights = (wq_ref, wk_ref, wv_ref)

    bg0 = (*bg_sems[:3], buf0)
    older3 = stage3(me, da_ref, bg0)
    if b:
        operands = []
        for blk, chip in enumerate((peer_of(me, 6) // 2, first_dev // 2)):
            operands += [pltpu.make_async_copy(d.at[block_rows(chip), :], d_two.at[blk, n], ld_sems.at[2 * blk + n])
                         for n, d in enumerate((d0_ref, pd0_ref))]
        operands += [pltpu.make_async_copy(w.at[half_rows(core), :], w_all.at[0, :, pl.ds(n * LOC, LOC)], ld_sems.at[4 + n])
                     for n, w in enumerate(weights)]
        operands.append(pltpu.make_async_copy(pw_ref, w_all.at[1], ld_sems.at[7]))
        moved = [pltpu.make_async_remote_copy(
            src_ref=sbuf.at[blk, pl.ds(lo, count), :], dst_ref=got_ref.at[blk, pl.ds(lo, count), :], send_sem=rs_sems.at[n],
            recv_sem=rs_sems.at[3 + n], device_id=(first_dev,), device_id_type=MESH)
            for n, (blk, lo, count) in enumerate(((0, 0, BLK), (1, 0, BLK * 3 // 4), (1, BLK * 3 // 4, BLK // 4)))]
    else:
        bg = (*bg_sems[3:], buf1)
        older2 = stage2(me, da_ref, bg0)
        gather = stage1(me, shard_ref.at[1], full_ref, bg)
        operands = [pltpu.make_async_copy(w.at[half_rows(1 - core), :], w_half.at[:, pl.ds(n * LOC, LOC)], ld_sems.at[n])
                    for n, w in enumerate(weights)]
        moved = [pltpu.make_async_remote_copy(
            src_ref=w_half, dst_ref=pw_ref, send_sem=rs_sems.at[0], recv_sem=rs_sems.at[3], device_id=(partner,),
            device_id_type=MESH)]

    @pl.when(jnp.logical_and(h == 0, step == 0))
    def _():
        entry_signal(me)
        if b:
            needed, rest_of = operands[:2] + operands[4:], operands[2:4]
            start(needed)
            fetch(0).start()
            start(rest_of)
            older3.load()
            start(tables)
            wait(needed)
            sbuf[0] = dot(d_two[0, 0], w_all[0], NT) + dot(d_two[0, 1], w_all[1], NT)
            entry_wait()
            moved[0].start()
            older3.send()
            wait(rest_of)
            sbuf[1] = dot(d_two[1, 0], w_all[0], NT) + dot(d_two[1, 1], w_all[1], NT)
            moved[1].start()
        else:
            older2.load()
            fetch(0).start()
            gather.load()
            start(operands)
            start(tables)
            entry_wait()
            older2.send()
            gather.send()
            wait(operands)
            start(moved)
        dots_scr[...] = jnp.zeros_like(dots_scr)

    if not b:
        @pl.when(jnp.logical_and(h == 1, step == NB - 1))
        def _():
            gather.wait()
            early = stage2(me, full_ref, bg, 0)
            early.load()
            early.send()

    @pl.when(jnp.logical_and(h == 0, step == NB - 1))
    def _():
        older3.wait()
        fetch(NB - 1).start()

    @pl.when(h == 0)
    def _():
        fetch(step).wait()
        dh_scr[block_rows(qi), :] = dot(dbuf[step % 2], wo_ref[...], NT).astype(BF)
        if b:
            @pl.when(step < NB - 2)
            def _():
                fetch(step + 1).start()
        else:
            @pl.when(step == 0)
            def _():
                older2.wait(2, 3)

            @pl.when(step < NB - 2)
            def _():
                fetch(step + 1).start()

            @pl.when(step == NB - 2)
            def _():
                older2.wait(0, 1)
                older3.load()
                older3.send()

    @pl.when(step == 0)
    def _():
        kt_scr[...] = qkv_ref[1].T
        dk_scr[...] = jnp.zeros_like(dk_scr)
        dv_scr[...] = jnp.zeros_like(dv_scr)

    qb = qkv_ref[0, block_rows(qi), :]
    dob = dh_scr[block_rows(qi), head_cols(h)]
    lse = lse_ref[pl.ds(h * NB + qi, 1), :]

    def first(j, acc, diag=False):
        rows = block_rows(j)
        p = jnp.exp2(dot(qkv_ref[1, rows, :], qb, NT) * C2 - lse)
        if diag:
            p = jnp.where(causal_mask(), p, 0.0)
        dp = dot(qkv_ref[2, rows, :], dob, NT)
        p_scr[j] = p
        dp_scr[j] = dp
        dv_scr[rows, :] += dot(p.astype(BF), dob)
        return acc + jnp.sum((p * dp).reshape(BLK // 8, 8, BLK), axis=0)

    acc = first(qi, jnp.zeros((8, BLK), F32), True)
    acc = lax.fori_loop(0, qi, first, acc)
    delta = jnp.sum(acc, axis=0, keepdims=True)
    dqt_scr[...] = jnp.zeros_like(dqt_scr)

    def second(j, carry):
        rows = block_rows(j)
        ds = (p_scr[j] * (dp_scr[j] - delta) * SCALE).astype(BF)
        dk_scr[rows, :] += dot(ds, qb)
        dqt_scr[...] += dot(kt_scr[:, rows], ds)
        return carry

    lax.fori_loop(0, qi + 1, second, 0)
    dq_scr[block_rows(qi), :] = dqt_scr[...].T

    @pl.when(step == NB - 1)
    def _():
        d_scr[:, pl.ds(pl.multiple_of(2 * LOC + h * HD, HD), HD)] = dv_scr[...].astype(BF)
        gg_ref[...] = jnp.zeros_like(gg_ref)
        cols = head_cols(h)

        @pl.when(h == 0)
        def _():
            wait(tables)


        inverse = columns_of(inv_ref[...])
        for i in range(NB):
            rows = pl.ds(i * BLK, BLK)
            cos, sin = cos_ref[rows, :], sin_ref[rows, :]
            for n, from_scr in enumerate((dq_scr, dk_scr)):
                d = from_scr[rows, :]
                hat = d * cos - pltpu.roll(d, HD // 2, 1) * sin
                unit = raw_ref[n, rows, cols] * inverse[i + n * NB]
                gg_ref[n:n + 1, :] += jnp.sum(hat * unit, axis=0, keepdims=True)
                du = hat * gains_ref[n:n + 1, :]
                du_scr[n, h, rows, :] = du
                dots_scr[i + n * NB:i + n * NB + 1, :] += row_sums(du * unit)

    @pl.when(jnp.logical_and(h == 1, step == NB - 1))
    def _():
        srcs, slots = ([dots_scr], [slot]) if b else ([dots_scr, gga_ref], [slot, ga_slot])
        sums = exchange(me, srcs, slots, ex_send, ex_recv)
        start(sums)
        if b:
            moved[2].start()
        else:
            stage2(me, full_ref, bg, 1).send()
        wait(sums)
        total[...] = ordered_total(me, dots_scr, slot) / DIM
        gout_ref[...] = gga_ref[...] if b else ordered_total(me, gga_ref, ga_slot)

        def copies(i):
            rows = block_rows(i)
            return [pltpu.make_async_copy(d_scr.at[rows, :], d_ref.at[rows, :], d_sems.at[i]),
                    pltpu.make_async_remote_copy(
                        src_ref=d_scr.at[rows, :], dst_ref=pd_ref.at[rows, :], send_sem=pd_send.at[i],
                        recv_sem=pd_recv.at[i], device_id=(peer_of(me, 1),), device_id_type=MESH)]

        inverse, dots = columns_of(inv_ref[...]), columns_of(total[...])
        for i in range(NB):
            rows = pl.ds(i * BLK, BLK)
            for n in range(2):
                inv = inverse[i + n * NB]
                for hh in range(LOC // HD):
                    sl = slice(hh * HD, (hh + 1) * HD)
                    unit = raw_ref[n, rows, sl] * inv
                    val = inv * (du_scr[n, hh, rows, :] - unit * dots[i + n * NB])
                    d_scr[rows, n * LOC + hh * HD:n * LOC + (hh + 1) * HD] = val.astype(BF)
            start(copies(i))
        for i in range(NB):
            wait(copies(i))
        wait(moved)
        if not b:
            stage2(me, full_ref, bg, 0).wait()
            stage2(me, full_ref, bg, 1).wait()


def backward(b, da, qkv, wo, lse, raw, inv, gains, cos, sin, gga, weights, others, cid):
    def whole(*shape):
        return pl.BlockSpec(shape, lambda h, i: (0,) * len(shape))

    def picked(*shape):
        return pl.BlockSpec((None,) + shape, lambda h, i: (b,) + (0,) * len(shape))

    gsp = whole(8, DIM // 8)
    half = (DIM // 2, 3 * LOC)
    if b:
        extra = [sds((2, BLK, DIM // 2), F32), sds((SEQ, DIM), BF)]
        own = [pltpu.VMEM((2, TOK, DIM), BF), pltpu.VMEM((2,) + half, BF), pltpu.VMEM((2, 2, BLK, 3 * LOC), BF), pltpu.VMEM((2, BLK, DIM // 2), F32)]
    else:
        extra = [sds((SEQ, DIM), BF), sds(half, BF), sds((SEQ, DIM), BF)]
        own = [pltpu.VMEM((2, TOK, DIM), BF), pltpu.VMEM((2, TOK, DIM), BF), pltpu.VMEM(half, BF)]
    return pl.pallas_call(
        functools.partial(backward_kernel, b),
        grid=(2, NB),
        in_specs=[pl.BlockSpec((None, 3, SEQ, HD), lambda h, i: (b, 0, 0, h)),
                  whole(LOC, DIM),
                  picked(2 * NB, BLK), ANYWHERE, picked(2 * NB, BLK),
                  pl.BlockSpec((2 + DIM // LOC, HD), lambda h, i: (0, h)), ANYWHERE, ANYWHERE, gsp]
        + [ANYWHERE] * (4 + len(others)),
        out_specs=[ANYWHERE, ANYWHERE, pl.BlockSpec((8, HD), lambda h, i: (0, h)), gsp] + [ANYWHERE] * len(extra),
        out_shape=[sds((SEQ, 3 * LOC), BF), sds((SEQ, 3 * LOC), BF), sds((8, LOC), F32), sds((8, DIM // 8), F32)] + extra,
        input_output_aliases={12: 5 if b else 6},
        scratch_shapes=own + [
            pltpu.VMEM((NB, BLK, BLK), F32), pltpu.VMEM((NB, BLK, BLK), F32), pltpu.VMEM((HD, SEQ), BF),
            pltpu.VMEM((HD, BLK), F32), pltpu.VMEM((SEQ, HD), F32), pltpu.VMEM((SEQ, HD), F32),
            pltpu.VMEM((SEQ, HD), F32), pltpu.VMEM((2, 2, SEQ, HD), F32), pltpu.VMEM((SEQ, 3 * LOC), BF),
            pltpu.VMEM((SEQ, LOC), BF), pltpu.VMEM((2, BLK, DIM), BF), pltpu.VMEM((2 * NB, BLK), F32), pltpu.VMEM((2 * NB, BLK), F32),
            pltpu.VMEM((NDEV - 1, 2 * NB, BLK), F32), pltpu.VMEM((NDEV - 1, 8, DIM // 8), F32),
            DMA((2, NDEV - 1)), DMA((2, NDEV - 1)), DMA((NB,)), DMA((NB,)), DMA((NB,)), DMA((6,)), DMA((8,)), DMA((2,)),
            pltpu.VMEM((2, SEQ, LOC), F32), pltpu.VMEM((SEQ, HD), F32), pltpu.VMEM((SEQ, HD), F32), DMA((3,))]
        + BG_SEMS * (1 if b else 2),
        compiler_params=params(dimension_semantics=("arbitrary", "arbitrary"), collective_id=cid, has_side_effects=True),
        cost_estimate=cost(25e9, 30e6),
        name="backward",
    )(qkv, wo, lse, raw, inv, gains, cos, sin, gga, *weights, da, *others)


HALF = DIM // 2
CH = 256


def grads_kernel(d0, d1, pd0, pd1, wq, wk, wv, pw, got, x_full, o_all, da0, da1, dy_ref, dx_out, gwq_out, gwk_out, gwv_out, gwo_out,
                 d_all, w_all, sbuf, r1, r2, fin, acc, xbuf, obuf,
                 dl_sems, w_sems, s1_sems, r1_sems, s2_sems, r2_sems, fs_sems, fr_sems, x_sems, o_sems, dx_ref, gwq_ref, gwk_ref, gwv_ref, gwo_ref, out_sems):
    me = lax.axis_index('tp')
    core, partner, first, second = route(me)
    chip = me // 2
    diag_chip, first_chip, second_chip = peer_of(me, 6) // 2, first // 2, second // 2

    barrier = pltpu.get_barrier_semaphore()
    for dev in (partner, first, second):
        pl.semaphore_signal(barrier, inc=1, device_id=(dev,), device_id_type=MESH)

    def rows_of(blk):
        return pl.ds(pl.multiple_of(blk * BLK, BLK), BLK)

    results = [pltpu.make_async_copy(src, dst, out_sems.at[n]) for n, (src, dst) in enumerate((
        (gwq_ref, gwq_out), (gwk_ref, gwk_out), (gwv_ref, gwv_out), (gwo_ref, gwo_out)))]
    chips = (diag_chip, first_chip, second_chip, chip)
    w_copies = [pltpu.make_async_copy(w.at[half_rows(core), :], w_all.at[0, :, pl.ds(n * LOC, LOC)], w_sems.at[n])
                for n, w in enumerate((wq, wk, wv))]
    w_copies.append(pltpu.make_async_copy(pw, w_all.at[1], w_sems.at[3]))
    loads = []
    for n in range(8):
        rows, b = rows_of(chips[n // 2]), n % 2
        loads.append([pltpu.make_async_copy(d.at[rows, :], d_all.at[side, b, rows, :], dl_sems.at[side, n])
                      for side, d in enumerate(((d0, d1)[b], (pd0, pd1)[b]))])
    start(w_copies)
    start(loads[1])
    pl.semaphore_wait(barrier, 3)
    wait(w_copies)

    def partial(b, blk):
        rows = rows_of(blk)
        return dot(d_all[0, b, rows, :], w_all[0], NT) + dot(d_all[1, b, rows, :], w_all[1], NT)

    def to_first(n):
        return pltpu.make_async_remote_copy(
            src_ref=sbuf.at[n // 2], dst_ref=r1.at[n], send_sem=s1_sems.at[n], recv_sem=r1_sems.at[n],
            device_id=(first,), device_id_type=MESH)

    def to_second(b):
        return pltpu.make_async_remote_copy(
            src_ref=r1.at[b], dst_ref=r2.at[b], send_sem=s2_sems.at[b], recv_sem=r2_sems.at[b],
            device_id=(second,), device_id_type=MESH)

    def to_partner(b):
        return pltpu.make_async_remote_copy(
            src_ref=r1.at[2 + b, pl.ds(pl.multiple_of((1 - core) * TOK, TOK), TOK), :], dst_ref=fin.at[b],
            send_sem=fs_sems.at[b], recv_sem=fr_sems.at[b], device_id=(partner,), device_id_type=MESH)

    taken = [pltpu.make_async_copy(got.at[n], r1.at[2 * n], w_sems.at[4 + n]) for n in range(2)]
    for n in (1, 3):
        wait(loads[n])
        if n == 1:
            start(loads[3])
        sbuf[n // 2] = partial(1, chips[n // 2])
        to_first(n).start()
        if n == 1:
            start(taken)
            for later in (4, 0, 2, 5, 6, 7):
                start(loads[later])
    for n in (0, 2, 4, 5, 6, 7):
        wait(loads[n])
    wait(taken)

    steps = SEQ // CH

    def chunk(i):
        return pl.ds(pl.multiple_of(i * CH, CH), CH)

    def stream(pairs, body):
        def fetch(i):
            return [pltpu.make_async_copy(src.at[chunk(i), :], buf.at[i % 2], sems.at[i % 2]) for src, buf, sems in pairs]

        for c in fetch(0):
            c.start()

        def it(i, carry):
            @pl.when(i + 1 < steps)
            def _():
                for c in fetch(i + 1):
                    c.start()

            for c in fetch(i):
                c.wait()
            body(i)
            return carry

        lax.fori_loop(0, steps, it, 0)

    def wgrad(b, src):
        def body(i):
            left = d_all[0, b, chunk(i), :].T
            for c in range(3):
                part = slice(c * LOC, (c + 1) * LOC)
                acc[part, :] += dot(left[part, :], xbuf[i % 2])

        stream([(src, xbuf, x_sems)], body)

    def forward_second(b):
        if b:
            to_first(b).wait_recv()
        r1[b] += partial(b, second_chip)
        to_second(b).start()

    forward_second(0)
    acc[...] = jnp.zeros_like(acc)
    wgrad(0, x_full.at[0])
    wgrad(1, x_full.at[1])
    for n, ref in enumerate((gwq_ref, gwk_ref, gwv_ref)):
        ref[...] = acc[n * LOC:(n + 1) * LOC, :].T.astype(BF)
        results[n].start()
    forward_second(1)
    acc[:LOC, :] = jnp.zeros((LOC, DIM), F32)

    def wo_body(i):
        acc[:LOC, :] += dot(obuf[i % 2].T, xbuf[i % 2])

    for o_src, da_src in ((o_all.at[0], da0), (o_all.at[1], da1)):
        stream([(da_src, xbuf, x_sems), (o_src, obuf, o_sems)], wo_body)
    gwo_ref[...] = acc[:LOC, :].astype(BF)
    results[3].start()

    def own_part(b, carry):
        r1_own = partial(b, chip)
        pl.when(b == 1)(to_first(3).wait_recv)
        to_second(b).wait_recv()
        r1[2 + b] += r1_own + r2[b]
        to_partner(b).start()
        cols = half_rows(core)
        rows = pl.ds(pl.multiple_of(core * TOK, TOK), TOK)
        dx_ref[b, :, cols] = (r1[2 + b, rows, :] + dy_ref[b, :, cols].astype(F32)).astype(BF)
        return carry

    lax.fori_loop(0, 2, own_part, 0)

    def finish(b, carry):
        to_partner(b).wait()
        cols = half_rows(1 - core)
        dx_ref[b, :, cols] = (fin[b] + dy_ref[b, :, cols].astype(F32)).astype(BF)
        pltpu.make_async_copy(dx_ref.at[b], dx_out.at[b], out_sems.at[4 + b]).start()
        to_second(b).wait_send()
        return carry

    to_first(1).wait_send()
    to_first(3).wait_send()
    lax.fori_loop(0, 2, finish, 0)
    wait(results)
    for b in range(2):
        pltpu.make_async_copy(dx_ref.at[b], dx_out.at[b], out_sems.at[4 + b]).wait()


def grads(d0, d1, pd0, pd1, wq, wk, wv, pw, got, x_full, o_all, da0, da1, dy, cid):
    vm = pl.BlockSpec(memory_space=pltpu.VMEM)
    far = pl.BlockSpec(memory_space=pl.ANY)
    dma = pltpu.SemaphoreType.DMA
    return pl.pallas_call(
        grads_kernel,
        in_specs=[far] * 13 + [vm],
        out_specs=[far] * 5,
        out_shape=[sds((2, TOK, DIM), BF)] + [sds((DIM, LOC), BF)] * 3 + [sds((LOC, DIM), BF)],
        scratch_shapes=[pltpu.VMEM((2, 2, SEQ, 3 * LOC), BF), pltpu.VMEM((2, HALF, 3 * LOC), BF),
                        pltpu.VMEM((2, BLK, HALF), F32), pltpu.VMEM((4, BLK, HALF), F32), pltpu.VMEM((2, BLK, HALF), F32),
                        pltpu.VMEM((2, TOK, HALF), F32), pltpu.VMEM((3 * LOC, DIM), F32),
                        pltpu.VMEM((2, CH, DIM), BF), pltpu.VMEM((2, CH, LOC), BF),
                        dma((2, 8)), dma((9,)), dma((4,)), dma((4,)), dma((2,)), dma((2,)),
                        dma((2,)), dma((2,)), dma((2,)), dma((2,)), pltpu.VMEM((2, TOK, DIM), BF),
                        pltpu.VMEM((DIM, LOC), BF), pltpu.VMEM((DIM, LOC), BF), pltpu.VMEM((DIM, LOC), BF),
                        pltpu.VMEM((LOC, DIM), BF), dma((6,))],
        compiler_params=pltpu.CompilerParams(vmem_limit_bytes=67043328, collective_id=cid, has_side_effects=True),
        cost_estimate=cost(100e9, 40e6),
        name="grads",
    )(d0, d1, pd0, pd1, wq, wk, wv, pw, got, x_full, o_all, da0, da1, dy)


def deliver_kernel(*refs):
    count = (len(refs) - 2) // 3
    loads, stores = [], []
    for src, dst, buf in zip(refs[:count], refs[count:2 * count], refs[2 * count:3 * count]):
        for part in range(2):
            piece = (part,) if len(src.shape) == 3 else (pl.ds(part * (src.shape[0] // 2), src.shape[0] // 2),)
            n = len(loads)
            loads.append(pltpu.make_async_copy(src.at[piece], buf.at[piece], refs[-2].at[n]))
            stores.append(pltpu.make_async_copy(buf.at[piece], dst.at[piece], refs[-1].at[n]))
    ahead = 4
    start(loads[:ahead])
    for n, (load, store) in enumerate(zip(loads, stores)):
        load.wait()
        store.start()
        start(loads[n + ahead:n + ahead + 1])
    wait(stores)


def deliver(*arrays):
    return pl.pallas_call(
        deliver_kernel,
        in_specs=[ANYWHERE] * len(arrays),
        out_specs=[ANYWHERE] * len(arrays),
        out_shape=[sds(t.shape, t.dtype) for t in arrays],
        scratch_shapes=[pltpu.VMEM(t.shape, t.dtype) for t in arrays] + [DMA((2 * len(arrays),)), DMA((2 * len(arrays),))],
        compiler_params=params(),
        cost_estimate=cost(1e9, 16e6),
        name="deliver",
    )(*arrays)


def local_block(x_loc, wq, wk, wv, wo, gq, gk, ga, dy_loc):
    gains = jnp.concatenate([gq, gk, ga]).astype(F32).reshape(2 + DIM // LOC, LOC)
    weights = (wq, wk, wv)
    cos, sin, inv, o, lse, raw, qkv, o_recv, x_full, wo_full = forward(x_loc, wq, wk, wv, wo, gains, 0)
    y, da, gga, da0 = out_block(o_recv, wo_full, x_loc, dy_loc, gains, 1)
    state = (qkv, wo, lse, raw, inv, gains, cos, sin, gga, weights)
    d0, pd0, gg0, gout, da1, pw, da0 = backward(0, da0, *state, (da,), 2)
    d1, pd1, gg1, _, got, da1 = backward(1, da1, *state, (d0, pd0, pw), 3)
    grad_ga = gout.reshape(DIM).astype(BF)
    big = grads(d0, d1, pd0, pd1, *weights, pw, got, x_full, o, da0, da1, dy_loc, 4)
    y, dx, gwq, gwk, gwv, gwo = deliver(y, *big)
    gg = gg0 + gg1
    return (y, dx, gwq, gwk, gwv, gwo, gg[0].astype(BF), gg[1].astype(BF), grad_ga)


def solution(mesh):
    act, col, row, vec = P(None, 'tp', None), P(None, 'tp'), P('tp', None), P('tp')
    in_specs = (act, col, col, col, row, vec, vec, P(), act)
    out_specs = (act, act, col, col, col, row, vec, vec, P())
    return jax.shard_map(local_block, mesh=mesh, in_specs=in_specs, out_specs=out_specs, check_vma=False)
```

```python
import functools
import math

import jax
import jax.numpy as jnp
import numpy as np
from jax import lax
from jax.experimental import pallas as pl
from jax.experimental.pallas import tpu as pltpu
from jax.sharding import PartitionSpec as P

HD = 128
ROPE_THETA = 500000.0
EPS = 1e-6
DIM = 2048
SEQ = 2048
LOC = 256
TOK = 256
BLK = 512
NB = SEQ // BLK
NDEV = 8
SCALE = HD ** -0.5
C2 = SCALE * math.log2(math.e)
MESH = pl.DeviceIdType.MESH
BF = jnp.bfloat16
F32 = jnp.float32
VMEM_MAX = 60 * 1024 * 1024

NT = (((1,), (1,)), ((), ()))
NN = (((1,), (0,)), ((), ()))


def dot(a, b, dims=NN):
    return lax.dot_general(a, b, dims, preferred_element_type=F32)


def sds(shape, dtype):
    return jax.ShapeDtypeStruct(shape, dtype)


def cost(flops, nbytes, trans=0):
    return pl.CostEstimate(flops=int(flops), bytes_accessed=int(nbytes), transcendentals=int(trans))


def params(**kw):
    return pltpu.CompilerParams(vmem_limit_bytes=VMEM_MAX, **kw)


def peer_of(me, mask):
    core, ax, ay = me % 2, (me // 2) % 2, me // 4
    core = 1 - core if mask & 1 else core
    ax = 1 - ax if mask & 2 else ax
    ay = 1 - ay if mask & 4 else ay
    return ay * 4 + ax * 2 + core


ORDER = (6, 7, 2, 4, 3, 5, 1)


def entry_signal(me):
    for mask in ORDER:
        pl.semaphore_signal(pltpu.get_barrier_semaphore(), inc=1, device_id=(peer_of(me, mask),), device_id_type=MESH)


def entry_wait():
    pl.semaphore_wait(pltpu.get_barrier_semaphore(), NDEV - 1)


def nbr_signal(me):
    for mask in (1, 2, 4):
        pl.semaphore_signal(pltpu.get_barrier_semaphore(), inc=1, device_id=(peer_of(me, mask),), device_id_type=MESH)


def nbr_wait():
    pl.semaphore_wait(pltpu.get_barrier_semaphore(), 3)


DMA = pltpu.SemaphoreType.DMA
ANYWHERE = pl.BlockSpec(memory_space=pl.ANY)
BG_SEMS = [DMA((11,)), DMA((11,)), DMA((5,))]
BG = BG_SEMS + [pltpu.VMEM((2, TOK, DIM), BF)]


def shard_rows(dev, lo=0, count=TOK):
    return pl.ds(pl.multiple_of(dev * TOK + lo, TOK // 4), count)


class Stage:
    def __init__(self, loads, copies):
        self.loads, self.copies = loads, copies

    def load(self):
        start(self.loads)

    def send(self):
        wait(self.loads)
        start(self.copies)

    def wait(self, *which):
        wait([self.copies[n] for n in which] or self.copies)


def stage1(me, src, full, bg, part=None):
    send, recv, own, buf = bg
    lo, count, at = (0, TOK, 0) if part is None else (part * (TOK // 2), TOK // 2, 8 * part)
    there = full.at[shard_rows(me, lo, count), :]
    mine = buf.at[0, pl.ds(lo, count), :]
    copies = [pltpu.make_async_remote_copy(
        src_ref=mine, dst_ref=there, send_sem=send.at[at + k], recv_sem=recv.at[at + k],
        device_id=(peer_of(me, mask),), device_id_type=MESH) for k, mask in enumerate((2, 4, 1))]
    loads = [] if part == 1 or src is None else [pltpu.make_async_copy(src, buf.at[0], own.at[0])]
    return Stage(loads, copies + [pltpu.make_async_copy(mine, there, own.at[3 if part == 1 else 2])])


def stage2(me, full, bg, part=None):
    send, recv, own, buf = bg
    xn, yn = peer_of(me, 2), peer_of(me, 4)
    half = TOK // 2
    lo, count = (0, half) if part is None else (part * (half // 2), half // 2)
    at = 8 if part == 1 else 3
    plan = [(1, half + lo, count, yn, 2, at), (0, lo, count, xn, 4, at + 1)]
    if part != 0:
        plan += [(0, 0, TOK, xn, 1, 5), (1, 0, TOK, yn, 1, 6)]
    loads = [pltpu.make_async_copy(full.at[shard_rows(dev), :], buf.at[n], own.at[n]) for n, dev in enumerate((xn, yn))]
    return Stage([] if part == 1 else loads, [pltpu.make_async_remote_copy(
        src_ref=buf.at[slot, pl.ds(first, rows), :], dst_ref=full.at[shard_rows(dev, first, rows), :],
        send_sem=send.at[sem], recv_sem=recv.at[sem], device_id=(peer_of(me, mask),), device_id_type=MESH)
        for slot, first, rows, dev, mask, sem in plan])


def stage3(me, full, bg):
    send, recv, own, buf = bg
    rows = full.at[shard_rows(peer_of(me, 6)), :]
    return Stage([pltpu.make_async_copy(rows, buf.at[1], own.at[1])], [pltpu.make_async_remote_copy(
        src_ref=buf.at[1], dst_ref=rows, send_sem=send.at[7], recv_sem=recv.at[7],
        device_id=(peer_of(me, 1),), device_id_type=MESH)])


def route(me):
    core = me % 2
    first = peer_of(me, 2) * (1 - core) + peer_of(me, 4) * core
    second = peer_of(me, 4) * (1 - core) + peer_of(me, 2) * core
    return core, peer_of(me, 1), first, second


def half_rows(c):
    return pl.ds(pl.multiple_of(c * (DIM // 2), DIM // 2), DIM // 2)


def start(copies):
    for c in copies:
        c.start()


def wait(copies):
    for c in copies:
        c.wait()


def row_sums(vals):
    folded = vals[:, :HD]
    for start in range(HD, vals.shape[1], HD):
        folded = folded + vals[:, start:start + HD]
    return jnp.sum(folded.T, axis=0, keepdims=True)


def columns_of(rows):
    turned = rows.T
    return [jnp.broadcast_to(turned[:, c:c + 1], (rows.shape[1], HD)) for c in range(rows.shape[0])]


def as_column(row):
    return jnp.broadcast_to(row, (HD, row.shape[1])).T


def exchange(me, srcs, slots, send_sems, recv_sems):
    copies = []
    for n, (src, slot) in enumerate(zip(srcs, slots)):
        for p, mask in enumerate(ORDER):
            copies.append(pltpu.make_async_remote_copy(
                src_ref=src, dst_ref=slot.at[p], send_sem=send_sems.at[n, p], recv_sem=recv_sems.at[n, p],
                device_id=(peer_of(me, mask),), device_id_type=MESH))
    return copies


def ordered_total(me, src, slot):
    own = src[...]
    total = jnp.zeros_like(own)
    for dev in range(NDEV):
        term = jnp.where(me == dev, own, 0.0)
        for p, mask in enumerate(ORDER):
            term = term + jnp.where(peer_of(me, mask) == dev, slot[p], 0.0)
        total = total + term
    return total


def causal_mask():
    keys = lax.broadcasted_iota(jnp.int32, (BLK, BLK), 0)
    queries = lax.broadcasted_iota(jnp.int32, (BLK, BLK), 1)
    return keys <= queries


def block_rows(i):
    return pl.ds(pl.multiple_of(i * BLK, BLK), BLK)


def head_cols(h):
    return pl.ds(pl.multiple_of(h * HD, HD), HD)


def forward_kernel(freq_ref, wq_ref, wk_ref, wv_ref, gains_ref, x_ref, wo_ref,
                   cos_ref, sin_ref, inv_ref, o_ref, lse_ref, raw_ref, qkv_ref, both_ref, full_ref, wof_ref,
                   raw, qkv, xbuf, sums_scr, slot, p_scr, vt_scr, acc_scr, o_scr, buf0, buf1,
                   ex_send, ex_recv, out_sems, send_sems, recv_sems, own_sems, x_sems, *bg_sems):
    g = pl.program_id(0)
    b, t = g // (4 * NB), g % (4 * NB)
    me = lax.axis_index('tp')
    bg0, bg1, bg2 = (*bg_sems[:3], buf0), (*bg_sems[3:6], buf1), (*bg_sems[6:], buf0)
    x0f, x1f = full_ref.at[0], full_ref.at[1]

    def x_gather(part=None):
        return stage1(me, x_ref.at[1], x1f, bg1, part)

    def wo_gather(part=None):
        return stage1(me, wo_ref, wof_ref, bg2, part)

    def keep(bb):
        return [pltpu.make_async_copy(raw, raw_ref.at[bb], out_sems.at[0]),
                pltpu.make_async_copy(qkv, qkv_ref.at[bb], out_sems.at[1])]

    def sums(bb):
        return exchange(me, [sums_scr.at[bb]], [slot.at[bb]], ex_send.at[bb], ex_recv.at[bb])

    def fetch(bb, i):
        return pltpu.make_async_copy(full_ref.at[bb, block_rows(i), :], xbuf.at[i % 2], x_sems.at[i % 2])

    def block_copy(bb, hh, st, half):
        dest = 2 * ((me // 2 + 1 + st) % NB) + half
        part = o_scr.at[bb, hh, st, pl.ds(half * TOK, TOK), :]
        dst = both_ref.at[bb, :, pl.ds(pl.multiple_of(me * LOC + hh * HD, HD), HD)]
        away = pltpu.make_async_remote_copy(
            src_ref=part, dst_ref=dst, send_sem=send_sems.at[bb, hh, st, half], recv_sem=recv_sems.at[bb, hh, me],
            device_id=(dest,), device_id_type=MESH)
        return dest, away, pltpu.make_async_copy(part, dst, own_sems.at[bb, hh])

    def run(stage):
        stage.load()
        stage.send()

    @pl.when(g == 0)
    def _():
        first = stage1(me, x_ref.at[0], x0f, bg0)
        entry_signal(me)
        first.load()
        entry_wait()
        first.send()
        x_gather(0).load()
        freq = freq_ref[...]
        sign = jnp.where(lax.broadcasted_iota(jnp.int32, (TOK, HD), 1) < HD // 2, -1.0, 1.0)

        def table(i, carry):
            rows = pl.ds(pl.multiple_of(i * TOK, TOK), TOK)
            pos = (lax.broadcasted_iota(jnp.int32, (TOK, HD), 0) + i * TOK).astype(F32)
            angle = pos * freq
            cos_ref[rows, :] = jnp.cos(angle)
            sin_ref[rows, :] = jnp.sin(angle) * sign
            return carry

        lax.fori_loop(0, SEQ // TOK, table, 0)
        first.wait()
        second, third = stage2(me, x0f, bg0), stage3(me, x0f, bg0)
        run(second)
        x_gather(0).send()
        second.wait()
        run(third)
        third.wait()
        fetch(0, 0).start()

    @pl.when(g == 2 * NB + 2)
    def _():
        x_gather(0).wait()
        x_gather(1).wait()
        run(stage2(me, x1f, bg1))
        run(wo_gather(0))

    @pl.when(g == 4 * NB)
    def _():
        stage2(me, x1f, bg1).wait()
        third = stage3(me, x1f, bg1)
        run(third)
        for c in keep(0):
            c.wait()
        third.wait()
        fetch(1, 0).start()

    @pl.when(g == 6 * NB + 2)
    def _():
        wo_gather(0).wait()
        wo_gather(1).wait()
        run(stage2(me, wof_ref, bg2))

    @pl.when(t < NB)
    def _():
        rows = block_rows(t)

        @pl.when(t < NB - 1)
        def _():
            fetch(b, t + 1).start()

        fetch(b, t).wait()
        x = xbuf[t % 2]
        for n, w_ref in enumerate((wq_ref, wk_ref)):
            val = dot(x, w_ref[...])
            raw[n, rows, :] = val
            sums_scr[b, pl.ds(t + n * NB, 1), :] = row_sums(val * val)
        qkv[2, rows, :] = dot(x, wv_ref[...]).astype(BF)

    @pl.when(t == NB)
    def _():
        start(sums(b))
        keep(b)[0].start()
        pl.when(b == 0)(x_gather(1).send)
        pl.when(b == 1)(wo_gather(1).send)
        wait(sums(b))
        inv_ref[...] = lax.rsqrt(ordered_total(me, sums_scr.at[b], slot.at[b]) / DIM + EPS)

    @pl.when(jnp.logical_and(t >= NB, t < 2 * NB))
    def _():
        i = t - NB
        rows = block_rows(i)
        cos, sin = cos_ref[rows, :], sin_ref[rows, :]
        for n in range(2):
            inv = as_column(inv_ref[pl.ds(i + n * NB, 1), :])
            gain = gains_ref[n:n + 1, :]
            for h in range(LOC // HD):
                sl = slice(h * HD, (h + 1) * HD)
                hat = raw[n, rows, sl] * inv * gain[:, sl]
                qkv[n, rows, sl] = (hat * cos + pltpu.roll(hat, HD // 2, 1) * sin).astype(BF)

    @pl.when(t == 2 * NB)
    def _():
        keep(b)[1].start()

    @pl.when(t >= 2 * NB)
    def _():
        h, step = t // NB - 2, t % NB
        qi = (me // 2 + 1 + step) % NB
        cols = head_cols(h)

        @pl.when(step == 0)
        def _():
            vt_scr[...] = qkv[2, :, cols].T

        qb = qkv[0, block_rows(qi), cols]

        def scores(j):
            return dot(qkv[1, block_rows(j), cols], qb, NT)

        def first(j, m):
            s = scores(j)
            p_scr[j] = s
            return jnp.maximum(m, jnp.max(s.reshape(BLK // 8, 8, BLK), axis=0))

        s = jnp.where(causal_mask(), scores(qi), -1e30)
        p_scr[qi] = s
        m = lax.fori_loop(0, qi, first, jnp.max(s.reshape(BLK // 8, 8, BLK), axis=0))
        m = jnp.max(m, axis=0, keepdims=True)

        def second(j, l):
            p = jnp.exp2((p_scr[j] - m) * C2)
            p_scr[j] = p
            return l + jnp.sum(p.reshape(BLK // 8, 8, BLK), axis=0)

        l = lax.fori_loop(0, qi + 1, second, jnp.zeros((8, BLK), F32))
        l = jnp.sum(l, axis=0, keepdims=True)
        rl = 1.0 / l
        lse_ref[pl.ds(h * NB + qi, 1), :] = m * C2 + jnp.log2(l)

        acc_scr[...] = jnp.zeros_like(acc_scr)

        def third(j, carry):
            p = (p_scr[j] * rl).astype(BF)
            acc_scr[...] += dot(vt_scr[:, block_rows(j)], p)
            return carry

        lax.fori_loop(0, qi + 1, third, 0)
        out = acc_scr[...].T.astype(BF)
        o_scr[b, h, step] = out
        o_ref[block_rows(qi), cols] = out

        for half in range(2):
            dest, away, here = block_copy(b, h, step, half)
            pl.when(dest != me)(away.start)
            pl.when(dest == me)(here.start)

    @pl.when(g == 8 * NB - 1)
    def _():
        stage2(me, wof_ref, bg2).wait()
        third = stage3(me, wof_ref, bg2)
        run(third)
        for c in keep(1):
            c.wait()

        def drain(n, carry):
            bb, hh = n // 2, n % 2
            for st in range(NB):
                for half in range(2):
                    dest, away, here = block_copy(bb, hh, st, half)
                    if st < NB - 1:
                        away.wait_send()
                    else:
                        pl.when(dest != me)(away.wait_send)
                        pl.when(dest == me)(here.wait)
            for mask in ORDER:
                peer = peer_of(me, mask)
                pltpu.make_async_remote_copy(
                    src_ref=o_scr.at[0, 0, 0, pl.ds(0, TOK), :],
                    dst_ref=both_ref.at[bb, :, pl.ds(pl.multiple_of(peer * LOC + hh * HD, HD), HD)],
                    send_sem=send_sems.at[0, 0, 0, 0], recv_sem=recv_sems.at[bb, hh, peer],
                    device_id=(peer,), device_id_type=MESH).wait_recv()
            return carry

        lax.fori_loop(0, 4, drain, 0)
        third.wait()


def forward(x, wq, wk, wv, wo, gains, cid):
    inv_freq = np.float32(1.0) / np.float32(ROPE_THETA) ** (np.arange(HD // 2, dtype=np.float32) / np.float32(HD // 2))
    freq = jnp.asarray(np.concatenate([inv_freq, inv_freq])[None, :], F32)

    def whole(*shape):
        return pl.BlockSpec(shape, lambda g: (0,) * len(shape))

    def per_batch(*shape):
        return pl.BlockSpec((None,) + shape, lambda g: (g // (4 * NB),) + (0,) * len(shape))

    wspec, rows = whole(DIM, LOC), per_batch(2 * NB, BLK)
    return pl.pallas_call(
        forward_kernel,
        grid=(8 * NB,),
        in_specs=[whole(1, HD), wspec, wspec, wspec, whole(2 + DIM // LOC, LOC), ANYWHERE, ANYWHERE],
        out_specs=[whole(SEQ, HD), whole(SEQ, HD), rows, per_batch(SEQ, LOC), rows] + [ANYWHERE] * 5,
        out_shape=[sds((SEQ, HD), F32), sds((SEQ, HD), F32), sds((2, 2 * NB, BLK), F32), sds((2, SEQ, LOC), BF),
                   sds((2, 2 * NB, BLK), F32), sds((2, 2, SEQ, LOC), F32), sds((2, 3, SEQ, LOC), BF),
                   sds((2, TOK, DIM), BF), sds((2, SEQ, DIM), BF), sds((SEQ, DIM), BF)],
        scratch_shapes=[pltpu.VMEM((2, SEQ, LOC), F32), pltpu.VMEM((3, SEQ, LOC), BF), pltpu.VMEM((2, BLK, DIM), BF),
                        pltpu.VMEM((2, 2 * NB, BLK), F32), pltpu.VMEM((2, NDEV - 1, 2 * NB, BLK), F32),
                        pltpu.VMEM((NB, BLK, BLK), F32), pltpu.VMEM((HD, SEQ), BF), pltpu.VMEM((HD, BLK), F32),
                        pltpu.VMEM((2, 2, NB, BLK, HD), BF), pltpu.VMEM((2, TOK, DIM), BF), pltpu.VMEM((2, TOK, DIM), BF),
                        DMA((2, 1, NDEV - 1)), DMA((2, 1, NDEV - 1)), DMA((2,)),
                        DMA((2, 2, NB, 2)), DMA((2, 2, NDEV)), DMA((2, 2)), DMA((2,))] + BG_SEMS * 3,
        compiler_params=params(dimension_semantics=("arbitrary",), collective_id=cid, has_side_effects=True),
        cost_estimate=cost(60e9, 60e6),
        name="forward",
    )(freq, wq, wk, wv, gains, x, wo)


def out_kernel(o_ref, x_ref, dy_ref, gains_ref, wo_ref, y_ref, da_ref, gga_ref, full_ref, wo_scr, a_scr, wo_sems, buf, *bg_sems):
    b = pl.program_id(0)
    me = lax.axis_index('tp')
    bg = (*bg_sems, buf)
    step = DIM // NB

    def piece(j):
        cols = pl.ds(pl.multiple_of(j * step, step), step)
        return cols, pltpu.make_async_copy(wo_ref.at[:, cols], wo_scr.at[:, cols], wo_sems.at[j])

    @pl.when(b == 0)
    def _():
        nbr_signal(me)
        for j in range(NB):
            piece(j)[1].start()
        gga_ref[...] = jnp.zeros_like(gga_ref)

    o = o_ref[0]

    def fwd(j, carry):
        cols, load = piece(j)
        pl.when(b == 0)(load.wait)
        a_scr[:, cols] = dot(o, wo_scr[:, cols])
        return carry

    lax.fori_loop(0, NB, fwd, 0)
    a = a_scr[...]
    r = lax.rsqrt(jnp.mean(a * a, axis=-1, keepdims=True) + EPS)
    n = a * r
    ga = jnp.concatenate([gains_ref[2 + i:3 + i, :] for i in range(8)], axis=1)
    dy = dy_ref[0].astype(F32)
    gn = dy * ga
    da = (r * (gn - n * jnp.mean(gn * n, axis=-1, keepdims=True))).astype(BF)
    da_ref[0] = da

    @pl.when(b == 0)
    def _():
        buf[0] = da
        nbr_wait()
        stage1(me, None, full_ref, bg).send()

    y_ref[0] = (x_ref[0].astype(F32) + n * ga).astype(BF)
    col = jnp.sum(dy * n, axis=0, keepdims=True)
    for i in range(8):
        gga_ref[i:i + 1, :] += col[:, i * LOC:(i + 1) * LOC]

    @pl.when(b == 1)
    def _():
        stage1(me, None, full_ref, bg).wait()


def out_block(o, wo, x, dy, gains, cid):
    def whole(*shape):
        return pl.BlockSpec(shape, lambda i: (0,) * len(shape))

    batch = pl.BlockSpec((1, TOK, DIM), lambda i: (i, 0, 0))
    return pl.pallas_call(
        out_kernel,
        grid=(2,),
        in_specs=[batch, batch, batch, whole(2 + DIM // LOC, LOC), ANYWHERE],
        out_specs=[batch, batch, whole(8, DIM // 8), ANYWHERE],
        out_shape=[sds((2, TOK, DIM), BF), sds((2, TOK, DIM), BF), sds((8, DIM // 8), F32), sds((SEQ, DIM), BF)],
        scratch_shapes=[pltpu.VMEM((DIM, DIM), BF), pltpu.VMEM((TOK, DIM), F32), DMA((NB,)),
                        pltpu.VMEM((2, TOK, DIM), BF)] + BG_SEMS,
        compiler_params=params(dimension_semantics=("arbitrary",), collective_id=cid, has_side_effects=True),
        cost_estimate=cost(8 * TOK * DIM * DIM + 5e9, 18e6),
        name="out_block",
    )(o, x, dy, gains, wo)


def backward_kernel(b, qkv_ref, wo_ref, lse_ref, raw_hbm, inv_ref, gains_ref, cos_hbm, sin_hbm, gga_ref,
                    wq_ref, wk_ref, wv_ref, da_ref, *rest):
    if b:
        d0_ref, pd0_ref, pw_ref, d_ref, pd_ref, gg_ref, gout_ref, got_ref, da_ref, buf0, w_all, d_two, sbuf, *rest = rest
    else:
        shard_ref, d_ref, pd_ref, gg_ref, gout_ref, full_ref, pw_ref, da_ref, buf0, buf1, w_half, *rest = rest
    (p_scr, dp_scr, kt_scr, dqt_scr, dq_scr, dk_scr, dv_scr, du_scr, d_scr, dh_scr, dbuf, dots_scr, total, slot, ga_slot,
     ex_send, ex_recv, pd_send, pd_recv, d_sems, rs_sems, ld_sems, db_sems, raw_ref, cos_ref, sin_ref, tb_sems, *bg_sems) = rest
    h, step = pl.program_id(0), pl.program_id(1)
    me = lax.axis_index('tp')

    def chip_at(n):
        ax, ay = (me // 2) % 2, me // 4
        return (ay + (n // 2) * (1 - 2 * ay)) * 2 + ax + (n % 2) * (1 - 2 * ax)

    def fetch(n):
        return pltpu.make_async_copy(da_ref.at[block_rows(chip_at(n)), :], dbuf.at[n % 2], db_sems.at[n % 2])

    qi = chip_at(step)
    tables = [pltpu.make_async_copy(src, dst, tb_sems.at[n]) for n, (src, dst) in enumerate(
        ((raw_hbm.at[b], raw_ref), (cos_hbm, cos_ref), (sin_hbm, sin_ref)))]
    core, partner, first_dev, _ = route(me)
    weights = (wq_ref, wk_ref, wv_ref)

    bg0 = (*bg_sems[:3], buf0)
    older3 = stage3(me, da_ref, bg0)
    if b:
        operands = []
        for blk, chip in enumerate((peer_of(me, 6) // 2, first_dev // 2)):
            operands += [pltpu.make_async_copy(d.at[block_rows(chip), :], d_two.at[blk, n], ld_sems.at[2 * blk + n])
                         for n, d in enumerate((d0_ref, pd0_ref))]
        operands += [pltpu.make_async_copy(w.at[half_rows(core), :], w_all.at[0, :, pl.ds(n * LOC, LOC)], ld_sems.at[4 + n])
                     for n, w in enumerate(weights)]
        operands.append(pltpu.make_async_copy(pw_ref, w_all.at[1], ld_sems.at[7]))
        moved = [pltpu.make_async_remote_copy(
            src_ref=sbuf.at[blk, pl.ds(lo, count), :], dst_ref=got_ref.at[blk, pl.ds(lo, count), :], send_sem=rs_sems.at[n],
            recv_sem=rs_sems.at[3 + n], device_id=(first_dev,), device_id_type=MESH)
            for n, (blk, lo, count) in enumerate(((0, 0, BLK), (1, 0, BLK * 3 // 4), (1, BLK * 3 // 4, BLK // 4)))]
    else:
        bg = (*bg_sems[3:], buf1)
        older2 = stage2(me, da_ref, bg0)
        gather = stage1(me, shard_ref.at[1], full_ref, bg)
        operands = [pltpu.make_async_copy(w.at[half_rows(1 - core), :], w_half.at[:, pl.ds(n * LOC, LOC)], ld_sems.at[n])
                    for n, w in enumerate(weights)]
        moved = [pltpu.make_async_remote_copy(
            src_ref=w_half, dst_ref=pw_ref, send_sem=rs_sems.at[0], recv_sem=rs_sems.at[3], device_id=(partner,),
            device_id_type=MESH)]

    @pl.when(jnp.logical_and(h == 0, step == 0))
    def _():
        entry_signal(me)
        if b:
            needed, rest_of = operands[:2] + operands[4:], operands[2:4]
            start(needed)
            fetch(0).start()
            start(rest_of)
            older3.load()
            start(tables)
            wait(needed)
            sbuf[0] = dot(d_two[0, 0], w_all[0], NT) + dot(d_two[0, 1], w_all[1], NT)
            entry_wait()
            moved[0].start()
            older3.send()
            wait(rest_of)
            sbuf[1] = dot(d_two[1, 0], w_all[0], NT) + dot(d_two[1, 1], w_all[1], NT)
            moved[1].start()
        else:
            older2.load()
            fetch(0).start()
            gather.load()
            start(operands)
            start(tables)
            entry_wait()
            older2.send()
            gather.send()
            wait(operands)
            start(moved)
        dots_scr[...] = jnp.zeros_like(dots_scr)

    if not b:
        @pl.when(jnp.logical_and(h == 1, step == NB - 1))
        def _():
            gather.wait()
            early = stage2(me, full_ref, bg, 0)
            early.load()
            early.send()

    @pl.when(jnp.logical_and(h == 0, step == NB - 1))
    def _():
        older3.wait()
        fetch(NB - 1).start()

    @pl.when(h == 0)
    def _():
        fetch(step).wait()
        dh_scr[block_rows(qi), :] = dot(dbuf[step % 2], wo_ref[...], NT).astype(BF)
        if b:
            @pl.when(step < NB - 2)
            def _():
                fetch(step + 1).start()
        else:
            @pl.when(step == 0)
            def _():
                older2.wait(2, 3)

            @pl.when(step < NB - 2)
            def _():
                fetch(step + 1).start()

            @pl.when(step == NB - 2)
            def _():
                older2.wait(0, 1)
                older3.load()
                older3.send()

    @pl.when(step == 0)
    def _():
        kt_scr[...] = qkv_ref[1].T
        dk_scr[...] = jnp.zeros_like(dk_scr)
        dv_scr[...] = jnp.zeros_like(dv_scr)

    qb = qkv_ref[0, block_rows(qi), :]
    dob = dh_scr[block_rows(qi), head_cols(h)]
    lse = lse_ref[pl.ds(h * NB + qi, 1), :]

    def first(j, acc, diag=False):
        rows = block_rows(j)
        p = jnp.exp2(dot(qkv_ref[1, rows, :], qb, NT) * C2 - lse)
        if diag:
            p = jnp.where(causal_mask(), p, 0.0)
        dp = dot(qkv_ref[2, rows, :], dob, NT)
        p_scr[j] = p
        dp_scr[j] = dp
        dv_scr[rows, :] += dot(p.astype(BF), dob)
        return acc + jnp.sum((p * dp).reshape(BLK // 8, 8, BLK), axis=0)

    acc = first(qi, jnp.zeros((8, BLK), F32), True)
    acc = lax.fori_loop(0, qi, first, acc)
    delta = jnp.sum(acc, axis=0, keepdims=True)
    dqt_scr[...] = jnp.zeros_like(dqt_scr)

    def second(j, carry):
        rows = block_rows(j)
        ds = (p_scr[j] * (dp_scr[j] - delta) * SCALE).astype(BF)
        dk_scr[rows, :] += dot(ds, qb)
        dqt_scr[...] += dot(kt_scr[:, rows], ds)
        return carry

    lax.fori_loop(0, qi + 1, second, 0)
    dq_scr[block_rows(qi), :] = dqt_scr[...].T

    @pl.when(step == NB - 1)
    def _():
        d_scr[:, pl.ds(pl.multiple_of(2 * LOC + h * HD, HD), HD)] = dv_scr[...].astype(BF)
        gg_ref[...] = jnp.zeros_like(gg_ref)
        cols = head_cols(h)

        @pl.when(h == 0)
        def _():
            wait(tables)


        inverse = columns_of(inv_ref[...])
        for i in range(NB):
            rows = pl.ds(i * BLK, BLK)
            cos, sin = cos_ref[rows, :], sin_ref[rows, :]
            for n, from_scr in enumerate((dq_scr, dk_scr)):
                d = from_scr[rows, :]
                hat = d * cos - pltpu.roll(d, HD // 2, 1) * sin
                unit = raw_ref[n, rows, cols] * inverse[i + n * NB]
                gg_ref[n:n + 1, :] += jnp.sum(hat * unit, axis=0, keepdims=True)
                du = hat * gains_ref[n:n + 1, :]
                du_scr[n, h, rows, :] = du
                dots_scr[i + n * NB:i + n * NB + 1, :] += row_sums(du * unit)

    @pl.when(jnp.logical_and(h == 1, step == NB - 1))
    def _():
        srcs, slots = ([dots_scr], [slot]) if b else ([dots_scr, gga_ref], [slot, ga_slot])
        sums = exchange(me, srcs, slots, ex_send, ex_recv)
        start(sums)
        if b:
            moved[2].start()
        else:
            stage2(me, full_ref, bg, 1).send()
        wait(sums)
        total[...] = ordered_total(me, dots_scr, slot) / DIM
        gout_ref[...] = gga_ref[...] if b else ordered_total(me, gga_ref, ga_slot)

        def copies(i):
            rows = block_rows(i)
            return [pltpu.make_async_copy(d_scr.at[rows, :], d_ref.at[rows, :], d_sems.at[i]),
                    pltpu.make_async_remote_copy(
                        src_ref=d_scr.at[rows, :], dst_ref=pd_ref.at[rows, :], send_sem=pd_send.at[i],
                        recv_sem=pd_recv.at[i], device_id=(peer_of(me, 1),), device_id_type=MESH)]

        inverse, dots = columns_of(inv_ref[...]), columns_of(total[...])
        for i in range(NB):
            rows = pl.ds(i * BLK, BLK)
            for n in range(2):
                inv = inverse[i + n * NB]
                for hh in range(LOC // HD):
                    sl = slice(hh * HD, (hh + 1) * HD)
                    unit = raw_ref[n, rows, sl] * inv
                    val = inv * (du_scr[n, hh, rows, :] - unit * dots[i + n * NB])
                    d_scr[rows, n * LOC + hh * HD:n * LOC + (hh + 1) * HD] = val.astype(BF)
            start(copies(i))
        for i in range(NB):
            wait(copies(i))
        wait(moved)
        if not b:
            stage2(me, full_ref, bg, 0).wait()
            stage2(me, full_ref, bg, 1).wait()


def backward(b, da, qkv, wo, lse, raw, inv, gains, cos, sin, gga, weights, others, cid):
    def whole(*shape):
        return pl.BlockSpec(shape, lambda h, i: (0,) * len(shape))

    def picked(*shape):
        return pl.BlockSpec((None,) + shape, lambda h, i: (b,) + (0,) * len(shape))

    gsp = whole(8, DIM // 8)
    half = (DIM // 2, 3 * LOC)
    if b:
        extra = [sds((2, BLK, DIM // 2), F32), sds((SEQ, DIM), BF)]
        own = [pltpu.VMEM((2, TOK, DIM), BF), pltpu.VMEM((2,) + half, BF), pltpu.VMEM((2, 2, BLK, 3 * LOC), BF), pltpu.VMEM((2, BLK, DIM // 2), F32)]
    else:
        extra = [sds((SEQ, DIM), BF), sds(half, BF), sds((SEQ, DIM), BF)]
        own = [pltpu.VMEM((2, TOK, DIM), BF), pltpu.VMEM((2, TOK, DIM), BF), pltpu.VMEM(half, BF)]
    return pl.pallas_call(
        functools.partial(backward_kernel, b),
        grid=(2, NB),
        in_specs=[pl.BlockSpec((None, 3, SEQ, HD), lambda h, i: (b, 0, 0, h)),
                  whole(LOC, DIM),
                  picked(2 * NB, BLK), ANYWHERE, picked(2 * NB, BLK),
                  pl.BlockSpec((2 + DIM // LOC, HD), lambda h, i: (0, h)), ANYWHERE, ANYWHERE, gsp]
        + [ANYWHERE] * (4 + len(others)),
        out_specs=[ANYWHERE, ANYWHERE, pl.BlockSpec((8, HD), lambda h, i: (0, h)), gsp] + [ANYWHERE] * len(extra),
        out_shape=[sds((SEQ, 3 * LOC), BF), sds((SEQ, 3 * LOC), BF), sds((8, LOC), F32), sds((8, DIM // 8), F32)] + extra,
        input_output_aliases={12: 5 if b else 6},
        scratch_shapes=own + [
            pltpu.VMEM((NB, BLK, BLK), F32), pltpu.VMEM((NB, BLK, BLK), F32), pltpu.VMEM((HD, SEQ), BF),
            pltpu.VMEM((HD, BLK), F32), pltpu.VMEM((SEQ, HD), F32), pltpu.VMEM((SEQ, HD), F32),
            pltpu.VMEM((SEQ, HD), F32), pltpu.VMEM((2, 2, SEQ, HD), F32), pltpu.VMEM((SEQ, 3 * LOC), BF),
            pltpu.VMEM((SEQ, LOC), BF), pltpu.VMEM((2, BLK, DIM), BF), pltpu.VMEM((2 * NB, BLK), F32), pltpu.VMEM((2 * NB, BLK), F32),
            pltpu.VMEM((NDEV - 1, 2 * NB, BLK), F32), pltpu.VMEM((NDEV - 1, 8, DIM // 8), F32),
            DMA((2, NDEV - 1)), DMA((2, NDEV - 1)), DMA((NB,)), DMA((NB,)), DMA((NB,)), DMA((6,)), DMA((8,)), DMA((2,)),
            pltpu.VMEM((2, SEQ, LOC), F32), pltpu.VMEM((SEQ, HD), F32), pltpu.VMEM((SEQ, HD), F32), DMA((3,))]
        + BG_SEMS * (1 if b else 2),
        compiler_params=params(dimension_semantics=("arbitrary", "arbitrary"), collective_id=cid, has_side_effects=True),
        cost_estimate=cost(25e9, 30e6),
        name="backward",
    )(qkv, wo, lse, raw, inv, gains, cos, sin, gga, *weights, da, *others)


HALF = DIM // 2
CH = 256


def grads_kernel(d0, d1, pd0, pd1, wq, wk, wv, pw, got, x_full, o_all, da0, da1, dy_ref, dx_out, gwq_out, gwk_out, gwv_out, gwo_out,
                 d_all, w_all, sbuf, r1, r2, fin, acc, xbuf, obuf,
                 dl_sems, w_sems, s1_sems, r1_sems, s2_sems, r2_sems, fs_sems, fr_sems, x_sems, o_sems, dx_ref, gwq_ref, gwk_ref, gwv_ref, gwo_ref, out_sems):
    me = lax.axis_index('tp')
    core, partner, first, second = route(me)
    chip = me // 2
    diag_chip, first_chip, second_chip = peer_of(me, 6) // 2, first // 2, second // 2

    barrier = pltpu.get_barrier_semaphore()
    for dev in (partner, first, second):
        pl.semaphore_signal(barrier, inc=1, device_id=(dev,), device_id_type=MESH)

    def rows_of(blk):
        return pl.ds(pl.multiple_of(blk * BLK, BLK), BLK)

    results = [pltpu.make_async_copy(src, dst, out_sems.at[n]) for n, (src, dst) in enumerate((
        (gwq_ref, gwq_out), (gwk_ref, gwk_out), (gwv_ref, gwv_out), (gwo_ref, gwo_out)))]
    chips = (diag_chip, first_chip, second_chip, chip)
    w_copies = [pltpu.make_async_copy(w.at[half_rows(core), :], w_all.at[0, :, pl.ds(n * LOC, LOC)], w_sems.at[n])
                for n, w in enumerate((wq, wk, wv))]
    w_copies.append(pltpu.make_async_copy(pw, w_all.at[1], w_sems.at[3]))
    loads = []
    for n in range(8):
        rows, b = rows_of(chips[n // 2]), n % 2
        loads.append([pltpu.make_async_copy(d.at[rows, :], d_all.at[side, b, rows, :], dl_sems.at[side, n])
                      for side, d in enumerate(((d0, d1)[b], (pd0, pd1)[b]))])
    start(w_copies)
    start(loads[1])
    pl.semaphore_wait(barrier, 3)
    wait(w_copies)

    def partial(b, blk):
        rows = rows_of(blk)
        return dot(d_all[0, b, rows, :], w_all[0], NT) + dot(d_all[1, b, rows, :], w_all[1], NT)

    def to_first(n):
        return pltpu.make_async_remote_copy(
            src_ref=sbuf.at[n // 2], dst_ref=r1.at[n], send_sem=s1_sems.at[n], recv_sem=r1_sems.at[n],
            device_id=(first,), device_id_type=MESH)

    def to_second(b):
        return pltpu.make_async_remote_copy(
            src_ref=r1.at[b], dst_ref=r2.at[b], send_sem=s2_sems.at[b], recv_sem=r2_sems.at[b],
            device_id=(second,), device_id_type=MESH)

    def to_partner(b):
        return pltpu.make_async_remote_copy(
            src_ref=r1.at[2 + b, pl.ds(pl.multiple_of((1 - core) * TOK, TOK), TOK), :], dst_ref=fin.at[b],
            send_sem=fs_sems.at[b], recv_sem=fr_sems.at[b], device_id=(partner,), device_id_type=MESH)

    taken = [pltpu.make_async_copy(got.at[n], r1.at[2 * n], w_sems.at[4 + n]) for n in range(2)]
    for n in (1, 3):
        wait(loads[n])
        if n == 1:
            start(loads[3])
        sbuf[n // 2] = partial(1, chips[n // 2])
        to_first(n).start()
        if n == 1:
            start(taken)
            for later in (4, 0, 2, 5, 6, 7):
                start(loads[later])
    for n in (0, 2, 4, 5, 6, 7):
        wait(loads[n])
    wait(taken)

    steps = SEQ // CH

    def chunk(i):
        return pl.ds(pl.multiple_of(i * CH, CH), CH)

    def stream(pairs, body):
        def fetch(i):
            return [pltpu.make_async_copy(src.at[chunk(i), :], buf.at[i % 2], sems.at[i % 2]) for src, buf, sems in pairs]

        for c in fetch(0):
            c.start()

        def it(i, carry):
            @pl.when(i + 1 < steps)
            def _():
                for c in fetch(i + 1):
                    c.start()

            for c in fetch(i):
                c.wait()
            body(i)
            return carry

        lax.fori_loop(0, steps, it, 0)

    def wgrad(b, src):
        def body(i):
            left = d_all[0, b, chunk(i), :].T
            for c in range(3):
                part = slice(c * LOC, (c + 1) * LOC)
                acc[part, :] += dot(left[part, :], xbuf[i % 2])

        stream([(src, xbuf, x_sems)], body)

    def forward_second(b):
        if b:
            to_first(b).wait_recv()
        r1[b] += partial(b, second_chip)
        to_second(b).start()

    forward_second(0)
    acc[...] = jnp.zeros_like(acc)
    wgrad(0, x_full.at[0])
    wgrad(1, x_full.at[1])
    for n, ref in enumerate((gwq_ref, gwk_ref, gwv_ref)):
        ref[...] = acc[n * LOC:(n + 1) * LOC, :].T.astype(BF)
        results[n].start()
    forward_second(1)
    acc[:LOC, :] = jnp.zeros((LOC, DIM), F32)

    def wo_body(i):
        acc[:LOC, :] += dot(obuf[i % 2].T, xbuf[i % 2])

    for o_src, da_src in ((o_all.at[0], da0), (o_all.at[1], da1)):
        stream([(da_src, xbuf, x_sems), (o_src, obuf, o_sems)], wo_body)
    gwo_ref[...] = acc[:LOC, :].astype(BF)
    results[3].start()

    def own_part(b, carry):
        r1_own = partial(b, chip)
        pl.when(b == 1)(to_first(3).wait_recv)
        to_second(b).wait_recv()
        r1[2 + b] += r1_own + r2[b]
        to_partner(b).start()
        cols = half_rows(core)
        rows = pl.ds(pl.multiple_of(core * TOK, TOK), TOK)
        dx_ref[b, :, cols] = (r1[2 + b, rows, :] + dy_ref[b, :, cols].astype(F32)).astype(BF)
        return carry

    lax.fori_loop(0, 2, own_part, 0)

    def finish(b, carry):
        to_partner(b).wait()
        cols = half_rows(1 - core)
        dx_ref[b, :, cols] = (fin[b] + dy_ref[b, :, cols].astype(F32)).astype(BF)
        pltpu.make_async_copy(dx_ref.at[b], dx_out.at[b], out_sems.at[4 + b]).start()
        to_second(b).wait_send()
        return carry

    to_first(1).wait_send()
    to_first(3).wait_send()
    lax.fori_loop(0, 2, finish, 0)
    wait(results)
    for b in range(2):
        pltpu.make_async_copy(dx_ref.at[b], dx_out.at[b], out_sems.at[4 + b]).wait()


def grads(d0, d1, pd0, pd1, wq, wk, wv, pw, got, x_full, o_all, da0, da1, dy, cid):
    vm = pl.BlockSpec(memory_space=pltpu.VMEM)
    far = pl.BlockSpec(memory_space=pl.ANY)
    dma = pltpu.SemaphoreType.DMA
    return pl.pallas_call(
        grads_kernel,
        in_specs=[far] * 13 + [vm],
        out_specs=[far] * 5,
        out_shape=[sds((2, TOK, DIM), BF)] + [sds((DIM, LOC), BF)] * 3 + [sds((LOC, DIM), BF)],
        scratch_shapes=[pltpu.VMEM((2, 2, SEQ, 3 * LOC), BF), pltpu.VMEM((2, HALF, 3 * LOC), BF),
                        pltpu.VMEM((2, BLK, HALF), F32), pltpu.VMEM((4, BLK, HALF), F32), pltpu.VMEM((2, BLK, HALF), F32),
                        pltpu.VMEM((2, TOK, HALF), F32), pltpu.VMEM((3 * LOC, DIM), F32),
                        pltpu.VMEM((2, CH, DIM), BF), pltpu.VMEM((2, CH, LOC), BF),
                        dma((2, 8)), dma((9,)), dma((4,)), dma((4,)), dma((2,)), dma((2,)),
                        dma((2,)), dma((2,)), dma((2,)), dma((2,)), pltpu.VMEM((2, TOK, DIM), BF),
                        pltpu.VMEM((DIM, LOC), BF), pltpu.VMEM((DIM, LOC), BF), pltpu.VMEM((DIM, LOC), BF),
                        pltpu.VMEM((LOC, DIM), BF), dma((6,))],
        compiler_params=pltpu.CompilerParams(vmem_limit_bytes=67043328, collective_id=cid, has_side_effects=True),
        cost_estimate=cost(100e9, 40e6),
        name="grads",
    )(d0, d1, pd0, pd1, wq, wk, wv, pw, got, x_full, o_all, da0, da1, dy)


def deliver_kernel(*refs):
    count = (len(refs) - 2) // 3
    loads, stores = [], []
    for src, dst, buf in zip(refs[:count], refs[count:2 * count], refs[2 * count:3 * count]):
        for part in range(2):
            piece = (part,) if len(src.shape) == 3 else (pl.ds(part * (src.shape[0] // 2), src.shape[0] // 2),)
            n = len(loads)
            loads.append(pltpu.make_async_copy(src.at[piece], buf.at[piece], refs[-2].at[n]))
            stores.append(pltpu.make_async_copy(buf.at[piece], dst.at[piece], refs[-1].at[n]))
    ahead = len(loads)
    start(loads[:ahead])
    for n, (load, store) in enumerate(zip(loads, stores)):
        load.wait()
        store.start()
        start(loads[n + ahead:n + ahead + 1])
    wait(stores)


def deliver(*arrays):
    return pl.pallas_call(
        deliver_kernel,
        in_specs=[ANYWHERE] * len(arrays),
        out_specs=[ANYWHERE] * len(arrays),
        out_shape=[sds(t.shape, t.dtype) for t in arrays],
        scratch_shapes=[pltpu.VMEM(t.shape, t.dtype) for t in arrays] + [DMA((2 * len(arrays),)), DMA((2 * len(arrays),))],
        compiler_params=params(),
        cost_estimate=cost(1e9, 16e6),
        name="deliver",
    )(*arrays)


def local_block(x_loc, wq, wk, wv, wo, gq, gk, ga, dy_loc):
    gains = jnp.concatenate([gq, gk, ga]).astype(F32).reshape(2 + DIM // LOC, LOC)
    weights = (wq, wk, wv)
    cos, sin, inv, o, lse, raw, qkv, o_recv, x_full, wo_full = forward(x_loc, wq, wk, wv, wo, gains, 0)
    y, da, gga, da0 = out_block(o_recv, wo_full, x_loc, dy_loc, gains, 1)
    state = (qkv, wo, lse, raw, inv, gains, cos, sin, gga, weights)
    d0, pd0, gg0, gout, da1, pw, da0 = backward(0, da0, *state, (da,), 2)
    d1, pd1, gg1, _, got, da1 = backward(1, da1, *state, (d0, pd0, pw), 3)
    grad_ga = gout.reshape(DIM).astype(BF)
    big = grads(d0, d1, pd0, pd1, *weights, pw, got, x_full, o, da0, da1, dy_loc, 4)
    y, dx, gwq, gwk, gwv, gwo = deliver(y, *big)
    gg = gg0 + gg1
    return (y, dx, gwq, gwk, gwv, gwo, gg[0].astype(BF), gg[1].astype(BF), grad_ga)


def solution(mesh):
    act, col, row, vec = P(None, 'tp', None), P(None, 'tp'), P('tp', None), P('tp')
    in_specs = (act, col, col, col, row, vec, vec, P(), act)
    out_specs = (act, act, col, col, col, row, vec, vec, P())
    return jax.shard_map(local_block, mesh=mesh, in_specs=in_specs, out_specs=out_specs, check_vma=False)
```
